32 devices in a mesh: dp: 1 (over z), ep2: 4 (over y), ep: 8 (over x, core).
Axes of the slice: x: 4, y: 4, z: 1, core: 2. Of those that a mesh axis runs over, the one named last changes fastest.
The devices are a block of a 4x4x8 slice.
Arguments:
- x_tok: bfloat16 [32768, 2048], P(('dp', 'ep2', 'ep'))
- expert_ids: int32 [32768, 8], P(('dp', 'ep2', 'ep'))
- gate_w: float32 [32768, 8], P(('dp', 'ep2', 'ep'))
- w_in: bfloat16 [128, 2048, 768], P(('ep2', 'ep'))
- w_out: bfloat16 [128, 768, 2048], P(('ep2', 'ep'))
Outputs:
- output: bfloat16 [32768, 2048], P(('dp', 'ep2', 'ep'))
All inputs are finite; a program needn't handle non-finite values.
Results may differ from the reference program's by a relative error of at most 0.00112.
Values are sent between devices in bfloat16 or wider.
A program may use at most 768 MiB of HBM per device.

```python
import math
import jax
import jax.numpy as jnp
from jax import lax

TOKENS = 1024
GROUP = 32
D_MODEL = 2048
FF = 768
EXPERTS = 128
TOP = 8
CAP = 2560


def draw_routing(route_key):
    k_perm, k_shift, k_tok, k_roll = jax.random.split(route_key, 4)
    avg_count = TOKENS * TOP // EXPERTS
    spread = avg_count - 1
    rank_of = jax.random.permutation(k_perm, EXPERTS)
    shifts = jax.random.randint(k_shift, (GROUP, 1), 0, EXPERTS // 16 + 2)
    prof_pos = (rank_of[None, :] + shifts) % EXPERTS
    near_end = jnp.minimum(prof_pos, EXPERTS - 1 - prof_pos)
    step_mag = (spread * (EXPERTS - 1 - 2 * near_end)) // (EXPERTS - 1)
    dev_counts = avg_count + jnp.where(prof_pos < EXPERTS - 1 - prof_pos, step_mag, -step_mag)
    run_end = jnp.cumsum(dev_counts, axis=1)
    list_pos = jnp.arange(TOKENS * TOP)
    sorted_ids = jax.vmap(lambda end_row: jnp.searchsorted(end_row, list_pos, side='right'))(run_end)
    id_grid = jnp.swapaxes(sorted_ids.reshape(GROUP, TOP, TOKENS), 1, 2)
    tok_keys = jax.random.split(k_tok, GROUP)
    tok_perm = jax.vmap(lambda tok_key: jax.random.permutation(tok_key, TOKENS))(tok_keys)
    id_grid = jnp.take_along_axis(id_grid, jnp.broadcast_to(tok_perm[:, :, None], (GROUP, TOKENS, TOP)), axis=1)
    roll_by = jax.random.randint(k_roll, (GROUP, TOKENS, 1), 0, TOP)
    col_ids = (jnp.arange(TOP)[None, None, :] + roll_by) % TOP
    id_grid = jnp.take_along_axis(id_grid, col_ids, axis=2)
    return id_grid.reshape(GROUP * TOKENS, TOP).astype(jnp.int32)


def setup_inputs(seed: int = 0, part: int = 0) -> dict:
    key_part = jax.random.fold_in(jax.random.key(seed), part)
    k_x, k_gate, k_route = jax.random.split(key_part, 3)
    k_in, k_out = jax.random.split(jax.random.key(seed + 1), 2)
    x_tok = jax.random.normal(k_x, (GROUP * TOKENS, D_MODEL), jnp.float32).astype(jnp.bfloat16)
    gate_w = jax.random.uniform(k_gate, (GROUP * TOKENS, TOP), jnp.float32, 0.5, 1.5) * (2.0 / math.sqrt(TOP))
    w_in = (jax.random.normal(k_in, (EXPERTS, D_MODEL, FF), jnp.float32) * (D_MODEL ** -0.5)).astype(jnp.bfloat16)
    w_out = (jax.random.normal(k_out, (EXPERTS, FF, D_MODEL), jnp.float32) * (FF ** -0.5)).astype(jnp.bfloat16)
    return {'x_tok': x_tok, 'expert_ids': draw_routing(k_route), 'gate_w': gate_w, 'w_in': w_in, 'w_out': w_out}


def reference(x_tok, expert_ids, gate_w, w_in, w_out):
    flat_e = expert_ids.reshape(-1)
    n_pair = flat_e.shape[0]
    pair_order = jnp.argsort(flat_e, stable=True)
    counts = jnp.bincount(flat_e, length=EXPERTS)
    starts = jnp.cumsum(counts) - counts
    slot_ids = jnp.arange(CAP)
    flat_gate = gate_w.reshape(-1)

    def one_expert(acc_y, inputs):
        start_at, n_count, w_a, w_b = inputs
        pair_ids = pair_order[jnp.minimum(start_at + slot_ids, n_pair - 1)]
        is_kept = slot_ids < jnp.minimum(n_count, CAP)
        tok_ids = pair_ids // TOP
        tok_rows = jnp.where(is_kept[:, None], x_tok[tok_ids], jnp.zeros((), x_tok.dtype))
        hidden = jax.nn.gelu(jnp.dot(tok_rows, w_a, preferred_element_type=jnp.float32), approximate=True).astype(jnp.bfloat16)
        out_rows = jnp.dot(hidden, w_b, preferred_element_type=jnp.float32).astype(jnp.bfloat16)
        weight = jnp.where(is_kept, flat_gate[pair_ids], 0.0)
        acc_y = acc_y.at[tok_ids].add(weight[:, None] * out_rows.astype(jnp.float32))
        return acc_y, None

    acc_y, _ = lax.scan(one_expert, x_tok.astype(jnp.float32), (starts, counts, w_in, w_out))
    return acc_y.astype(jnp.bfloat16)
```

```python
import functools
import math

import jax
import jax.numpy as jnp
from jax import lax
from jax.experimental import pallas as pl
from jax.experimental.pallas import tpu as pltpu
from jax.sharding import PartitionSpec as P

LANES = 128
CHUNKS = 4
TILE = 256
PREFIX_ROWS = 8
BF16 = jnp.bfloat16
F32 = jnp.float32
I32 = jnp.int32
HBM = pl.BlockSpec(memory_space=pl.ANY)
SMEM = pl.BlockSpec(memory_space=pltpu.SMEM)
VMEM = pl.BlockSpec(memory_space=pltpu.VMEM)
VMEM_LIMIT = 64_000_000


def capacity_of(group_size, n_tok, n_top, experts):
    return 8 * ((5 * group_size * n_tok * n_top) // (32 * experts))


def route_kernel(ids_ref, gate_ref, tok_ref, wgt_ref, cnt_ref, code_t, gate_t, tok_acc, wgt_acc):
    n_tok, n_top = ids_ref.shape
    step = n_tok // CHUNKS
    lane = lax.broadcasted_iota(I32, (n_tok, LANES), 1)
    member = jnp.zeros((n_tok, LANES), F32)
    gates = jnp.zeros((n_tok, LANES), F32)
    for j in range(n_top):
        hit = ids_ref[:, j:j + 1] == lane
        member = member + jnp.where(hit, 1.0, 0.0)
        gates = gates + jnp.where(hit, gate_ref[:, j:j + 1], 0.0)
    member_b = member.astype(BF16)
    row_block = min(n_tok, 128)
    for i in range(n_tok // row_block):
        rows = pl.ds(i * row_block, row_block)
        later = lax.broadcasted_iota(I32, (row_block, n_tok), 0) + i * row_block
        earlier = lax.broadcasted_iota(I32, (row_block, n_tok), 1)
        tri = jnp.where(earlier < later, 1.0, 0.0).astype(BF16)
        rank = jnp.dot(tri, member_b, preferred_element_type=F32)
        mem = member[i * row_block:(i + 1) * row_block]
        code_t[:, rows] = jnp.where(mem > 0.5, rank, -1.0).T
        gate_t[:, rows] = gates[i * row_block:(i + 1) * row_block].T
    total = jnp.zeros((1, LANES), F32)
    rows_out = [total]
    for k in range(CHUNKS):
        total = total + jnp.sum(member[k * step:(k + 1) * step], axis=0, keepdims=True)
        rows_out.append(total)
    while len(rows_out) < PREFIX_ROWS:
        rows_out.append(total)
    cnt_ref[...] = jnp.concatenate(rows_out, axis=0).astype(I32)
    tok_acc[...] = jnp.zeros_like(tok_acc)
    wgt_acc[...] = jnp.zeros_like(wgt_acc)
    slot = lax.broadcasted_iota(I32, (LANES, n_tok), 0).astype(F32)
    token = lax.broadcasted_iota(I32, (1, n_tok), 1).astype(F32)
    out_lane = lax.broadcasted_iota(I32, (LANES, LANES), 1)

    def one_expert(e, carry):
        hit = slot == code_t[pl.ds(e, 1), :]
        tok = jnp.sum(jnp.where(hit, token, 0.0), axis=1, keepdims=True)
        wgt = jnp.sum(jnp.where(hit, gate_t[pl.ds(e, 1), :], 0.0), axis=1, keepdims=True)
        tok_acc[...] = jnp.where(out_lane == e, tok, tok_acc[...])
        wgt_acc[...] = jnp.where(out_lane == e, wgt, wgt_acc[...])
        return carry

    lax.fori_loop(0, LANES, one_expert, 0)
    tok_ref[...] = tok_acc[...].T.astype(I32)
    wgt_ref[...] = wgt_acc[...].T


def route(ids, gate):
    n_tok = ids.shape[0]
    return pl.pallas_call(
        route_kernel,
        out_shape=(
            jax.ShapeDtypeStruct((LANES, LANES), I32),
            jax.ShapeDtypeStruct((LANES, LANES), F32),
            jax.ShapeDtypeStruct((PREFIX_ROWS, LANES), I32),
        ),
        in_specs=[VMEM, VMEM],
        out_specs=(VMEM, VMEM, VMEM),
        scratch_shapes=[
            pltpu.VMEM((LANES, n_tok), F32),
            pltpu.VMEM((LANES, n_tok), F32),
            pltpu.VMEM((LANES, LANES), F32),
            pltpu.VMEM((LANES, LANES), F32),
        ],
        cost_estimate=pl.CostEstimate(flops=2 * 10 ** 10, bytes_accessed=10 ** 6, transcendentals=0),
        name='route',
    )(ids, gate)


def list_kernel(cap, slots, n_tok, group, sub, cnt_ref, core_ref, tok_ref, src_ref, dst_ref, cs_ref, kept_ref, base_ref):
    core = core_ref[0]
    n_dst = group // 2
    step = n_tok // CHUNKS
    rows = CHUNKS + 1

    def per_expert(e, carry):
        def per_dev(g, off):
            n = cnt_ref[(g * rows + CHUNKS) * sub + e]
            kept = jnp.clip(cap - off, 0, n)

            @pl.when(g % 2 == core)
            def _():
                kept_ref[(g // 2) * sub + e] = kept
            return off + n
        return carry + lax.fori_loop(0, group, per_dev, 0) * 0

    lax.fori_loop(0, sub, per_expert, 0)

    def per_dst(i, carry):
        def add(e, acc):
            base_ref[i * sub + e] = acc
            return acc + kept_ref[i * sub + e]
        return carry + lax.fori_loop(0, sub, add, 0) * 0

    lax.fori_loop(0, n_dst, per_dst, 0)

    def expert_lists(e, carry):
        def chunk_lists(k, pos):
            cs_ref[e, k] = pos

            def segment(i, o):
                g = 2 * i + core
                kept = kept_ref[i * sub + e]
                s0 = jnp.minimum(cnt_ref[(g * rows + k) * sub + e], kept)
                s1 = jnp.minimum(cnt_ref[(g * rows + k + 1) * sub + e], kept)
                src0 = g * step - k * step
                dst0 = i * slots + base_ref[i * sub + e]

                def block(b, c):
                    for q in range(8):
                        s = s0 + b * 8 + q
                        v = tok_ref[i * sub + e, jnp.minimum(s, LANES - 1)]
                        src_ref[e, o + b * 8 + q] = src0 + v
                        dst_ref[e, o + b * 8 + q] = dst0 + s
                    return c

                n = s1 - s0
                lax.fori_loop(0, (n + 7) // 8, block, 0)
                return o + n

            return lax.fori_loop(0, n_dst, segment, pos)

        end = lax.fori_loop(0, CHUNKS, chunk_lists, 0)
        cs_ref[e, CHUNKS] = end
        return carry

    lax.fori_loop(0, sub, expert_lists, 0)


def build_lists(cnt, core, toks, cap, slots, n_tok, group, sub):
    width = LANES * (group // 2) + LANES
    return pl.pallas_call(
        functools.partial(list_kernel, cap, slots, n_tok, group, sub),
        out_shape=(
            jax.ShapeDtypeStruct((sub, width), I32),
            jax.ShapeDtypeStruct((sub, width), I32),
            jax.ShapeDtypeStruct((sub, LANES), I32),
        ),
        in_specs=[SMEM, SMEM, SMEM],
        out_specs=(SMEM, SMEM, SMEM),
        scratch_shapes=[
            pltpu.SMEM((group // 2 * sub,), I32),
            pltpu.SMEM((group // 2 * sub,), I32),
        ],
        cost_estimate=pl.CostEstimate(flops=2 * 10 ** 10, bytes_accessed=10 ** 6, transcendentals=0),
        name='row_lists',
    )(cnt, core, toks)


def rows_loop(n, fn):
    def block(b, c):
        for q in range(8):
            fn(b * 8 + q)
        return c

    def single(r, c):
        fn(r)
        return c

    full = n // 8
    lax.fori_loop(0, full, block, 0)
    lax.fori_loop(full * 8, n, single, 0)


def gelu(v):
    return 0.5 * v * (1.0 + jnp.tanh(math.sqrt(2.0 / math.pi) * (v + 0.044715 * v * v * v)))


def expert_kernel(k, first, *refs):
    if first:
        (src, dst, cs, core_ref, x_hbm, wa_own, wa_sib, wb_own, wb_sib, send,
         xbuf, obuf, wa, wb, t_e, t_base, t_cnt, gsem, ssem, wsem) = refs
    else:
        (src, dst, cs, core_ref, x_hbm, wa_own, wa_sib, wb_own, wb_sib, _, send,
         xbuf, obuf, wa, wb, t_e, t_base, t_cnt, gsem, ssem, wsem) = refs
    e_loc, d_model, _ = wa_own.shape
    sub = 2 * e_loc
    core = core_ref[0]
    sublanes = d_model // LANES

    def weight_copies(e, act):
        slot = e % 2
        q = e % e_loc

        @pl.when(e // e_loc == core)
        def _():
            act(pltpu.make_async_copy(wa_own.at[q], wa.at[slot], wsem.at[slot, 0]))
            act(pltpu.make_async_copy(wb_own.at[q], wb.at[slot], wsem.at[slot, 1]))

        @pl.when(e // e_loc != core)
        def _():
            act(pltpu.make_async_copy(wa_sib.at[q], wa.at[slot], wsem.at[slot, 0]))
            act(pltpu.make_async_copy(wb_sib.at[q], wb.at[slot], wsem.at[slot, 1]))

    weight_copies(0, lambda c: c.start())

    def plan(e, t):
        lo = cs[e, k]
        n = cs[e, k + 1] - lo

        def put(i, c):
            t_e[t + i] = e
            t_base[t + i] = lo + i * TILE
            t_cnt[t + i] = jnp.minimum(n - i * TILE, TILE)
            return c

        n_tiles = (n + TILE - 1) // TILE
        lax.fori_loop(0, n_tiles, put, 0)
        return t + n_tiles

    n_all = lax.fori_loop(0, sub, plan, 0)

    def gather_start(t):
        e, base, slot = t_e[t], t_base[t], t % 2
        rows_loop(t_cnt[t], lambda r: pltpu.make_async_copy(
            x_hbm.at[src[e, base + r]], xbuf.at[slot, r], gsem.at[slot]).start())

    def gather_wait(t):
        n, slot = t_cnt[t], t % 2
        pltpu.make_async_copy(x_hbm.at[pl.ds(0, n)], xbuf.at[slot, pl.ds(0, n)], gsem.at[slot]).wait()

    def scatter_start(t):
        e, base, slot = t_e[t], t_base[t], t % 2
        rows_loop(t_cnt[t], lambda r: pltpu.make_async_copy(
            obuf.at[slot, r], send.at[dst[e, base + r]], ssem.at[slot]).start())

    def scatter_wait(t):
        n, slot = t_cnt[t], t % 2
        pltpu.make_async_copy(obuf.at[slot, pl.ds(0, n)], send.at[pl.ds(0, n)], ssem.at[slot]).wait()

    for t in range(2):
        @pl.when(t < n_all)
        def _():
            gather_start(t)

    def one_expert(e, t_first):
        weight_copies(e, lambda c: c.wait())

        @pl.when(e + 1 < sub)
        def _():
            weight_copies(e + 1, lambda c: c.start())

        ws = e % 2
        n = cs[e, k + 1] - cs[e, k]

        def one_tile(i, t):
            slot = t % 2
            gather_wait(t)

            @pl.when(t >= 2)
            def _():
                scatter_wait(t - 2)

            rows = xbuf[slot].reshape(TILE, d_model)
            hidden = gelu(jnp.dot(rows, wa[ws], preferred_element_type=F32)).astype(BF16)
            out = jnp.dot(hidden, wb[ws], preferred_element_type=F32).astype(BF16)
            obuf[slot] = out.reshape(TILE, sublanes, LANES)

            @pl.when(t + 2 < n_all)
            def _():
                gather_start(t + 2)

            scatter_start(t)
            return t + 1

        return lax.fori_loop(0, (n + TILE - 1) // TILE, one_tile, t_first)

    lax.fori_loop(0, sub, one_expert, 0)
    for back in (2, 1):
        @pl.when(n_all >= back)
        def _():
            scatter_wait(n_all - back)


def run_experts(k, src, dst, cs, core, x_rows, wa, wa_sib, wb, wb_sib, send, send_rows):
    e_loc, d_model, ff = wa.shape
    sub = 2 * e_loc
    sublanes = d_model // LANES
    first = send is None
    ops = (src, dst, cs, core, x_rows, wa, wa_sib, wb, wb_sib) + (() if first else (send,))
    max_tiles = sub * (pl.cdiv(src.shape[1], TILE) + 1)
    flops = 4 * d_model * ff * x_rows.shape[0]
    return pl.pallas_call(
        functools.partial(expert_kernel, k, first),
        out_shape=jax.ShapeDtypeStruct((send_rows, sublanes, LANES), BF16),
        in_specs=[SMEM] * 4 + [HBM] * (len(ops) - 4),
        out_specs=HBM,
        scratch_shapes=[
            pltpu.VMEM((2, TILE, sublanes, LANES), BF16),
            pltpu.VMEM((2, TILE, sublanes, LANES), BF16),
            pltpu.VMEM((2, d_model, ff), BF16),
            pltpu.VMEM((2, ff, d_model), BF16),
            pltpu.SMEM((max_tiles,), I32),
            pltpu.SMEM((max_tiles,), I32),
            pltpu.SMEM((max_tiles,), I32),
            pltpu.SemaphoreType.DMA((2,)),
            pltpu.SemaphoreType.DMA((2,)),
            pltpu.SemaphoreType.DMA((2, 2)),
        ],
        input_output_aliases={} if first else {len(ops) - 1: 0},
        compiler_params=pltpu.CompilerParams(vmem_limit_bytes=VMEM_LIMIT),
        cost_estimate=pl.CostEstimate(flops=flops, bytes_accessed=6 * 10 ** 7, transcendentals=0),
        name='experts',
    )(*ops)


def return_kernel(rows_main, rows_last, n_y, n_x, send, recv, ssem, rsem):
    y = lax.axis_index('ep2')
    ec = lax.axis_index('ep')
    x, core = ec // 2, ec % 2
    me = y * n_x + x
    offsets = [(dy, dx) for dy in range(n_y) for dx in range(n_x) if (dy, dx) != (0, 0)]
    half_y, half_x = n_y // 2, n_x // 2
    near = lambda d, n: min(d, n - d)
    offsets.sort(key=lambda o: (near(o[0], n_y) + near(o[1], n_x), o[0] > half_y, o[1] > half_x))

    def peer(dy, dx):
        return {'ep2': lax.rem(y + dy, n_y), 'ep': lax.rem(x + dx, n_x) * 2 + core}

    barrier = pltpu.get_barrier_semaphore()
    for dy, dx in offsets:
        pl.semaphore_signal(barrier, inc=1, device_id=peer(dy, dx), device_id_type=pl.DeviceIdType.MESH)
    pl.semaphore_wait(barrier, len(offsets))

    def copy(i, dy, dx, rows):
        ty, tx = lax.rem(y + dy, n_y), lax.rem(x + dx, n_x)
        return pltpu.make_async_remote_copy(
            src_ref=send.at[ty * n_x + tx, pl.ds(0, rows)],
            dst_ref=recv.at[me, pl.ds(0, rows)],
            send_sem=ssem.at[i],
            recv_sem=rsem.at[i],
            device_id=peer(dy, dx),
            device_id_type=pl.DeviceIdType.MESH,
        )

    def sized(row, fn):
        if rows_main == rows_last:
            fn(rows_main)
            return

        @pl.when(row < n_y - 1)
        def _():
            fn(rows_main)

        @pl.when(row == n_y - 1)
        def _():
            fn(rows_last)

    for i, (dy, dx) in enumerate(offsets):
        sized(lax.rem(y + dy, n_y), lambda rows: copy(i, dy, dx, rows).start())
    for i, (dy, dx) in enumerate(offsets):
        sized(lax.rem(y + dy, n_y), lambda rows: copy(i, dy, dx, rows).wait_send())
    for i, (dy, dx) in enumerate(offsets):
        sized(y, lambda rows: copy(i, dy, dx, rows).wait_recv())


def send_back(rows_main, rows_last, cid, n_y, n_x, send):
    n = n_y * n_x - 1
    return pl.pallas_call(
        functools.partial(return_kernel, rows_main, rows_last, n_y, n_x),
        out_shape=jax.ShapeDtypeStruct(send.shape, BF16),
        in_specs=[HBM],
        out_specs=HBM,
        scratch_shapes=[pltpu.SemaphoreType.DMA((n,)), pltpu.SemaphoreType.DMA((n,))],
        compiler_params=pltpu.CompilerParams(collective_id=cid, has_side_effects=True),
        name='send_back_%d_%d' % (rows_main, rows_last),
    )(send)


def combine_kernel(tok, wgt, kept, chip_ref, recv, send, x_ref, y_ref, rbuf, acc0, acc1, acc2, acc3, sem):
    n_tok, d_model = x_ref.shape
    n_chip, slots, sublanes, _ = recv.shape
    sub = kept.shape[0] // n_chip
    accs = (acc0, acc1, acc2, acc3)
    mine = chip_ref[0]
    blk = 16

    def count(i):
        n = kept[i * sub]
        for q in range(1, sub):
            n = n + kept[i * sub + q]
        return n

    def fetch(i, act):
        slot = i % 2
        n = count(i)

        @pl.when(jnp.logical_and(i == mine, n > 0))
        def _():
            act(pltpu.make_async_copy(send.at[i, pl.ds(0, n)], rbuf.at[slot, pl.ds(0, n)], sem.at[slot]))

        @pl.when(jnp.logical_and(i != mine, n > 0))
        def _():
            act(pltpu.make_async_copy(recv.at[i, pl.ds(0, n)], rbuf.at[slot, pl.ds(0, n)], sem.at[slot]))

    fetch(0, lambda c: c.start())

    def zero(b, c):
        for acc in accs:
            acc[pl.ds(b * blk, blk)] = jnp.zeros((blk, sublanes, LANES), F32)
        return c

    lax.fori_loop(0, n_tok // blk, zero, 0)

    def one_chip(i, c):
        slot = i % 2

        @pl.when(i + 1 < n_chip)
        def _():
            fetch(i + 1, lambda d: d.start())

        fetch(i, lambda d: d.wait())

        def one_expert(q, base):
            e = i * sub + q
            n = kept[e]

            def quad(b, cc):
                for p in range(4):
                    s = b * 4 + p
                    s_in = jnp.minimum(s, LANES - 1)
                    t = jnp.where(s < n, tok[e, s_in], n_tok)
                    row = rbuf[slot, base + s].astype(F32)
                    accs[p][t] = accs[p][t] + wgt[e, s_in] * row
                return cc

            lax.fori_loop(0, (n + 3) // 4, quad, 0)
            return base + n

        lax.fori_loop(0, sub, one_expert, 0)
        return c

    lax.fori_loop(0, n_chip, one_chip, 0)

    def finish(b, c):
        rows = pl.ds(pl.multiple_of(b * blk, blk), blk)
        total = (acc0[rows] + acc1[rows]) + (acc2[rows] + acc3[rows])
        y_ref[rows, :] = (x_ref[rows, :].astype(F32) + total.reshape(blk, d_model)).astype(BF16)
        return c

    lax.fori_loop(0, n_tok // blk, finish, 0)


def combine(tok, wgt, kept, chip, recv, send, x):
    n_tok, d_model = x.shape
    n_chip, slots, sublanes, _ = recv.shape
    acc = pltpu.VMEM((n_tok + 8, sublanes, LANES), F32)
    return pl.pallas_call(
        combine_kernel,
        out_shape=jax.ShapeDtypeStruct((n_tok, d_model), BF16),
        in_specs=[SMEM, SMEM, SMEM, SMEM, HBM, HBM, VMEM],
        out_specs=VMEM,
        scratch_shapes=[
            pltpu.VMEM((2, slots + 8, sublanes, LANES), BF16),
            acc, acc, acc, acc,
            pltpu.SemaphoreType.DMA((2,)),
        ],
        compiler_params=pltpu.CompilerParams(vmem_limit_bytes=VMEM_LIMIT),
        cost_estimate=pl.CostEstimate(flops=2 * 10 ** 10, bytes_accessed=6 * 10 ** 7, transcendentals=0),
        name='combine',
    )(tok, wgt, kept, chip, recv, send, x)


def solution(mesh):
    dev_axes = ('ep2', 'ep')
    n_y, n_ep = mesh.shape['ep2'], mesh.shape['ep']
    n_x = n_ep // 2
    group = n_y * n_ep
    n_chip = n_y * n_x

    def local_step(x_loc, ids_loc, gate_loc, w_a, w_b):
        n_tok, d_model = x_loc.shape
        n_top = ids_loc.shape[1]
        e_loc = w_a.shape[0]
        sub = 2 * e_loc
        experts = e_loc * group
        cap = capacity_of(group, n_tok, n_top, experts)
        sublanes = d_model // LANES
        slots = sub * LANES
        step = n_tok // CHUNKS
        me = lax.axis_index(dev_axes)
        core, chip = me % 2, me // 2

        x3 = x_loc.reshape(n_tok, sublanes, LANES)
        chunks = [lax.all_gather(x3[k * step:(k + 1) * step], dev_axes, tiled=True) for k in range(CHUNKS)]
        swap = [(i, i ^ 1) for i in range(n_ep)]
        w_a_sib = lax.ppermute(w_a, 'ep', swap)
        w_b_sib = lax.ppermute(w_b, 'ep', swap)

        toks, wgts, cnts = route(ids_loc, gate_loc)
        info = jnp.concatenate([toks[:experts].reshape(n_chip, sub, LANES), jnp.pad(cnts, ((0, sub - PREFIX_ROWS), (0, 0)))[None]], axis=0)
        info, chunks[0] = lax.optimization_barrier((info, chunks[0]))
        every = lax.all_gather(info, dev_axes, tiled=False)
        cnt_all = every[:, n_chip, :CHUNKS + 1, :]
        my_cnt = lax.dynamic_slice(cnt_all, (0, 0, chip * sub), (group, CHUNKS + 1, sub)).reshape(-1)
        by_core = every.reshape(n_chip, 2, n_chip + 1, sub, LANES)
        my_tok = lax.dynamic_slice(by_core, (0, core, chip, 0, 0), (n_chip, 1, 1, sub, LANES)).reshape(n_chip * sub, LANES)
        core1 = core.reshape(1).astype(I32)
        src, dst, cs = build_lists(my_cnt, core1, my_tok, cap, slots, n_tok, group, sub)

        totals = cnt_all[:, CHUNKS, :experts]
        offs = jnp.cumsum(totals, axis=0) - totals
        kept = jnp.clip(cap - offs, 0, totals)
        kept_own = lax.dynamic_slice(kept, (me, 0), (1, experts)).reshape(experts)
        need = jnp.sum(kept.reshape(n_y, n_ep, n_chip, sub), axis=3)
        need_main = jnp.max(need[:n_y - 1])
        need_last = jnp.max(need[n_y - 1])

        send = None
        for k in range(CHUNKS):
            send = run_experts(k, src, dst, cs, core1, chunks[k], w_a, w_a_sib, w_b, w_b_sib, send, n_chip * slots)
        send = send.reshape(n_chip, slots, sublanes, LANES)

        tiers = [(slots * a // 64, slots * b // 64) for a, b in ((43, 32), (45, 36), (49, 36), (53, 40))] + [(slots, slots)]
        index = jnp.int32(len(tiers) - 1)
        for i in range(len(tiers) - 2, -1, -1):
            fits = jnp.logical_and(need_main <= tiers[i][0], need_last <= tiers[i][1])
            index = jnp.where(fits, jnp.int32(i), index)
        recv = lax.switch(index, [functools.partial(send_back, a, b, i, n_y, n_x) for i, (a, b) in enumerate(tiers)], send)
        return combine(toks, wgts, kept_own, chip.reshape(1).astype(I32), recv, send, x_loc)

    tok_spec = P(('dp', 'ep2', 'ep'), None)
    w_spec = P(dev_axes, None, None)
    return jax.shard_map(local_step, mesh=mesh, in_specs=(tok_spec, tok_spec, tok_spec, w_spec, w_spec), out_specs=tok_spec, check_vma=False)
```

```python
import functools
import math

import jax
import jax.numpy as jnp
from jax import lax
from jax.experimental import pallas as pl
from jax.experimental.pallas import tpu as pltpu
from jax.sharding import PartitionSpec as P

LANES = 128
CHUNK_UNITS = 16
CHUNK_ENDS = (0, 4, 12, 16)
TILE = 256
PREFIX_ROWS = 8
BF16 = jnp.bfloat16
F32 = jnp.float32
I32 = jnp.int32
HBM = pl.BlockSpec(memory_space=pl.ANY)
SMEM = pl.BlockSpec(memory_space=pltpu.SMEM)
VMEM = pl.BlockSpec(memory_space=pltpu.VMEM)
VMEM_LIMIT = 64_000_000


def capacity_of(group_size, n_tok, n_top, experts):
    return 8 * ((5 * group_size * n_tok * n_top) // (32 * experts))


def route_kernel(bounds, ids_ref, gate_ref, tok_ref, wgt_ref, cnt_ref, code_t, gate_t, tok_acc, wgt_acc):
    n_tok, n_top = ids_ref.shape
    lane = lax.broadcasted_iota(I32, (n_tok, LANES), 1)
    member = jnp.zeros((n_tok, LANES), F32)
    gates = jnp.zeros((n_tok, LANES), F32)
    for j in range(n_top):
        hit = ids_ref[:, j:j + 1] == lane
        member = member + jnp.where(hit, 1.0, 0.0)
        gates = gates + jnp.where(hit, gate_ref[:, j:j + 1], 0.0)
    member_b = member.astype(BF16)
    row_block = min(n_tok, 128)
    for i in range(n_tok // row_block):
        rows = pl.ds(i * row_block, row_block)
        later = lax.broadcasted_iota(I32, (row_block, n_tok), 0) + i * row_block
        earlier = lax.broadcasted_iota(I32, (row_block, n_tok), 1)
        tri = jnp.where(earlier < later, 1.0, 0.0).astype(BF16)
        rank = jnp.dot(tri, member_b, preferred_element_type=F32)
        mem = member[i * row_block:(i + 1) * row_block]
        code_t[:, rows] = jnp.where(mem > 0.5, rank, -1.0).T
        gate_t[:, rows] = gates[i * row_block:(i + 1) * row_block].T
    total = jnp.zeros((1, LANES), F32)
    rows_out = [total]
    for lo, hi in zip(bounds[:-1], bounds[1:]):
        total = total + jnp.sum(member[lo:hi], axis=0, keepdims=True)
        rows_out.append(total)
    while len(rows_out) < PREFIX_ROWS:
        rows_out.append(total)
    cnt_ref[...] = jnp.concatenate(rows_out, axis=0).astype(I32)
    tok_acc[...] = jnp.zeros_like(tok_acc)
    wgt_acc[...] = jnp.zeros_like(wgt_acc)
    slot = lax.broadcasted_iota(I32, (LANES, n_tok), 0).astype(F32)
    token = lax.broadcasted_iota(I32, (1, n_tok), 1).astype(F32)
    out_lane = lax.broadcasted_iota(I32, (LANES, LANES), 1)

    def one_expert(e, carry):
        hit = slot == code_t[pl.ds(e, 1), :]
        tok = jnp.sum(jnp.where(hit, token, 0.0), axis=1, keepdims=True)
        wgt = jnp.sum(jnp.where(hit, gate_t[pl.ds(e, 1), :], 0.0), axis=1, keepdims=True)
        tok_acc[...] = jnp.where(out_lane == e, tok, tok_acc[...])
        wgt_acc[...] = jnp.where(out_lane == e, wgt, wgt_acc[...])
        return carry

    lax.fori_loop(0, LANES, one_expert, 0)
    tok_ref[...] = tok_acc[...].T.astype(I32)
    wgt_ref[...] = wgt_acc[...].T


def route(ids, gate, bounds):
    n_tok = ids.shape[0]
    return pl.pallas_call(
        functools.partial(route_kernel, bounds),
        out_shape=(
            jax.ShapeDtypeStruct((LANES, LANES), I32),
            jax.ShapeDtypeStruct((LANES, LANES), F32),
            jax.ShapeDtypeStruct((PREFIX_ROWS, LANES), I32),
        ),
        in_specs=[VMEM, VMEM],
        out_specs=(VMEM, VMEM, VMEM),
        scratch_shapes=[
            pltpu.VMEM((LANES, n_tok), F32),
            pltpu.VMEM((LANES, n_tok), F32),
            pltpu.VMEM((LANES, LANES), F32),
            pltpu.VMEM((LANES, LANES), F32),
        ],
        cost_estimate=pl.CostEstimate(flops=2 * 10 ** 10, bytes_accessed=10 ** 6, transcendentals=0),
        name='route',
    )(ids, gate)


def list_kernel(cap, slots, bounds, group, sub, place_ref, info_ref, src_ref, start_ref, len_ref, dst_ref, cs_ref, kept_ref, base_ref):
    core, chip = place_ref[0], place_ref[1]
    n_dst = group // 2
    n_chunk = len(bounds) - 1
    dev_words = (sub + PREFIX_ROWS) * LANES
    width = src_ref.shape[0] // sub

    def count(g, k, e):
        return info_ref[g * dev_words + (sub + k) * LANES + chip * sub + e]

    def per_expert(e, carry):
        def per_dev(i, off):
            for c in range(2):
                n = count(2 * i + c, n_chunk, e)
                kept = jnp.clip(cap - off, 0, n)
                off = off + n

                @pl.when(core == c)
                def _():
                    kept_ref[i * sub + e] = kept
            return off
        lax.fori_loop(0, n_dst, per_dev, 0)
        return carry

    lax.fori_loop(0, sub, per_expert, 0)

    def per_dst(i, carry):
        def add(e, acc):
            base_ref[i * sub + e] = acc
            return acc + kept_ref[i * sub + e]
        lax.fori_loop(0, sub, add, i * slots)
        return carry

    lax.fori_loop(0, n_dst, per_dst, 0)

    def expert_lists(e, carry):
        pos = e * width
        for k in range(n_chunk):
            cs_ref[e * (n_chunk + 1) + k] = pos
            size = bounds[k + 1] - bounds[k]

            def segment(i, o):
                g = 2 * i + core
                kept = kept_ref[i * sub + e]
                s0 = jnp.minimum(count(g, k, e), kept)
                n = jnp.minimum(count(g, k + 1, e), kept) - s0
                j = (e * n_chunk + k) * n_dst + i
                start_ref[j] = o
                len_ref[j] = n
                dst_ref[j] = base_ref[i * sub + e] + s0
                src0 = g * size - bounds[k]
                tok0 = g * dev_words + e * LANES + s0

                def block(b, c):
                    vals = [info_ref[tok0 + b * 8 + q] for q in range(8)]
                    for q in range(8):
                        src_ref[o + b * 8 + q] = src0 + vals[q]
                    return c

                lax.fori_loop(0, (n + 7) // 8, block, 0)
                return o + n

            pos = lax.fori_loop(0, n_dst, segment, pos)
        cs_ref[e * (n_chunk + 1) + n_chunk] = pos
        return carry

    lax.fori_loop(0, sub, expert_lists, 0)


def build_lists(place, info, cap, slots, bounds, group, sub):
    n_dst, n_chunk = group // 2, len(bounds) - 1
    width = LANES * n_dst + 8
    segs = sub * n_chunk * n_dst
    return pl.pallas_call(
        functools.partial(list_kernel, cap, slots, bounds, group, sub),
        out_shape=(
            jax.ShapeDtypeStruct((sub * width,), I32),
            jax.ShapeDtypeStruct((segs,), I32),
            jax.ShapeDtypeStruct((segs,), I32),
            jax.ShapeDtypeStruct((segs,), I32),
            jax.ShapeDtypeStruct((sub * (n_chunk + 1),), I32),
        ),
        in_specs=[SMEM, SMEM],
        out_specs=(SMEM,) * 5,
        scratch_shapes=[
            pltpu.SMEM((n_dst * sub,), I32),
            pltpu.SMEM((n_dst * sub,), I32),
        ],
        cost_estimate=pl.CostEstimate(flops=2 * 10 ** 10, bytes_accessed=10 ** 6, transcendentals=0),
        name='row_lists',
    )(place, info)


def rows_loop(n, fn):
    def block(b, c):
        for q in range(8):
            fn(b * 8 + q)
        return c

    def single(r, c):
        fn(r)
        return c

    full = n // 8
    lax.fori_loop(0, full, block, 0)
    lax.fori_loop(full * 8, n, single, 0)


def gelu(v):
    return 0.5 * v * (1.0 + jnp.tanh(math.sqrt(2.0 / math.pi) * (v + 0.044715 * v * v * v)))


def expert_kernel(k, n_chunk, first, *refs):
    (src, seg_start, seg_len, seg_dst, cs, place, x_hbm, wa_own, wa_sib, wb_own, wb_sib) = refs[:11]
    (send, xbuf, obuf, wa, wb, t_e, t_base, t_cnt, gsem, ssem, wsem) = refs[11 if first else 12:]
    e_loc, d_model, _ = wa_own.shape
    sub = 2 * e_loc
    core = place[0]
    sublanes = d_model // LANES
    n_dst = seg_start.shape[0] // (sub * n_chunk)

    def weight_copies(e, act):
        slot = e % 2
        q = e % e_loc

        @pl.when(e // e_loc == core)
        def _():
            act(pltpu.make_async_copy(wa_own.at[q], wa.at[slot], wsem.at[slot, 0]))
            act(pltpu.make_async_copy(wb_own.at[q], wb.at[slot], wsem.at[slot, 1]))

        @pl.when(e // e_loc != core)
        def _():
            act(pltpu.make_async_copy(wa_sib.at[q], wa.at[slot], wsem.at[slot, 0]))
            act(pltpu.make_async_copy(wb_sib.at[q], wb.at[slot], wsem.at[slot, 1]))

    weight_copies(0, lambda c: c.start())

    def plan(e, t):
        lo = cs[e * (n_chunk + 1) + k]
        n = cs[e * (n_chunk + 1) + k + 1] - lo

        def put(i, c):
            t_e[t + i] = e
            t_base[t + i] = lo + i * TILE
            t_cnt[t + i] = jnp.minimum(n - i * TILE, TILE)
            return c

        n_tiles = (n + TILE - 1) // TILE
        lax.fori_loop(0, n_tiles, put, 0)
        return t + n_tiles

    n_all = lax.fori_loop(0, sub, plan, 0)

    def gather_start(t):
        base, slot = t_base[t], t % 2
        rows_loop(t_cnt[t], lambda r: pltpu.make_async_copy(
            x_hbm.at[src[base + r]], xbuf.at[slot, r], gsem.at[slot]).start())

    def gather_wait(t):
        n, slot = t_cnt[t], t % 2
        pltpu.make_async_copy(x_hbm.at[pl.ds(0, n)], xbuf.at[slot, pl.ds(0, n)], gsem.at[slot]).wait()

    def scatter_start(t):
        base, slot = t_base[t], t % 2
        end = base + t_cnt[t]

        def segment(i, c):
            j = (t_e[t] * n_chunk + k) * n_dst + i
            first_row = seg_start[j]
            lo = jnp.maximum(first_row, base)
            n = jnp.minimum(first_row + seg_len[j], end) - lo

            @pl.when(n > 0)
            def _():
                pltpu.make_async_copy(
                    obuf.at[slot, pl.ds(lo - base, n)],
                    send.at[pl.ds(seg_dst[j] + lo - first_row, n)],
                    ssem.at[slot],
                ).start()
            return c

        lax.fori_loop(0, n_dst, segment, 0)

    def scatter_wait(t):
        n, slot = t_cnt[t], t % 2
        pltpu.make_async_copy(obuf.at[slot, pl.ds(0, n)], send.at[pl.ds(0, n)], ssem.at[slot]).wait()

    for t in range(2):
        @pl.when(t < n_all)
        def _():
            gather_start(t)

    def one_expert(e, t_first):
        weight_copies(e, lambda c: c.wait())

        @pl.when(e + 1 < sub)
        def _():
            weight_copies(e + 1, lambda c: c.start())

        ws = e % 2
        n = cs[e * (n_chunk + 1) + k + 1] - cs[e * (n_chunk + 1) + k]

        def one_tile(i, t):
            slot = t % 2
            gather_wait(t)

            @pl.when(t >= 2)
            def _():
                scatter_wait(t - 2)

            rows = xbuf[slot].reshape(TILE, d_model)
            hidden = gelu(jnp.dot(rows, wa[ws], preferred_element_type=F32)).astype(BF16)
            out = jnp.dot(hidden, wb[ws], preferred_element_type=F32).astype(BF16)
            obuf[slot] = out.reshape(TILE, sublanes, LANES)

            @pl.when(t + 2 < n_all)
            def _():
                gather_start(t + 2)

            scatter_start(t)
            return t + 1

        return lax.fori_loop(0, (n + TILE - 1) // TILE, one_tile, t_first)

    lax.fori_loop(0, sub, one_expert, 0)
    for back in (2, 1):
        @pl.when(n_all >= back)
        def _():
            scatter_wait(n_all - back)


def run_experts(k, n_chunk, lists, place, x_rows, wa, wa_sib, wb, wb_sib, send, send_rows):
    e_loc, d_model, ff = wa.shape
    sub = 2 * e_loc
    sublanes = d_model // LANES
    first = send is None
    ops = (*lists, place, x_rows, wa, wa_sib, wb, wb_sib) + (() if first else (send,))
    max_tiles = sub * (pl.cdiv(lists[0].shape[0] // sub, TILE) + 1)
    flops = 4 * d_model * ff * x_rows.shape[0]
    return pl.pallas_call(
        functools.partial(expert_kernel, k, n_chunk, first),
        out_shape=jax.ShapeDtypeStruct((send_rows, sublanes, LANES), BF16),
        in_specs=[SMEM] * 6 + [HBM] * (len(ops) - 6),
        out_specs=HBM,
        scratch_shapes=[
            pltpu.VMEM((2, TILE, sublanes, LANES), BF16),
            pltpu.VMEM((2, TILE, sublanes, LANES), BF16),
            pltpu.VMEM((2, d_model, ff), BF16),
            pltpu.VMEM((2, ff, d_model), BF16),
            pltpu.SMEM((max_tiles,), I32),
            pltpu.SMEM((max_tiles,), I32),
            pltpu.SMEM((max_tiles,), I32),
            pltpu.SemaphoreType.DMA((2,)),
            pltpu.SemaphoreType.DMA((2,)),
            pltpu.SemaphoreType.DMA((2, 2)),
        ],
        input_output_aliases={} if first else {len(ops) - 1: 0},
        compiler_params=pltpu.CompilerParams(vmem_limit_bytes=VMEM_LIMIT),
        cost_estimate=pl.CostEstimate(flops=flops, bytes_accessed=6 * 10 ** 7, transcendentals=0),
        name='experts',
    )(*ops)


def flows_of(n_y, n_x):
    wrap = lambda d, n: d - n if 2 * d > n else d
    direct, relayed = [], []
    for dy in range(n_y):
        for dx in range(n_x):
            if (dy, dx) == (0, 0):
                continue
            tie_y, tie_x = n_y >= 4 and 2 * dy == n_y, n_x >= 4 and 2 * dx == n_x
            if not (tie_y or tie_x):
                direct.append((dy, dx))
                continue
            sy, sx = wrap(dy, n_y), wrap(dx, n_x)
            if tie_y and tie_x:
                leg = (sy // 2, sx // 2)
            elif tie_x:
                sx = sx if dy % 2 == 0 else -sx
                leg = (0, sx // 2)
            else:
                sy = sy if dx % 2 == 0 else -sy
                leg = (sy // 2, 0)
            relayed.append(((dy, dx), leg, (sy - leg[0], sx - leg[1])))
    direct.sort(key=lambda o: -abs(wrap(o[0], n_y)) - abs(wrap(o[1], n_x)))
    return direct, relayed


def return_kernel(rows_main, rows_last, n_y, n_x, send, recv, stage, dsem, lsem, fsem):
    y = lax.axis_index('ep2')
    ec = lax.axis_index('ep')
    x, core = ec // 2, ec % 2
    direct, relayed = flows_of(n_y, n_x)

    def at(dy, dx):
        return lax.rem(y + dy + n_y, n_y), lax.rem(x + dx + n_x, n_x)

    def chip(dy, dx):
        ty, tx = at(dy, dx)
        return ty * n_x + tx

    def peer(dy, dx):
        ty, tx = at(dy, dx)
        return {'ep2': ty, 'ep': tx * 2 + core}

    barrier = pltpu.get_barrier_semaphore()
    for dy in range(n_y):
        for dx in range(n_x):
            if (dy, dx) != (0, 0):
                pl.semaphore_signal(barrier, inc=1, device_id=peer(dy, dx), device_id_type=pl.DeviceIdType.MESH)
    pl.semaphore_wait(barrier, n_y * n_x - 1)

    def sized(row, fn):
        if rows_main == rows_last:
            fn(rows_main)
            return

        @pl.when(row < n_y - 1)
        def _():
            fn(rows_main)

        @pl.when(row == n_y - 1)
        def _():
            fn(rows_last)

    def part(p, rows):
        return pl.ds(p * (rows // 2), rows // 2)

    def remote(src, dst, sems, i, to):
        return pltpu.make_async_remote_copy(
            src_ref=src, dst_ref=dst, send_sem=sems.at[0, i], recv_sem=sems.at[1, i],
            device_id=peer(*to), device_id_type=pl.DeviceIdType.MESH)

    def straight(i, rows):
        d = direct[i]
        return remote(send.at[chip(*d), pl.ds(0, rows)], recv.at[chip(0, 0), pl.ds(0, rows)], dsem, i, d)

    def lead(i, p, rows):
        d, leg, _ = relayed[i]
        return remote(send.at[chip(*d), part(p, rows)], stage.at[i, part(p, rows)], lsem, 2 * i + p, leg)

    def follow(i, p, rows):
        _, leg, rest = relayed[i]
        return remote(stage.at[i, part(p, rows)], recv.at[chip(-leg[0], -leg[1]), part(p, rows)], fsem, 2 * i + p, rest)

    pieces = [(i, p) for p in range(2) for i in range(len(relayed))]
    for i, p in pieces:
        sized(at(*relayed[i][0])[0], lambda rows: lead(i, p, rows).start())
    for i, d in enumerate(direct):
        sized(at(*d)[0], lambda rows: straight(i, rows).start())
    for i, p in pieces:
        def forward(rows):
            lead(i, p, rows).wait_recv()
            follow(i, p, rows).start()
        sized(at(*relayed[i][2])[0], forward)
    for i, p in pieces:
        sized(at(*relayed[i][0])[0], lambda rows: lead(i, p, rows).wait_send())
    for i, d in enumerate(direct):
        sized(at(*d)[0], lambda rows: straight(i, rows).wait_send())
    for i, p in pieces:
        sized(at(*relayed[i][2])[0], lambda rows: follow(i, p, rows).wait_send())

    def arrivals(rows):
        for i in range(len(direct)):
            straight(i, rows).wait_recv()
        for i, p in pieces:
            follow(i, p, rows).wait_recv()

    sized(y, arrivals)


def send_back(rows_main, rows_last, cid, n_y, n_x, send):
    direct, relayed = flows_of(n_y, n_x)
    n_d, n_r = len(direct), max(1, len(relayed))
    return pl.pallas_call(
        functools.partial(return_kernel, rows_main, rows_last, n_y, n_x),
        out_shape=(
            jax.ShapeDtypeStruct(send.shape, BF16),
            jax.ShapeDtypeStruct((n_r, *send.shape[1:]), BF16),
        ),
        in_specs=[HBM],
        out_specs=(HBM, HBM),
        scratch_shapes=[
            pltpu.SemaphoreType.DMA((2, n_d)),
            pltpu.SemaphoreType.DMA((2, 2 * n_r)),
            pltpu.SemaphoreType.DMA((2, 2 * n_r)),
        ],
        compiler_params=pltpu.CompilerParams(collective_id=cid, has_side_effects=True),
        name='send_back_%d_%d' % (rows_main, rows_last),
    )(send)[0]


def combine_kernel(tok, wgt, kept, place, recv, send, x_ref, y_ref, rbuf, acc0, acc1, acc2, acc3, sem):
    n_tok, d_model = x_ref.shape
    n_chip, slots, sublanes, _ = recv.shape
    sub = kept.shape[0] // n_chip
    accs = (acc0, acc1, acc2, acc3)
    mine = place[1]
    blk = 16

    def count(i):
        n = kept[i * sub]
        for q in range(1, sub):
            n = n + kept[i * sub + q]
        return n

    def fetch(i, act):
        slot = i % 2
        n = count(i)

        @pl.when(jnp.logical_and(i == mine, n > 0))
        def _():
            act(pltpu.make_async_copy(send.at[i, pl.ds(0, n)], rbuf.at[slot, pl.ds(0, n)], sem.at[slot]))

        @pl.when(jnp.logical_and(i != mine, n > 0))
        def _():
            act(pltpu.make_async_copy(recv.at[i, pl.ds(0, n)], rbuf.at[slot, pl.ds(0, n)], sem.at[slot]))

    fetch(0, lambda c: c.start())

    def zero(b, c):
        for acc in accs:
            acc[pl.ds(b * blk, blk)] = jnp.zeros((blk, sublanes, LANES), F32)
        return c

    lax.fori_loop(0, n_tok // blk, zero, 0)

    def one_chip(i, c):
        slot = i % 2

        @pl.when(i + 1 < n_chip)
        def _():
            fetch(i + 1, lambda d: d.start())

        fetch(i, lambda d: d.wait())

        def one_expert(q, base):
            first = (i * sub + q) * LANES
            n = kept[i * sub + q]

            def quad(b, cc):
                at = first + b * 4
                toks = [tok[at + p] for p in range(4)]
                wgts = [wgt[at + p] for p in range(4)]
                rows = [wgts[p] * rbuf[slot, base + b * 4 + p].astype(F32) for p in range(4)]
                for p in range(4):
                    accs[p][toks[p]] = accs[p][toks[p]] + rows[p]
                return cc

            lax.fori_loop(0, (n + 3) // 4, quad, 0)
            return base + n

        lax.fori_loop(0, sub, one_expert, 0)
        return c

    lax.fori_loop(0, n_chip, one_chip, 0)

    def finish(b, c):
        rows = pl.ds(pl.multiple_of(b * blk, blk), blk)
        total = (acc0[rows] + acc1[rows]) + (acc2[rows] + acc3[rows])
        y_ref[rows, :] = (x_ref[rows, :].astype(F32) + total.reshape(blk, d_model)).astype(BF16)
        return c

    lax.fori_loop(0, n_tok // blk, finish, 0)


def combine(tok, wgt, kept, place, recv, send, x):
    n_tok, d_model = x.shape
    n_chip, slots, sublanes, _ = recv.shape
    acc = pltpu.VMEM((n_tok + 8, sublanes, LANES), F32)
    return pl.pallas_call(
        combine_kernel,
        out_shape=jax.ShapeDtypeStruct((n_tok, d_model), BF16),
        in_specs=[SMEM, SMEM, SMEM, SMEM, HBM, HBM, VMEM],
        out_specs=VMEM,
        scratch_shapes=[
            pltpu.VMEM((2, slots + 8, sublanes, LANES), BF16),
            acc, acc, acc, acc,
            pltpu.SemaphoreType.DMA((2,)),
        ],
        compiler_params=pltpu.CompilerParams(vmem_limit_bytes=VMEM_LIMIT),
        cost_estimate=pl.CostEstimate(flops=2 * 10 ** 10, bytes_accessed=6 * 10 ** 7, transcendentals=0),
        name='combine',
    )(tok, wgt, kept, place, recv, send, x)


def solution(mesh):
    dev_axes = ('ep2', 'ep')
    n_y, n_ep = mesh.shape['ep2'], mesh.shape['ep']
    n_x = n_ep // 2
    group = n_y * n_ep
    n_chip = n_y * n_x

    def local_step(x_loc, ids_loc, gate_loc, w_a, w_b):
        n_tok, d_model = x_loc.shape
        n_top = ids_loc.shape[1]
        e_loc = w_a.shape[0]
        sub = 2 * e_loc
        experts = e_loc * group
        cap = capacity_of(group, n_tok, n_top, experts)
        sublanes = d_model // LANES
        slots = sub * LANES
        bounds = tuple(n_tok * q // CHUNK_UNITS for q in CHUNK_ENDS)
        n_chunk = len(bounds) - 1
        me = lax.axis_index(dev_axes)
        core, chip = me % 2, me // 2
        place = jnp.stack([core, chip]).astype(I32)

        x3 = x_loc.reshape(n_tok, sublanes, LANES)
        chunks = [lax.all_gather(x3[bounds[k]:bounds[k + 1]], dev_axes, tiled=True) for k in range(n_chunk)]
        swap = [(i, i ^ 1) for i in range(n_ep)]
        w_a_sib = lax.ppermute(w_a, 'ep', swap)
        w_b_sib = lax.ppermute(w_b, 'ep', swap)

        toks, wgts, cnts = route(ids_loc, gate_loc, bounds)
        for_chip = toks[:experts].reshape(n_chip, 1, sub, LANES)
        table = jnp.concatenate([
            jnp.broadcast_to(for_chip, (n_chip, 2, sub, LANES)).reshape(group, sub, LANES),
            jnp.broadcast_to(cnts[None], (group, PREFIX_ROWS, LANES))], axis=1)
        table = lax.all_to_all(table, dev_axes, 0, 0, tiled=True)
        lists = build_lists(place, table.reshape(-1), cap, slots, bounds, group, sub)

        totals = table[:, sub + n_chunk, :experts]
        offs = jnp.cumsum(totals, axis=0) - totals
        kept = jnp.clip(cap - offs, 0, totals)
        kept_own = lax.dynamic_slice(kept, (me, 0), (1, experts)).reshape(experts)
        need = jnp.sum(kept.reshape(n_y, n_ep, n_chip, sub), axis=3)
        need_main = jnp.max(need[:n_y - 1])
        need_last = jnp.max(need[n_y - 1])

        send = None
        for k in range(n_chunk):
            send = run_experts(k, n_chunk, lists, place, chunks[k], w_a, w_a_sib, w_b, w_b_sib, send, n_chip * slots)
        send = send.reshape(n_chip, slots, sublanes, LANES)

        tiers = [(slots * a // 64, slots * b // 64) for a, b in ((43, 32), (45, 36), (49, 36), (53, 40))] + [(slots, slots)]
        index = jnp.int32(len(tiers) - 1)
        for i in range(len(tiers) - 2, -1, -1):
            fits = jnp.logical_and(need_main <= tiers[i][0], need_last <= tiers[i][1])
            index = jnp.where(fits, jnp.int32(i), index)
        recv = lax.switch(index, [functools.partial(send_back, a, b, i, n_y, n_x) for i, (a, b) in enumerate(tiers)], send)
        lane = jnp.arange(LANES)
        put_at = jnp.where(lane[None, :] < kept_own[:, None], toks[:experts], n_tok).reshape(-1)
        return combine(put_at, wgts[:experts].reshape(-1), kept_own, place, recv, send, x_loc)

    tok_spec = P(('dp', 'ep2', 'ep'), None)
    w_spec = P(dev_axes, None, None)
    return jax.shard_map(local_step, mesh=mesh, in_specs=(tok_spec, tok_spec, tok_spec, w_spec, w_spec), out_specs=tok_spec, check_vma=False)
```

```python
import functools
import math

import jax
import jax.numpy as jnp
from jax import lax
from jax.experimental import pallas as pl
from jax.experimental.pallas import tpu as pltpu
from jax.sharding import PartitionSpec as P

LANES = 128
CHUNK_UNITS = 16
CHUNK_ENDS = (0, 4, 12, 16)
SIZES = (40, 42, 44, 46, 48, 52, 64)
TILE = 256
PREFIX_ROWS = 8
BF16 = jnp.bfloat16
F32 = jnp.float32
I32 = jnp.int32
HBM = pl.BlockSpec(memory_space=pl.ANY)
SMEM = pl.BlockSpec(memory_space=pltpu.SMEM)
VMEM = pl.BlockSpec(memory_space=pltpu.VMEM)
VMEM_LIMIT = 64_000_000


def capacity_of(group_size, n_tok, n_top, experts):
    return 8 * ((5 * group_size * n_tok * n_top) // (32 * experts))


def route_kernel(bounds, ids_ref, gate_ref, tok_ref, wgt_ref, cnt_ref, code_t, gate_t, tok_acc, wgt_acc):
    n_tok, n_top = ids_ref.shape
    lane = lax.broadcasted_iota(I32, (n_tok, LANES), 1)
    member = jnp.zeros((n_tok, LANES), F32)
    gates = jnp.zeros((n_tok, LANES), F32)
    for j in range(n_top):
        hit = ids_ref[:, j:j + 1] == lane
        member = member + jnp.where(hit, 1.0, 0.0)
        gates = gates + jnp.where(hit, gate_ref[:, j:j + 1], 0.0)
    member_b = member.astype(BF16)
    row_block = min(n_tok, 128)
    for i in range(n_tok // row_block):
        rows = pl.ds(i * row_block, row_block)
        later = lax.broadcasted_iota(I32, (row_block, n_tok), 0) + i * row_block
        earlier = lax.broadcasted_iota(I32, (row_block, n_tok), 1)
        tri = jnp.where(earlier < later, 1.0, 0.0).astype(BF16)
        rank = jnp.dot(tri, member_b, preferred_element_type=F32)
        mem = member[i * row_block:(i + 1) * row_block]
        code_t[:, rows] = jnp.where(mem > 0.5, rank, -1.0).T
        gate_t[:, rows] = gates[i * row_block:(i + 1) * row_block].T
    total = jnp.zeros((1, LANES), F32)
    rows_out = [total]
    for lo, hi in zip(bounds[:-1], bounds[1:]):
        total = total + jnp.sum(member[lo:hi], axis=0, keepdims=True)
        rows_out.append(total)
    while len(rows_out) < PREFIX_ROWS:
        rows_out.append(total)
    cnt_ref[...] = jnp.concatenate(rows_out, axis=0).astype(I32)
    tok_acc[...] = jnp.zeros_like(tok_acc)
    wgt_acc[...] = jnp.zeros_like(wgt_acc)
    slot = lax.broadcasted_iota(I32, (LANES, n_tok), 0).astype(F32)
    token = lax.broadcasted_iota(I32, (1, n_tok), 1).astype(F32)
    out_lane = lax.broadcasted_iota(I32, (LANES, LANES), 1)

    def one_expert(e, carry):
        hit = slot == code_t[pl.ds(e, 1), :]
        tok = jnp.sum(jnp.where(hit, token, 0.0), axis=1, keepdims=True)
        wgt = jnp.sum(jnp.where(hit, gate_t[pl.ds(e, 1), :], 0.0), axis=1, keepdims=True)
        tok_acc[...] = jnp.where(out_lane == e, tok, tok_acc[...])
        wgt_acc[...] = jnp.where(out_lane == e, wgt, wgt_acc[...])
        return carry

    lax.fori_loop(0, LANES, one_expert, 0)
    tok_ref[...] = tok_acc[...].T.astype(I32)
    wgt_ref[...] = wgt_acc[...].T


def route(ids, gate, bounds):
    n_tok = ids.shape[0]
    return pl.pallas_call(
        functools.partial(route_kernel, bounds),
        out_shape=(
            jax.ShapeDtypeStruct((LANES, LANES), I32),
            jax.ShapeDtypeStruct((LANES, LANES), F32),
            jax.ShapeDtypeStruct((PREFIX_ROWS, LANES), I32),
        ),
        in_specs=[VMEM, VMEM],
        out_specs=(VMEM, VMEM, VMEM),
        scratch_shapes=[
            pltpu.VMEM((LANES, n_tok), F32),
            pltpu.VMEM((LANES, n_tok), F32),
            pltpu.VMEM((LANES, LANES), F32),
            pltpu.VMEM((LANES, LANES), F32),
        ],
        cost_estimate=pl.CostEstimate(flops=2 * 10 ** 10, bytes_accessed=10 ** 6, transcendentals=0),
        name='route',
    )(ids, gate)


def list_kernel(cap, slots_a, slots_b, bounds, n_y, n_x, sub, place_ref, info_ref, src_ref, start_ref, len_ref, dst_a_ref, dst_b_ref, cs_ref,
                kept_ref, base_a_ref, base_b_ref):
    core, chip = place_ref[0], place_ref[1]
    n_dst = n_y * n_x
    n_chunk = len(bounds) - 1
    dev_words = (sub + PREFIX_ROWS) * LANES
    width = src_ref.shape[0] // sub

    def count(g, k, e):
        return info_ref[g * dev_words + (sub + k) * LANES + chip * sub + e]

    def per_expert(e, carry):
        def per_dev(i, off):
            for c in range(2):
                n = count(2 * i + c, n_chunk, e)
                kept = jnp.clip(cap - off, 0, n)
                off = off + n

                @pl.when(core == c)
                def _():
                    kept_ref[i * sub + e] = kept
            return off
        lax.fori_loop(0, n_dst, per_dev, 0)
        return carry

    lax.fori_loop(0, sub, per_expert, 0)

    def add_up(base_ref, i, acc):
        def add(e, acc):
            base_ref[i * sub + e] = acc
            return acc + kept_ref[i * sub + e]
        return lax.fori_loop(0, sub, add, acc)

    for x in range(n_x):
        lax.fori_loop(0, n_y, lambda y, acc: add_up(base_a_ref, y * n_x + x, acc), x * slots_a)
    for y in range(n_y):
        lax.fori_loop(0, n_x, lambda x, acc: add_up(base_b_ref, y * n_x + x, acc), y * slots_b)

    def expert_lists(e, carry):
        pos = e * width
        for k in range(n_chunk):
            cs_ref[e * (n_chunk + 1) + k] = pos
            size = bounds[k + 1] - bounds[k]

            def segment(i, o):
                g = 2 * i + core
                kept = kept_ref[i * sub + e]
                s0 = jnp.minimum(count(g, k, e), kept)
                n = jnp.minimum(count(g, k + 1, e), kept) - s0
                j = (e * n_chunk + k) * n_dst + i
                start_ref[j] = o
                len_ref[j] = n
                dst_a_ref[j] = base_a_ref[i * sub + e] + s0
                dst_b_ref[j] = base_b_ref[i * sub + e] + s0
                src0 = g * size - bounds[k]
                tok0 = g * dev_words + e * LANES + s0

                def block(b, c):
                    vals = [info_ref[tok0 + b * 8 + q] for q in range(8)]
                    for q in range(8):
                        src_ref[o + b * 8 + q] = src0 + vals[q]
                    return c

                lax.fori_loop(0, (n + 7) // 8, block, 0)
                return o + n

            pos = lax.fori_loop(0, n_dst, segment, pos)
        cs_ref[e * (n_chunk + 1) + n_chunk] = pos
        return carry

    lax.fori_loop(0, sub, expert_lists, 0)


def build_lists(place, info, cap, slots_a, slots_b, bounds, n_y, n_x, sub):
    n_dst, n_chunk = n_y * n_x, len(bounds) - 1
    width = LANES * n_dst + 8
    segs = sub * n_chunk * n_dst
    return pl.pallas_call(
        functools.partial(list_kernel, cap, slots_a, slots_b, bounds, n_y, n_x, sub),
        out_shape=(
            jax.ShapeDtypeStruct((sub * width,), I32),
            jax.ShapeDtypeStruct((segs,), I32),
            jax.ShapeDtypeStruct((segs,), I32),
            jax.ShapeDtypeStruct((segs,), I32),
            jax.ShapeDtypeStruct((segs,), I32),
            jax.ShapeDtypeStruct((sub * (n_chunk + 1),), I32),
        ),
        in_specs=[SMEM, SMEM],
        out_specs=(SMEM,) * 6,
        scratch_shapes=[
            pltpu.SMEM((n_dst * sub,), I32),
            pltpu.SMEM((n_dst * sub,), I32),
            pltpu.SMEM((n_dst * sub,), I32),
        ],
        cost_estimate=pl.CostEstimate(flops=2 * 10 ** 10, bytes_accessed=10 ** 6, transcendentals=0),
        name='row_lists',
    )(place, info)


def rows_loop(n, fn):
    def block(b, c):
        for q in range(8):
            fn(b * 8 + q)
        return c

    def single(r, c):
        fn(r)
        return c

    full = n // 8
    lax.fori_loop(0, full, block, 0)
    lax.fori_loop(full * 8, n, single, 0)


def gelu(v):
    return 0.5 * v * (1.0 + jnp.tanh(math.sqrt(2.0 / math.pi) * (v + 0.044715 * v * v * v)))


def expert_kernel(k, n_chunk, first, *refs):
    (src, seg_start, seg_len, seg_dst_a, seg_dst_b, cs, place, x_hbm, wa_own, wa_sib, wb_own, wb_sib) = refs[:12]
    (send_a, send_b, xbuf, obuf_a, obuf_b, wa, wb, t_e, t_base, t_cnt, gsem, ssem, wsem) = refs[12 if first else 14:]
    e_loc, d_model, _ = wa_own.shape
    sub = 2 * e_loc
    core = place[0]
    sublanes = d_model // LANES
    n_dst = seg_start.shape[0] // (sub * n_chunk)

    def weight_copies(e, act):
        slot = e % 2
        q = e % e_loc

        @pl.when(e // e_loc == core)
        def _():
            act(pltpu.make_async_copy(wa_own.at[q], wa.at[slot], wsem.at[slot, 0]))
            act(pltpu.make_async_copy(wb_own.at[q], wb.at[slot], wsem.at[slot, 1]))

        @pl.when(e // e_loc != core)
        def _():
            act(pltpu.make_async_copy(wa_sib.at[q], wa.at[slot], wsem.at[slot, 0]))
            act(pltpu.make_async_copy(wb_sib.at[q], wb.at[slot], wsem.at[slot, 1]))

    sides = ((obuf_a, send_a, seg_dst_a), (obuf_b, send_b, seg_dst_b))
    weight_copies(0, lambda c: c.start())

    def plan(e, t):
        lo = cs[e * (n_chunk + 1) + k]
        n = cs[e * (n_chunk + 1) + k + 1] - lo

        def put(i, c):
            t_e[t + i] = e
            t_base[t + i] = lo + i * TILE
            t_cnt[t + i] = jnp.minimum(n - i * TILE, TILE)
            return c

        n_tiles = (n + TILE - 1) // TILE
        lax.fori_loop(0, n_tiles, put, 0)
        return t + n_tiles

    n_all = lax.fori_loop(0, sub, plan, 0)

    def gather_start(t):
        base, slot = t_base[t], t % 2
        rows_loop(t_cnt[t], lambda r: pltpu.make_async_copy(
            x_hbm.at[src[base + r]], xbuf.at[slot, r], gsem.at[slot]).start())

    def gather_wait(t):
        n, slot = t_cnt[t], t % 2
        pltpu.make_async_copy(x_hbm.at[pl.ds(0, n)], xbuf.at[slot, pl.ds(0, n)], gsem.at[slot]).wait()

    def scatter_start(t):
        base, slot = t_base[t], t % 2
        end = base + t_cnt[t]

        def segment(i, c):
            j = (t_e[t] * n_chunk + k) * n_dst + i
            first_row = seg_start[j]
            lo = jnp.maximum(first_row, base)
            n = jnp.minimum(first_row + seg_len[j], end) - lo

            @pl.when(n > 0)
            def _():
                for half, (obuf, send, seg_dst) in enumerate(sides):
                    pltpu.make_async_copy(
                        obuf.at[slot, pl.ds(lo - base, n)],
                        send.at[pl.ds(seg_dst[j] + lo - first_row, n)],
                        ssem.at[half, slot],
                    ).start()
            return c

        lax.fori_loop(0, n_dst, segment, 0)

    def scatter_wait(t):
        n, slot = t_cnt[t], t % 2
        for half, (obuf, send, _) in enumerate(sides):
            pltpu.make_async_copy(obuf.at[slot, pl.ds(0, n)], send.at[pl.ds(0, n)], ssem.at[half, slot]).wait()

    for t in range(2):
        @pl.when(t < n_all)
        def _():
            gather_start(t)

    def one_expert(e, t_first):
        weight_copies(e, lambda c: c.wait())

        @pl.when(e + 1 < sub)
        def _():
            weight_copies(e + 1, lambda c: c.start())

        ws = e % 2
        n = cs[e * (n_chunk + 1) + k + 1] - cs[e * (n_chunk + 1) + k]

        def one_tile(i, t):
            slot = t % 2
            gather_wait(t)

            @pl.when(t >= 2)
            def _():
                scatter_wait(t - 2)

            rows = xbuf[slot].reshape(TILE, d_model)
            hidden = gelu(jnp.dot(rows, wa[ws], preferred_element_type=F32)).astype(BF16)
            out = jnp.dot(hidden, wb[ws], preferred_element_type=F32).astype(BF16)
            obuf_a[slot] = out[:, :d_model // 2].reshape(TILE, sublanes // 2, LANES)
            obuf_b[slot] = out[:, d_model // 2:].reshape(TILE, sublanes // 2, LANES)

            @pl.when(t + 2 < n_all)
            def _():
                gather_start(t + 2)

            scatter_start(t)
            return t + 1

        return lax.fori_loop(0, (n + TILE - 1) // TILE, one_tile, t_first)

    lax.fori_loop(0, sub, one_expert, 0)
    for back in (2, 1):
        @pl.when(n_all >= back)
        def _():
            scatter_wait(n_all - back)


def run_experts(k, n_chunk, lists, place, x_rows, wa, wa_sib, wb, wb_sib, sends, rows_a, rows_b):
    e_loc, d_model, ff = wa.shape
    sub = 2 * e_loc
    sublanes = d_model // LANES
    half = sublanes // 2
    first = sends is None
    ops = (*lists, place, x_rows, wa, wa_sib, wb, wb_sib) + (() if first else tuple(sends))
    n_smem = len(lists) + 1
    max_tiles = sub * (pl.cdiv(lists[0].shape[0] // sub, TILE) + 1)
    flops = 4 * d_model * ff * x_rows.shape[0]
    return pl.pallas_call(
        functools.partial(expert_kernel, k, n_chunk, first),
        out_shape=(
            jax.ShapeDtypeStruct((rows_a, half, LANES), BF16),
            jax.ShapeDtypeStruct((rows_b, half, LANES), BF16),
        ),
        in_specs=[SMEM] * n_smem + [HBM] * (len(ops) - n_smem),
        out_specs=(HBM, HBM),
        scratch_shapes=[
            pltpu.VMEM((2, TILE, sublanes, LANES), BF16),
            pltpu.VMEM((2, TILE, half, LANES), BF16),
            pltpu.VMEM((2, TILE, half, LANES), BF16),
            pltpu.VMEM((2, d_model, ff), BF16),
            pltpu.VMEM((2, ff, d_model), BF16),
            pltpu.SMEM((max_tiles,), I32),
            pltpu.SMEM((max_tiles,), I32),
            pltpu.SMEM((max_tiles,), I32),
            pltpu.SemaphoreType.DMA((2,)),
            pltpu.SemaphoreType.DMA((2, 2)),
            pltpu.SemaphoreType.DMA((2, 2)),
        ],
        input_output_aliases={} if first else {len(ops) - 2: 0, len(ops) - 1: 1},
        compiler_params=pltpu.CompilerParams(vmem_limit_bytes=VMEM_LIMIT),
        cost_estimate=pl.CostEstimate(flops=flops, bytes_accessed=6 * 10 ** 7, transcendentals=0),
        name='experts',
    )(*ops)


PIECES = 4


class Ring:
    def __init__(self, axis, n_y, n_x):
        y, ec = lax.axis_index('ep2'), lax.axis_index('ep')
        self.axis, self.core = axis, ec % 2
        self.n = n_x if axis == 'x' else n_y
        self.pos = ec // 2 if axis == 'x' else y
        far = self.n // 2 if self.n % 2 == 0 and self.n >= 4 else None
        self.direct = [d for d in range(1, self.n) if d != far]
        self.far = far

    def place(self, d):
        return lax.rem(self.pos + d + self.n, self.n)

    def device(self, d):
        if self.axis == 'x':
            return {'ep': self.place(d) * 2 + self.core}
        return {'ep2': self.place(d)}

    def remote(self, src, dst, sems, i, d):
        return pltpu.make_async_remote_copy(
            src_ref=src, dst_ref=dst, send_sem=sems.at[0, i], recv_sem=sems.at[1, i],
            device_id=self.device(d), device_id_type=pl.DeviceIdType.MESH)

    def signal(self, barrier):
        for d in range(1, self.n):
            pl.semaphore_signal(barrier, inc=1, device_id=self.device(d), device_id_type=pl.DeviceIdType.MESH)


def spread_kernel(rows_a, rows_b, n_y, n_x, send_a, send_b, recv_a, recv_b, stage_a, stage_b, sem_a, sem_b):
    rings = (Ring('x', n_y, n_x), Ring('y', n_y, n_x))
    barrier = pltpu.get_barrier_semaphore()
    for ring in rings:
        ring.signal(barrier)
    pl.semaphore_wait(barrier, n_x + n_y - 2)

    sides = list(zip(rings, (rows_a, rows_b), (send_a, send_b), (recv_a, recv_b), (stage_a, stage_b), (sem_a, sem_b)))

    def lead(side, p):
        ring, rows, send, _, stage, sem = side
        hop = ring.far // 2 if p % 2 == 0 else -(ring.far // 2)
        part = pl.ds(p * (rows // PIECES), rows // PIECES)
        return ring.remote(send.at[ring.place(ring.far), part], stage.at[part], sem, p, hop)

    def follow(side, p):
        ring, rows, _, recv, stage, sem = side
        hop = ring.far // 2 if p % 2 == 0 else -(ring.far // 2)
        part = pl.ds(p * (rows // PIECES), rows // PIECES)
        return ring.remote(stage.at[part], recv.at[ring.place(-hop), part], sem, PIECES + p, hop)

    def straight(side, i):
        ring, rows, send, recv, _, sem = side
        d = ring.direct[i]
        return ring.remote(send.at[ring.place(d), pl.ds(0, rows)], recv.at[ring.pos, pl.ds(0, rows)], sem, 2 * PIECES + i, d)

    relayed = [(side, p) for p in range(PIECES) for side in sides if side[0].far]
    direct = [(side, i) for side in sides for i in range(len(side[0].direct))]
    for job in relayed:
        lead(*job).start()
    for job in direct:
        straight(*job).start()
    for job in relayed:
        lead(*job).wait_recv()
        follow(*job).start()
    for job in relayed:
        lead(*job).wait_send()
    for job in direct:
        straight(*job).wait()
    for job in relayed:
        follow(*job).wait()


def spread(rows_a, rows_b, cid, n_y, n_x, send_a, send_b):
    return pl.pallas_call(
        functools.partial(spread_kernel, rows_a, rows_b, n_y, n_x),
        out_shape=tuple(jax.ShapeDtypeStruct(s, BF16) for s in (send_a.shape, send_b.shape, send_a.shape[1:], send_b.shape[1:])),
        in_specs=[HBM, HBM],
        out_specs=(HBM,) * 4,
        scratch_shapes=[
            pltpu.SemaphoreType.DMA((2, 2 * PIECES + n_x)),
            pltpu.SemaphoreType.DMA((2, 2 * PIECES + n_y)),
        ],
        compiler_params=pltpu.CompilerParams(collective_id=cid, has_side_effects=True),
        name='spread_%d_%d' % (rows_a, rows_b),
    )(send_a, send_b)[:2]


def sum_kernel(n_y, n_x, kept_a, kept_b, place, tok_hbm, wgt_hbm, recv_a, recv_b, send_a, send_b, z_a, z_b,
               tok, wgt, rbuf, acc0, acc1, tsem, rsem, zsem):
    core, chip = place[0], place[1]
    my_y, my_x = chip // n_x, chip % n_x
    n_chip = n_y * n_x
    sub = kept_a.shape[0] // n_chip
    n_tok = z_a.shape[1]
    words = sub * LANES
    per_dev = tok_hbm.shape[0] // (2 * n_chip)
    blk = 16
    accs = (acc0, acc1)

    def tables(half, act):
        for i in range(n_y if half == 0 else n_x):
            g = (i * n_x + my_x) * 2 + core if half == 0 else (my_y * n_x + i) * 2 + core
            for q in range(n_x if half == 0 else n_y):
                owner = my_y * n_x + q if half == 0 else q * n_x + my_x
                src = pl.ds(pl.multiple_of(g * per_dev + owner * words, words), words)
                dst = pl.ds((half * n_chip + i * (n_x if half == 0 else n_y) + q) * words, words)
                act(pltpu.make_async_copy(tok_hbm.at[src], tok.at[dst], tsem.at[half]))
                act(pltpu.make_async_copy(wgt_hbm.at[src], wgt.at[dst], tsem.at[half]))

    for half in range(2):
        tables(half, lambda c: c.start())

    def one_half(half, kept, recv, send, z, mine, n_dst, n_src):
        def count(q):
            def add(i, n):
                for e in range(sub):
                    n = n + kept[(i * n_src + q) * sub + e]
                return n
            return lax.fori_loop(0, n_dst, add, 0)

        def fetch(q, act):
            slot, n = q % 2, count(q)

            @pl.when(jnp.logical_and(q == mine, n > 0))
            def _():
                act(pltpu.make_async_copy(send.at[q, pl.ds(0, n)], rbuf.at[slot, pl.ds(0, n)], rsem.at[slot]))

            @pl.when(jnp.logical_and(q != mine, n > 0))
            def _():
                act(pltpu.make_async_copy(recv.at[q, pl.ds(0, n)], rbuf.at[slot, pl.ds(0, n)], rsem.at[slot]))

        fetch(0, lambda c: c.start())

        def zero(b, c):
            for acc in accs:
                acc[pl.ds(b * blk, blk)] = jnp.zeros((blk, *acc.shape[1:]), F32)
            return c

        lax.fori_loop(0, n_dst * n_tok // blk, zero, 0)
        tables(half, lambda c: c.wait())
        dummy = n_dst * n_tok

        def one_source(q, c):
            slot = q % 2

            @pl.when(q + 1 < n_src)
            def _():
                fetch(q + 1, lambda d: d.start())

            fetch(q, lambda d: d.wait())

            def one_list(j, base):
                i, e = j // sub, j % sub
                n = kept[(i * n_src + q) * sub + e]
                first = (half * n_chip + i * n_src + q) * words + e * LANES
                shift = i * n_tok

                def quad(b, cc):
                    at = first + b * 4
                    toks = [jnp.where(b * 4 + p < n, shift + tok[at + p], dummy) for p in range(4)]
                    wgts = [wgt[at + p] for p in range(4)]
                    rows = [wgts[p] * rbuf[slot, base + b * 4 + p].astype(F32) for p in range(4)]
                    for p in range(4):
                        acc = accs[p % 2]
                        acc[toks[p]] = acc[toks[p]] + rows[p]
                    return cc

                lax.fori_loop(0, (n + 3) // 4, quad, 0)
                return base + n

            lax.fori_loop(0, n_dst * sub, one_list, 0)
            return c

        lax.fori_loop(0, n_src, one_source, 0)

        def put(i):
            return pltpu.make_async_copy(acc0.at[pl.ds(i * n_tok, n_tok)], z.at[i], zsem.at[i])

        for i in range(n_dst):
            def merge(b, c):
                rows = pl.ds(i * n_tok + b * blk, blk)
                acc0[rows] = acc0[rows] + acc1[rows]
                return c
            lax.fori_loop(0, n_tok // blk, merge, 0)
            put(i).start()
        for i in range(n_dst):
            put(i).wait()

    one_half(0, kept_a, recv_a, send_a, z_a, my_x, n_y, n_x)
    one_half(1, kept_b, recv_b, send_b, z_b, my_y, n_x, n_y)


def weighted_sums(n_y, n_x, kept_a, kept_b, place, tok, wgt, recv_a, recv_b, send_a, send_b, n_tok):
    half = recv_a.shape[2]
    n_dst = max(n_y, n_x)
    slots = max(recv_a.shape[1], recv_b.shape[1])
    words = kept_a.shape[0] * LANES
    acc = pltpu.VMEM((n_dst * n_tok + 8, half, LANES), F32)
    return pl.pallas_call(
        functools.partial(sum_kernel, n_y, n_x),
        out_shape=(
            jax.ShapeDtypeStruct((n_y, n_tok, half, LANES), F32),
            jax.ShapeDtypeStruct((n_x, n_tok, half, LANES), F32),
        ),
        in_specs=[SMEM] * 3 + [HBM] * 6,
        out_specs=(HBM, HBM),
        scratch_shapes=[
            pltpu.SMEM((2 * words,), I32),
            pltpu.SMEM((2 * words,), F32),
            pltpu.VMEM((2, slots + 8, half, LANES), BF16),
            acc, acc,
            pltpu.SemaphoreType.DMA((2,)),
            pltpu.SemaphoreType.DMA((2,)),
            pltpu.SemaphoreType.DMA((n_dst,)),
        ],
        compiler_params=pltpu.CompilerParams(vmem_limit_bytes=VMEM_LIMIT),
        cost_estimate=pl.CostEstimate(flops=2 * 10 ** 10, bytes_accessed=6 * 10 ** 7, transcendentals=0),
        name='weighted_sums',
    )(kept_a, kept_b, place, tok, wgt, recv_a, recv_b, send_a, send_b)


SUM_CHUNKS = 4


def reduce_kernel(n_y, n_x, z_a, z_b, x_ref, y_ref, own, part, zsem, rsem):
    rings = (Ring('y', n_y, n_x), Ring('x', n_y, n_x))
    zs = (z_a, z_b)
    n_tok, d_model = x_ref.shape
    rows = n_tok // (2 * SUM_CHUNKS)
    half = d_model // 2
    blk = 16
    lanes = [(a, w) for a in range(2) for w in range(2)]
    steps = [ring.n - 1 for ring in rings]

    barrier = pltpu.get_barrier_semaphore()
    for ring in rings:
        for d in (1, -1):
            pl.semaphore_signal(barrier, inc=1, device_id=ring.device(d), device_id_type=pl.DeviceIdType.MESH)
    pl.semaphore_wait(barrier, 4)

    def sign(w):
        return 1 if w == 0 else -1

    def chunk(w, j):
        return pl.ds((w * SUM_CHUNKS + j) * rows, rows)

    def load(a, w, s, j):
        block = rings[a].place(-sign(w) * (s + 1)) if s < steps[a] else rings[a].pos
        return pltpu.make_async_copy(zs[a].at[block, chunk(w, j)], own.at[a, w, s - 1, j], zsem.at[a, w, s - 1, j])

    def hop(a, w, s, j):
        ring = rings[a]
        src = zs[a].at[ring.place(-sign(w)), chunk(w, j)] if s == 0 else part.at[a, w, s - 1, j]
        return pltpu.make_async_remote_copy(
            src_ref=src, dst_ref=part.at[a, w, s, j], send_sem=rsem.at[0, a, w, s, j], recv_sem=rsem.at[1, a, w, s, j],
            device_id=ring.device(sign(w)), device_id_type=pl.DeviceIdType.MESH)

    for j in range(SUM_CHUNKS):
        for a, w in lanes:
            hop(a, w, 0, j).start()
    for s in range(1, max(steps) + 1):
        for j in range(SUM_CHUNKS):
            for a, w in lanes:
                if s <= steps[a]:
                    load(a, w, s, j).start()

    for s in range(1, max(steps)):
        for j in range(SUM_CHUNKS):
            for a, w in lanes:
                if s >= steps[a]:
                    continue
                load(a, w, s, j).wait()
                hop(a, w, s - 1, j).wait_recv()

                def add(b, c):
                    r = pl.ds(b * blk, blk)
                    part[a, w, s - 1, j, r] = part[a, w, s - 1, j, r] + own[a, w, s - 1, j, r]
                    return c

                lax.fori_loop(0, rows // blk, add, 0)
                hop(a, w, s, j).start()

    for j in range(SUM_CHUNKS):
        for a, w in lanes:
            s = steps[a]
            load(a, w, s, j).wait()
            hop(a, w, s - 1, j).wait_recv()
            first = (w * SUM_CHUNKS + j) * rows

            def finish(b, c):
                r = pl.ds(b * blk, blk)
                out = pl.ds(pl.multiple_of(first + b * blk, blk), blk)
                cols = pl.ds(a * half, half)
                total = part[a, w, s - 1, j, r] + own[a, w, s - 1, j, r]
                y_ref[out, cols] = (x_ref[out, cols].astype(F32) + total.reshape(blk, half)).astype(BF16)
                return c

            lax.fori_loop(0, rows // blk, finish, 0)
    for s in range(max(steps)):
        for j in range(SUM_CHUNKS):
            for a, w in lanes:
                if s < steps[a]:
                    hop(a, w, s, j).wait_send()


def reduce_back(cid, n_y, n_x, z_a, z_b, x):
    n_tok, d_model = x.shape
    rows = n_tok // (2 * SUM_CHUNKS)
    steps = max(n_y, n_x) - 1
    buf = pltpu.VMEM((2, 2, steps, SUM_CHUNKS, rows, z_a.shape[2], LANES), F32)
    return pl.pallas_call(
        functools.partial(reduce_kernel, n_y, n_x),
        out_shape=jax.ShapeDtypeStruct((n_tok, d_model), BF16),
        in_specs=[HBM, HBM, VMEM],
        out_specs=VMEM,
        scratch_shapes=[
            buf, buf,
            pltpu.SemaphoreType.DMA((2, 2, steps, SUM_CHUNKS)),
            pltpu.SemaphoreType.DMA((2, 2, 2, steps, SUM_CHUNKS)),
        ],
        compiler_params=pltpu.CompilerParams(collective_id=cid, has_side_effects=True, vmem_limit_bytes=VMEM_LIMIT),
        name='reduce_back',
    )(z_a, z_b, x)


def solution(mesh):
    dev_axes = ('ep2', 'ep')
    n_y, n_ep = mesh.shape['ep2'], mesh.shape['ep']
    n_x = n_ep // 2
    group = n_y * n_ep
    n_chip = n_y * n_x

    def local_step(x_loc, ids_loc, gate_loc, w_a, w_b):
        n_tok, d_model = x_loc.shape
        n_top = ids_loc.shape[1]
        e_loc = w_a.shape[0]
        sub = 2 * e_loc
        experts = e_loc * group
        cap = capacity_of(group, n_tok, n_top, experts)
        sublanes = d_model // LANES
        slots_a, slots_b = n_y * sub * LANES, n_x * sub * LANES
        bounds = tuple(n_tok * q // CHUNK_UNITS for q in CHUNK_ENDS)
        n_chunk = len(bounds) - 1
        me = lax.axis_index(dev_axes)
        core, chip = me % 2, me // 2
        place = jnp.stack([core, chip]).astype(I32)

        x3 = x_loc.reshape(n_tok, sublanes, LANES)
        chunks = [lax.all_gather(x3[bounds[k]:bounds[k + 1]], dev_axes, tiled=True) for k in range(n_chunk)]
        swap = [(i, i ^ 1) for i in range(n_ep)]
        w_a_sib = lax.ppermute(w_a, 'ep', swap)
        w_b_sib = lax.ppermute(w_b, 'ep', swap)

        toks, wgts, cnts = route(ids_loc, gate_loc, bounds)
        for_chip = toks[:experts].reshape(n_chip, 1, sub, LANES)
        table = jnp.concatenate([
            jnp.broadcast_to(for_chip, (n_chip, 2, sub, LANES)).reshape(group, sub, LANES),
            jnp.broadcast_to(cnts[None], (group, PREFIX_ROWS, LANES))], axis=1)
        table = lax.all_to_all(table, dev_axes, 0, 0, tiled=True)
        lists = build_lists(place, table.reshape(-1), cap, slots_a, slots_b, bounds, n_y, n_x, sub)

        totals = table[:, sub + n_chunk, :experts]
        offs = jnp.cumsum(totals, axis=0) - totals
        kept = jnp.clip(cap - offs, 0, totals)
        by_place = kept.reshape(n_y, n_x, 2, n_y, n_x, sub)
        y, x = chip // n_x, chip % n_x
        kept_a = lax.dynamic_slice(by_place, (0, x, core, y, 0, 0), (n_y, 1, 1, 1, n_x, sub)).reshape(-1)
        kept_b = lax.dynamic_slice(by_place, (y, 0, core, 0, x, 0), (1, n_x, 1, n_y, 1, sub)).reshape(-1)
        per_chip = jnp.sum(by_place, axis=5)
        need_a = jnp.max(jnp.sum(per_chip, axis=0))
        need_b = jnp.max(jnp.sum(per_chip, axis=1))

        sends = None
        for k in range(n_chunk):
            if k == n_chunk - 1:
                toks, wgts, sends = lax.optimization_barrier((toks, wgts, sends))
            sends = run_experts(k, n_chunk, lists, place, chunks[k], w_a, w_a_sib, w_b, w_b_sib, sends, n_x * slots_a, n_y * slots_b)
        tok_all = lax.all_gather(toks[:experts].reshape(-1), dev_axes, tiled=True)
        wgt_all = lax.all_gather(wgts[:experts].reshape(-1), dev_axes, tiled=True)
        send_a = sends[0].reshape(n_x, slots_a, sublanes // 2, LANES)
        send_b = sends[1].reshape(n_y, slots_b, sublanes // 2, LANES)

        tiers = [(slots_a * q // 64, slots_b * q // 64) for q in SIZES]
        index = jnp.int32(len(tiers) - 1)
        for i in range(len(tiers) - 2, -1, -1):
            fits = jnp.logical_and(need_a <= tiers[i][0], need_b <= tiers[i][1])
            index = jnp.where(fits, jnp.int32(i), index)
        recv_a, recv_b = lax.switch(index, [functools.partial(spread, a, b, i, n_y, n_x) for i, (a, b) in enumerate(tiers)], send_a, send_b)
        recv_a, tok_all, wgt_all = lax.optimization_barrier((recv_a, tok_all, wgt_all))
        z_a, z_b = weighted_sums(n_y, n_x, kept_a, kept_b, place, tok_all, wgt_all, recv_a, recv_b, send_a, send_b, n_tok)
        return reduce_back(len(tiers), n_y, n_x, z_a, z_b, x_loc)

    tok_spec = P(('dp', 'ep2', 'ep'), None)
    w_spec = P(dev_axes, None, None)
    return jax.shard_map(local_step, mesh=mesh, in_specs=(tok_spec, tok_spec, tok_spec, w_spec, w_spec), out_specs=tok_spec, check_vma=False)
```

```python
import functools
import math

import jax
import jax.numpy as jnp
from jax import lax
from jax.experimental import pallas as pl
from jax.experimental.pallas import tpu as pltpu
from jax.sharding import PartitionSpec as P

LANES = 128
CHUNK_UNITS = 32
CHUNK_ENDS = (0, 25, 32)
SIZES = (40, 42, 44, 46, 48, 52, 64)
TILE = 256
PREFIX_ROWS = 8
BF16 = jnp.bfloat16
F32 = jnp.float32
I32 = jnp.int32
HBM = pl.BlockSpec(memory_space=pl.ANY)
SMEM = pl.BlockSpec(memory_space=pltpu.SMEM)
VMEM = pl.BlockSpec(memory_space=pltpu.VMEM)
VMEM_LIMIT = 64_000_000


def capacity_of(group_size, n_tok, n_top, experts):
    return 8 * ((5 * group_size * n_tok * n_top) // (32 * experts))


def route_kernel(bounds, ids_ref, gate_ref, tok_ref, wgt_ref, cnt_ref, code_t, gate_t, tok_acc, wgt_acc):
    n_tok, n_top = ids_ref.shape
    lane = lax.broadcasted_iota(I32, (n_tok, LANES), 1)
    member = jnp.zeros((n_tok, LANES), F32)
    gates = jnp.zeros((n_tok, LANES), F32)
    for j in range(n_top):
        hit = ids_ref[:, j:j + 1] == lane
        member = member + jnp.where(hit, 1.0, 0.0)
        gates = gates + jnp.where(hit, gate_ref[:, j:j + 1], 0.0)
    member_b = member.astype(BF16)
    row_block = min(n_tok, 128)
    for i in range(n_tok // row_block):
        rows = pl.ds(i * row_block, row_block)
        later = lax.broadcasted_iota(I32, (row_block, n_tok), 0) + i * row_block
        earlier = lax.broadcasted_iota(I32, (row_block, n_tok), 1)
        tri = jnp.where(earlier < later, 1.0, 0.0).astype(BF16)
        rank = jnp.dot(tri, member_b, preferred_element_type=F32)
        mem = member[i * row_block:(i + 1) * row_block]
        code_t[:, rows] = jnp.where(mem > 0.5, rank, -1.0).T
        gate_t[:, rows] = gates[i * row_block:(i + 1) * row_block].T
    total = jnp.zeros((1, LANES), F32)
    rows_out = [total]
    for lo, hi in zip(bounds[:-1], bounds[1:]):
        total = total + jnp.sum(member[lo:hi], axis=0, keepdims=True)
        rows_out.append(total)
    while len(rows_out) < PREFIX_ROWS:
        rows_out.append(total)
    cnt_ref[...] = jnp.concatenate(rows_out, axis=0).astype(I32)
    tok_acc[...] = jnp.zeros_like(tok_acc)
    wgt_acc[...] = jnp.zeros_like(wgt_acc)
    slot = lax.broadcasted_iota(I32, (LANES, n_tok), 0).astype(F32)
    token = lax.broadcasted_iota(I32, (1, n_tok), 1).astype(F32)
    out_lane = lax.broadcasted_iota(I32, (LANES, LANES), 1)

    def one_expert(e, carry):
        hit = slot == code_t[pl.ds(e, 1), :]
        tok = jnp.sum(jnp.where(hit, token, 0.0), axis=1, keepdims=True)
        wgt = jnp.sum(jnp.where(hit, gate_t[pl.ds(e, 1), :], 0.0), axis=1, keepdims=True)
        tok_acc[...] = jnp.where(out_lane == e, tok, tok_acc[...])
        wgt_acc[...] = jnp.where(out_lane == e, wgt, wgt_acc[...])
        return carry

    lax.fori_loop(0, LANES, one_expert, 0)
    tok_ref[...] = tok_acc[...].T.astype(I32)
    wgt_ref[...] = wgt_acc[...].T


def route(ids, gate, bounds):
    n_tok = ids.shape[0]
    return pl.pallas_call(
        functools.partial(route_kernel, bounds),
        out_shape=(
            jax.ShapeDtypeStruct((LANES, LANES), I32),
            jax.ShapeDtypeStruct((LANES, LANES), F32),
            jax.ShapeDtypeStruct((PREFIX_ROWS, LANES), I32),
        ),
        in_specs=[VMEM, VMEM],
        out_specs=(VMEM, VMEM, VMEM),
        scratch_shapes=[
            pltpu.VMEM((LANES, n_tok), F32),
            pltpu.VMEM((LANES, n_tok), F32),
            pltpu.VMEM((LANES, LANES), F32),
            pltpu.VMEM((LANES, LANES), F32),
        ],
        cost_estimate=pl.CostEstimate(flops=2 * 10 ** 10, bytes_accessed=10 ** 6, transcendentals=0),
        name='route',
    )(ids, gate)


def list_kernel(cap, slots_a, slots_b, bounds, n_y, n_x, sub, place_ref, info_ref, src_ref, start_ref, len_ref, dst_a_ref, dst_b_ref, cs_ref,
                kept_ref, base_a_ref, base_b_ref):
    core, chip = place_ref[0], place_ref[1]
    n_dst = n_y * n_x
    n_chunk = len(bounds) - 1
    dev_words = (sub + PREFIX_ROWS) * LANES
    width = src_ref.shape[0] // sub

    def count(g, k, e):
        return info_ref[g * dev_words + (sub + k) * LANES + chip * sub + e]

    def per_expert(e, carry):
        def per_dev(i, off):
            for c in range(2):
                n = count(2 * i + c, n_chunk, e)
                kept = jnp.clip(cap - off, 0, n)
                off = off + n

                @pl.when(core == c)
                def _():
                    kept_ref[i * sub + e] = kept
            return off
        lax.fori_loop(0, n_dst, per_dev, 0)
        return carry

    lax.fori_loop(0, sub, per_expert, 0)

    def add_up(base_ref, i, acc):
        def add(e, acc):
            base_ref[i * sub + e] = acc
            return acc + kept_ref[i * sub + e]
        return lax.fori_loop(0, sub, add, acc)

    for x in range(n_x):
        lax.fori_loop(0, n_y, lambda y, acc: add_up(base_a_ref, y * n_x + x, acc), x * slots_a)
    for y in range(n_y):
        lax.fori_loop(0, n_x, lambda x, acc: add_up(base_b_ref, y * n_x + x, acc), y * slots_b)

    def expert_lists(e, carry):
        pos = e * width
        for k in range(n_chunk):
            cs_ref[e * (n_chunk + 1) + k] = pos
            size = bounds[k + 1] - bounds[k]

            def segment(i, o):
                g = 2 * i + core
                kept = kept_ref[i * sub + e]
                s0 = jnp.minimum(count(g, k, e), kept)
                n = jnp.minimum(count(g, k + 1, e), kept) - s0
                j = (e * n_chunk + k) * n_dst + i
                start_ref[j] = o
                len_ref[j] = n
                dst_a_ref[j] = base_a_ref[i * sub + e] + s0
                dst_b_ref[j] = base_b_ref[i * sub + e] + s0
                src0 = g * size - bounds[k]
                tok0 = g * dev_words + e * LANES + s0

                def block(b, c):
                    vals = [info_ref[tok0 + b * 8 + q] for q in range(8)]
                    for q in range(8):
                        src_ref[o + b * 8 + q] = src0 + vals[q]
                    return c

                lax.fori_loop(0, (n + 7) // 8, block, 0)
                return o + n

            pos = lax.fori_loop(0, n_dst, segment, pos)
        cs_ref[e * (n_chunk + 1) + n_chunk] = pos
        return carry

    lax.fori_loop(0, sub, expert_lists, 0)


def build_lists(place, info, cap, slots_a, slots_b, bounds, n_y, n_x, sub):
    n_dst, n_chunk = n_y * n_x, len(bounds) - 1
    width = LANES * n_dst + 8
    segs = sub * n_chunk * n_dst
    return pl.pallas_call(
        functools.partial(list_kernel, cap, slots_a, slots_b, bounds, n_y, n_x, sub),
        out_shape=(
            jax.ShapeDtypeStruct((sub * width,), I32),
            jax.ShapeDtypeStruct((segs,), I32),
            jax.ShapeDtypeStruct((segs,), I32),
            jax.ShapeDtypeStruct((segs,), I32),
            jax.ShapeDtypeStruct((segs,), I32),
            jax.ShapeDtypeStruct((sub * (n_chunk + 1),), I32),
        ),
        in_specs=[SMEM, SMEM],
        out_specs=(SMEM,) * 6,
        scratch_shapes=[
            pltpu.SMEM((n_dst * sub,), I32),
            pltpu.SMEM((n_dst * sub,), I32),
            pltpu.SMEM((n_dst * sub,), I32),
        ],
        cost_estimate=pl.CostEstimate(flops=2 * 10 ** 10, bytes_accessed=10 ** 6, transcendentals=0),
        name='row_lists',
    )(place, info)


def rows_loop(n, fn):
    def block(b, c):
        for q in range(8):
            fn(b * 8 + q)
        return c

    def single(r, c):
        fn(r)
        return c

    full = n // 8
    lax.fori_loop(0, full, block, 0)
    lax.fori_loop(full * 8, n, single, 0)


def gelu(v):
    return 0.5 * v * (1.0 + jnp.tanh(math.sqrt(2.0 / math.pi) * (v + 0.044715 * v * v * v)))


def expert_kernel(k, n_chunk, first, *refs):
    (src, seg_start, seg_len, seg_dst_a, seg_dst_b, cs, place, x_hbm, wa_own, wa_sib, wb_own, wb_sib) = refs[:12]
    (send_a, send_b, xbuf, obuf_a, obuf_b, wa, wb, t_e, t_base, t_cnt, gsem, ssem, wsem) = refs[12 if first else 14:]
    e_loc, d_model, _ = wa_own.shape
    sub = 2 * e_loc
    core = place[0]
    sublanes = d_model // LANES
    n_dst = seg_start.shape[0] // (sub * n_chunk)

    def weight_copies(e, act):
        slot = e % 2
        q = e % e_loc

        @pl.when(e // e_loc == core)
        def _():
            act(pltpu.make_async_copy(wa_own.at[q], wa.at[slot], wsem.at[slot, 0]))
            act(pltpu.make_async_copy(wb_own.at[q], wb.at[slot], wsem.at[slot, 1]))

        @pl.when(e // e_loc != core)
        def _():
            act(pltpu.make_async_copy(wa_sib.at[q], wa.at[slot], wsem.at[slot, 0]))
            act(pltpu.make_async_copy(wb_sib.at[q], wb.at[slot], wsem.at[slot, 1]))

    sides = ((obuf_a, send_a, seg_dst_a), (obuf_b, send_b, seg_dst_b))
    weight_copies(0, lambda c: c.start())

    def plan(e, t):
        lo = cs[e * (n_chunk + 1) + k]
        n = cs[e * (n_chunk + 1) + k + 1] - lo

        def put(i, c):
            t_e[t + i] = e
            t_base[t + i] = lo + i * TILE
            t_cnt[t + i] = jnp.minimum(n - i * TILE, TILE)
            return c

        n_tiles = (n + TILE - 1) // TILE
        lax.fori_loop(0, n_tiles, put, 0)
        return t + n_tiles

    n_all = lax.fori_loop(0, sub, plan, 0)

    def gather_start(t):
        base, slot = t_base[t], t % 2
        rows_loop(t_cnt[t], lambda r: pltpu.make_async_copy(
            x_hbm.at[src[base + r]], xbuf.at[slot, r], gsem.at[slot]).start())

    def gather_wait(t):
        n, slot = t_cnt[t], t % 2
        pltpu.make_async_copy(x_hbm.at[pl.ds(0, n)], xbuf.at[slot, pl.ds(0, n)], gsem.at[slot]).wait()

    def scatter_start(t):
        base, slot = t_base[t], t % 2
        end = base + t_cnt[t]

        def segment(i, c):
            j = (t_e[t] * n_chunk + k) * n_dst + i
            first_row = seg_start[j]
            lo = jnp.maximum(first_row, base)
            n = jnp.minimum(first_row + seg_len[j], end) - lo

            @pl.when(n > 0)
            def _():
                for half, (obuf, send, seg_dst) in enumerate(sides):
                    pltpu.make_async_copy(
                        obuf.at[slot, pl.ds(lo - base, n)],
                        send.at[pl.ds(seg_dst[j] + lo - first_row, n)],
                        ssem.at[half, slot],
                    ).start()
            return c

        lax.fori_loop(0, n_dst, segment, 0)

    def scatter_wait(t):
        n, slot = t_cnt[t], t % 2
        for half, (obuf, send, _) in enumerate(sides):
            pltpu.make_async_copy(obuf.at[slot, pl.ds(0, n)], send.at[pl.ds(0, n)], ssem.at[half, slot]).wait()

    for t in range(2):
        @pl.when(t < n_all)
        def _():
            gather_start(t)

    def one_expert(e, t_first):
        weight_copies(e, lambda c: c.wait())

        @pl.when(e + 1 < sub)
        def _():
            weight_copies(e + 1, lambda c: c.start())

        ws = e % 2
        n = cs[e * (n_chunk + 1) + k + 1] - cs[e * (n_chunk + 1) + k]

        def one_tile(i, t):
            slot = t % 2
            gather_wait(t)

            @pl.when(t >= 2)
            def _():
                scatter_wait(t - 2)

            rows = xbuf[slot].reshape(TILE, d_model)
            hidden = gelu(jnp.dot(rows, wa[ws], preferred_element_type=F32)).astype(BF16)
            out = jnp.dot(hidden, wb[ws], preferred_element_type=F32).astype(BF16)
            obuf_a[slot] = out[:, :d_model // 2].reshape(TILE, sublanes // 2, LANES)
            obuf_b[slot] = out[:, d_model // 2:].reshape(TILE, sublanes // 2, LANES)

            @pl.when(t + 2 < n_all)
            def _():
                gather_start(t + 2)

            scatter_start(t)
            return t + 1

        return lax.fori_loop(0, (n + TILE - 1) // TILE, one_tile, t_first)

    lax.fori_loop(0, sub, one_expert, 0)
    for back in (2, 1):
        @pl.when(n_all >= back)
        def _():
            scatter_wait(n_all - back)


def run_experts(k, n_chunk, lists, place, x_rows, wa, wa_sib, wb, wb_sib, sends, rows_a, rows_b):
    e_loc, d_model, ff = wa.shape
    sub = 2 * e_loc
    sublanes = d_model // LANES
    half = sublanes // 2
    first = sends is None
    ops = (*lists, place, x_rows, wa, wa_sib, wb, wb_sib) + (() if first else tuple(sends))
    n_smem = len(lists) + 1
    max_tiles = sub * (pl.cdiv(lists[0].shape[0] // sub, TILE) + 1)
    flops = 4 * d_model * ff * x_rows.shape[0]
    return pl.pallas_call(
        functools.partial(expert_kernel, k, n_chunk, first),
        out_shape=(
            jax.ShapeDtypeStruct((rows_a, half, LANES), BF16),
            jax.ShapeDtypeStruct((rows_b, half, LANES), BF16),
        ),
        in_specs=[SMEM] * n_smem + [HBM] * (len(ops) - n_smem),
        out_specs=(HBM, HBM),
        scratch_shapes=[
            pltpu.VMEM((2, TILE, sublanes, LANES), BF16),
            pltpu.VMEM((2, TILE, half, LANES), BF16),
            pltpu.VMEM((2, TILE, half, LANES), BF16),
            pltpu.VMEM((2, d_model, ff), BF16),
            pltpu.VMEM((2, ff, d_model), BF16),
            pltpu.SMEM((max_tiles,), I32),
            pltpu.SMEM((max_tiles,), I32),
            pltpu.SMEM((max_tiles,), I32),
            pltpu.SemaphoreType.DMA((2,)),
            pltpu.SemaphoreType.DMA((2, 2)),
            pltpu.SemaphoreType.DMA((2, 2)),
        ],
        input_output_aliases={} if first else {len(ops) - 2: 0, len(ops) - 1: 1},
        compiler_params=pltpu.CompilerParams(vmem_limit_bytes=VMEM_LIMIT),
        cost_estimate=pl.CostEstimate(flops=flops, bytes_accessed=6 * 10 ** 7, transcendentals=0),
        name='experts',
    )(*ops)


PIECES = 4


class Ring:
    def __init__(self, axis, n_y, n_x):
        y, ec = lax.axis_index('ep2'), lax.axis_index('ep')
        self.axis, self.core = axis, ec % 2
        self.n = n_x if axis == 'x' else n_y
        self.pos = ec // 2 if axis == 'x' else y
        far = self.n // 2 if self.n % 2 == 0 and self.n >= 4 else None
        self.direct = [d for d in range(1, self.n) if d != far]
        self.far = far

    def place(self, d):
        return lax.rem(self.pos + d + self.n, self.n)

    def device(self, d):
        if self.axis == 'x':
            return {'ep': self.place(d) * 2 + self.core}
        return {'ep2': self.place(d)}

    def remote(self, src, dst, sems, i, d):
        return pltpu.make_async_remote_copy(
            src_ref=src, dst_ref=dst, send_sem=sems.at[0, i], recv_sem=sems.at[1, i],
            device_id=self.device(d), device_id_type=pl.DeviceIdType.MESH)

    def signal(self, barrier):
        for d in range(1, self.n):
            pl.semaphore_signal(barrier, inc=1, device_id=self.device(d), device_id_type=pl.DeviceIdType.MESH)


def spread_kernel(rows_a, rows_b, n_y, n_x, send_a, send_b, recv_a, recv_b, stage_a, stage_b, sem_a, sem_b):
    rings = (Ring('x', n_y, n_x), Ring('y', n_y, n_x))
    barrier = pltpu.get_barrier_semaphore()
    for ring in rings:
        ring.signal(barrier)
    pl.semaphore_wait(barrier, n_x + n_y - 2)

    sides = list(zip(rings, (rows_a, rows_b), (send_a, send_b), (recv_a, recv_b), (stage_a, stage_b), (sem_a, sem_b)))

    def lead(side, p):
        ring, rows, send, _, stage, sem = side
        hop = ring.far // 2 if p % 2 == 0 else -(ring.far // 2)
        part = pl.ds(p * (rows // PIECES), rows // PIECES)
        return ring.remote(send.at[ring.place(ring.far), part], stage.at[part], sem, p, hop)

    def follow(side, p):
        ring, rows, _, recv, stage, sem = side
        hop = ring.far // 2 if p % 2 == 0 else -(ring.far // 2)
        part = pl.ds(p * (rows // PIECES), rows // PIECES)
        return ring.remote(stage.at[part], recv.at[ring.place(-hop), part], sem, PIECES + p, hop)

    def straight(side, i):
        ring, rows, send, recv, _, sem = side
        d = ring.direct[i]
        return ring.remote(send.at[ring.place(d), pl.ds(0, rows)], recv.at[ring.pos, pl.ds(0, rows)], sem, 2 * PIECES + i, d)

    relayed = [(side, p) for p in range(PIECES) for side in sides if side[0].far]
    direct = [(side, i) for side in sides for i in range(len(side[0].direct))]
    for job in relayed:
        lead(*job).start()
    for job in direct:
        straight(*job).start()
    for job in relayed:
        lead(*job).wait_recv()
        follow(*job).start()
    for job in relayed:
        lead(*job).wait_send()
    for job in direct:
        straight(*job).wait()
    for job in relayed:
        follow(*job).wait()


def spread(rows_a, rows_b, cid, n_y, n_x, send_a, send_b):
    return pl.pallas_call(
        functools.partial(spread_kernel, rows_a, rows_b, n_y, n_x),
        out_shape=tuple(jax.ShapeDtypeStruct(s, BF16) for s in (send_a.shape, send_b.shape, send_a.shape[1:], send_b.shape[1:])),
        in_specs=[HBM, HBM],
        out_specs=(HBM,) * 4,
        scratch_shapes=[
            pltpu.SemaphoreType.DMA((2, 2 * PIECES + n_x)),
            pltpu.SemaphoreType.DMA((2, 2 * PIECES + n_y)),
        ],
        compiler_params=pltpu.CompilerParams(collective_id=cid, has_side_effects=True),
        name='spread_%d_%d' % (rows_a, rows_b),
    )(send_a, send_b)[:2]


def sum_kernel(n_y, n_x, kept_a, kept_b, place, tok_hbm, wgt_hbm, recv_a, recv_b, send_a, send_b, z_a, z_b, *scratch):
    n_acc = 2 * max(n_y, n_x)
    tok, wgt, rbuf = scratch[:3]
    accs = scratch[3:3 + n_acc]
    tsem, rsem, zsem = scratch[3 + n_acc:]
    core, chip = place[0], place[1]
    my_y, my_x = chip // n_x, chip % n_x
    n_chip = n_y * n_x
    sub = kept_a.shape[0] // n_chip
    n_tok = z_a.shape[1]
    words = sub * LANES
    per_dev = tok_hbm.shape[0] // (2 * n_chip)
    blk = 16
    halves = (
        (kept_a, recv_a, send_a, z_a, my_x, n_y, n_x),
        (kept_b, recv_b, send_b, z_b, my_y, n_x, n_y),
    )

    def tables(half, act):
        n_dst, n_src = halves[half][5:]
        for i in range(n_dst):
            g = (i * n_x + my_x) * 2 + core if half == 0 else (my_y * n_x + i) * 2 + core
            for q in range(n_src):
                owner = my_y * n_x + q if half == 0 else q * n_x + my_x
                src = pl.ds(pl.multiple_of(g * per_dev + owner * words, words), words)
                dst = pl.ds((half * n_chip + i * n_src + q) * words, words)
                act(pltpu.make_async_copy(tok_hbm.at[src], tok.at[dst], tsem.at[half]))
                act(pltpu.make_async_copy(wgt_hbm.at[src], wgt.at[dst], tsem.at[half]))

    def rows_of(half, i, q):
        kept, n_src = halves[half][0], halves[half][6]
        n = kept[(i * n_src + q) * sub]
        for e in range(1, sub):
            n = n + kept[(i * n_src + q) * sub + e]
        return n

    def fetch(half, q, act):
        _, recv, send, _, mine, n_dst, _ = halves[half]
        slot, n = q % 2, rows_of(half, 0, q)
        for i in range(1, n_dst):
            n = n + rows_of(half, i, q)

        @pl.when(jnp.logical_and(q == mine, n > 0))
        def _():
            act(pltpu.make_async_copy(send.at[q, pl.ds(0, n)], rbuf.at[slot, pl.ds(0, n)], rsem.at[slot]))

        @pl.when(jnp.logical_and(q != mine, n > 0))
        def _():
            act(pltpu.make_async_copy(recv.at[q, pl.ds(0, n)], rbuf.at[slot, pl.ds(0, n)], rsem.at[slot]))

    def zero(acc):
        def body(b, c):
            acc[pl.ds(b * blk, blk)] = jnp.zeros((blk, *acc.shape[1:]), F32)
            return c
        lax.fori_loop(0, n_tok // blk, body, 0)

    fetch(0, 0, lambda c: c.start())
    for half in range(2):
        tables(half, lambda c: c.start())
    puts = []
    for half in range(2):
        kept, _, _, z, _, n_dst, n_src = halves[half]
        for i in range(n_dst):
            zero(accs[2 * i + 1])
        for put in puts:
            put.wait()
        for i in range(n_dst):
            zero(accs[2 * i])
        tables(half, lambda c: c.wait())
        for q in range(n_src):
            slot = q % 2
            fetch(half, q, lambda d: d.wait())
            if q + 1 < n_src:
                fetch(half, q + 1, lambda d: d.start())
            elif half == 0 and n_src % 2 == 0:
                fetch(1, 0, lambda d: d.start())
            bases = [jnp.int32(0)]
            for i in range(n_dst - 1):
                bases.append(bases[-1] + rows_of(half, i, q))

            def one_expert(e, bases):
                counts = [kept[(i * n_src + q) * sub + e] for i in range(n_dst)]
                most = counts[0]
                for n in counts[1:]:
                    most = jnp.maximum(most, n)
                firsts = [(half * n_chip + i * n_src + q) * words + e * LANES for i in range(n_dst)]

                def pair(b, cc):
                    jobs = []
                    for i in range(n_dst):
                        for p in range(2):
                            s = b * 2 + p
                            row = rbuf[slot, bases[i] + s].astype(F32)
                            jobs.append((accs[2 * i + p], tok[firsts[i] + s], wgt[firsts[i] + s] * row))
                    for acc, t, row in jobs:
                        acc[t] = acc[t] + row
                    return cc

                lax.fori_loop(0, (most + 1) // 2, pair, 0)
                return tuple(base + n for base, n in zip(bases, counts))

            lax.fori_loop(0, sub, one_expert, tuple(bases))
        if half == 0 and n_src % 2:
            fetch(1, 0, lambda d: d.start())
        puts = []
        for i in range(n_dst):
            even, odd = accs[2 * i], accs[2 * i + 1]

            def merge(b, c):
                rows = pl.ds(b * blk, blk)
                even[rows] = even[rows] + odd[rows]
                return c

            lax.fori_loop(0, n_tok // blk, merge, 0)
            puts.append(pltpu.make_async_copy(even.at[pl.ds(0, n_tok)], z.at[i], zsem.at[i]))
            puts[-1].start()
    for put in puts:
        put.wait()


def weighted_sums(n_y, n_x, kept_a, kept_b, place, tok, wgt, recv_a, recv_b, send_a, send_b, n_tok):
    half = recv_a.shape[2]
    n_dst = max(n_y, n_x)
    slots = max(recv_a.shape[1], recv_b.shape[1])
    words = kept_a.shape[0] * LANES
    return pl.pallas_call(
        functools.partial(sum_kernel, n_y, n_x),
        out_shape=(
            jax.ShapeDtypeStruct((n_y, n_tok, half, LANES), F32),
            jax.ShapeDtypeStruct((n_x, n_tok, half, LANES), F32),
        ),
        in_specs=[SMEM] * 3 + [HBM] * 6,
        out_specs=(HBM, HBM),
        scratch_shapes=[
            pltpu.SMEM((2 * words,), I32),
            pltpu.SMEM((2 * words,), F32),
            pltpu.VMEM((2, slots + LANES, half, LANES), BF16),
            *[pltpu.VMEM((n_tok + 8, half, LANES), F32) for _ in range(2 * n_dst)],
            pltpu.SemaphoreType.DMA((2,)),
            pltpu.SemaphoreType.DMA((2,)),
            pltpu.SemaphoreType.DMA((n_dst,)),
        ],
        compiler_params=pltpu.CompilerParams(vmem_limit_bytes=VMEM_LIMIT),
        cost_estimate=pl.CostEstimate(flops=2 * 10 ** 10, bytes_accessed=6 * 10 ** 7, transcendentals=0),
        name='weighted_sums',
    )(kept_a, kept_b, place, tok, wgt, recv_a, recv_b, send_a, send_b)


SUM_CHUNKS = 4


def reduce_kernel(n_y, n_x, z_a, z_b, x_ref, y_ref, own, part, zsem, rsem):
    rings = (Ring('y', n_y, n_x), Ring('x', n_y, n_x))
    zs = (z_a, z_b)
    n_tok, d_model = x_ref.shape
    rows = n_tok // (2 * SUM_CHUNKS)
    half = d_model // 2
    blk = 16
    lanes = [(a, w) for a in range(2) for w in range(2)]
    steps = [ring.n - 1 for ring in rings]

    barrier = pltpu.get_barrier_semaphore()
    for ring in rings:
        for d in (1, -1):
            pl.semaphore_signal(barrier, inc=1, device_id=ring.device(d), device_id_type=pl.DeviceIdType.MESH)
    pl.semaphore_wait(barrier, 4)

    def sign(w):
        return 1 if w == 0 else -1

    def chunk(w, j):
        return pl.ds((w * SUM_CHUNKS + j) * rows, rows)

    def load(a, w, s, j):
        block = rings[a].place(-sign(w) * (s + 1)) if s < steps[a] else rings[a].pos
        return pltpu.make_async_copy(zs[a].at[block, chunk(w, j)], own.at[a, w, s - 1, j], zsem.at[a, w, s - 1, j])

    def hop(a, w, s, j):
        ring = rings[a]
        src = zs[a].at[ring.place(-sign(w)), chunk(w, j)] if s == 0 else part.at[a, w, s - 1, j]
        return pltpu.make_async_remote_copy(
            src_ref=src, dst_ref=part.at[a, w, s, j], send_sem=rsem.at[0, a, w, s, j], recv_sem=rsem.at[1, a, w, s, j],
            device_id=ring.device(sign(w)), device_id_type=pl.DeviceIdType.MESH)

    for j in range(SUM_CHUNKS):
        for a, w in lanes:
            hop(a, w, 0, j).start()
    for s in range(1, max(steps) + 1):
        for j in range(SUM_CHUNKS):
            for a, w in lanes:
                if s <= steps[a]:
                    load(a, w, s, j).start()

    for s in range(1, max(steps)):
        for j in range(SUM_CHUNKS):
            for a, w in lanes:
                if s >= steps[a]:
                    continue
                load(a, w, s, j).wait()
                hop(a, w, s - 1, j).wait_recv()

                def add(b, c):
                    r = pl.ds(b * blk, blk)
                    part[a, w, s - 1, j, r] = part[a, w, s - 1, j, r] + own[a, w, s - 1, j, r]
                    return c

                lax.fori_loop(0, rows // blk, add, 0)
                hop(a, w, s, j).start()

    for j in range(SUM_CHUNKS):
        for a, w in lanes:
            s = steps[a]
            load(a, w, s, j).wait()
            hop(a, w, s - 1, j).wait_recv()
            first = (w * SUM_CHUNKS + j) * rows

            def finish(b, c):
                r = pl.ds(b * blk, blk)
                out = pl.ds(pl.multiple_of(first + b * blk, blk), blk)
                cols = pl.ds(a * half, half)
                total = part[a, w, s - 1, j, r] + own[a, w, s - 1, j, r]
                y_ref[out, cols] = (x_ref[out, cols].astype(F32) + total.reshape(blk, half)).astype(BF16)
                return c

            lax.fori_loop(0, rows // blk, finish, 0)
    for s in range(max(steps)):
        for j in range(SUM_CHUNKS):
            for a, w in lanes:
                if s < steps[a]:
                    hop(a, w, s, j).wait_send()


def reduce_back(cid, n_y, n_x, z_a, z_b, x):
    n_tok, d_model = x.shape
    rows = n_tok // (2 * SUM_CHUNKS)
    steps = max(n_y, n_x) - 1
    buf = pltpu.VMEM((2, 2, steps, SUM_CHUNKS, rows, z_a.shape[2], LANES), F32)
    return pl.pallas_call(
        functools.partial(reduce_kernel, n_y, n_x),
        out_shape=jax.ShapeDtypeStruct((n_tok, d_model), BF16),
        in_specs=[HBM, HBM, VMEM],
        out_specs=VMEM,
        scratch_shapes=[
            buf, buf,
            pltpu.SemaphoreType.DMA((2, 2, steps, SUM_CHUNKS)),
            pltpu.SemaphoreType.DMA((2, 2, 2, steps, SUM_CHUNKS)),
        ],
        compiler_params=pltpu.CompilerParams(collective_id=cid, has_side_effects=True, vmem_limit_bytes=VMEM_LIMIT),
        name='reduce_back',
    )(z_a, z_b, x)


def solution(mesh):
    dev_axes = ('ep2', 'ep')
    n_y, n_ep = mesh.shape['ep2'], mesh.shape['ep']
    n_x = n_ep // 2
    group = n_y * n_ep
    n_chip = n_y * n_x

    def local_step(x_loc, ids_loc, gate_loc, w_a, w_b):
        n_tok, d_model = x_loc.shape
        n_top = ids_loc.shape[1]
        e_loc = w_a.shape[0]
        sub = 2 * e_loc
        experts = e_loc * group
        cap = capacity_of(group, n_tok, n_top, experts)
        sublanes = d_model // LANES
        slots_a, slots_b = n_y * sub * LANES, n_x * sub * LANES
        bounds = tuple(n_tok * q // CHUNK_UNITS for q in CHUNK_ENDS)
        n_chunk = len(bounds) - 1
        me = lax.axis_index(dev_axes)
        core, chip = me % 2, me // 2
        place = jnp.stack([core, chip]).astype(I32)

        x3 = x_loc.reshape(n_tok, sublanes, LANES)
        chunks = [lax.all_gather(x3[bounds[k]:bounds[k + 1]], dev_axes, tiled=True) for k in range(n_chunk)]
        swap = [(i, i ^ 1) for i in range(n_ep)]
        w_a_sib = lax.ppermute(w_a, 'ep', swap)
        w_b_sib = lax.ppermute(w_b, 'ep', swap)

        toks, wgts, cnts = route(ids_loc, gate_loc, bounds)
        for_chip = toks[:experts].reshape(n_chip, 1, sub, LANES)
        table = jnp.concatenate([
            jnp.broadcast_to(for_chip, (n_chip, 2, sub, LANES)).reshape(group, sub, LANES),
            jnp.broadcast_to(cnts[None], (group, PREFIX_ROWS, LANES))], axis=1)
        table = lax.all_to_all(table, dev_axes, 0, 0, tiled=True)
        lists = build_lists(place, table.reshape(-1), cap, slots_a, slots_b, bounds, n_y, n_x, sub)

        totals = table[:, sub + n_chunk, :experts]
        offs = jnp.cumsum(totals, axis=0) - totals
        kept = jnp.clip(cap - offs, 0, totals)
        kept_own = lax.dynamic_slice(kept, (me, 0), (1, experts)).reshape(experts, 1)
        toks = jnp.where(jnp.arange(LANES)[None, :] < kept_own, toks[:experts], n_tok)
        by_place = kept.reshape(n_y, n_x, 2, n_y, n_x, sub)
        y, x = chip // n_x, chip % n_x
        kept_a = lax.dynamic_slice(by_place, (0, x, core, y, 0, 0), (n_y, 1, 1, 1, n_x, sub)).reshape(-1)
        kept_b = lax.dynamic_slice(by_place, (y, 0, core, 0, x, 0), (1, n_x, 1, n_y, 1, sub)).reshape(-1)
        per_chip = jnp.sum(by_place, axis=5)
        need_a = jnp.max(jnp.sum(per_chip, axis=0))
        need_b = jnp.max(jnp.sum(per_chip, axis=1))

        sends = None
        for k in range(n_chunk):
            if k == n_chunk - 1:
                toks, wgts, sends = lax.optimization_barrier((toks, wgts, sends))
            sends = run_experts(k, n_chunk, lists, place, chunks[k], w_a, w_a_sib, w_b, w_b_sib, sends, n_x * slots_a, n_y * slots_b)
        tok_all = lax.all_gather(toks.reshape(-1), dev_axes, tiled=True)
        wgt_all = lax.all_gather(wgts[:experts].reshape(-1), dev_axes, tiled=True)
        send_a = sends[0].reshape(n_x, slots_a, sublanes // 2, LANES)
        send_b = sends[1].reshape(n_y, slots_b, sublanes // 2, LANES)

        tiers = [(slots_a * q // 64, slots_b * q // 64) for q in SIZES]
        index = jnp.int32(len(tiers) - 1)
        for i in range(len(tiers) - 2, -1, -1):
            fits = jnp.logical_and(need_a <= tiers[i][0], need_b <= tiers[i][1])
            index = jnp.where(fits, jnp.int32(i), index)
        recv_a, recv_b = lax.switch(index, [functools.partial(spread, a, b, i, n_y, n_x) for i, (a, b) in enumerate(tiers)], send_a, send_b)
        recv_a, tok_all, wgt_all = lax.optimization_barrier((recv_a, tok_all, wgt_all))
        z_a, z_b = weighted_sums(n_y, n_x, kept_a, kept_b, place, tok_all, wgt_all, recv_a, recv_b, send_a, send_b, n_tok)
        return reduce_back(len(tiers), n_y, n_x, z_a, z_b, x_loc)

    tok_spec = P(('dp', 'ep2', 'ep'), None)
    w_spec = P(dev_axes, None, None)
    return jax.shard_map(local_step, mesh=mesh, in_specs=(tok_spec, tok_spec, tok_spec, w_spec, w_spec), out_specs=tok_spec, check_vma=False)
```

```python
import functools
import math

import jax
import jax.numpy as jnp
from jax import lax
from jax.experimental import pallas as pl
from jax.experimental.pallas import tpu as pltpu
from jax.sharding import PartitionSpec as P

LANES = 128
CHUNK_UNITS = 32
CHUNK_ENDS = (0, 25, 32)
SIZES = (38, 40, 41, 42, 43, 44, 45, 46, 48, 50, 52, 56)
TILE = 256
PREFIX_ROWS = 8
BF16 = jnp.bfloat16
F32 = jnp.float32
I32 = jnp.int32
HBM = pl.BlockSpec(memory_space=pl.ANY)
SMEM = pl.BlockSpec(memory_space=pltpu.SMEM)
VMEM = pl.BlockSpec(memory_space=pltpu.VMEM)
VMEM_LIMIT = 64_000_000


def capacity_of(group_size, n_tok, n_top, experts):
    return 8 * ((5 * group_size * n_tok * n_top) // (32 * experts))


def far_of(n):
    return n // 2 if n % 2 == 0 and n >= 4 else 0


def direct_of(n):
    return [d for d in range(1, n) if d != far_of(n)]


def first_of(n):
    return sorted({1 % n, (n - 1) % n} - {0})


def rest_of(n):
    return [r for r in range(n) if r not in first_of(n)]


def route_kernel(bounds, ids_ref, gate_ref, tok_ref, wgt_ref, cnt_ref, code_t, gate_t, tok_acc, wgt_acc):
    n_tok, n_top = ids_ref.shape
    lane = lax.broadcasted_iota(I32, (n_tok, LANES), 1)
    member = jnp.zeros((n_tok, LANES), F32)
    gates = jnp.zeros((n_tok, LANES), F32)
    for j in range(n_top):
        hit = ids_ref[:, j:j + 1] == lane
        member = member + jnp.where(hit, 1.0, 0.0)
        gates = gates + jnp.where(hit, gate_ref[:, j:j + 1], 0.0)
    member_b = member.astype(BF16)
    row_block = min(n_tok, 128)
    for i in range(n_tok // row_block):
        rows = pl.ds(i * row_block, row_block)
        later = lax.broadcasted_iota(I32, (row_block, n_tok), 0) + i * row_block
        earlier = lax.broadcasted_iota(I32, (row_block, n_tok), 1)
        tri = jnp.where(earlier < later, 1.0, 0.0).astype(BF16)
        rank = jnp.dot(tri, member_b, preferred_element_type=F32)
        mem = member[i * row_block:(i + 1) * row_block]
        code_t[:, rows] = jnp.where(mem > 0.5, rank, -1.0).T
        gate_t[:, rows] = gates[i * row_block:(i + 1) * row_block].T
    total = jnp.zeros((1, LANES), F32)
    rows_out = [total]
    for lo, hi in zip(bounds[:-1], bounds[1:]):
        total = total + jnp.sum(member[lo:hi], axis=0, keepdims=True)
        rows_out.append(total)
    while len(rows_out) < PREFIX_ROWS:
        rows_out.append(total)
    cnt_ref[...] = jnp.concatenate(rows_out, axis=0).astype(I32)
    tok_acc[...] = jnp.zeros_like(tok_acc)
    wgt_acc[...] = jnp.zeros_like(wgt_acc)
    slot = lax.broadcasted_iota(I32, (LANES, n_tok), 0).astype(F32)
    token = lax.broadcasted_iota(I32, (1, n_tok), 1).astype(F32)
    out_lane = lax.broadcasted_iota(I32, (LANES, LANES), 1)

    def one_expert(e, carry):
        hit = slot == code_t[pl.ds(e, 1), :]
        tok = jnp.sum(jnp.where(hit, token, 0.0), axis=1, keepdims=True)
        wgt = jnp.sum(jnp.where(hit, gate_t[pl.ds(e, 1), :], 0.0), axis=1, keepdims=True)
        tok_acc[...] = jnp.where(out_lane == e, tok, tok_acc[...])
        wgt_acc[...] = jnp.where(out_lane == e, wgt, wgt_acc[...])
        return carry

    lax.fori_loop(0, LANES, one_expert, 0)
    tok_ref[...] = tok_acc[...].T.astype(I32)
    wgt_ref[...] = wgt_acc[...].T


def route(ids, gate, bounds):
    n_tok = ids.shape[0]
    return pl.pallas_call(
        functools.partial(route_kernel, bounds),
        out_shape=(
            jax.ShapeDtypeStruct((LANES, LANES), I32),
            jax.ShapeDtypeStruct((LANES, LANES), F32),
            jax.ShapeDtypeStruct((PREFIX_ROWS, LANES), I32),
        ),
        in_specs=[VMEM, VMEM],
        out_specs=(VMEM, VMEM, VMEM),
        scratch_shapes=[
            pltpu.VMEM((LANES, n_tok), F32),
            pltpu.VMEM((LANES, n_tok), F32),
            pltpu.VMEM((LANES, LANES), F32),
            pltpu.VMEM((LANES, LANES), F32),
        ],
        cost_estimate=pl.CostEstimate(flops=2 * 10 ** 10, bytes_accessed=10 ** 6, transcendentals=0),
        name='route',
    )(ids, gate)


def list_kernel(cap, slots_a, slots_b, early, bounds, n_y, n_x, sub, place_ref, info_ref, src_ref, start_ref, len_ref, dst_a_ref, dst_b_ref, cs_ref,
                kept_ref, base_a_ref, base_b_ref):
    core, chip = place_ref[0], place_ref[1]
    n_dst = n_y * n_x
    n_chunk = len(bounds) - 1
    dev_words = (sub + PREFIX_ROWS) * LANES
    width = src_ref.shape[0] // sub

    def count(g, k, e):
        return info_ref[g * dev_words + (sub + k) * LANES + chip * sub + e]

    def per_expert(e, carry):
        def per_dev(i, off):
            for c in range(2):
                n = count(2 * i + c, n_chunk, e)
                kept = jnp.clip(cap - off, 0, n)
                off = off + n

                @pl.when(core == c)
                def _():
                    kept_ref[i * sub + e] = kept
            return off
        lax.fori_loop(0, n_dst, per_dev, 0)
        return carry

    lax.fori_loop(0, sub, per_expert, 0)

    my_y, my_x = chip // n_x, chip % n_x

    def rows_in(k, i, e):
        g, kept = 2 * i + core, kept_ref[i * sub + e]
        return jnp.minimum(count(g, k + 1, e), kept) - jnp.minimum(count(g, k, e), kept)

    def block_bases(base_ref, n_blocks, n_inner, slots, index):
        for d in range(n_blocks):
            acc = jnp.int32(d * slots)
            for k in range(n_chunk):
                for r in first_of(n_inner) + rest_of(n_inner):
                    i = index(d, r)

                    def add(e, acc):
                        base_ref[(k * n_dst + i) * sub + e] = acc
                        return acc + rows_in(k, i, e)

                    acc = lax.fori_loop(0, sub, add, acc)
                if k == 0:
                    acc = jnp.maximum(acc, d * slots + early)

    block_bases(base_a_ref, n_x, n_y, slots_a, lambda d, r: lax.rem(my_y + r, n_y) * n_x + lax.rem(my_x + d, n_x))
    block_bases(base_b_ref, n_y, n_x, slots_b, lambda d, r: lax.rem(my_y + d, n_y) * n_x + lax.rem(my_x + r, n_x))

    def expert_lists(e, carry):
        pos = e * width
        for k in range(n_chunk):
            cs_ref[e * (n_chunk + 1) + k] = pos
            size = bounds[k + 1] - bounds[k]

            def segment(i, o):
                g = 2 * i + core
                kept = kept_ref[i * sub + e]
                s0 = jnp.minimum(count(g, k, e), kept)
                n = jnp.minimum(count(g, k + 1, e), kept) - s0
                j = (e * n_chunk + k) * n_dst + i
                start_ref[j] = o
                len_ref[j] = n
                dst_a_ref[j] = base_a_ref[(k * n_dst + i) * sub + e]
                dst_b_ref[j] = base_b_ref[(k * n_dst + i) * sub + e]
                src0 = g * size - bounds[k]
                tok0 = g * dev_words + e * LANES + s0

                def block(b, c):
                    vals = [info_ref[tok0 + b * 8 + q] for q in range(8)]
                    for q in range(8):
                        src_ref[o + b * 8 + q] = src0 + vals[q]
                    return c

                lax.fori_loop(0, (n + 7) // 8, block, 0)
                return o + n

            pos = lax.fori_loop(0, n_dst, segment, pos)
        cs_ref[e * (n_chunk + 1) + n_chunk] = pos
        return carry

    lax.fori_loop(0, sub, expert_lists, 0)


def build_lists(place, info, cap, slots_a, slots_b, early, bounds, n_y, n_x, sub):
    n_dst, n_chunk = n_y * n_x, len(bounds) - 1
    width = LANES * n_dst + 8
    segs = sub * n_chunk * n_dst
    return pl.pallas_call(
        functools.partial(list_kernel, cap, slots_a, slots_b, early, bounds, n_y, n_x, sub),
        out_shape=(
            jax.ShapeDtypeStruct((sub * width,), I32),
            jax.ShapeDtypeStruct((segs,), I32),
            jax.ShapeDtypeStruct((segs,), I32),
            jax.ShapeDtypeStruct((segs,), I32),
            jax.ShapeDtypeStruct((segs,), I32),
            jax.ShapeDtypeStruct((sub * (n_chunk + 1),), I32),
        ),
        in_specs=[SMEM, SMEM],
        out_specs=(SMEM,) * 6,
        scratch_shapes=[
            pltpu.SMEM((n_dst * sub,), I32),
            pltpu.SMEM((n_chunk * n_dst * sub,), I32),
            pltpu.SMEM((n_chunk * n_dst * sub,), I32),
        ],
        cost_estimate=pl.CostEstimate(flops=2 * 10 ** 10, bytes_accessed=10 ** 6, transcendentals=0),
        name='row_lists',
    )(place, info)


def rows_loop(n, fn):
    def block(b, c):
        for q in range(8):
            fn(b * 8 + q)
        return c

    def single(r, c):
        fn(r)
        return c

    full = n // 8
    lax.fori_loop(0, full, block, 0)
    lax.fori_loop(full * 8, n, single, 0)


def gelu(v):
    return 0.5 * v * (1.0 + jnp.tanh(math.sqrt(2.0 / math.pi) * (v + 0.044715 * v * v * v)))


def expert_kernel(k, n_chunk, first, *refs):
    (src, seg_start, seg_len, seg_dst_a, seg_dst_b, cs, place, x_hbm, wa_own, wa_sib, wb_own, wb_sib) = refs[:12]
    (send_a, send_b, xbuf, obuf_a, obuf_b, wa, wb, t_e, t_base, t_cnt, gsem, ssem, wsem) = refs[12 if first else 14:]
    e_loc, d_model, _ = wa_own.shape
    sub = 2 * e_loc
    core = place[0]
    sublanes = d_model // LANES
    n_dst = seg_start.shape[0] // (sub * n_chunk)

    def weight_copies(e, act):
        slot = e % 2
        q = e % e_loc

        @pl.when(e // e_loc == core)
        def _():
            act(pltpu.make_async_copy(wa_own.at[q], wa.at[slot], wsem.at[slot, 0]))
            act(pltpu.make_async_copy(wb_own.at[q], wb.at[slot], wsem.at[slot, 1]))

        @pl.when(e // e_loc != core)
        def _():
            act(pltpu.make_async_copy(wa_sib.at[q], wa.at[slot], wsem.at[slot, 0]))
            act(pltpu.make_async_copy(wb_sib.at[q], wb.at[slot], wsem.at[slot, 1]))

    sides = ((obuf_a, send_a, seg_dst_a), (obuf_b, send_b, seg_dst_b))
    weight_copies(0, lambda c: c.start())

    def plan(e, t):
        lo = cs[e * (n_chunk + 1) + k]
        n = cs[e * (n_chunk + 1) + k + 1] - lo

        def put(i, c):
            t_e[t + i] = e
            t_base[t + i] = lo + i * TILE
            t_cnt[t + i] = jnp.minimum(n - i * TILE, TILE)
            return c

        n_tiles = (n + TILE - 1) // TILE
        lax.fori_loop(0, n_tiles, put, 0)
        return t + n_tiles

    n_all = lax.fori_loop(0, sub, plan, 0)

    def gather_start(t):
        base, slot = t_base[t], t % 2
        rows_loop(t_cnt[t], lambda r: pltpu.make_async_copy(
            x_hbm.at[src[base + r]], xbuf.at[slot, r], gsem.at[slot]).start())

    def gather_wait(t):
        n, slot = t_cnt[t], t % 2
        pltpu.make_async_copy(x_hbm.at[pl.ds(0, n)], xbuf.at[slot, pl.ds(0, n)], gsem.at[slot]).wait()

    def scatter_start(t):
        base, slot = t_base[t], t % 2
        end = base + t_cnt[t]

        def segment(i, c):
            j = (t_e[t] * n_chunk + k) * n_dst + i
            first_row = seg_start[j]
            lo = jnp.maximum(first_row, base)
            n = jnp.minimum(first_row + seg_len[j], end) - lo

            @pl.when(n > 0)
            def _():
                for half, (obuf, send, seg_dst) in enumerate(sides):
                    pltpu.make_async_copy(
                        obuf.at[slot, pl.ds(lo - base, n)],
                        send.at[pl.ds(seg_dst[j] + lo - first_row, n)],
                        ssem.at[half, slot],
                    ).start()
            return c

        lax.fori_loop(0, n_dst, segment, 0)

    def scatter_wait(t):
        n, slot = t_cnt[t], t % 2
        for half, (obuf, send, _) in enumerate(sides):
            pltpu.make_async_copy(obuf.at[slot, pl.ds(0, n)], send.at[pl.ds(0, n)], ssem.at[half, slot]).wait()

    for t in range(2):
        @pl.when(t < n_all)
        def _():
            gather_start(t)

    def one_expert(e, t_first):
        weight_copies(e, lambda c: c.wait())

        @pl.when(e + 1 < sub)
        def _():
            weight_copies(e + 1, lambda c: c.start())

        ws = e % 2
        n = cs[e * (n_chunk + 1) + k + 1] - cs[e * (n_chunk + 1) + k]

        def one_tile(i, t):
            slot = t % 2
            gather_wait(t)

            @pl.when(t >= 2)
            def _():
                scatter_wait(t - 2)

            rows = xbuf[slot].reshape(TILE, d_model)
            hidden = gelu(jnp.dot(rows, wa[ws], preferred_element_type=F32)).astype(BF16)
            out = jnp.dot(hidden, wb[ws], preferred_element_type=F32).astype(BF16)
            obuf_a[slot] = out[:, :d_model // 2].reshape(TILE, sublanes // 2, LANES)
            obuf_b[slot] = out[:, d_model // 2:].reshape(TILE, sublanes // 2, LANES)

            @pl.when(t + 2 < n_all)
            def _():
                gather_start(t + 2)

            scatter_start(t)
            return t + 1

        return lax.fori_loop(0, (n + TILE - 1) // TILE, one_tile, t_first)

    lax.fori_loop(0, sub, one_expert, 0)
    for back in (2, 1):
        @pl.when(n_all >= back)
        def _():
            scatter_wait(n_all - back)


def run_experts(k, n_chunk, lists, place, x_rows, wa, wa_sib, wb, wb_sib, sends, rows_a, rows_b):
    e_loc, d_model, ff = wa.shape
    sub = 2 * e_loc
    sublanes = d_model // LANES
    half = sublanes // 2
    first = sends is None
    ops = (*lists, place, x_rows, wa, wa_sib, wb, wb_sib) + (() if first else tuple(sends))
    n_smem = len(lists) + 1
    max_tiles = sub * (pl.cdiv(lists[0].shape[0] // sub, TILE) + 1)
    flops = 4 * d_model * ff * x_rows.shape[0]
    return pl.pallas_call(
        functools.partial(expert_kernel, k, n_chunk, first),
        out_shape=(
            jax.ShapeDtypeStruct((rows_a, half, LANES), BF16),
            jax.ShapeDtypeStruct((rows_b, half, LANES), BF16),
        ),
        in_specs=[SMEM] * n_smem + [HBM] * (len(ops) - n_smem),
        out_specs=(HBM, HBM),
        scratch_shapes=[
            pltpu.VMEM((2, TILE, sublanes, LANES), BF16),
            pltpu.VMEM((2, TILE, half, LANES), BF16),
            pltpu.VMEM((2, TILE, half, LANES), BF16),
            pltpu.VMEM((2, d_model, ff), BF16),
            pltpu.VMEM((2, ff, d_model), BF16),
            pltpu.SMEM((max_tiles,), I32),
            pltpu.SMEM((max_tiles,), I32),
            pltpu.SMEM((max_tiles,), I32),
            pltpu.SemaphoreType.DMA((2,)),
            pltpu.SemaphoreType.DMA((2, 2)),
            pltpu.SemaphoreType.DMA((2, 2)),
        ],
        input_output_aliases={} if first else {len(ops) - 2: 0, len(ops) - 1: 1},
        compiler_params=pltpu.CompilerParams(vmem_limit_bytes=VMEM_LIMIT),
        cost_estimate=pl.CostEstimate(flops=flops, bytes_accessed=6 * 10 ** 7, transcendentals=0),
        name='experts',
    )(*ops)


PIECES = 4


class Ring:
    def __init__(self, axis, n_y, n_x):
        y, ec = lax.axis_index('ep2'), lax.axis_index('ep')
        self.axis, self.core = axis, ec % 2
        self.n = n_x if axis == 'x' else n_y
        self.pos = ec // 2 if axis == 'x' else y
        self.direct, self.far = direct_of(self.n), far_of(self.n)

    def place(self, d):
        return lax.rem(self.pos + d + self.n, self.n)

    def device(self, d):
        if self.axis == 'x':
            return {'ep': self.place(d) * 2 + self.core}
        return {'ep2': self.place(d)}

    def remote(self, src, dst, sems, i, d):
        return pltpu.make_async_remote_copy(
            src_ref=src, dst_ref=dst, send_sem=sems.at[0, i], recv_sem=sems.at[1, i],
            device_id=self.device(d), device_id_type=pl.DeviceIdType.MESH)

    def signal(self, barrier):
        for d in range(1, self.n):
            pl.semaphore_signal(barrier, inc=1, device_id=self.device(d), device_id_type=pl.DeviceIdType.MESH)


def spread_kernel(rows_a, rows_b, early, n_y, n_x, send_a, send_b, recv_a, recv_b, stage_a, stage_b, sem_a, sem_b):
    rings = (Ring('x', n_y, n_x), Ring('y', n_y, n_x))
    barrier = pltpu.get_barrier_semaphore()
    for ring in rings:
        ring.signal(barrier)
    pl.semaphore_wait(barrier, n_x + n_y - 2)

    sides = list(zip(rings, (rows_a, rows_b), (send_a, send_b), (recv_a, recv_b), (stage_a, stage_b), (sem_a, sem_b)))

    def lead(side, p):
        ring, rows, send, _, stage, sem = side
        hop = ring.far // 2 if p % 2 == 0 else -(ring.far // 2)
        part = pl.ds(p * (rows // PIECES), rows // PIECES)
        return ring.remote(send.at[ring.far, part], stage.at[part], sem, p, hop)

    def follow(side, p):
        ring, rows, _, recv, stage, sem = side
        hop = ring.far // 2 if p % 2 == 0 else -(ring.far // 2)
        part = pl.ds(p * (rows // PIECES), rows // PIECES)
        return ring.remote(stage.at[part], recv.at[ring.far, part], sem, PIECES + p, hop)

    def straight(side, i):
        ring, rows, send, recv, _, sem = side
        d = ring.direct[i]
        part = pl.ds(early, rows - early)
        return ring.remote(send.at[d, part], recv.at[d, part], sem, 2 * PIECES + i, d)

    relayed = [(side, p) for p in range(PIECES) for side in sides if side[0].far]
    direct = [(side, i) for side in sides for i in range(len(side[0].direct))]
    for job in relayed:
        lead(*job).start()
    for job in direct:
        straight(*job).start()
    for job in relayed:
        lead(*job).wait_recv()
        follow(*job).start()
    for job in relayed:
        lead(*job).wait_send()
    for job in direct:
        straight(*job).wait()
    for job in relayed:
        follow(*job).wait()


def spread(rows_a, rows_b, early, cid, n_y, n_x, send_a, send_b):
    return pl.pallas_call(
        functools.partial(spread_kernel, rows_a, rows_b, early, n_y, n_x),
        out_shape=tuple(jax.ShapeDtypeStruct(s, BF16) for s in (send_a.shape, send_b.shape, send_a.shape[1:], send_b.shape[1:])),
        in_specs=[HBM, HBM],
        out_specs=(HBM,) * 4,
        scratch_shapes=[
            pltpu.SemaphoreType.DMA((2, 2 * PIECES + n_x)),
            pltpu.SemaphoreType.DMA((2, 2 * PIECES + n_y)),
        ],
        compiler_params=pltpu.CompilerParams(collective_id=cid, has_side_effects=True),
        name='spread_%d_%d' % (rows_a, rows_b),
    )(send_a, send_b)[:2]


WAYS = 4


def sum_kernel(n_y, n_x, which, early, *refs):
    (kept_a, kept_b, kept0_a, kept0_b, place, tok_hbm, wgt_hbm, recv_a, recv_b, send_a, send_b), refs = refs[:11], refs[11:]
    early_a, refs = refs[:len(direct_of(n_x))], refs[len(direct_of(n_x)):]
    early_b, refs = refs[:len(direct_of(n_y))], refs[len(direct_of(n_y)):]
    pick = first_of if which == 0 else rest_of
    n_out = (2 if which == 0 else 1) * (len(pick(n_y)) + len(pick(n_x)))
    outs, refs = refs[:n_out], refs[n_out:]
    n_acc = WAYS * max(len(pick(n_y)), len(pick(n_x)))
    tok, wgt, rbuf = refs[:3]
    accs = refs[3:3 + n_acc]
    tsem, rsem, zsem = refs[3 + n_acc:]
    core, chip = place[0], place[1]
    my_y, my_x = chip // n_x, chip % n_x
    n_chip = n_y * n_x
    sub = kept_a.shape[0] // n_chip
    n_tok = accs[0].shape[0] - 8
    words = sub * LANES
    per_dev = tok_hbm.shape[0] // (2 * n_chip)
    blk = 16
    halves = (
        (kept_a, kept0_a, recv_a, send_a, early_a, my_x, n_x, my_y, n_y),
        (kept_b, kept0_b, recv_b, send_b, early_b, my_y, n_y, my_x, n_x),
    )
    table_base = (0, len(pick(n_y)) * n_x * words)

    def dest(half, r):
        return lax.rem(halves[half][7] + r, halves[half][8])

    def source(half, d):
        n = halves[half][6]
        return lax.rem(halves[half][5] + n - d, n)

    def table_at(half, j, d):
        return table_base[half] + (j * halves[half][6] + d) * words

    def tables(half, act):
        for j, r in enumerate(pick(halves[half][8])):
            i = dest(half, r)
            g = (i * n_x + my_x) * 2 + core if half == 0 else (my_y * n_x + i) * 2 + core
            for d in range(halves[half][6]):
                q = source(half, d)
                owner = my_y * n_x + q if half == 0 else q * n_x + my_x
                src = pl.ds(pl.multiple_of(g * per_dev + owner * words, words), words)
                dst = pl.ds(table_at(half, j, d), words)
                act(pltpu.make_async_copy(tok_hbm.at[src], tok.at[dst], tsem.at[half]))
                act(pltpu.make_async_copy(wgt_hbm.at[src], wgt.at[dst], tsem.at[half]))

    def group_rows(half, d):
        kept, kept0, n_src, n_dst = halves[half][0], halves[half][1], halves[half][6], halves[half][8]
        q = source(half, d)
        head, tail = {}, {}
        for r in first_of(n_dst) + rest_of(n_dst):
            at = (dest(half, r) * n_src + q) * sub
            n0 = n = jnp.int32(0)
            for e in range(sub):
                n0 = n0 + kept0[at + e]
                n = n + kept[at + e]
            head[r], tail[r] = n0, n - n0
        all_head = sum(head.values(), jnp.int32(0))
        return head, tail, jnp.maximum(all_head, early)

    def fetch(half, d, act):
        _, _, recv, send, early_rows, _, n_src, _, _ = halves[half]
        slot = d % 2
        _, tail, second = group_rows(half, d)
        n = second + sum(tail.values(), jnp.int32(0))
        to = rbuf.at[slot]
        if d == 0:
            act(pltpu.make_async_copy(send.at[0, pl.ds(0, n)], to.at[pl.ds(0, n)], rsem.at[slot]))
        elif d == far_of(n_src):
            act(pltpu.make_async_copy(recv.at[d, pl.ds(0, n)], to.at[pl.ds(0, n)], rsem.at[slot]))
        else:
            rows = early_rows[direct_of(n_src).index(d)]
            act(pltpu.make_async_copy(rows, to.at[pl.ds(0, early)], rsem.at[slot]))

            @pl.when(n > early)
            def _():
                late = pl.ds(early, n - early)
                act(pltpu.make_async_copy(recv.at[d, late], to.at[late], rsem.at[slot]))

    def zero(acc):
        def body(b, c):
            acc[pl.ds(b * blk, blk)] = jnp.zeros((blk, *acc.shape[1:]), F32)
            return c
        lax.fori_loop(0, n_tok // blk, body, 0)

    fetch(0, 0, lambda c: c.start())
    for half in range(2):
        tables(half, lambda c: c.start())
    puts, out_at = [], 0
    for half in range(2):
        kept, kept0, _, _, _, _, n_src, _, n_dst = halves[half]
        picked = pick(n_dst)
        for acc in accs[:WAYS * len(picked)]:
            if not any(acc is accs[j * WAYS] for j in range(n_acc // WAYS)):
                zero(acc)
        for put in puts:
            put.wait()
        for j in range(len(picked)):
            zero(accs[j * WAYS])
        tables(half, lambda c: c.wait())
        for d in range(n_src):
            slot = d % 2
            fetch(half, d, lambda c: c.wait())
            if d + 1 < n_src:
                fetch(half, d + 1, lambda c: c.start())
            elif half == 0 and n_src % 2 == 0:
                fetch(1, 0, lambda c: c.start())
            q = source(half, d)
            head, tail, second = group_rows(half, d)
            for part, counts_of, start in ((0, head, jnp.int32(0)), (1, tail, second)):
                bases = {}
                for r in first_of(n_dst) + rest_of(n_dst):
                    bases[r], start = start, start + counts_of[r]

                def one_expert(e, bases):
                    counts, firsts = [], []
                    for j, r in enumerate(picked):
                        at = (dest(half, r) * n_src + q) * sub + e
                        counts.append(kept0[at] if part == 0 else kept[at] - kept0[at])
                        firsts.append(table_at(half, j, d) + e * LANES + (0 if part == 0 else kept0[at]))
                    most = counts[0]
                    for n in counts[1:]:
                        most = jnp.maximum(most, n)

                    def group(b, cc):
                        jobs = []
                        for j in range(len(picked)):
                            for p in range(WAYS):
                                s = b * WAYS + p
                                row = rbuf[slot, bases[j] + s].astype(F32)
                                t = jnp.where(s < counts[j], tok[firsts[j] + s], n_tok)
                                jobs.append((accs[j * WAYS + p], t, wgt[firsts[j] + s] * row))
                        for acc, t, row in jobs:
                            acc[t] = acc[t] + row
                        return cc

                    lax.fori_loop(0, (most + WAYS - 1) // WAYS, group, 0)
                    return tuple(base + n for base, n in zip(bases, counts))

                lax.fori_loop(0, sub, one_expert, tuple(bases[r] for r in picked))
        if half == 0 and n_src % 2:
            fetch(1, 0, lambda c: c.start())
        puts = []
        for j in range(len(picked)):
            group_accs = accs[j * WAYS:(j + 1) * WAYS]

            def merge(b, c):
                rows = pl.ds(b * blk, blk)
                total = group_accs[0][rows] + group_accs[1][rows]
                for acc in group_accs[2:]:
                    total = total + acc[rows]
                group_accs[0][rows] = total
                return c

            lax.fori_loop(0, n_tok // blk, merge, 0)
            pieces = 2 if which == 0 else 1
            size = n_tok // pieces
            for p in range(pieces):
                puts.append(pltpu.make_async_copy(group_accs[0].at[pl.ds(p * size, size)], outs[out_at], zsem.at[j, p]))
                puts[-1].start()
                out_at += 1
    for put in puts:
        put.wait()


def weighted_sums(n_y, n_x, which, early, counts, place, tok, wgt, recvs, sends, earlies, n_tok):
    half = recvs[0].shape[2]
    pick = first_of if which == 0 else rest_of
    sub = counts[0].shape[0] // (n_y * n_x)
    slots = max(recvs[0].shape[1], recvs[1].shape[1])
    table = (len(pick(n_y)) * n_x + len(pick(n_x)) * n_y) * sub * LANES + 2 * LANES
    most = max(len(pick(n_y)), len(pick(n_x)))
    pieces = 2 if which == 0 else 1
    n_out = pieces * (len(pick(n_y)) + len(pick(n_x)))
    ops = (*counts, place, tok, wgt, *recvs, *sends, *earlies)
    return pl.pallas_call(
        functools.partial(sum_kernel, n_y, n_x, which, early),
        out_shape=tuple(jax.ShapeDtypeStruct((n_tok // pieces, half, LANES), F32) for _ in range(n_out)),
        in_specs=[SMEM] * 5 + [HBM] * (len(ops) - 5),
        out_specs=(HBM,) * n_out,
        scratch_shapes=[
            pltpu.SMEM((table,), I32),
            pltpu.SMEM((table,), F32),
            pltpu.VMEM((2, slots + LANES + 8, half, LANES), BF16),
            *[pltpu.VMEM((n_tok + 8, half, LANES), F32) for _ in range(WAYS * most)],
            pltpu.SemaphoreType.DMA((2,)),
            pltpu.SemaphoreType.DMA((2,)),
            pltpu.SemaphoreType.DMA((most, 2)),
        ],
        compiler_params=pltpu.CompilerParams(vmem_limit_bytes=VMEM_LIMIT),
        cost_estimate=pl.CostEstimate(flops=5 * 10 ** 10, bytes_accessed=6 * 10 ** 7, transcendentals=0),
        name='weighted_sums',
    )(*ops)


SUM_CHUNKS = 4


def reduce_kernel(n_y, n_x, *refs):
    sizes = (n_y, n_x)
    got, refs = refs[:4], refs[4:]
    sums = []
    for n in sizes:
        split, refs = refs[:2 * len(first_of(n))], refs[2 * len(first_of(n)):]
        sums.append({(r, w): split[2 * j + w] for j, r in enumerate(first_of(n)) for w in range(2)})
    for a, n in enumerate(sizes):
        whole, refs = refs[:len(rest_of(n))], refs[len(rest_of(n)):]
        sums[a].update({(r, None): ref for r, ref in zip(rest_of(n), whole)})
    x_ref, y_ref, own, part, zsem, gsem, rsem = refs
    rings = (Ring('y', n_y, n_x), Ring('x', n_y, n_x))
    n_tok, d_model = x_ref.shape
    half_tok = n_tok // 2
    rows = half_tok // SUM_CHUNKS
    half = d_model // 2
    blk = min(16, rows)
    lanes = [(a, w) for a in range(2) for w in range(2)]
    steps = [n - 1 for n in sizes]

    barrier = pltpu.get_barrier_semaphore()
    for ring in rings:
        for d in (1, -1):
            pl.semaphore_signal(barrier, inc=1, device_id=ring.device(d), device_id_type=pl.DeviceIdType.MESH)
    pl.semaphore_wait(barrier, 4)

    def sign(w):
        return 1 if w == 0 else -1

    def load(a, w, s, j):
        n = sizes[a]
        r = 0 if s == steps[a] else (n - 1 - s if w == 0 else 1 + s)
        if (r, w) in sums[a]:
            src = sums[a][r, w].at[pl.ds(j * rows, rows)]
        else:
            src = sums[a][r, None].at[pl.ds(w * half_tok + j * rows, rows)]
        return pltpu.make_async_copy(src, own.at[a, w, s - 1, j], zsem.at[a, w, s - 1, j])

    def start(a, w, j):
        return pltpu.make_async_copy(got[2 * a + w].at[pl.ds(j * rows, rows)], part.at[a, w, 0, j], gsem.at[a, w, j])

    def hop(a, w, s, j):
        return pltpu.make_async_remote_copy(
            src_ref=part.at[a, w, s - 1, j], dst_ref=part.at[a, w, s, j], send_sem=rsem.at[0, a, w, s, j], recv_sem=rsem.at[1, a, w, s, j],
            device_id=rings[a].device(sign(w)), device_id_type=pl.DeviceIdType.MESH)

    def arrive(a, w, s, j):
        if s == 0:
            start(a, w, j).wait()
        else:
            hop(a, w, s, j).wait_recv()

    for s in range(1, max(steps) + 1):
        for j in range(SUM_CHUNKS):
            for a, w in lanes:
                if s == 1:
                    start(a, w, j).start()
                if s <= steps[a]:
                    load(a, w, s, j).start()

    for s in range(1, max(steps)):
        for j in range(SUM_CHUNKS):
            for a, w in lanes:
                if s >= steps[a]:
                    continue
                load(a, w, s, j).wait()
                arrive(a, w, s - 1, j)

                def add(b, c):
                    r = pl.ds(b * blk, blk)
                    part[a, w, s - 1, j, r] = part[a, w, s - 1, j, r] + own[a, w, s - 1, j, r]
                    return c

                lax.fori_loop(0, rows // blk, add, 0)
                hop(a, w, s, j).start()

    for j in range(SUM_CHUNKS):
        for a, w in lanes:
            s = steps[a]
            load(a, w, s, j).wait()
            arrive(a, w, s - 1, j)
            first = w * half_tok + j * rows

            def finish(b, c):
                r = pl.ds(b * blk, blk)
                out = pl.ds(pl.multiple_of(first + b * blk, blk), blk)
                cols = pl.ds(a * half, half)
                total = part[a, w, s - 1, j, r] + own[a, w, s - 1, j, r]
                y_ref[out, cols] = (x_ref[out, cols].astype(F32) + total.reshape(blk, half)).astype(BF16)
                return c

            lax.fori_loop(0, rows // blk, finish, 0)
    for s in range(1, max(steps)):
        for j in range(SUM_CHUNKS):
            for a, w in lanes:
                if s < steps[a]:
                    hop(a, w, s, j).wait_send()


def reduce_back(cid, n_y, n_x, got, split, whole, x):
    n_tok, d_model = x.shape
    rows = n_tok // (2 * SUM_CHUNKS)
    steps = max(n_y, n_x) - 1
    buf = pltpu.VMEM((2, 2, steps, SUM_CHUNKS, rows, d_model // 2 // LANES, LANES), F32)
    ops = (*got, *split, *whole, x)
    return pl.pallas_call(
        functools.partial(reduce_kernel, n_y, n_x),
        out_shape=jax.ShapeDtypeStruct((n_tok, d_model), BF16),
        in_specs=[HBM] * (len(ops) - 1) + [VMEM],
        out_specs=VMEM,
        scratch_shapes=[
            buf, buf,
            pltpu.SemaphoreType.DMA((2, 2, steps, SUM_CHUNKS)),
            pltpu.SemaphoreType.DMA((2, 2, SUM_CHUNKS)),
            pltpu.SemaphoreType.DMA((2, 2, 2, steps, SUM_CHUNKS)),
        ],
        compiler_params=pltpu.CompilerParams(collective_id=cid, has_side_effects=True, vmem_limit_bytes=VMEM_LIMIT),
        name='reduce_back',
    )(*ops)


def solution(mesh):
    dev_axes = ('ep2', 'ep')
    n_y, n_ep = mesh.shape['ep2'], mesh.shape['ep']
    n_x = n_ep // 2
    group = n_y * n_ep
    n_chip = n_y * n_x

    def local_step(x_loc, ids_loc, gate_loc, w_a, w_b):
        n_tok, d_model = x_loc.shape
        n_top = ids_loc.shape[1]
        e_loc = w_a.shape[0]
        sub = 2 * e_loc
        experts = e_loc * group
        cap = capacity_of(group, n_tok, n_top, experts)
        sublanes = d_model // LANES
        base_a, base_b = n_y * sub * LANES, n_x * sub * LANES
        early = min(base_a, base_b) // 4
        slots_a, slots_b = base_a + early, base_b + early
        bounds = tuple(n_tok * q // CHUNK_UNITS for q in CHUNK_ENDS)
        n_chunk = len(bounds) - 1
        me = lax.axis_index(dev_axes)
        core, chip = me % 2, me // 2
        place = jnp.stack([core, chip]).astype(I32)

        x3 = x_loc.reshape(n_tok, sublanes, LANES)
        chunks = [lax.all_gather(x3[bounds[k]:bounds[k + 1]], dev_axes, tiled=True) for k in range(n_chunk)]
        swap = [(i, i ^ 1) for i in range(n_ep)]
        w_a_sib = lax.ppermute(w_a, 'ep', swap)
        w_b_sib = lax.ppermute(w_b, 'ep', swap)

        toks, wgts, cnts = route(ids_loc, gate_loc, bounds)
        for_chip = toks[:experts].reshape(n_chip, 1, sub, LANES)
        table = jnp.concatenate([
            jnp.broadcast_to(for_chip, (n_chip, 2, sub, LANES)).reshape(group, sub, LANES),
            jnp.broadcast_to(cnts[None], (group, PREFIX_ROWS, LANES))], axis=1)
        table = lax.all_to_all(table, dev_axes, 0, 0, tiled=True)
        lists = build_lists(place, table.reshape(-1), cap, slots_a, slots_b, early, bounds, n_y, n_x, sub)

        totals = table[:, sub + n_chunk, :experts]
        offs = jnp.cumsum(totals, axis=0) - totals
        kept = jnp.clip(cap - offs, 0, totals)
        kept0 = jnp.minimum(table[:, sub + 1, :experts], kept)
        y, x = chip // n_x, chip % n_x

        def counts_of(n):
            by_place = n.reshape(n_y, n_x, 2, n_y, n_x, sub)
            along_y = lax.dynamic_slice(by_place, (0, x, core, y, 0, 0), (n_y, 1, 1, 1, n_x, sub)).reshape(-1)
            along_x = lax.dynamic_slice(by_place, (y, 0, core, 0, x, 0), (1, n_x, 1, n_y, 1, sub)).reshape(-1)
            per_chip = jnp.sum(by_place, axis=5)
            return along_y, along_x, jnp.sum(per_chip, axis=0), jnp.sum(per_chip, axis=1)

        kept_a, kept_b, rows_a, rows_b = counts_of(kept)
        kept0_a, kept0_b, rows0_a, rows0_b = counts_of(kept0)
        need_a = jnp.max(jnp.maximum(rows0_a, early) + rows_a - rows0_a)
        need_b = jnp.max(jnp.maximum(rows0_b, early) + rows_b - rows0_b)

        tiers = [(base_a * q // 64, base_b * q // 64) for q in SIZES] + [(slots_a, slots_b)]
        limits = jnp.array(tiers[:-1], I32)
        index = jnp.sum(jnp.logical_or(need_a > limits[:, 0], need_b > limits[:, 1]).astype(I32))
        counts = (kept_a, kept_b, kept0_a, kept0_b)
        lists, counts, index = lax.optimization_barrier((lists, counts, index))

        def up_x(v, d):
            return lax.ppermute(v, 'ep', [(i, (i + 2 * d) % n_ep) for i in range(n_ep)])

        def up_y(v, d):
            return lax.ppermute(v, 'ep2', [(i, (i + d) % n_y) for i in range(n_y)])

        half = sublanes // 2
        sends, earlies = None, ()
        for k in range(n_chunk):
            sends = run_experts(k, n_chunk, lists, place, chunks[k], w_a, w_a_sib, w_b, w_b_sib, sends, n_x * slots_a, n_y * slots_b)
            if k == 0:
                early_a = [lax.slice_in_dim(sends[0], d * slots_a, d * slots_a + early) for d in direct_of(n_x)]
                early_b = [lax.slice_in_dim(sends[1], d * slots_b, d * slots_b + early) for d in direct_of(n_y)]
                sends, early_a, early_b, toks, wgts = lax.optimization_barrier((sends, early_a, early_b, toks, wgts))
                earlies = [up_x(v, d) for v, d in zip(early_a, direct_of(n_x))] + [up_y(v, d) for v, d in zip(early_b, direct_of(n_y))]
        tok_all = lax.all_gather(toks[:experts].reshape(-1), dev_axes, tiled=True)
        wgt_all = lax.all_gather(wgts[:experts].reshape(-1), dev_axes, tiled=True)
        sends = (sends[0].reshape(n_x, slots_a, half, LANES), sends[1].reshape(n_y, slots_b, half, LANES))

        recvs = lax.switch(index, [functools.partial(spread, a, b, early, i, n_y, n_x) for i, (a, b) in enumerate(tiers)], *sends)
        recvs, tok_all, wgt_all = lax.optimization_barrier((recvs, tok_all, wgt_all))
        sums = functools.partial(weighted_sums, n_y, n_x)
        common = (early, counts, place, tok_all, wgt_all, recvs, sends, earlies, n_tok)
        split = sums(0, *common)
        cut = 2 * len(first_of(n_y))
        got = (
            up_y(split[cut - 2], 1), up_y(split[1], -1),
            up_x(split[-2], 1), up_x(split[cut + 1], -1),
        )
        whole = sums(1, *common)
        return reduce_back(len(tiers), n_y, n_x, got, split, whole, x_loc)

    tok_spec = P(('dp', 'ep2', 'ep'), None)
    w_spec = P(dev_axes, None, None)
    return jax.shard_map(local_step, mesh=mesh, in_specs=(tok_spec, tok_spec, tok_spec, w_spec, w_spec), out_specs=tok_spec, check_vma=False)
```

```python
import collections
import functools
import math

import jax
import jax.numpy as jnp
from jax import lax
from jax.experimental import pallas as pl
from jax.experimental.pallas import tpu as pltpu
from jax.sharding import PartitionSpec as P

LANES = 128
SEGMENTS = (0, 17, 34, 49, 64)
CHUNKS = (0, 3, 4)
SIZES = (78, 80, 82, 84, 86, 88, 90, 94, 100)
TILE = 256
PREFIX_ROWS = 8
BF16 = jnp.bfloat16
F32 = jnp.float32
I32 = jnp.int32
HBM = pl.BlockSpec(memory_space=pl.ANY)
SMEM = pl.BlockSpec(memory_space=pltpu.SMEM)
VMEM = pl.BlockSpec(memory_space=pltpu.VMEM)
BOTH = range(2)
UNROLL = 8
BLOCK = 16
PAIR = pltpu.SemaphoreType.DMA((2,))
COST = pl.CostEstimate(flops=2 * 10 ** 10, bytes_accessed=10 ** 7, transcendentals=0)
VMEM_LIMIT = 64_000_000
LOCAL = pltpu.CompilerParams(vmem_limit_bytes=VMEM_LIMIT)
MIXED = pltpu.CompilerParams(vmem_limit_bytes=VMEM_LIMIT)


def remote_params(cid):
    return pltpu.CompilerParams(collective_id=cid, has_side_effects=True, vmem_limit_bytes=VMEM_LIMIT)


def take(refs, n):
    return refs[:n], refs[n:]


def start(copy):
    copy.start()


def wait(copy):
    copy.wait()


def capacity_of(group_size, n_tok, n_top, experts):
    return 8 * ((5 * group_size * n_tok * n_top) // (32 * experts))


def far_of(n):
    return n // 2 if n % 2 == 0 and n >= 4 else 0


def direct_of(n):
    return [d for d in range(1, n) if d != far_of(n)]


def bounds_of(n_tok):
    return tuple(16 * ((n_tok * q + 512) // 1024) for q in SEGMENTS)


def tokens_of(bounds, path, w):
    lo, hi = bounds[2 * path + w:][:2]
    return hi - lo


def order_of(n, w):
    return [n - 1 - s if w == 0 else (1 + s) % n for s in range(n)]


def route_kernel(bounds, ids_ref, gate_ref, tok_ref, wgt_ref, cnt_ref, code_t, gate_t, tok_acc, wgt_acc):
    n_tok, n_top = ids_ref.shape
    lane = lax.broadcasted_iota(I32, (n_tok, LANES), 1)
    member = jnp.zeros((n_tok, LANES), F32)
    gates = jnp.zeros((n_tok, LANES), F32)
    for j in range(n_top):
        hit = ids_ref[:, j:j + 1] == lane
        member = member + jnp.where(hit, 1.0, 0.0)
        gates = gates + jnp.where(hit, gate_ref[:, j:j + 1], 0.0)
    member_b = member.astype(BF16)
    row_block = min(n_tok, 128)
    for i in range(n_tok // row_block):
        rows = pl.ds(i * row_block, row_block)
        later = lax.broadcasted_iota(I32, (row_block, n_tok), 0) + i * row_block
        earlier = lax.broadcasted_iota(I32, (row_block, n_tok), 1)
        tri = jnp.where(earlier < later, 1.0, 0.0).astype(BF16)
        rank = jnp.dot(tri, member_b, preferred_element_type=F32)
        mem = member[i * row_block:(i + 1) * row_block]
        code_t[:, rows] = jnp.where(mem > 0.5, rank, -1.0).T
        gate_t[:, rows] = gates[i * row_block:(i + 1) * row_block].T
    total = jnp.zeros((1, LANES), F32)
    rows_out = [total]
    for lo, hi in zip(bounds[:-1], bounds[1:]):
        total = total + jnp.sum(member[lo:hi], axis=0, keepdims=True)
        rows_out.append(total)
    while len(rows_out) < PREFIX_ROWS:
        rows_out.append(total)
    cnt_ref[...] = jnp.concatenate(rows_out, axis=0).astype(I32)
    tok_acc[...] = jnp.zeros_like(tok_acc)
    wgt_acc[...] = jnp.zeros_like(wgt_acc)
    slot = lax.broadcasted_iota(I32, (LANES, n_tok), 0).astype(F32)
    token = lax.broadcasted_iota(I32, (1, n_tok), 1).astype(F32)
    out_lane = lax.broadcasted_iota(I32, (LANES, LANES), 1)

    def one_expert(e, carry):
        hit = slot == code_t[pl.ds(e, 1), :]
        tok = jnp.sum(jnp.where(hit, token, 0.0), axis=1, keepdims=True)
        wgt = jnp.sum(jnp.where(hit, gate_t[pl.ds(e, 1), :], 0.0), axis=1, keepdims=True)
        tok_acc[...] = jnp.where(out_lane == e, tok, tok_acc[...])
        wgt_acc[...] = jnp.where(out_lane == e, wgt, wgt_acc[...])
        return carry

    lax.fori_loop(0, LANES, one_expert, 0)
    tok_ref[...] = tok_acc[...].T.astype(I32)
    wgt_ref[...] = wgt_acc[...].T


def route(ids, gate, bounds):
    n_tok = ids.shape[0]
    return pl.pallas_call(
        functools.partial(route_kernel, bounds),
        out_shape=(
            jax.ShapeDtypeStruct((LANES, LANES), I32),
            jax.ShapeDtypeStruct((LANES, LANES), F32),
            jax.ShapeDtypeStruct((PREFIX_ROWS, LANES), I32),
        ),
        in_specs=[VMEM, VMEM],
        out_specs=(VMEM, VMEM, VMEM),
        scratch_shapes=[
            pltpu.VMEM((LANES, n_tok), F32),
            pltpu.VMEM((LANES, n_tok), F32),
            pltpu.VMEM((LANES, LANES), F32),
            pltpu.VMEM((LANES, LANES), F32),
        ],
        cost_estimate=COST,
        name='route',
    )(ids, gate)


def list_kernel(cap, slots_a, slots_b, early, bounds, n_y, n_x, sub, place_ref, info_ref,
                src_ref, start_ref, len_ref, dst_ref, lim_ref, dir_ref, span_ref, kept_ref, base_ref, lim_tab, dir_tab):
    core, chip = place_ref[0], place_ref[1]
    n_dst = n_y * n_x
    n_seg, n_chunk = len(bounds) - 1, len(CHUNKS) - 1
    dev_words = (sub + PREFIX_ROWS) * LANES
    width = src_ref.shape[0] // sub
    my_y, my_x = chip // n_x, chip % n_x

    def count(g, k, e):
        return info_ref[g * dev_words + (sub + k) * LANES + chip * sub + e]

    def per_expert(e, carry):
        def per_dev(i, off):
            for c in BOTH:
                n = count(2 * i + c, n_seg, e)
                kept = jnp.clip(cap - off, 0, n)
                off = off + n

                @pl.when(core == c)
                def _():
                    kept_ref[i * sub + e] = kept
            return off
        lax.fori_loop(0, n_dst, per_dev, 0)
        return carry

    lax.fori_loop(0, sub, per_expert, 0)

    def rows_in(k, i, e):
        g, kept = 2 * i + core, kept_ref[i * sub + e]
        return jnp.minimum(count(g, k + 1, e), kept) - jnp.minimum(count(g, k, e), kept)

    def block_bases(path, n_blocks, n_inner, slots, index):
        for d in range(n_blocks):
            acc = jnp.int32(d * slots)
            for w in BOTH:
                for r in order_of(n_inner, w):
                    i = index(d, r)

                    def add(e, acc):
                        base_ref[((2 * path + w) * n_dst + i) * sub + e] = acc
                        return acc + rows_in(2 * path + w, i, e)

                    acc = lax.fori_loop(0, sub, add, acc)
                    direct = direct_of(n_blocks)
                    lim_tab[path * n_dst + i] = d * slots + early if d in direct else 0
                    dir_tab[path * n_dst + i] = direct.index(d) if d in direct else 0
                if w == 0:
                    acc = jnp.maximum(acc, d * slots + early)

    block_bases(0, n_x, n_y, slots_a, lambda d, r: lax.rem(my_y + r, n_y) * n_x + lax.rem(my_x + d, n_x))
    block_bases(1, n_y, n_x, slots_b, lambda d, r: lax.rem(my_y + d, n_y) * n_x + lax.rem(my_x + r, n_x))

    def expert_lists(e, carry):
        pos = e * width
        for chunk, (chunk_lo, chunk_hi) in enumerate(zip(CHUNKS[:-1], CHUNKS[1:])):
            size = bounds[chunk_hi] - bounds[chunk_lo]
            start_at = pos
            for k in range(chunk_lo, chunk_hi):

                def segment(i, o):
                    g = 2 * i + core
                    kept = kept_ref[i * sub + e]
                    s0 = jnp.minimum(count(g, k, e), kept)
                    n = jnp.minimum(count(g, k + 1, e), kept) - s0
                    j = (e * n_seg + k) * n_dst + i
                    start_ref[j] = o
                    len_ref[j] = n
                    dst_ref[j] = base_ref[(k * n_dst + i) * sub + e]
                    lim_ref[j] = lim_tab[(k // 2) * n_dst + i]
                    dir_ref[j] = dir_tab[(k // 2) * n_dst + i]
                    src0 = g * size - bounds[chunk_lo]
                    tok0 = g * dev_words + e * LANES + s0

                    def block(b, c):
                        vals = [info_ref[tok0 + b * UNROLL + q] for q in range(UNROLL)]
                        for q in range(UNROLL):
                            src_ref[o + b * UNROLL + q] = src0 + vals[q]
                        return c

                    lax.fori_loop(0, pl.cdiv(n, UNROLL), block, 0)
                    return o + n

                pos = lax.fori_loop(0, n_dst, segment, pos)
            span_ref[(e * n_chunk + chunk) * 2] = start_at
            span_ref[(e * n_chunk + chunk) * 2 + 1] = pos - start_at

            def pad(b, c):
                for q in range(UNROLL):
                    src_ref[pos + b * UNROLL + q] = 0
                return c

            lax.fori_loop(0, TILE // UNROLL, pad, 0)
            pos = pos + TILE
        return carry

    lax.fori_loop(0, sub, expert_lists, 0)


def build_lists(place, info, cap, slots_a, slots_b, early, bounds, n_y, n_x, sub):
    n_dst, n_seg = n_y * n_x, len(bounds) - 1
    n_chunk = len(CHUNKS) - 1
    width = LANES * n_dst + n_chunk * TILE + UNROLL
    segs = sub * n_seg * n_dst + UNROLL
    return pl.pallas_call(
        functools.partial(list_kernel, cap, slots_a, slots_b, early, bounds, n_y, n_x, sub),
        out_shape=(
            jax.ShapeDtypeStruct((sub * width,), I32),
            *[jax.ShapeDtypeStruct((segs,), I32) for _ in range(5)],
            jax.ShapeDtypeStruct((sub * n_chunk * 2,), I32),
        ),
        in_specs=[SMEM, SMEM],
        out_specs=(SMEM,) * 7,
        scratch_shapes=[
            pltpu.SMEM((n_dst * sub,), I32),
            pltpu.SMEM((n_seg * n_dst * sub,), I32),
            pltpu.SMEM((2 * n_dst,), I32),
            pltpu.SMEM((2 * n_dst,), I32),
        ],
        cost_estimate=COST,
        name='row_lists',
    )(place, info)


def gelu(v):
    return 0.5 * v * (1.0 + jnp.tanh(math.sqrt(2.0 / math.pi) * (v + 0.044715 * v * v * v)))


def expert_kernel(chunk, n_seg, early, n_early, *refs):
    lo_seg, hi_seg = CHUNKS[chunk:][:2]
    (src, seg_start, seg_len, seg_dst, seg_lim, seg_dir, span, place, x_hbm, wa_own, wa_sib, wb_own, wb_sib), refs = take(refs, 13)
    if lo_seg > 0:
        refs = refs[1:]
    paths, at = [], 0
    for path in BOTH:
        first, last = max(lo_seg, 2 * path), min(hi_seg, 2 * path + 2)
        if first < last:
            n = n_early[path] if lo_seg == 0 else 0
            paths.append((first, last, refs[at], refs[at + 1:at + 1 + n]))
            at += 1 + n
    xbuf, xrows, obuf, wa, wb, t_e, t_base, t_cnt, ptr, gsem, ssem, wsem = refs[at:]
    e_loc, d_model, _ = wa_own.shape
    sub = 2 * e_loc
    core = place[0]
    sublanes = d_model // LANES
    n_dst = (seg_start.shape[0] - UNROLL) // (sub * n_seg)

    def span_of(e):
        at = (e * (len(CHUNKS) - 1) + chunk) * 2
        return span[at], span[at + 1]

    def weight_copies(e, act):
        slot = e % 2
        q = e % e_loc

        @pl.when(e // e_loc == core)
        def _():
            act(pltpu.make_async_copy(wa_own.at[q], wa.at[slot], wsem.at[slot, 0]))
            act(pltpu.make_async_copy(wb_own.at[q], wb.at[slot], wsem.at[slot, 1]))

        @pl.when(e // e_loc != core)
        def _():
            act(pltpu.make_async_copy(wa_sib.at[q], wa.at[slot], wsem.at[slot, 0]))
            act(pltpu.make_async_copy(wb_sib.at[q], wb.at[slot], wsem.at[slot, 1]))

    weight_copies(0, start)

    def plan(e, t):
        lo, n = span_of(e)

        def put(i, c):
            t_e[t + i] = e
            t_base[t + i] = lo + i * TILE
            t_cnt[t + i] = jnp.minimum(n - i * TILE, TILE)
            return c

        n_tiles = (n + TILE - 1) // TILE
        lax.fori_loop(0, n_tiles, put, 0)
        return t + n_tiles

    n_all = lax.fori_loop(0, sub, plan, 0)
    for t in BOTH:
        t_base[n_all + t], _ = span_of(0)

    def fetch_row(t, r):
        slot = t % 2
        pltpu.make_async_copy(x_hbm.at[src[t_base[t] + r]], xbuf.at[slot, r], gsem.at[slot]).start()

    def gather_wait(t):
        slot = t % 2
        pltpu.make_async_copy(x_hbm.at[pl.ds(0, TILE)], xbuf.at[slot], gsem.at[slot]).wait()

    def scatter_start(t):
        base, slot = t_base[t], t % 2
        end = base + t_cnt[t]

        for path, (_, last, send, earlies) in enumerate(paths):
            j_end = (t_e[t] * n_seg + last) * n_dst

            def more(j):
                return jnp.logical_and(j < j_end, seg_start[j] < end)

            def segment(j):
                first_row = seg_start[j]
                lo = jnp.maximum(first_row, base)
                n = jnp.minimum(first_row + seg_len[j], end) - lo
                to = seg_dst[j] + lo - first_row
                n_early = jnp.clip(seg_lim[j] - to, 0, jnp.maximum(n, 0)) if earlies else 0

                for q, rows in enumerate(earlies):
                    @pl.when(jnp.logical_and(n_early > 0, seg_dir[j] == q))
                    def _():
                        pltpu.make_async_copy(
                            obuf.at[slot, pl.ds(lo - base, n_early)],
                            rows.at[pl.ds(to - seg_lim[j] + early, n_early)],
                            ssem.at[slot],
                        ).start()

                @pl.when(n > n_early)
                def _():
                    pltpu.make_async_copy(
                        obuf.at[slot, pl.ds(lo - base + n_early, n - n_early)],
                        send.at[pl.ds(to + n_early, n - n_early)],
                        ssem.at[slot],
                    ).start()
                return j + 1

            start = ptr[path]
            ptr[path] = jnp.maximum(lax.while_loop(more, segment, start) - 1, start)

    def scatter_wait(t):
        n, slot = t_cnt[t], t % 2
        send = paths[0][2]
        pltpu.make_async_copy(obuf.at[slot, pl.ds(0, n)], send.at[pl.ds(0, n)], ssem.at[slot]).wait()

    def prime(r, c):
        for t in BOTH:
            fetch_row(t, r)
        return c

    lax.fori_loop(0, TILE, prime, 0, unroll=UNROLL)

    def one_expert(e, t_first):
        weight_copies(e, wait)

        @pl.when(e + 1 < sub)
        def _():
            weight_copies(e + 1, start)

        ws = e % 2
        _, n = span_of(e)
        for path, (first, _, _, _) in enumerate(paths):
            ptr[path] = (e * n_seg + first) * n_dst

        def one_tile(i, t):
            slot = t % 2
            gather_wait(t)

            @pl.when(t >= 2)
            def _():
                scatter_wait(t - 2)

            xrows[...] = xbuf[slot].reshape(TILE, d_model)
            for r in range(TILE):
                fetch_row(t + 2, r)
            hidden = gelu(jnp.dot(xrows[...], wa[ws], preferred_element_type=F32)).astype(BF16)
            out = jnp.dot(hidden, wb[ws], preferred_element_type=F32).astype(BF16)
            obuf[slot] = out.reshape(TILE, sublanes, LANES)
            scatter_start(t)
            return t + 1

        return lax.fori_loop(0, (n + TILE - 1) // TILE, one_tile, t_first)

    lax.fori_loop(0, sub, one_expert, 0)
    for back in (2, 1):
        gather_wait(n_all + back)

        @pl.when(n_all >= back)
        def _():
            scatter_wait(n_all - back)


def run_experts(chunk, early, n_early, lists, place, x_rows, wa, wa_sib, wb, wb_sib, rows):
    e_loc, d_model, ff = wa.shape
    sub = 2 * e_loc
    sublanes = d_model // LANES
    ops = (*lists, place, x_rows, wa, wa_sib, wb, wb_sib) + (() if chunk == 0 else (rows,))
    n_smem = len(lists) + 1
    max_tiles = sub * (pl.cdiv(lists[0].shape[0] // sub, TILE) + 1) + 2
    if chunk == 0:
        sizes = [rows[0]] + [early] * n_early[0] + [rows[1]] + [early] * n_early[1]
    else:
        sizes = [rows.shape[0]]
    return pl.pallas_call(
        functools.partial(expert_kernel, chunk, len(SEGMENTS) - 1, early, n_early),
        out_shape=tuple(jax.ShapeDtypeStruct((n, sublanes, LANES), BF16) for n in sizes),
        in_specs=[SMEM] * n_smem + [HBM] * (len(ops) - n_smem),
        out_specs=(HBM,) * len(sizes),
        scratch_shapes=[
            pltpu.VMEM((2, TILE, sublanes, LANES), BF16),
            pltpu.VMEM((TILE, d_model), BF16),
            pltpu.VMEM((2, TILE, sublanes, LANES), BF16),
            pltpu.VMEM((2, d_model, ff), BF16),
            pltpu.VMEM((2, ff, d_model), BF16),
            pltpu.SMEM((max_tiles,), I32),
            pltpu.SMEM((max_tiles,), I32),
            pltpu.SMEM((max_tiles,), I32),
            pltpu.SMEM((2,), I32),
            PAIR, PAIR,
            pltpu.SemaphoreType.DMA((2, 2)),
        ],
        input_output_aliases={} if chunk == 0 else {len(ops) - 1: 0},
        compiler_params=MIXED,
        cost_estimate=COST,
        name='experts',
    )(*ops)


PIECES = 4


class Ring:
    def __init__(self, axis, n_y, n_x):
        y, ec = lax.axis_index('ep2'), lax.axis_index('ep')
        self.axis, self.core = axis, ec % 2
        self.n = n_x if axis == 'x' else n_y
        self.pos = ec // 2 if axis == 'x' else y
        self.direct, self.far = direct_of(self.n), far_of(self.n)

    def place(self, d):
        return lax.rem(self.pos + d + self.n, self.n)

    def device(self, d):
        if self.axis == 'x':
            return {'ep': self.place(d) * 2 + self.core}
        return {'ep2': self.place(d)}

    def remote(self, src, dst, sems, i, d):
        return pltpu.make_async_remote_copy(
            src_ref=src, dst_ref=dst, send_sem=sems.at[0, i], recv_sem=sems.at[1, i],
            device_id=self.device(d), device_id_type=pl.DeviceIdType.MESH)

    def signal(self, barrier):
        for d in range(1, self.n):
            pl.semaphore_signal(barrier, inc=1, device_id=self.device(d), device_id_type=pl.DeviceIdType.MESH)


def spread_kernel(rows_a, rows_b, early, n_y, n_x, send_a, send_b, recv_a, recv_b, stage_a, stage_b, sem_a, sem_b):
    rings = (Ring('x', n_y, n_x), Ring('y', n_y, n_x))
    barrier = pltpu.get_barrier_semaphore()
    for ring in rings:
        ring.signal(barrier)
    pl.semaphore_wait(barrier, n_x + n_y - 2)

    sides = list(zip(rings, (rows_a, rows_b), (send_a, send_b), (recv_a, recv_b), (stage_a, stage_b), (sem_a, sem_b)))

    def lead(side, p):
        ring, rows, send, _, stage, sem = side
        hop = ring.far // 2 if p % 2 == 0 else -(ring.far // 2)
        part = pl.ds(p * (rows // PIECES), rows // PIECES)
        return ring.remote(send.at[ring.far, part], stage.at[part], sem, p, hop)

    def follow(side, p):
        ring, rows, _, recv, stage, sem = side
        hop = ring.far // 2 if p % 2 == 0 else -(ring.far // 2)
        part = pl.ds(p * (rows // PIECES), rows // PIECES)
        return ring.remote(stage.at[part], recv.at[ring.far, part], sem, PIECES + p, hop)

    def straight(side, i):
        ring, rows, send, recv, _, sem = side
        d = ring.direct[i]
        part = pl.ds(early, rows - early)
        return ring.remote(send.at[d, part], recv.at[d, part], sem, 2 * PIECES + i, d)

    relayed = [(side, p) for p in range(PIECES) for side in sides if side[0].far]
    direct = [(side, i) for side in sides for i in range(len(side[0].direct))]
    for job in relayed:
        lead(*job).start()
    for job in direct:
        straight(*job).start()
    for job in relayed:
        lead(*job).wait_recv()
        follow(*job).start()
    for job in relayed:
        lead(*job).wait_send()
    for job in direct:
        straight(*job).wait()
    for job in relayed:
        follow(*job).wait()


def spread(rows_a, rows_b, early, cid, n_y, n_x, send_a, send_b):
    return pl.pallas_call(
        functools.partial(spread_kernel, rows_a, rows_b, early, n_y, n_x),
        out_shape=tuple(jax.ShapeDtypeStruct(s, BF16) for s in (send_a.shape, send_b.shape, send_a.shape[1:], send_b.shape[1:])),
        in_specs=[HBM, HBM],
        out_specs=(HBM,) * 4,
        scratch_shapes=[
            pltpu.SemaphoreType.DMA((2, 2 * PIECES + n_x)),
            pltpu.SemaphoreType.DMA((2, 2 * PIECES + n_y)),
        ],
        compiler_params=remote_params(cid),
        name='spread_%d_%d' % (rows_a, rows_b),
    )(send_a, send_b)[:2]


WAYS = 4


Path = collections.namedtuple('Path', ('recv', 'send', 'earlies', 'at', 'blocks', 'out_at', 'steps'))


def spot(n_y, n_x, p, d, w, s):
    most = max(n_y, n_x)
    return (((p * most + d) * 2 + w) * most + s) * 2


def list_at(n_y, n_x, sub, my, p, s, w, d, level):
    at, blocks, out_at, steps = (my[1], n_x, my[0], n_y) if p == 0 else (my[0], n_y, my[1], n_x)
    out = lax.rem(out_at + order_of(steps, w)[s], steps)
    return ((out * 3 + level) * blocks + lax.rem(at + blocks - d, blocks)) * sub


def plan_kernel(n_y, n_x, early, lev_a, lev_b, place, rows_at):
    chip = place[1]
    sub = lev_a.shape[0] // (3 * n_y * n_x)
    for p, levels in enumerate((lev_a, lev_b)):
        blocks, steps = ((n_x, n_y), (n_y, n_x))[p]
        for d in range(blocks):
            acc = jnp.int32(0)
            for w in BOTH:
                for s in range(steps):
                    lower, upper = (list_at(n_y, n_x, sub, (chip // n_x, chip % n_x), p, s, w, d, w + up) for up in BOTH)

                    def add(e, n):
                        return n + levels[upper + e] - levels[lower + e]

                    n = lax.fori_loop(0, sub, add, jnp.int32(0))
                    at = spot(n_y, n_x, p, d, w, s)
                    rows_at[at] = acc
                    rows_at[at + 1] = n
                    acc = acc + n
                if not w:
                    acc = jnp.maximum(acc, early)


def plan_rows(n_y, n_x, early, levels, place):
    most = max(n_y, n_x)
    return pl.pallas_call(
        functools.partial(plan_kernel, n_y, n_x, early),
        out_shape=jax.ShapeDtypeStruct((8 * most * most,), I32),
        in_specs=[SMEM] * 3,
        out_specs=SMEM,
        cost_estimate=COST,
        name='plan_rows',
    )(*levels, place)


def sum_kernel(n_y, n_x, passes, early, bounds, *refs):
    (lev_a, lev_b, rows_at, place, tok_hbm, wgt_hbm, recv_a, recv_b, send_a, send_b), refs = take(refs, 10)
    early_a, refs = take(refs, len(direct_of(n_x)))
    early_b, refs = take(refs, len(direct_of(n_y)))
    core, chip = place[0], place[1]
    my_y, my_x = chip // n_x, chip % n_x
    n_chip = n_y * n_x
    sub = lev_a.shape[0] // (3 * n_chip)
    words = sub * LANES
    per_dev = tok_hbm.shape[0] // (2 * n_chip)
    paths = (
        Path(recv_a, send_a, early_a, my_x, n_x, my_y, n_y),
        Path(recv_b, send_b, early_b, my_y, n_y, my_x, n_x),
    )
    todo = [(p, s) for p in BOTH for s in passes if s < paths[p].steps]
    outs, refs = take(refs, 2 * len(todo))
    (tok, wgt, *bufs), refs = take(refs, 4)
    accs, (tsem, rsem, zsem) = take(refs, 2 * WAYS)
    ways = [accs[:WAYS], accs[WAYS:]]
    table_of, size = {}, 0
    for p, s in todo:
        for w in BOTH:
            table_of[p, s, w] = size
            size += paths[p].blocks * words

    def dest(p, s, w):
        return lax.rem(paths[p].out_at + order_of(paths[p].steps, w)[s], paths[p].steps)

    def source(p, d):
        return lax.rem(paths[p].at + paths[p].blocks - d, paths[p].blocks)

    def tables(p, s, act):
        for w in BOTH:
            i = dest(p, s, w)
            g = (i * n_x + my_x) * 2 + core if p == 0 else (my_y * n_x + i) * 2 + core
            for d in range(paths[p].blocks):
                q = source(p, d)
                owner = my_y * n_x + q if p == 0 else q * n_x + my_x
                src = pl.ds(pl.multiple_of(g * per_dev + owner * words, words), words)
                dst = pl.ds(table_of[p, s, w] + d * words, words)
                act(pltpu.make_async_copy(tok_hbm.at[src], tok.at[dst], tsem.at[todo.index((p, s))]))
                act(pltpu.make_async_copy(wgt_hbm.at[src], wgt.at[dst], tsem.at[todo.index((p, s))]))

    jobs = [(p, s, d) for p, s in todo for d in range(paths[p].blocks)]

    def fetch(job, act):
        p, s, d = jobs[job]
        path = paths[p]
        slot = job % 2
        for w in BOTH:
            first, n = (rows_at[spot(n_y, n_x, p, d, w, s) + i] for i in BOTH)
            to = bufs[w].at[slot]
            main = path.recv if d else path.send
            n_early = 0
            if not w and d in direct_of(path.blocks):
                rows = path.earlies[direct_of(path.blocks).index(d)]
                n_early = jnp.clip(early - first, 0, n)

                @pl.when(n_early > 0)
                def _():
                    act(pltpu.make_async_copy(rows.at[pl.ds(first, n_early)], to.at[pl.ds(0, n_early)], rsem.at[slot]))

            @pl.when(n > n_early)
            def _():
                act(pltpu.make_async_copy(
                    main.at[d, pl.ds(first + n_early, n - n_early)], to.at[pl.ds(n_early, n - n_early)], rsem.at[slot]))

    def zero(acc):
        def body(b, c):
            acc[pl.ds(b * BLOCK, BLOCK)] = jnp.zeros((BLOCK, *acc.shape[1:]), F32)
            return c
        lax.fori_loop(0, (acc.shape[0] - 8) // BLOCK, body, 0)

    fetch(0, start)
    for p, s in todo:
        tables(p, s, start)
    puts = []
    for job, (p, s, d) in enumerate(jobs):
        slot = job % 2
        levels = (lev_a, lev_b)[p]
        dummy = accs[0].shape[0] - 8
        if not d:
            for _, *others in ways:
                for acc in others:
                    zero(acc)
            for put in puts:
                put.wait()
            for target, *_ in ways:
                zero(target)
            tables(p, s, wait)
        fetch(job, wait)
        if job + 1 < len(jobs):
            fetch(job + 1, start)

        def one_expert(e, bases):
            counts, firsts = [], []
            for w in BOTH:
                lower, upper = (levels[list_at(n_y, n_x, sub, (my_y, my_x), p, s, w, d, w + up) + e] for up in BOTH)
                counts.append(upper - lower)
                firsts.append(table_of[p, s, w] + d * words + e * LANES + lower)
            longest = jnp.maximum(counts[0], counts[1])

            def group(b, cc):
                adds = []
                for w in BOTH:
                    for q in range(WAYS):
                        r = b * WAYS + q
                        row = bufs[w][slot, bases[w] + r].astype(F32)
                        t = jnp.where(r < counts[w], tok[firsts[w] + r], dummy)
                        adds.append((ways[w][q], t, wgt[firsts[w] + r] * row))
                for acc, t, row in adds:
                    acc[t] = acc[t] + row
                return cc

            lax.fori_loop(0, lax.shift_right_logical(longest + (WAYS - 1), 2), group, 0)
            return bases[0] + counts[0], bases[1] + counts[1]

        lax.fori_loop(0, sub, one_expert, (jnp.int32(0), jnp.int32(0)))
        if d + 1 == paths[p].blocks:
            puts = []
            for w in BOTH:
                target, second, third, fourth = ways[w]
                size = tokens_of(bounds, p, w)

                def merge(b, c):
                    rows = pl.ds(b * BLOCK, BLOCK)
                    target[rows] = (target[rows] + second[rows]) + (third[rows] + fourth[rows])
                    return c

                lax.fori_loop(0, size // BLOCK, merge, 0)
                out = outs[2 * todo.index((p, s)) + w]
                puts.append(pltpu.make_async_copy(target.at[pl.ds(0, size)], out, zsem.at[w]))
                puts[-1].start()
    for put in puts:
        put.wait()


def weighted_sums(n_y, n_x, passes, early, bounds, levels, rows_at, place, tok, wgt, recvs, sends, earlies):
    sublanes = recvs[0].shape[2]
    sub = levels[0].shape[0] // (3 * n_y * n_x)
    todo = [(p, s) for p, n in enumerate((n_y, n_x)) for s in passes if s < n]
    sizes = [tokens_of(bounds, p, w) for p, _ in todo for w in BOTH]
    table = sum((n_x if p == 0 else n_y) * 2 * sub * LANES for p, _ in todo) + 2 * LANES
    tokens = max(b - a for a, b in zip(bounds[:-1], bounds[1:]))
    ops = (*levels, rows_at, place, tok, wgt, *recvs, *sends, *earlies)
    return pl.pallas_call(
        functools.partial(sum_kernel, n_y, n_x, passes, early, bounds),
        out_shape=tuple(jax.ShapeDtypeStruct((n, sublanes, LANES), F32) for n in sizes),
        in_specs=[SMEM] * 4 + [HBM] * (len(ops) - 4),
        out_specs=(HBM,) * len(sizes),
        scratch_shapes=[
            pltpu.SMEM((table,), I32),
            pltpu.SMEM((table,), F32),
            *[pltpu.VMEM((2, sub * LANES + LANES, sublanes, LANES), BF16) for _ in BOTH],
            *[pltpu.VMEM((tokens + 8, sublanes, LANES), F32) for _ in range(2 * WAYS)],
            pltpu.SemaphoreType.DMA((len(todo),)),
            PAIR, PAIR,
        ],
        compiler_params=LOCAL,
        cost_estimate=COST,
        name='weighted_sums',
    )(*ops)


SUM_CHUNKS = 8


def pieces_of(n):
    cuts = [BLOCK * ((n // BLOCK * j) // SUM_CHUNKS) for j in range(SUM_CHUNKS + 1)]
    return [(a, b - a) for a, b in zip(cuts[:-1], cuts[1:]) if b > a]


def reduce_kernel(n_y, n_x, bounds, *refs):
    sizes = (n_y, n_x)
    lanes = [(p, w) for p in BOTH for w in BOTH]
    got, refs = take(refs, len(lanes))
    got = dict(zip(lanes, got))
    sums = {}
    for p, n in enumerate(sizes):
        for s in range(1, n):
            for w in BOTH:
                (sums[p, s, w],), refs = take(refs, 1)
    (x_ref, y_ref), refs = take(refs, 2)
    part, own = {}, {}
    for p, w in lanes:
        for s in range(sizes[p] - 1):
            (part[p, w, s], own[p, w, s]), refs = take(refs, 2)
    zsem, gsem, rsem = refs
    rings = (Ring('y', n_y, n_x), Ring('x', n_y, n_x))
    d_model = x_ref.shape[1]
    pieces = {(p, w): pieces_of(tokens_of(bounds, p, w)) for p, w in lanes}
    order = [(p, w, j) for j in range(SUM_CHUNKS) for p, w in lanes if j < len(pieces[p, w])]

    barrier = pltpu.get_barrier_semaphore()
    for ring in rings:
        for d in (1, -1):
            pl.semaphore_signal(barrier, inc=1, device_id=ring.device(d), device_id_type=pl.DeviceIdType.MESH)
    pl.semaphore_wait(barrier, 4)

    def rows_of(p, w, j):
        return pl.ds(*pieces[p, w][j])

    def load(p, w, s, j):
        r = rows_of(p, w, j)
        return pltpu.make_async_copy(sums[p, s, w].at[r], own[p, w, s - 1].at[r], zsem.at[p, w, s - 1, j])

    def begin(p, w, j):
        r = rows_of(p, w, j)
        return pltpu.make_async_copy(got[p, w].at[r], part[p, w, 0].at[r], gsem.at[p, w, j])

    def hop(p, w, s, j):
        r = rows_of(p, w, j)
        return pltpu.make_async_remote_copy(
            src_ref=part[p, w, s - 1].at[r], dst_ref=part[p, w, s].at[r],
            send_sem=rsem.at[0, p, w, s, j], recv_sem=rsem.at[1, p, w, s, j],
            device_id=rings[p].device(1 if w == 0 else -1), device_id_type=pl.DeviceIdType.MESH)

    def arrive(p, w, s, j):
        if s == 0:
            begin(p, w, j).wait()
        else:
            hop(p, w, s, j).wait_recv()

    last = max(sizes) - 1
    for s in range(1, last + 1):
        for p, w, j in order:
            if s == 1:
                begin(p, w, j).start()
            if s < sizes[p]:
                load(p, w, s, j).start()

    for s in range(1, last):
        for p, w, j in order:
            if s >= sizes[p] - 1:
                continue
            load(p, w, s, j).wait()
            arrive(p, w, s - 1, j)
            into, more = part[p, w, s - 1], own[p, w, s - 1]
            first, n = pieces[p, w][j]

            def add(b, c):
                r = pl.ds(first + b * BLOCK, BLOCK)
                into[r] = into[r] + more[r]
                return c

            lax.fori_loop(0, n // BLOCK, add, 0)
            hop(p, w, s, j).start()

    for p, w, j in order:
        s = sizes[p] - 1
        load(p, w, s, j).wait()
        arrive(p, w, s - 1, j)
        into, more = part[p, w, s - 1], own[p, w, s - 1]
        first, n = pieces[p, w][j]
        token = bounds[2 * p + w] + first

        def finish(b, c):
            r = pl.ds(first + b * BLOCK, BLOCK)
            out = pl.ds(pl.multiple_of(token + b * BLOCK, BLOCK), BLOCK)
            total = into[r] + more[r]
            y_ref[out, :] = (x_ref[out, :].astype(F32) + total.reshape(BLOCK, d_model)).astype(BF16)
            return c

        lax.fori_loop(0, n // BLOCK, finish, 0)
    for s in range(1, last):
        for p, w, j in order:
            if s < sizes[p] - 1:
                hop(p, w, s, j).wait_send()


def reduce_back(cid, n_y, n_x, bounds, got, sums, x):
    n_tok, d_model = x.shape
    sublanes = d_model // LANES
    bufs = []
    for p, n in enumerate((n_y, n_x)):
        for w in BOTH:
            size = tokens_of(bounds, p, w)
            bufs += [pltpu.VMEM((size, sublanes, LANES), F32)] * (2 * (n - 1))
    steps = max(n_y, n_x) - 1
    ops = (*got, *sums, x)
    return pl.pallas_call(
        functools.partial(reduce_kernel, n_y, n_x, bounds),
        out_shape=jax.ShapeDtypeStruct((n_tok, d_model), BF16),
        in_specs=[HBM] * (len(ops) - 1) + [VMEM],
        out_specs=VMEM,
        scratch_shapes=[
            *bufs,
            pltpu.SemaphoreType.DMA((2, 2, steps, SUM_CHUNKS)),
            pltpu.SemaphoreType.DMA((2, 2, SUM_CHUNKS)),
            pltpu.SemaphoreType.DMA((2, 2, 2, steps, SUM_CHUNKS)),
        ],
        compiler_params=remote_params(cid),
        name='reduce_back',
    )(*ops)


def solution(mesh):
    dev_axes = ('ep2', 'ep')
    n_y, n_ep = mesh.shape['ep2'], mesh.shape['ep']
    n_x = n_ep // 2
    group = n_y * n_ep
    n_chip = n_y * n_x

    def local_step(x_loc, ids_loc, gate_loc, w_a, w_b):
        n_tok, d_model = x_loc.shape
        n_top = ids_loc.shape[1]
        e_loc = w_a.shape[0]
        sub = 2 * e_loc
        experts = e_loc * group
        cap = capacity_of(group, n_tok, n_top, experts)
        sublanes = d_model // LANES
        base_a, base_b = n_y * sub * LANES, n_x * sub * LANES
        early = min(base_a, base_b) // 8
        slots_a, slots_b = base_a + early, base_b + early
        bounds = bounds_of(n_tok)
        n_seg, n_chunk = len(bounds) - 1, len(CHUNKS) - 1
        me = lax.axis_index(dev_axes)
        core, chip = me % 2, me // 2
        place = jnp.stack([core, chip]).astype(I32)

        x3 = x_loc.reshape(n_tok, sublanes, LANES)
        chunks = [lax.all_gather(x3[bounds[CHUNKS[k]]:bounds[CHUNKS[k + 1]]], dev_axes, tiled=True) for k in range(n_chunk)]
        swap = [(i, i ^ 1) for i in range(n_ep)]
        w_a_sib = lax.ppermute(w_a, 'ep', swap)
        w_b_sib = lax.ppermute(w_b, 'ep', swap)

        toks, wgts, cnts = route(ids_loc, gate_loc, bounds)
        for_chip = toks[:experts].reshape(n_chip, 1, sub, LANES)
        table = jnp.concatenate([
            jnp.broadcast_to(for_chip, (n_chip, 2, sub, LANES)).reshape(group, sub, LANES),
            jnp.broadcast_to(cnts[None], (group, PREFIX_ROWS, LANES))], axis=1)
        table = lax.all_to_all(table, dev_axes, 0, 0, tiled=True)
        lists = build_lists(place, table.reshape(-1), cap, slots_a, slots_b, early, bounds, n_y, n_x, sub)

        prefix = table[:, sub:sub + n_seg + 1, :experts]
        totals = prefix[:, n_seg]
        offs = jnp.cumsum(totals, axis=0) - totals
        kept = jnp.clip(cap - offs, 0, totals)
        upto = jnp.minimum(prefix, kept[:, None])
        y, x = chip // n_x, chip % n_x
        level_a = lax.dynamic_slice(upto.reshape(n_y, n_ep, n_seg + 1, experts), (0, x * 2 + core, 0, y * n_x * sub), (n_y, 1, 3, n_x * sub))
        level_b = lax.dynamic_slice(upto.reshape(n_y, n_x, 2, n_seg + 1, experts), (y, 0, core, 2, 0), (1, n_x, 1, 3, experts))
        level_b = lax.dynamic_slice(level_b.reshape(n_x, 3, n_y, n_x * sub), (0, 0, 0, x * sub), (n_x, 3, n_y, sub))
        levels = (level_a.reshape(-1), level_b.reshape(-1))
        of_chip = (jnp.arange(experts)[:, None] // sub == jnp.arange(n_chip)[None, :]).astype(F32)
        per_chip = jnp.dot(upto.reshape(-1, experts).astype(F32), of_chip).reshape(group, n_seg + 1, n_chip)
        rows = (per_chip[:, 1:] - per_chip[:, :-1]).astype(I32)
        rows_a = jnp.sum(rows.reshape(n_y, n_ep, n_seg, n_chip), axis=0)
        rows_b = jnp.sum(rows.reshape(n_y, n_x, 2, n_seg, n_chip), axis=1)
        need_a = jnp.max(jnp.maximum(rows_a[:, 0], early) + rows_a[:, 1])
        need_b = jnp.max(jnp.maximum(rows_b[:, :, 2], early) + rows_b[:, :, 3])
        tiers = [(base_a * q // 256, base_b * q // 256) for q in SIZES] + [(slots_a, slots_b)]
        limits = jnp.array(tiers[:-1], I32)
        index = jnp.sum(jnp.logical_or(need_a > limits[:, 0], need_b > limits[:, 1]).astype(I32))
        within = toks[:experts]
        for lo, hi in zip(bounds[1:-1], bounds[:-2]):
            within = jnp.where(toks[:experts] >= lo, within - (lo - hi), within)
        rows_at = plan_rows(n_y, n_x, early, levels, place)
        lists, levels, rows_at, index, within = lax.optimization_barrier((lists, levels, rows_at, index, within))

        def up_x(v, d):
            return lax.ppermute(v, 'ep', [(i, (i + 2 * d) % n_ep) for i in range(n_ep)])

        def up_y(v, d):
            return lax.ppermute(v, 'ep2', [(i, (i + d) % n_y) for i in range(n_y)])

        weights = (w_a, w_a_sib, w_b, w_b_sib)
        direct_x, direct_y = direct_of(n_x), direct_of(n_y)
        n_early = (len(direct_x), len(direct_y))
        first = run_experts(0, early, n_early, lists, place, chunks[0], *weights, (n_x * slots_a, n_y * slots_b))
        first, within, wgts = lax.optimization_barrier((first, within, wgts))
        send_a, early_a = first[0], first[1:1 + n_early[0]]
        send_b, early_b = first[1 + n_early[0]], first[2 + n_early[0]:]
        earlies = [up_x(v, d) for v, d in zip(early_a, direct_x)] + [up_y(v, d) for v, d in zip(early_b, direct_y)]
        send_b, = run_experts(1, early, n_early, lists, place, chunks[1], *weights, send_b)
        tok_all = lax.all_gather(within.reshape(-1), dev_axes, tiled=True)
        wgt_all = lax.all_gather(wgts[:experts].reshape(-1), dev_axes, tiled=True)
        sends = (send_a.reshape(n_x, slots_a, sublanes, LANES), send_b.reshape(n_y, slots_b, sublanes, LANES))

        recvs = lax.switch(index, [functools.partial(spread, a, b, early, i, n_y, n_x) for i, (a, b) in enumerate(tiers)], *sends)
        recvs, tok_all, wgt_all = lax.optimization_barrier((recvs, tok_all, wgt_all))
        common = (early, bounds, levels, rows_at, place, tok_all, wgt_all, recvs, sends, earlies)
        head = weighted_sums(n_y, n_x, (0,), *common)
        got = (up_y(head[0], 1), up_y(head[1], -1), up_x(head[2], 1), up_x(head[3], -1))
        rest = weighted_sums(n_y, n_x, tuple(range(1, max(n_y, n_x))), *common)
        return reduce_back(len(tiers), n_y, n_x, bounds, got, rest, x_loc)

    tok_spec = P(('dp', 'ep2', 'ep'), None)
    w_spec = P(dev_axes, None, None)
    return jax.shard_map(local_step, mesh=mesh, in_specs=(tok_spec, tok_spec, tok_spec, w_spec, w_spec), out_specs=tok_spec, check_vma=False)
```

```python
import collections
import functools
import math

import jax
import jax.numpy as jnp
from jax import lax
from jax.experimental import pallas as pl
from jax.experimental.pallas import tpu as pltpu
from jax.sharding import PartitionSpec as P

LANES = 128
SEGMENTS = (0, 17, 34, 51, 64)
CHUNKS = (0, 3, 4)
SIZES = (78, 80, 82, 84, 86, 88, 90, 94, 100)
TILE = 256
PREFIX_ROWS = 8
BF16 = jnp.bfloat16
F32 = jnp.float32
I32 = jnp.int32
HBM = pl.BlockSpec(memory_space=pl.ANY)
SMEM = pl.BlockSpec(memory_space=pltpu.SMEM)
VMEM = pl.BlockSpec(memory_space=pltpu.VMEM)
BOTH = range(2)
UNROLL = 8
BLOCK = 16
PAIR = pltpu.SemaphoreType.DMA((2,))
COST = pl.CostEstimate(flops=2 * 10 ** 10, bytes_accessed=10 ** 7, transcendentals=0)
VMEM_LIMIT = 64_000_000
LOCAL = pltpu.CompilerParams(vmem_limit_bytes=VMEM_LIMIT)
MIXED = pltpu.CompilerParams(vmem_limit_bytes=VMEM_LIMIT)


def remote_params(cid):
    return pltpu.CompilerParams(collective_id=cid, has_side_effects=True, vmem_limit_bytes=VMEM_LIMIT)


def take(refs, n):
    return refs[:n], refs[n:]


def start(copy):
    copy.start()


def wait(copy):
    copy.wait()


def capacity_of(group_size, n_tok, n_top, experts):
    return 8 * ((5 * group_size * n_tok * n_top) // (32 * experts))


def far_of(n):
    return n // 2 if n % 2 == 0 and n >= 4 else 0


def direct_of(n):
    return [d for d in range(1, n) if d != far_of(n)]


def bounds_of(n_tok):
    return tuple(16 * ((n_tok * q + 512) // 1024) for q in SEGMENTS)


def tokens_of(bounds, path, w):
    lo, hi = bounds[2 * path + w:][:2]
    return hi - lo


def order_of(n, w):
    return [n - 1 - s if w == 0 else (1 + s) % n for s in range(n)]


def route_kernel(bounds, ids_ref, gate_ref, tok_ref, wgt_ref, cnt_ref, code_t, gate_t, tok_acc, wgt_acc):
    n_tok, n_top = ids_ref.shape
    lane = lax.broadcasted_iota(I32, (n_tok, LANES), 1)
    member = jnp.zeros((n_tok, LANES), F32)
    gates = jnp.zeros((n_tok, LANES), F32)
    for j in range(n_top):
        hit = ids_ref[:, j:j + 1] == lane
        member = member + jnp.where(hit, 1.0, 0.0)
        gates = gates + jnp.where(hit, gate_ref[:, j:j + 1], 0.0)
    member_b = member.astype(BF16)
    row_block = min(n_tok, 128)
    for i in range(n_tok // row_block):
        rows = pl.ds(i * row_block, row_block)
        later = lax.broadcasted_iota(I32, (row_block, n_tok), 0) + i * row_block
        earlier = lax.broadcasted_iota(I32, (row_block, n_tok), 1)
        tri = jnp.where(earlier < later, 1.0, 0.0).astype(BF16)
        rank = jnp.dot(tri, member_b, preferred_element_type=F32)
        mem = member[i * row_block:(i + 1) * row_block]
        code_t[:, rows] = jnp.where(mem > 0.5, rank, -1.0).T
        gate_t[:, rows] = gates[i * row_block:(i + 1) * row_block].T
    total = jnp.zeros((1, LANES), F32)
    rows_out = [total]
    for lo, hi in zip(bounds[:-1], bounds[1:]):
        total = total + jnp.sum(member[lo:hi], axis=0, keepdims=True)
        rows_out.append(total)
    while len(rows_out) < PREFIX_ROWS:
        rows_out.append(total)
    cnt_ref[...] = jnp.concatenate(rows_out, axis=0).astype(I32)
    tok_acc[...] = jnp.zeros_like(tok_acc)
    wgt_acc[...] = jnp.zeros_like(wgt_acc)
    slot = lax.broadcasted_iota(I32, (LANES, n_tok), 0).astype(F32)
    token = lax.broadcasted_iota(I32, (1, n_tok), 1).astype(F32)
    out_lane = lax.broadcasted_iota(I32, (LANES, LANES), 1)

    def one_expert(e, carry):
        hit = slot == code_t[pl.ds(e, 1), :]
        tok = jnp.sum(jnp.where(hit, token, 0.0), axis=1, keepdims=True)
        wgt = jnp.sum(jnp.where(hit, gate_t[pl.ds(e, 1), :], 0.0), axis=1, keepdims=True)
        tok_acc[...] = jnp.where(out_lane == e, tok, tok_acc[...])
        wgt_acc[...] = jnp.where(out_lane == e, wgt, wgt_acc[...])
        return carry

    lax.fori_loop(0, LANES, one_expert, 0)
    tok_ref[...] = tok_acc[...].T.astype(I32)
    wgt_ref[...] = wgt_acc[...].T


def route(ids, gate, bounds):
    n_tok = ids.shape[0]
    return pl.pallas_call(
        functools.partial(route_kernel, bounds),
        out_shape=(
            jax.ShapeDtypeStruct((LANES, LANES), I32),
            jax.ShapeDtypeStruct((LANES, LANES), F32),
            jax.ShapeDtypeStruct((PREFIX_ROWS, LANES), I32),
        ),
        in_specs=[VMEM, VMEM],
        out_specs=(VMEM, VMEM, VMEM),
        scratch_shapes=[
            pltpu.VMEM((LANES, n_tok), F32),
            pltpu.VMEM((LANES, n_tok), F32),
            pltpu.VMEM((LANES, LANES), F32),
            pltpu.VMEM((LANES, LANES), F32),
        ],
        cost_estimate=COST,
        name='route',
    )(ids, gate)


def list_kernel(cap, slots_a, slots_b, early, bounds, n_y, n_x, sub, place_ref, info_ref,
                src_ref, start_ref, len_ref, dst_ref, lim_ref, dir_ref, span_ref, kept_ref, base_ref, lim_tab, dir_tab):
    core, chip = place_ref[0], place_ref[1]
    n_dst = n_y * n_x
    n_seg, n_chunk = len(bounds) - 1, len(CHUNKS) - 1
    dev_words = (sub + PREFIX_ROWS) * LANES
    width = src_ref.shape[0] // sub
    my_y, my_x = chip // n_x, chip % n_x

    def count(g, k, e):
        return info_ref[g * dev_words + (sub + k) * LANES + chip * sub + e]

    def per_expert(e, carry):
        def per_dev(i, off):
            for c in BOTH:
                n = count(2 * i + c, n_seg, e)
                kept = jnp.clip(cap - off, 0, n)
                off = off + n

                @pl.when(core == c)
                def _():
                    kept_ref[i * sub + e] = kept
            return off
        lax.fori_loop(0, n_dst, per_dev, 0)
        return carry

    lax.fori_loop(0, sub, per_expert, 0)

    def rows_in(k, i, e):
        g, kept = 2 * i + core, kept_ref[i * sub + e]
        return jnp.minimum(count(g, k + 1, e), kept) - jnp.minimum(count(g, k, e), kept)

    def block_bases(path, n_blocks, n_inner, slots, index):
        for d in range(n_blocks):
            acc = jnp.int32(d * slots)
            for w in BOTH:
                for r in order_of(n_inner, w):
                    i = index(d, r)

                    def add(e, acc):
                        base_ref[((2 * path + w) * n_dst + i) * sub + e] = acc
                        return acc + rows_in(2 * path + w, i, e)

                    acc = lax.fori_loop(0, sub, add, acc)
                    direct = direct_of(n_blocks)
                    lim_tab[path * n_dst + i] = d * slots + early if d in direct else 0
                    dir_tab[path * n_dst + i] = direct.index(d) if d in direct else 0
                if w == 0:
                    acc = jnp.maximum(acc, d * slots + early)

    block_bases(0, n_x, n_y, slots_a, lambda d, r: lax.rem(my_y + r, n_y) * n_x + lax.rem(my_x + d, n_x))
    block_bases(1, n_y, n_x, slots_b, lambda d, r: lax.rem(my_y + d, n_y) * n_x + lax.rem(my_x + r, n_x))

    def expert_lists(e, carry):
        pos = e * width
        for chunk, (chunk_lo, chunk_hi) in enumerate(zip(CHUNKS[:-1], CHUNKS[1:])):
            size = bounds[chunk_hi] - bounds[chunk_lo]
            start_at = pos
            for k in range(chunk_lo, chunk_hi):

                def segment(i, o):
                    g = 2 * i + core
                    kept = kept_ref[i * sub + e]
                    s0 = jnp.minimum(count(g, k, e), kept)
                    n = jnp.minimum(count(g, k + 1, e), kept) - s0
                    j = (e * n_seg + k) * n_dst + i
                    start_ref[j] = o
                    len_ref[j] = n
                    dst_ref[j] = base_ref[(k * n_dst + i) * sub + e]
                    lim_ref[j] = lim_tab[(k // 2) * n_dst + i]
                    dir_ref[j] = dir_tab[(k // 2) * n_dst + i]
                    src0 = g * size - bounds[chunk_lo]
                    tok0 = g * dev_words + e * LANES + s0

                    def block(b, c):
                        vals = [info_ref[tok0 + b * UNROLL + q] for q in range(UNROLL)]
                        for q in range(UNROLL):
                            src_ref[o + b * UNROLL + q] = src0 + vals[q]
                        return c

                    lax.fori_loop(0, pl.cdiv(n, UNROLL), block, 0)
                    return o + n

                pos = lax.fori_loop(0, n_dst, segment, pos)
            span_ref[(e * n_chunk + chunk) * 2] = start_at
            span_ref[(e * n_chunk + chunk) * 2 + 1] = pos - start_at

            def pad(b, c):
                for q in range(UNROLL):
                    src_ref[pos + b * UNROLL + q] = b * UNROLL + q
                return c

            lax.fori_loop(0, TILE // UNROLL, pad, 0)
            pos = pos + TILE
        return carry

    lax.fori_loop(0, sub, expert_lists, 0)


def build_lists(place, info, cap, slots_a, slots_b, early, bounds, n_y, n_x, sub):
    n_dst, n_seg = n_y * n_x, len(bounds) - 1
    n_chunk = len(CHUNKS) - 1
    width = LANES * n_dst + n_chunk * TILE + UNROLL
    segs = sub * n_seg * n_dst + UNROLL
    return pl.pallas_call(
        functools.partial(list_kernel, cap, slots_a, slots_b, early, bounds, n_y, n_x, sub),
        out_shape=(
            jax.ShapeDtypeStruct((sub * width,), I32),
            *[jax.ShapeDtypeStruct((segs,), I32) for _ in range(5)],
            jax.ShapeDtypeStruct((sub * n_chunk * 2,), I32),
        ),
        in_specs=[SMEM, SMEM],
        out_specs=(SMEM,) * 7,
        scratch_shapes=[
            pltpu.SMEM((n_dst * sub,), I32),
            pltpu.SMEM((n_seg * n_dst * sub,), I32),
            pltpu.SMEM((2 * n_dst,), I32),
            pltpu.SMEM((2 * n_dst,), I32),
        ],
        cost_estimate=COST,
        name='row_lists',
    )(place, info)


def gelu(v):
    return 0.5 * v * (1.0 + jnp.tanh(math.sqrt(2.0 / math.pi) * (v + 0.044715 * v * v * v)))


def expert_kernel(chunk, n_seg, early, n_early, *refs):
    lo_seg, hi_seg = CHUNKS[chunk:][:2]
    (src, seg_start, seg_len, seg_dst, seg_lim, seg_dir, span, place, x_hbm, wa_own, wa_sib, wb_own, wb_sib), refs = take(refs, 13)
    if lo_seg > 0:
        refs = refs[1:]
    paths, at = [], 0
    for path in BOTH:
        first, last = max(lo_seg, 2 * path), min(hi_seg, 2 * path + 2)
        if first < last:
            n = n_early[path] if lo_seg == 0 else 0
            paths.append((first, last, refs[at], refs[at + 1:at + 1 + n]))
            at += 1 + n
    xbuf, xrows, obuf, wa, wb, t_e, t_base, t_cnt, ptr, gsem, ssem, wsem = refs[at:]
    e_loc, d_model, _ = wa_own.shape
    sub = 2 * e_loc
    core = place[0]
    sublanes = d_model // LANES
    n_dst = (seg_start.shape[0] - UNROLL) // (sub * n_seg)

    def span_of(e):
        at = (e * (len(CHUNKS) - 1) + chunk) * 2
        return span[at], span[at + 1]

    def weight_copies(e, act):
        slot = e % 2
        q = e % e_loc

        @pl.when(e // e_loc == core)
        def _():
            act(pltpu.make_async_copy(wa_own.at[q], wa.at[slot], wsem.at[slot, 0]))
            act(pltpu.make_async_copy(wb_own.at[q], wb.at[slot], wsem.at[slot, 1]))

        @pl.when(e // e_loc != core)
        def _():
            act(pltpu.make_async_copy(wa_sib.at[q], wa.at[slot], wsem.at[slot, 0]))
            act(pltpu.make_async_copy(wb_sib.at[q], wb.at[slot], wsem.at[slot, 1]))

    weight_copies(0, start)

    def plan(e, t):
        lo, n = span_of(e)

        def put(i, c):
            t_e[t + i] = e
            t_base[t + i] = lo + i * TILE
            t_cnt[t + i] = jnp.minimum(n - i * TILE, TILE)
            return c

        n_tiles = (n + TILE - 1) // TILE
        lax.fori_loop(0, n_tiles, put, 0)
        return t + n_tiles

    n_all = lax.fori_loop(0, sub, plan, 0)
    for t in BOTH:
        t_base[n_all + t], _ = span_of(0)

    def fetch_row(t, r):
        slot = t % 2
        pltpu.make_async_copy(x_hbm.at[src[t_base[t] + r]], xbuf.at[slot, r], gsem.at[slot]).start()

    def gather_wait(t):
        slot = t % 2
        pltpu.make_async_copy(x_hbm.at[pl.ds(0, TILE)], xbuf.at[slot], gsem.at[slot]).wait()

    def scatter_start(t):
        base, slot = t_base[t], t % 2
        end = base + t_cnt[t]

        for path, (_, last, send, earlies) in enumerate(paths):
            j_end = (t_e[t] * n_seg + last) * n_dst

            def more(j):
                return jnp.logical_and(j < j_end, seg_start[j] < end)

            def segment(j):
                first_row = seg_start[j]
                lo = jnp.maximum(first_row, base)
                n = jnp.minimum(first_row + seg_len[j], end) - lo
                to = seg_dst[j] + lo - first_row
                n_early = jnp.clip(seg_lim[j] - to, 0, jnp.maximum(n, 0)) if earlies else 0

                for q, rows in enumerate(earlies):
                    @pl.when(jnp.logical_and(n_early > 0, seg_dir[j] == q))
                    def _():
                        pltpu.make_async_copy(
                            obuf.at[slot, pl.ds(lo - base, n_early)],
                            rows.at[pl.ds(to - seg_lim[j] + early, n_early)],
                            ssem.at[slot],
                        ).start()

                @pl.when(n > n_early)
                def _():
                    pltpu.make_async_copy(
                        obuf.at[slot, pl.ds(lo - base + n_early, n - n_early)],
                        send.at[pl.ds(to + n_early, n - n_early)],
                        ssem.at[slot],
                    ).start()
                return j + 1

            start = ptr[path]
            ptr[path] = jnp.maximum(lax.while_loop(more, segment, start) - 1, start)

    def scatter_wait(t):
        n, slot = t_cnt[t], t % 2
        send = paths[0][2]
        pltpu.make_async_copy(obuf.at[slot, pl.ds(0, n)], send.at[pl.ds(0, n)], ssem.at[slot]).wait()

    def prime(r, c):
        for t in BOTH:
            fetch_row(t, r)
        return c

    lax.fori_loop(0, TILE, prime, 0, unroll=UNROLL)

    def one_expert(e, t_first):
        weight_copies(e, wait)

        @pl.when(e + 1 < sub)
        def _():
            weight_copies(e + 1, start)

        ws = e % 2
        _, n = span_of(e)
        for path, (first, _, _, _) in enumerate(paths):
            ptr[path] = (e * n_seg + first) * n_dst

        def one_tile(i, t):
            slot = t % 2
            gather_wait(t)

            @pl.when(t >= 2)
            def _():
                scatter_wait(t - 2)

            xrows[...] = xbuf[slot].reshape(TILE, d_model)
            for r in range(TILE):
                fetch_row(t + 2, r)
            hidden = gelu(jnp.dot(xrows[...], wa[ws], preferred_element_type=F32)).astype(BF16)
            out = jnp.dot(hidden, wb[ws], preferred_element_type=F32).astype(BF16)
            obuf[slot] = out.reshape(TILE, sublanes, LANES)
            scatter_start(t)
            return t + 1

        return lax.fori_loop(0, (n + TILE - 1) // TILE, one_tile, t_first)

    lax.fori_loop(0, sub, one_expert, 0)
    for back in (2, 1):
        gather_wait(n_all + back)

        @pl.when(n_all >= back)
        def _():
            scatter_wait(n_all - back)


def run_experts(chunk, early, n_early, lists, place, x_rows, wa, wa_sib, wb, wb_sib, rows):
    e_loc, d_model, ff = wa.shape
    sub = 2 * e_loc
    sublanes = d_model // LANES
    ops = (*lists, place, x_rows, wa, wa_sib, wb, wb_sib) + (() if chunk == 0 else (rows,))
    n_smem = len(lists) + 1
    max_tiles = sub * (pl.cdiv(lists[0].shape[0] // sub, TILE) + 1) + 2
    if chunk == 0:
        sizes = [rows[0]] + [early] * n_early[0] + [rows[1]] + [early] * n_early[1]
    else:
        sizes = [rows.shape[0]]
    return pl.pallas_call(
        functools.partial(expert_kernel, chunk, len(SEGMENTS) - 1, early, n_early),
        out_shape=tuple(jax.ShapeDtypeStruct((n, sublanes, LANES), BF16) for n in sizes),
        in_specs=[SMEM] * n_smem + [HBM] * (len(ops) - n_smem),
        out_specs=(HBM,) * len(sizes),
        scratch_shapes=[
            pltpu.VMEM((2, TILE, sublanes, LANES), BF16),
            pltpu.VMEM((TILE, d_model), BF16),
            pltpu.VMEM((2, TILE, sublanes, LANES), BF16),
            pltpu.VMEM((2, d_model, ff), BF16),
            pltpu.VMEM((2, ff, d_model), BF16),
            pltpu.SMEM((max_tiles,), I32),
            pltpu.SMEM((max_tiles,), I32),
            pltpu.SMEM((max_tiles,), I32),
            pltpu.SMEM((2,), I32),
            PAIR, PAIR,
            pltpu.SemaphoreType.DMA((2, 2)),
        ],
        input_output_aliases={} if chunk == 0 else {len(ops) - 1: 0},
        compiler_params=MIXED,
        cost_estimate=COST,
        name='experts',
    )(*ops)


PIECES = 4


class Ring:
    def __init__(self, axis, n_y, n_x):
        y, ec = lax.axis_index('ep2'), lax.axis_index('ep')
        self.axis, self.core = axis, ec % 2
        self.n = n_x if axis == 'x' else n_y
        self.pos = ec // 2 if axis == 'x' else y
        self.direct, self.far = direct_of(self.n), far_of(self.n)

    def place(self, d):
        return lax.rem(self.pos + d + self.n, self.n)

    def device(self, d):
        if self.axis == 'x':
            return {'ep': self.place(d) * 2 + self.core}
        return {'ep2': self.place(d)}

    def remote(self, src, dst, sems, i, d):
        return pltpu.make_async_remote_copy(
            src_ref=src, dst_ref=dst, send_sem=sems.at[0, i], recv_sem=sems.at[1, i],
            device_id=self.device(d), device_id_type=pl.DeviceIdType.MESH)

    def signal(self, barrier):
        for d in range(1, self.n):
            pl.semaphore_signal(barrier, inc=1, device_id=self.device(d), device_id_type=pl.DeviceIdType.MESH)


def spread_kernel(rows_a, rows_b, early, n_y, n_x, send_a, send_b, recv_a, recv_b, stage_a, stage_b, sem_a, sem_b):
    rings = (Ring('x', n_y, n_x), Ring('y', n_y, n_x))
    barrier = pltpu.get_barrier_semaphore()
    for ring in rings:
        ring.signal(barrier)
    pl.semaphore_wait(barrier, n_x + n_y - 2)

    sides = list(zip(rings, (rows_a, rows_b), (send_a, send_b), (recv_a, recv_b), (stage_a, stage_b), (sem_a, sem_b)))

    def lead(side, p):
        ring, rows, send, _, stage, sem = side
        hop = ring.far // 2 if p % 2 == 0 else -(ring.far // 2)
        part = pl.ds(p * (rows // PIECES), rows // PIECES)
        return ring.remote(send.at[ring.far, part], stage.at[part], sem, p, hop)

    def follow(side, p):
        ring, rows, _, recv, stage, sem = side
        hop = ring.far // 2 if p % 2 == 0 else -(ring.far // 2)
        part = pl.ds(p * (rows // PIECES), rows // PIECES)
        return ring.remote(stage.at[part], recv.at[ring.far, part], sem, PIECES + p, hop)

    def straight(side, i):
        ring, rows, send, recv, _, sem = side
        d = ring.direct[i]
        part = pl.ds(early, rows - early)
        return ring.remote(send.at[d, part], recv.at[d, part], sem, 2 * PIECES + i, d)

    relayed = [(side, p) for p in range(PIECES) for side in sides if side[0].far]
    direct = [(side, i) for side in sides for i in range(len(side[0].direct))]
    for job in relayed:
        lead(*job).start()
    for job in direct:
        straight(*job).start()
    for job in relayed:
        lead(*job).wait_recv()
        follow(*job).start()
    for job in relayed:
        lead(*job).wait_send()
    for job in direct:
        straight(*job).wait()
    for job in relayed:
        follow(*job).wait()


def spread(rows_a, rows_b, early, cid, n_y, n_x, send_a, send_b):
    return pl.pallas_call(
        functools.partial(spread_kernel, rows_a, rows_b, early, n_y, n_x),
        out_shape=tuple(jax.ShapeDtypeStruct(s, BF16) for s in (send_a.shape, send_b.shape, send_a.shape[1:], send_b.shape[1:])),
        in_specs=[HBM, HBM],
        out_specs=(HBM,) * 4,
        scratch_shapes=[
            pltpu.SemaphoreType.DMA((2, 2 * PIECES + n_x)),
            pltpu.SemaphoreType.DMA((2, 2 * PIECES + n_y)),
        ],
        compiler_params=remote_params(cid),
        name='spread_%d_%d' % (rows_a, rows_b),
    )(send_a, send_b)[:2]


WAYS = 4


Path = collections.namedtuple('Path', ('recv', 'send', 'earlies', 'at', 'blocks', 'out_at', 'steps'))


def spot(n_y, n_x, p, d, w, s):
    most = max(n_y, n_x)
    return (((p * most + d) * 2 + w) * most + s) * 2


def list_at(n_y, n_x, sub, my, p, s, w, d, level):
    at, blocks, out_at, steps = (my[1], n_x, my[0], n_y) if p == 0 else (my[0], n_y, my[1], n_x)
    out = lax.rem(out_at + order_of(steps, w)[s], steps)
    return ((out * 3 + level) * blocks + lax.rem(at + blocks - d, blocks)) * sub


def plan_kernel(n_y, n_x, early, lev_a, lev_b, place, rows_at):
    chip = place[1]
    sub = lev_a.shape[0] // (3 * n_y * n_x)
    for p, levels in enumerate((lev_a, lev_b)):
        blocks, steps = ((n_x, n_y), (n_y, n_x))[p]
        for d in range(blocks):
            acc = jnp.int32(0)
            for w in BOTH:
                for s in range(steps):
                    lower, upper = (list_at(n_y, n_x, sub, (chip // n_x, chip % n_x), p, s, w, d, w + up) for up in BOTH)

                    def add(e, n):
                        return n + levels[upper + e] - levels[lower + e]

                    n = lax.fori_loop(0, sub, add, jnp.int32(0))
                    at = spot(n_y, n_x, p, d, w, s)
                    rows_at[at] = acc
                    rows_at[at + 1] = n
                    acc = acc + n
                if not w:
                    acc = jnp.maximum(acc, early)


def plan_rows(n_y, n_x, early, levels, place):
    most = max(n_y, n_x)
    return pl.pallas_call(
        functools.partial(plan_kernel, n_y, n_x, early),
        out_shape=jax.ShapeDtypeStruct((8 * most * most,), I32),
        in_specs=[SMEM] * 3,
        out_specs=SMEM,
        cost_estimate=COST,
        name='plan_rows',
    )(*levels, place)


def sum_kernel(n_y, n_x, passes, early, bounds, *refs):
    (lev_a, lev_b, rows_at, place, tok_hbm, wgt_hbm, recv_a, recv_b, send_a, send_b), refs = take(refs, 10)
    early_a, refs = take(refs, len(direct_of(n_x)))
    early_b, refs = take(refs, len(direct_of(n_y)))
    core, chip = place[0], place[1]
    my_y, my_x = chip // n_x, chip % n_x
    n_chip = n_y * n_x
    sub = lev_a.shape[0] // (3 * n_chip)
    words = sub * LANES
    per_dev = tok_hbm.shape[0] // (2 * n_chip)
    paths = (
        Path(recv_a, send_a, early_a, my_x, n_x, my_y, n_y),
        Path(recv_b, send_b, early_b, my_y, n_y, my_x, n_x),
    )
    todo = [(p, s) for p in BOTH for s in passes if s < paths[p].steps]
    outs, refs = take(refs, 2 * len(todo))
    (tok, wgt, *bufs), refs = take(refs, 4)
    accs, (tsem, rsem, zsem) = take(refs, 2 * WAYS)
    ways = [accs[:WAYS], accs[WAYS:]]
    table_of, size = {}, 0
    for p, s in todo:
        for w in BOTH:
            table_of[p, s, w] = size
            size += paths[p].blocks * words

    def dest(p, s, w):
        return lax.rem(paths[p].out_at + order_of(paths[p].steps, w)[s], paths[p].steps)

    def source(p, d):
        return lax.rem(paths[p].at + paths[p].blocks - d, paths[p].blocks)

    def tables(p, s, act):
        for w in BOTH:
            i = dest(p, s, w)
            g = (i * n_x + my_x) * 2 + core if p == 0 else (my_y * n_x + i) * 2 + core
            for d in range(paths[p].blocks):
                q = source(p, d)
                owner = my_y * n_x + q if p == 0 else q * n_x + my_x
                src = pl.ds(pl.multiple_of(g * per_dev + owner * words, words), words)
                dst = pl.ds(table_of[p, s, w] + d * words, words)
                act(pltpu.make_async_copy(tok_hbm.at[src], tok.at[dst], tsem.at[todo.index((p, s))]))
                act(pltpu.make_async_copy(wgt_hbm.at[src], wgt.at[dst], tsem.at[todo.index((p, s))]))

    jobs = [(p, s, d) for p, s in todo for d in range(paths[p].blocks)]

    def fetch(job, act):
        p, s, d = jobs[job]
        path = paths[p]
        slot = job % 2
        for w in BOTH:
            first, n = (rows_at[spot(n_y, n_x, p, d, w, s) + i] for i in BOTH)
            to = bufs[w].at[slot]
            main = path.recv if d else path.send
            n_early = 0
            if not w and d in direct_of(path.blocks):
                rows = path.earlies[direct_of(path.blocks).index(d)]
                n_early = jnp.clip(early - first, 0, n)

                @pl.when(n_early > 0)
                def _():
                    act(pltpu.make_async_copy(rows.at[pl.ds(first, n_early)], to.at[pl.ds(0, n_early)], rsem.at[slot]))

            @pl.when(n > n_early)
            def _():
                act(pltpu.make_async_copy(
                    main.at[d, pl.ds(first + n_early, n - n_early)], to.at[pl.ds(n_early, n - n_early)], rsem.at[slot]))

    def zero(acc):
        def body(b, c):
            acc[pl.ds(b * BLOCK, BLOCK)] = jnp.zeros((BLOCK, *acc.shape[1:]), F32)
            return c
        lax.fori_loop(0, (acc.shape[0] - 8) // BLOCK, body, 0)

    fetch(0, start)
    for p, s in todo:
        tables(p, s, start)
    puts = []
    for job, (p, s, d) in enumerate(jobs):
        slot = job % 2
        levels = (lev_a, lev_b)[p]
        dummy = accs[0].shape[0] - 8
        if not d:
            for _, *others in ways:
                for acc in others:
                    zero(acc)
            for put in puts:
                put.wait()
            for target, *_ in ways:
                zero(target)
            tables(p, s, wait)
        fetch(job, wait)
        if job + 1 < len(jobs):
            fetch(job + 1, start)

        def one_expert(e, bases):
            counts, firsts = [], []
            for w in BOTH:
                lower, upper = (levels[list_at(n_y, n_x, sub, (my_y, my_x), p, s, w, d, w + up) + e] for up in BOTH)
                counts.append(upper - lower)
                firsts.append(table_of[p, s, w] + d * words + e * LANES + lower)
            longest = jnp.maximum(counts[0], counts[1])

            def group(b, cc):
                adds = []
                for w in BOTH:
                    for q in range(WAYS):
                        r = b * WAYS + q
                        row = bufs[w][slot, bases[w] + r].astype(F32)
                        t = jnp.where(r < counts[w], tok[firsts[w] + r], dummy)
                        adds.append((ways[w][q], t, wgt[firsts[w] + r] * row))
                for acc, t, row in adds:
                    acc[t] = acc[t] + row
                return cc

            lax.fori_loop(0, lax.shift_right_logical(longest + (WAYS - 1), 2), group, 0)
            return bases[0] + counts[0], bases[1] + counts[1]

        lax.fori_loop(0, sub, one_expert, (jnp.int32(0), jnp.int32(0)))
        if d + 1 == paths[p].blocks:
            puts = []
            for w in BOTH:
                target, second, third, fourth = ways[w]
                size = tokens_of(bounds, p, w)

                def merge(b, c):
                    rows = pl.ds(b * BLOCK, BLOCK)
                    target[rows] = (target[rows] + second[rows]) + (third[rows] + fourth[rows])
                    return c

                lax.fori_loop(0, size // BLOCK, merge, 0)
                out = outs[2 * todo.index((p, s)) + w]
                puts.append(pltpu.make_async_copy(target.at[pl.ds(0, size)], out, zsem.at[w]))
                puts[-1].start()
    for put in puts:
        put.wait()


def weighted_sums(n_y, n_x, passes, early, bounds, levels, rows_at, place, tok, wgt, recvs, sends, earlies):
    sublanes = recvs[0].shape[2]
    sub = levels[0].shape[0] // (3 * n_y * n_x)
    todo = [(p, s) for p, n in enumerate((n_y, n_x)) for s in passes if s < n]
    sizes = [tokens_of(bounds, p, w) for p, _ in todo for w in BOTH]
    table = sum((n_x if p == 0 else n_y) * 2 * sub * LANES for p, _ in todo) + 2 * LANES
    tokens = max(b - a for a, b in zip(bounds[:-1], bounds[1:]))
    ops = (*levels, rows_at, place, tok, wgt, *recvs, *sends, *earlies)
    return pl.pallas_call(
        functools.partial(sum_kernel, n_y, n_x, passes, early, bounds),
        out_shape=tuple(jax.ShapeDtypeStruct((n, sublanes, LANES), F32) for n in sizes),
        in_specs=[SMEM] * 4 + [HBM] * (len(ops) - 4),
        out_specs=(HBM,) * len(sizes),
        scratch_shapes=[
            pltpu.SMEM((table,), I32),
            pltpu.SMEM((table,), F32),
            *[pltpu.VMEM((2, sub * LANES + LANES, sublanes, LANES), BF16) for _ in BOTH],
            *[pltpu.VMEM((tokens + 8, sublanes, LANES), F32) for _ in range(2 * WAYS)],
            pltpu.SemaphoreType.DMA((len(todo),)),
            PAIR, PAIR,
        ],
        compiler_params=LOCAL,
        cost_estimate=COST,
        name='weighted_sums',
    )(*ops)


SUM_CHUNKS = 8


def pieces_of(n):
    cuts = [BLOCK * ((n // BLOCK * j) // SUM_CHUNKS) for j in range(SUM_CHUNKS + 1)]
    return [(a, b - a) for a, b in zip(cuts[:-1], cuts[1:]) if b > a]


def reduce_kernel(n_y, n_x, bounds, *refs):
    sizes = (n_y, n_x)
    lanes = [(p, w) for p in BOTH for w in BOTH]
    got, refs = take(refs, len(lanes))
    got = dict(zip(lanes, got))
    sums = {}
    for p, n in enumerate(sizes):
        for s in range(1, n):
            for w in BOTH:
                (sums[p, s, w],), refs = take(refs, 1)
    (x_ref, y_ref), refs = take(refs, 2)
    part, own = {}, {}
    for p, w in lanes:
        for s in range(sizes[p] - 1):
            (part[p, w, s], own[p, w, s]), refs = take(refs, 2)
    zsem, gsem, rsem = refs
    rings = (Ring('y', n_y, n_x), Ring('x', n_y, n_x))
    d_model = x_ref.shape[1]
    pieces = {(p, w): pieces_of(tokens_of(bounds, p, w)) for p, w in lanes}
    order = [(p, w, j) for j in range(SUM_CHUNKS) for p, w in lanes if j < len(pieces[p, w])]

    barrier = pltpu.get_barrier_semaphore()
    for ring in rings:
        for d in (1, -1):
            pl.semaphore_signal(barrier, inc=1, device_id=ring.device(d), device_id_type=pl.DeviceIdType.MESH)
    pl.semaphore_wait(barrier, 4)

    def rows_of(p, w, j):
        return pl.ds(*pieces[p, w][j])

    def load(p, w, s, j):
        r = rows_of(p, w, j)
        return pltpu.make_async_copy(sums[p, s, w].at[r], own[p, w, s - 1].at[r], zsem.at[p, w, s - 1, j])

    def begin(p, w, j):
        r = rows_of(p, w, j)
        return pltpu.make_async_copy(got[p, w].at[r], part[p, w, 0].at[r], gsem.at[p, w, j])

    def hop(p, w, s, j):
        r = rows_of(p, w, j)
        return pltpu.make_async_remote_copy(
            src_ref=part[p, w, s - 1].at[r], dst_ref=part[p, w, s].at[r],
            send_sem=rsem.at[0, p, w, s, j], recv_sem=rsem.at[1, p, w, s, j],
            device_id=rings[p].device(1 if w == 0 else -1), device_id_type=pl.DeviceIdType.MESH)

    def arrive(p, w, s, j):
        if s == 0:
            begin(p, w, j).wait()
        else:
            hop(p, w, s, j).wait_recv()

    last = max(sizes) - 1
    for s in range(1, last + 1):
        for p, w, j in order:
            if s == 1:
                begin(p, w, j).start()
            if s < sizes[p]:
                load(p, w, s, j).start()

    for s in range(1, last):
        for p, w, j in order:
            if s >= sizes[p] - 1:
                continue
            load(p, w, s, j).wait()
            arrive(p, w, s - 1, j)
            into, more = part[p, w, s - 1], own[p, w, s - 1]
            first, n = pieces[p, w][j]

            def add(b, c):
                r = pl.ds(first + b * BLOCK, BLOCK)
                into[r] = into[r] + more[r]
                return c

            lax.fori_loop(0, n // BLOCK, add, 0)
            hop(p, w, s, j).start()

    for p, w, j in order:
        s = sizes[p] - 1
        load(p, w, s, j).wait()
        arrive(p, w, s - 1, j)
        into, more = part[p, w, s - 1], own[p, w, s - 1]
        first, n = pieces[p, w][j]
        token = bounds[2 * p + w] + first

        def finish(b, c):
            r = pl.ds(first + b * BLOCK, BLOCK)
            out = pl.ds(pl.multiple_of(token + b * BLOCK, BLOCK), BLOCK)
            total = into[r] + more[r]
            y_ref[out, :] = (x_ref[out, :].astype(F32) + total.reshape(BLOCK, d_model)).astype(BF16)
            return c

        lax.fori_loop(0, n // BLOCK, finish, 0)
    for s in range(1, last):
        for p, w, j in order:
            if s < sizes[p] - 1:
                hop(p, w, s, j).wait_send()


def reduce_back(cid, n_y, n_x, bounds, got, sums, x):
    n_tok, d_model = x.shape
    sublanes = d_model // LANES
    bufs = []
    for p, n in enumerate((n_y, n_x)):
        for w in BOTH:
            size = tokens_of(bounds, p, w)
            bufs += [pltpu.VMEM((size, sublanes, LANES), F32)] * (2 * (n - 1))
    steps = max(n_y, n_x) - 1
    ops = (*got, *sums, x)
    return pl.pallas_call(
        functools.partial(reduce_kernel, n_y, n_x, bounds),
        out_shape=jax.ShapeDtypeStruct((n_tok, d_model), BF16),
        in_specs=[HBM] * (len(ops) - 1) + [VMEM],
        out_specs=VMEM,
        scratch_shapes=[
            *bufs,
            pltpu.SemaphoreType.DMA((2, 2, steps, SUM_CHUNKS)),
            pltpu.SemaphoreType.DMA((2, 2, SUM_CHUNKS)),
            pltpu.SemaphoreType.DMA((2, 2, 2, steps, SUM_CHUNKS)),
        ],
        compiler_params=remote_params(cid),
        name='reduce_back',
    )(*ops)


def solution(mesh):
    dev_axes = ('ep2', 'ep')
    n_y, n_ep = mesh.shape['ep2'], mesh.shape['ep']
    n_x = n_ep // 2
    group = n_y * n_ep
    n_chip = n_y * n_x

    def local_step(x_loc, ids_loc, gate_loc, w_a, w_b):
        n_tok, d_model = x_loc.shape
        n_top = ids_loc.shape[1]
        e_loc = w_a.shape[0]
        sub = 2 * e_loc
        experts = e_loc * group
        cap = capacity_of(group, n_tok, n_top, experts)
        sublanes = d_model // LANES
        base_a, base_b = n_y * sub * LANES, n_x * sub * LANES
        early = min(base_a, base_b) // 8
        slots_a, slots_b = base_a + early, base_b + early
        bounds = bounds_of(n_tok)
        n_seg, n_chunk = len(bounds) - 1, len(CHUNKS) - 1
        me = lax.axis_index(dev_axes)
        core, chip = me % 2, me // 2
        place = jnp.stack([core, chip]).astype(I32)

        x3 = x_loc.reshape(n_tok, sublanes, LANES)
        chunks = [lax.all_gather(x3[bounds[CHUNKS[k]]:bounds[CHUNKS[k + 1]]], dev_axes, tiled=True) for k in range(n_chunk)]
        swap = [(i, i ^ 1) for i in range(n_ep)]
        w_a_sib = lax.ppermute(w_a, 'ep', swap)
        w_b_sib = lax.ppermute(w_b, 'ep', swap)

        toks, wgts, cnts = route(ids_loc, gate_loc, bounds)
        for_chip = toks[:experts].reshape(n_chip, 1, sub, LANES)
        table = jnp.concatenate([
            jnp.broadcast_to(for_chip, (n_chip, 2, sub, LANES)).reshape(group, sub, LANES),
            jnp.broadcast_to(cnts[None], (group, PREFIX_ROWS, LANES))], axis=1)
        table = lax.all_to_all(table, dev_axes, 0, 0, tiled=True)
        lists = build_lists(place, table.reshape(-1), cap, slots_a, slots_b, early, bounds, n_y, n_x, sub)

        prefix = table[:, sub:sub + n_seg + 1, :experts]
        totals = prefix[:, n_seg]
        offs = jnp.cumsum(totals, axis=0) - totals
        kept = jnp.clip(cap - offs, 0, totals)
        upto = jnp.minimum(prefix, kept[:, None])
        y, x = chip // n_x, chip % n_x
        level_a = lax.dynamic_slice(upto.reshape(n_y, n_ep, n_seg + 1, experts), (0, x * 2 + core, 0, y * n_x * sub), (n_y, 1, 3, n_x * sub))
        level_b = lax.dynamic_slice(upto.reshape(n_y, n_x, 2, n_seg + 1, experts), (y, 0, core, 2, 0), (1, n_x, 1, 3, experts))
        level_b = lax.dynamic_slice(level_b.reshape(n_x, 3, n_y, n_x * sub), (0, 0, 0, x * sub), (n_x, 3, n_y, sub))
        levels = (level_a.reshape(-1), level_b.reshape(-1))
        of_chip = (jnp.arange(experts)[:, None] // sub == jnp.arange(n_chip)[None, :]).astype(F32)
        per_chip = jnp.dot(upto.reshape(-1, experts).astype(F32), of_chip).reshape(group, n_seg + 1, n_chip)
        rows = (per_chip[:, 1:] - per_chip[:, :-1]).astype(I32)
        rows_a = jnp.sum(rows.reshape(n_y, n_ep, n_seg, n_chip), axis=0)
        rows_b = jnp.sum(rows.reshape(n_y, n_x, 2, n_seg, n_chip), axis=1)
        need_a = jnp.max(jnp.maximum(rows_a[:, 0], early) + rows_a[:, 1])
        need_b = jnp.max(jnp.maximum(rows_b[:, :, 2], early) + rows_b[:, :, 3])
        tiers = [(base_a * q // 256, base_b * q // 256) for q in SIZES] + [(slots_a, slots_b)]
        limits = jnp.array(tiers[:-1], I32)
        index = jnp.sum(jnp.logical_or(need_a > limits[:, 0], need_b > limits[:, 1]).astype(I32))
        within = toks[:experts]
        for lo, hi in zip(bounds[1:-1], bounds[:-2]):
            within = jnp.where(toks[:experts] >= lo, within - (lo - hi), within)
        rows_at = plan_rows(n_y, n_x, early, levels, place)
        lists, levels, rows_at, index, within = lax.optimization_barrier((lists, levels, rows_at, index, within))

        def up_x(v, d):
            return lax.ppermute(v, 'ep', [(i, (i + 2 * d) % n_ep) for i in range(n_ep)])

        def up_y(v, d):
            return lax.ppermute(v, 'ep2', [(i, (i + d) % n_y) for i in range(n_y)])

        weights = (w_a, w_a_sib, w_b, w_b_sib)
        direct_x, direct_y = direct_of(n_x), direct_of(n_y)
        n_early = (len(direct_x), len(direct_y))
        first = run_experts(0, early, n_early, lists, place, chunks[0], *weights, (n_x * slots_a, n_y * slots_b))
        first, within, wgts = lax.optimization_barrier((first, within, wgts))
        send_a, early_a = first[0], first[1:1 + n_early[0]]
        send_b, early_b = first[1 + n_early[0]], first[2 + n_early[0]:]
        earlies = [up_x(v, d) for v, d in zip(early_a, direct_x)] + [up_y(v, d) for v, d in zip(early_b, direct_y)]
        send_b, = run_experts(1, early, n_early, lists, place, chunks[1], *weights, send_b)
        tok_all = lax.all_gather(within.reshape(-1), dev_axes, tiled=True)
        wgt_all = lax.all_gather(wgts[:experts].reshape(-1), dev_axes, tiled=True)
        sends = (send_a.reshape(n_x, slots_a, sublanes, LANES), send_b.reshape(n_y, slots_b, sublanes, LANES))

        recvs = lax.switch(index, [functools.partial(spread, a, b, early, i, n_y, n_x) for i, (a, b) in enumerate(tiers)], *sends)
        recvs, tok_all, wgt_all = lax.optimization_barrier((recvs, tok_all, wgt_all))
        common = (early, bounds, levels, rows_at, place, tok_all, wgt_all, recvs, sends, earlies)
        head = weighted_sums(n_y, n_x, (0,), *common)
        got = (up_y(head[0], 1), up_y(head[1], -1), up_x(head[2], 1), up_x(head[3], -1))
        rest = weighted_sums(n_y, n_x, tuple(range(1, max(n_y, n_x))), *common)
        return reduce_back(len(tiers), n_y, n_x, bounds, got, rest, x_loc)

    tok_spec = P(('dp', 'ep2', 'ep'), None)
    w_spec = P(dev_axes, None, None)
    return jax.shard_map(local_step, mesh=mesh, in_specs=(tok_spec, tok_spec, tok_spec, w_spec, w_spec), out_specs=tok_spec, check_vma=False)
```

```python
import collections
import functools
import math

import jax
import jax.numpy as jnp
from jax import lax
from jax.experimental import pallas as pl
from jax.experimental.pallas import tpu as pltpu
from jax.sharding import PartitionSpec as P

LANES = 128
SEGMENTS = (0, 17, 34, 49, 64)
CHUNKS = (0, 3, 4)
SIZES = (80, 82, 84, 86, 88, 90, 92, 94, 97, 102)
TILE = 256
PREFIX_ROWS = 8
BF16 = jnp.bfloat16
F32 = jnp.float32
I32 = jnp.int32
HBM = pl.BlockSpec(memory_space=pl.ANY)
SMEM = pl.BlockSpec(memory_space=pltpu.SMEM)
VMEM = pl.BlockSpec(memory_space=pltpu.VMEM)
BOTH = range(2)
UNROLL = 8
BLOCK = 16
PAIR = pltpu.SemaphoreType.DMA((2,))
COST = pl.CostEstimate(flops=2 * 10 ** 10, bytes_accessed=10 ** 7, transcendentals=0)
VMEM_LIMIT = 64_000_000
LOCAL = pltpu.CompilerParams(vmem_limit_bytes=VMEM_LIMIT)
MIXED = pltpu.CompilerParams(vmem_limit_bytes=VMEM_LIMIT)


def remote_params(cid):
    return pltpu.CompilerParams(collective_id=cid, has_side_effects=True, vmem_limit_bytes=VMEM_LIMIT)


def take(refs, n):
    return refs[:n], refs[n:]


def start(copy):
    copy.start()


def wait(copy):
    copy.wait()


def capacity_of(group_size, n_tok, n_top, experts):
    return 8 * ((5 * group_size * n_tok * n_top) // (32 * experts))


def far_of(n):
    return n // 2 if n % 2 == 0 and n >= 4 else 0


def direct_of(n):
    return [d for d in range(1, n) if d != far_of(n)]


def bounds_of(n_tok):
    return tuple(16 * ((n_tok * q + 512) // 1024) for q in SEGMENTS)


def tokens_of(bounds, path, w):
    lo, hi = bounds[2 * path + w:][:2]
    return hi - lo


def order_of(n, w):
    return [n - 1 - s if w == 0 else (1 + s) % n for s in range(n)]


def route_kernel(bounds, ids_ref, gate_ref, tok_ref, wgt_ref, cnt_ref, code_t, gate_t, tok_acc, wgt_acc):
    n_tok, n_top = ids_ref.shape
    lane = lax.broadcasted_iota(I32, (n_tok, LANES), 1)
    member = jnp.zeros((n_tok, LANES), F32)
    gates = jnp.zeros((n_tok, LANES), F32)
    for j in range(n_top):
        hit = ids_ref[:, j:j + 1] == lane
        member = member + jnp.where(hit, 1.0, 0.0)
        gates = gates + jnp.where(hit, gate_ref[:, j:j + 1], 0.0)
    member_b = member.astype(BF16)
    row_block = min(n_tok, 128)
    for i in range(n_tok // row_block):
        rows = pl.ds(i * row_block, row_block)
        later = lax.broadcasted_iota(I32, (row_block, n_tok), 0) + i * row_block
        earlier = lax.broadcasted_iota(I32, (row_block, n_tok), 1)
        tri = jnp.where(earlier < later, 1.0, 0.0).astype(BF16)
        rank = jnp.dot(tri, member_b, preferred_element_type=F32)
        mem = member[i * row_block:(i + 1) * row_block]
        code_t[:, rows] = jnp.where(mem > 0.5, rank, -1.0).T
        gate_t[:, rows] = gates[i * row_block:(i + 1) * row_block].T
    total = jnp.zeros((1, LANES), F32)
    rows_out = [total]
    for lo, hi in zip(bounds[:-1], bounds[1:]):
        total = total + jnp.sum(member[lo:hi], axis=0, keepdims=True)
        rows_out.append(total)
    while len(rows_out) < PREFIX_ROWS:
        rows_out.append(total)
    cnt_ref[...] = jnp.concatenate(rows_out, axis=0).astype(I32)
    tok_acc[...] = jnp.zeros_like(tok_acc)
    wgt_acc[...] = jnp.zeros_like(wgt_acc)
    slot = lax.broadcasted_iota(I32, (LANES, n_tok), 0).astype(F32)
    token = lax.broadcasted_iota(I32, (1, n_tok), 1).astype(F32)
    out_lane = lax.broadcasted_iota(I32, (LANES, LANES), 1)

    def one_expert(e, carry):
        hit = slot == code_t[pl.ds(e, 1), :]
        tok = jnp.sum(jnp.where(hit, token, 0.0), axis=1, keepdims=True)
        wgt = jnp.sum(jnp.where(hit, gate_t[pl.ds(e, 1), :], 0.0), axis=1, keepdims=True)
        tok_acc[...] = jnp.where(out_lane == e, tok, tok_acc[...])
        wgt_acc[...] = jnp.where(out_lane == e, wgt, wgt_acc[...])
        return carry

    lax.fori_loop(0, LANES, one_expert, 0)
    tok_ref[...] = tok_acc[...].T.astype(I32)
    wgt_ref[...] = wgt_acc[...].T


def route(ids, gate, bounds):
    n_tok = ids.shape[0]
    return pl.pallas_call(
        functools.partial(route_kernel, bounds),
        out_shape=(
            jax.ShapeDtypeStruct((LANES, LANES), I32),
            jax.ShapeDtypeStruct((LANES, LANES), F32),
            jax.ShapeDtypeStruct((PREFIX_ROWS, LANES), I32),
        ),
        in_specs=[VMEM, VMEM],
        out_specs=(VMEM, VMEM, VMEM),
        scratch_shapes=[
            pltpu.VMEM((LANES, n_tok), F32),
            pltpu.VMEM((LANES, n_tok), F32),
            pltpu.VMEM((LANES, LANES), F32),
            pltpu.VMEM((LANES, LANES), F32),
        ],
        cost_estimate=COST,
        name='route',
    )(ids, gate)


def list_kernel(cap, slots_a, slots_b, early, bounds, n_y, n_x, sub, place_ref, info_ref,
                src_ref, start_ref, len_ref, dst_ref, lim_ref, dir_ref, span_ref, kept_ref, base_ref, lim_tab, dir_tab):
    core, chip = place_ref[0], place_ref[1]
    n_dst = n_y * n_x
    n_seg, n_chunk = len(bounds) - 1, len(CHUNKS) - 1
    dev_words = (sub + PREFIX_ROWS) * LANES
    width = src_ref.shape[0] // sub
    my_y, my_x = chip // n_x, chip % n_x

    def count(g, k, e):
        return info_ref[g * dev_words + (sub + k) * LANES + chip * sub + e]

    def per_expert(e, carry):
        def per_dev(i, off):
            for c in BOTH:
                n = count(2 * i + c, n_seg, e)
                kept = jnp.clip(cap - off, 0, n)
                off = off + n

                @pl.when(core == c)
                def _():
                    kept_ref[i * sub + e] = kept
            return off
        lax.fori_loop(0, n_dst, per_dev, 0)
        return carry

    lax.fori_loop(0, sub, per_expert, 0)

    def rows_in(k, i, e):
        g, kept = 2 * i + core, kept_ref[i * sub + e]
        return jnp.minimum(count(g, k + 1, e), kept) - jnp.minimum(count(g, k, e), kept)

    def block_bases(path, n_blocks, n_inner, slots, index):
        for d in range(n_blocks):
            acc = jnp.int32(d * slots)
            for w in BOTH:
                for r in order_of(n_inner, w):
                    i = index(d, r)

                    def add(e, acc):
                        base_ref[((2 * path + w) * n_dst + i) * sub + e] = acc
                        return acc + rows_in(2 * path + w, i, e)

                    acc = lax.fori_loop(0, sub, add, acc)
                    direct = direct_of(n_blocks)
                    lim_tab[path * n_dst + i] = d * slots + early if d in direct else 0
                    dir_tab[path * n_dst + i] = direct.index(d) if d in direct else 0
                if w == 0:
                    acc = jnp.maximum(acc, d * slots + early)

    block_bases(0, n_x, n_y, slots_a, lambda d, r: lax.rem(my_y + r, n_y) * n_x + lax.rem(my_x + d, n_x))
    block_bases(1, n_y, n_x, slots_b, lambda d, r: lax.rem(my_y + d, n_y) * n_x + lax.rem(my_x + r, n_x))

    def expert_lists(e, carry):
        pos = e * width
        for chunk, (chunk_lo, chunk_hi) in enumerate(zip(CHUNKS[:-1], CHUNKS[1:])):
            size = bounds[chunk_hi] - bounds[chunk_lo]
            start_at = pos
            for k in range(chunk_lo, chunk_hi):

                def segment(i, o):
                    g = 2 * i + core
                    kept = kept_ref[i * sub + e]
                    s0 = jnp.minimum(count(g, k, e), kept)
                    n = jnp.minimum(count(g, k + 1, e), kept) - s0
                    j = (e * n_seg + k) * n_dst + i
                    start_ref[j] = o
                    len_ref[j] = n
                    dst_ref[j] = base_ref[(k * n_dst + i) * sub + e]
                    lim_ref[j] = lim_tab[(k // 2) * n_dst + i]
                    dir_ref[j] = dir_tab[(k // 2) * n_dst + i]
                    src0 = g * size - bounds[chunk_lo]
                    tok0 = g * dev_words + e * LANES + s0

                    def block(b, c):
                        vals = [info_ref[tok0 + b * UNROLL + q] for q in range(UNROLL)]
                        for q in range(UNROLL):
                            src_ref[o + b * UNROLL + q] = src0 + vals[q]
                        return c

                    lax.fori_loop(0, pl.cdiv(n, UNROLL), block, 0)
                    return o + n

                pos = lax.fori_loop(0, n_dst, segment, pos)
            span_ref[(e * n_chunk + chunk) * 2] = start_at
            span_ref[(e * n_chunk + chunk) * 2 + 1] = pos - start_at

            def pad(b, c):
                for q in range(UNROLL):
                    src_ref[pos + b * UNROLL + q] = b * UNROLL + q
                return c

            lax.fori_loop(0, TILE // UNROLL, pad, 0)
            pos = pos + TILE
        return carry

    lax.fori_loop(0, sub, expert_lists, 0)


def build_lists(place, info, cap, slots_a, slots_b, early, bounds, n_y, n_x, sub):
    n_dst, n_seg = n_y * n_x, len(bounds) - 1
    n_chunk = len(CHUNKS) - 1
    width = LANES * n_dst + n_chunk * TILE + UNROLL
    segs = sub * n_seg * n_dst + UNROLL
    return pl.pallas_call(
        functools.partial(list_kernel, cap, slots_a, slots_b, early, bounds, n_y, n_x, sub),
        out_shape=(
            jax.ShapeDtypeStruct((sub * width,), I32),
            *[jax.ShapeDtypeStruct((segs,), I32) for _ in range(5)],
            jax.ShapeDtypeStruct((sub * n_chunk * 2,), I32),
        ),
        in_specs=[SMEM, SMEM],
        out_specs=(SMEM,) * 7,
        scratch_shapes=[
            pltpu.SMEM((n_dst * sub,), I32),
            pltpu.SMEM((n_seg * n_dst * sub,), I32),
            pltpu.SMEM((2 * n_dst,), I32),
            pltpu.SMEM((2 * n_dst,), I32),
        ],
        cost_estimate=COST,
        name='row_lists',
    )(place, info)


def gelu(v):
    return 0.5 * v * (1.0 + jnp.tanh(math.sqrt(2.0 / math.pi) * (v + 0.044715 * v * v * v)))


def expert_kernel(chunk, n_seg, early, n_early, *refs):
    lo_seg, hi_seg = CHUNKS[chunk:][:2]
    (src, seg_start, seg_len, seg_dst, seg_lim, seg_dir, span, place, x_hbm, wa_own, wa_sib, wb_own, wb_sib), refs = take(refs, 13)
    if lo_seg > 0:
        refs = refs[1:]
    paths, at = [], 0
    for path in BOTH:
        first, last = max(lo_seg, 2 * path), min(hi_seg, 2 * path + 2)
        if first < last:
            n = n_early[path] if lo_seg == 0 else 0
            paths.append((first, last, refs[at], refs[at + 1:at + 1 + n]))
            at += 1 + n
    xbuf, xrows, obuf, wa, wb, t_e, t_base, t_cnt, ptr, gsem, ssem, wsem = refs[at:]
    e_loc, d_model, _ = wa_own.shape
    sub = 2 * e_loc
    core = place[0]
    sublanes = d_model // LANES
    n_dst = (seg_start.shape[0] - UNROLL) // (sub * n_seg)

    def span_of(e):
        at = (e * (len(CHUNKS) - 1) + chunk) * 2
        return span[at], span[at + 1]

    def weight_copies(e, act):
        slot = e % 2
        q = e % e_loc

        @pl.when(e // e_loc == core)
        def _():
            act(pltpu.make_async_copy(wa_own.at[q], wa.at[slot], wsem.at[slot, 0]))
            act(pltpu.make_async_copy(wb_own.at[q], wb.at[slot], wsem.at[slot, 1]))

        @pl.when(e // e_loc != core)
        def _():
            act(pltpu.make_async_copy(wa_sib.at[q], wa.at[slot], wsem.at[slot, 0]))
            act(pltpu.make_async_copy(wb_sib.at[q], wb.at[slot], wsem.at[slot, 1]))

    weight_copies(0, start)

    def plan(e, t):
        lo, n = span_of(e)

        def put(i, c):
            t_e[t + i] = e
            t_base[t + i] = lo + i * TILE
            t_cnt[t + i] = jnp.minimum(n - i * TILE, TILE)
            return c

        n_tiles = (n + TILE - 1) // TILE
        lax.fori_loop(0, n_tiles, put, 0)
        return t + n_tiles

    n_all = lax.fori_loop(0, sub, plan, 0)
    for t in BOTH:
        t_base[n_all + t], _ = span_of(0)

    def fetch_row(t, r):
        slot = t % 2
        pltpu.make_async_copy(x_hbm.at[src[t_base[t] + r]], xbuf.at[slot, r], gsem.at[slot]).start()

    def gather_wait(t):
        slot = t % 2
        pltpu.make_async_copy(x_hbm.at[pl.ds(0, TILE)], xbuf.at[slot], gsem.at[slot]).wait()

    def scatter_start(t):
        base, slot = t_base[t], t % 2
        end = base + t_cnt[t]

        for path, (_, last, send, earlies) in enumerate(paths):
            j_end = (t_e[t] * n_seg + last) * n_dst

            def more(j):
                return jnp.logical_and(j < j_end, seg_start[j] < end)

            def segment(j):
                first_row = seg_start[j]
                lo = jnp.maximum(first_row, base)
                n = jnp.minimum(first_row + seg_len[j], end) - lo
                to = seg_dst[j] + lo - first_row
                n_early = jnp.clip(seg_lim[j] - to, 0, jnp.maximum(n, 0)) if earlies else 0

                def put_early(q, rows):
                    @pl.when(seg_dir[j] == q)
                    def _():
                        pltpu.make_async_copy(
                            obuf.at[slot, pl.ds(lo - base, n_early)],
                            rows.at[pl.ds(to - seg_lim[j] + early, n_early)],
                            ssem.at[slot],
                        ).start()

                if earlies:
                    @pl.when(n_early > 0)
                    def _():
                        for q, rows in enumerate(earlies):
                            put_early(q, rows)

                @pl.when(n > n_early)
                def _():
                    pltpu.make_async_copy(
                        obuf.at[slot, pl.ds(lo - base + n_early, n - n_early)],
                        send.at[pl.ds(to + n_early, n - n_early)],
                        ssem.at[slot],
                    ).start()
                return j + 1

            start = ptr[path]
            ptr[path] = jnp.maximum(lax.while_loop(more, segment, start) - 1, start)

    def scatter_wait(t):
        n, slot = t_cnt[t], t % 2
        send = paths[0][2]
        pltpu.make_async_copy(obuf.at[slot, pl.ds(0, n)], send.at[pl.ds(0, n)], ssem.at[slot]).wait()

    def prime(r, c):
        for t in BOTH:
            fetch_row(t, r)
        return c

    lax.fori_loop(0, TILE, prime, 0, unroll=UNROLL)

    def one_expert(e, t_first):
        weight_copies(e, wait)

        @pl.when(e + 1 < sub)
        def _():
            weight_copies(e + 1, start)

        ws = e % 2
        _, n = span_of(e)
        for path, (first, _, _, _) in enumerate(paths):
            ptr[path] = (e * n_seg + first) * n_dst

        def one_tile(i, t):
            slot = t % 2
            gather_wait(t)

            @pl.when(t >= 2)
            def _():
                scatter_wait(t - 2)

            xrows[...] = xbuf[slot].reshape(TILE, d_model)
            for r in range(TILE):
                fetch_row(t + 2, r)
            hidden = gelu(jnp.dot(xrows[...], wa[ws], preferred_element_type=F32)).astype(BF16)
            out = jnp.dot(hidden, wb[ws], preferred_element_type=F32).astype(BF16)
            obuf[slot] = out.reshape(TILE, sublanes, LANES)
            scatter_start(t)
            return t + 1

        return lax.fori_loop(0, (n + TILE - 1) // TILE, one_tile, t_first)

    lax.fori_loop(0, sub, one_expert, 0)
    for back in (2, 1):
        gather_wait(n_all + back)

        @pl.when(n_all >= back)
        def _():
            scatter_wait(n_all - back)


def run_experts(chunk, early, n_early, lists, place, x_rows, wa, wa_sib, wb, wb_sib, rows):
    e_loc, d_model, ff = wa.shape
    sub = 2 * e_loc
    sublanes = d_model // LANES
    ops = (*lists, place, x_rows, wa, wa_sib, wb, wb_sib) + (() if chunk == 0 else (rows,))
    n_smem = len(lists) + 1
    max_tiles = sub * (pl.cdiv(lists[0].shape[0] // sub, TILE) + 1) + 2
    if chunk == 0:
        sizes = [rows[0]] + [early] * n_early[0] + [rows[1]] + [early] * n_early[1]
    else:
        sizes = [rows.shape[0]]
    return pl.pallas_call(
        functools.partial(expert_kernel, chunk, len(SEGMENTS) - 1, early, n_early),
        out_shape=tuple(jax.ShapeDtypeStruct((n, sublanes, LANES), BF16) for n in sizes),
        in_specs=[SMEM] * n_smem + [HBM] * (len(ops) - n_smem),
        out_specs=(HBM,) * len(sizes),
        scratch_shapes=[
            pltpu.VMEM((2, TILE, sublanes, LANES), BF16),
            pltpu.VMEM((TILE, d_model), BF16),
            pltpu.VMEM((2, TILE, sublanes, LANES), BF16),
            pltpu.VMEM((2, d_model, ff), BF16),
            pltpu.VMEM((2, ff, d_model), BF16),
            pltpu.SMEM((max_tiles,), I32),
            pltpu.SMEM((max_tiles,), I32),
            pltpu.SMEM((max_tiles,), I32),
            pltpu.SMEM((2,), I32),
            PAIR, PAIR,
            pltpu.SemaphoreType.DMA((2, 2)),
        ],
        input_output_aliases={} if chunk == 0 else {len(ops) - 1: 0},
        compiler_params=MIXED,
        cost_estimate=COST,
        name='experts',
    )(*ops)


PIECES = 4


class Ring:
    def __init__(self, axis, n_y, n_x):
        y, ec = lax.axis_index('ep2'), lax.axis_index('ep')
        self.axis, self.core = axis, ec % 2
        self.n = n_x if axis == 'x' else n_y
        self.pos = ec // 2 if axis == 'x' else y
        self.direct, self.far = direct_of(self.n), far_of(self.n)

    def place(self, d):
        return lax.rem(self.pos + d + self.n, self.n)

    def device(self, d):
        if self.axis == 'x':
            return {'ep': self.place(d) * 2 + self.core}
        return {'ep2': self.place(d)}

    def remote(self, src, dst, sems, i, d):
        return pltpu.make_async_remote_copy(
            src_ref=src, dst_ref=dst, send_sem=sems.at[0, i], recv_sem=sems.at[1, i],
            device_id=self.device(d), device_id_type=pl.DeviceIdType.MESH)

    def signal(self, barrier):
        for d in range(1, self.n):
            pl.semaphore_signal(barrier, inc=1, device_id=self.device(d), device_id_type=pl.DeviceIdType.MESH)


def spread_kernel(rows_a, rows_b, early, n_y, n_x, send_a, send_b, recv_a, recv_b, stage_a, stage_b, sem_a, sem_b):
    rings = (Ring('x', n_y, n_x), Ring('y', n_y, n_x))
    barrier = pltpu.get_barrier_semaphore()
    for ring in rings:
        ring.signal(barrier)
    pl.semaphore_wait(barrier, n_x + n_y - 2)

    sides = list(zip(rings, (rows_a, rows_b), (send_a, send_b), (recv_a, recv_b), (stage_a, stage_b), (sem_a, sem_b)))

    def lead(side, p):
        ring, rows, send, _, stage, sem = side
        hop = ring.far // 2 if p % 2 == 0 else -(ring.far // 2)
        part = pl.ds(p * (rows // PIECES), rows // PIECES)
        return ring.remote(send.at[ring.far, part], stage.at[part], sem, p, hop)

    def follow(side, p):
        ring, rows, _, recv, stage, sem = side
        hop = ring.far // 2 if p % 2 == 0 else -(ring.far // 2)
        part = pl.ds(p * (rows // PIECES), rows // PIECES)
        return ring.remote(stage.at[part], recv.at[ring.far, part], sem, PIECES + p, hop)

    def straight(side, i):
        ring, rows, send, recv, _, sem = side
        d = ring.direct[i]
        part = pl.ds(early, rows - early)
        return ring.remote(send.at[d, part], recv.at[d, part], sem, 2 * PIECES + i, d)

    relayed = [(side, p) for p in range(PIECES) for side in sides if side[0].far]
    direct = [(side, i) for side in sides for i in range(len(side[0].direct))]
    for job in relayed:
        lead(*job).start()
    for job in direct:
        straight(*job).start()
    for job in relayed:
        lead(*job).wait_recv()
        follow(*job).start()
    for job in relayed:
        lead(*job).wait_send()
    for job in direct:
        straight(*job).wait()
    for job in relayed:
        follow(*job).wait()


def spread(rows_a, rows_b, early, cid, n_y, n_x, send_a, send_b):
    return pl.pallas_call(
        functools.partial(spread_kernel, rows_a, rows_b, early, n_y, n_x),
        out_shape=tuple(jax.ShapeDtypeStruct(s, BF16) for s in (send_a.shape, send_b.shape, send_a.shape[1:], send_b.shape[1:])),
        in_specs=[HBM, HBM],
        out_specs=(HBM,) * 4,
        scratch_shapes=[
            pltpu.SemaphoreType.DMA((2, 2 * PIECES + n_x)),
            pltpu.SemaphoreType.DMA((2, 2 * PIECES + n_y)),
        ],
        compiler_params=remote_params(cid),
        name='spread_%d_%d' % (rows_a, rows_b),
    )(send_a, send_b)[:2]


WAYS = 4


Path = collections.namedtuple('Path', ('recv', 'send', 'earlies', 'at', 'blocks', 'out_at', 'steps'))


def spot(n_y, n_x, p, d, w, s):
    most = max(n_y, n_x)
    return (((p * most + d) * 2 + w) * most + s) * 2


def list_at(n_y, n_x, sub, my, p, s, w, d, level):
    at, blocks, out_at, steps = (my[1], n_x, my[0], n_y) if p == 0 else (my[0], n_y, my[1], n_x)
    out = lax.rem(out_at + order_of(steps, w)[s], steps)
    return ((out * 3 + level) * blocks + lax.rem(at + blocks - d, blocks)) * sub


def plan_kernel(n_y, n_x, early, lev_a, lev_b, place, rows_at):
    chip = place[1]
    sub = lev_a.shape[0] // (3 * n_y * n_x)
    for p, levels in enumerate((lev_a, lev_b)):
        blocks, steps = ((n_x, n_y), (n_y, n_x))[p]
        for d in range(blocks):
            acc = jnp.int32(0)
            for w in BOTH:
                for s in range(steps):
                    lower, upper = (list_at(n_y, n_x, sub, (chip // n_x, chip % n_x), p, s, w, d, w + up) for up in BOTH)

                    def add(e, n):
                        return n + levels[upper + e] - levels[lower + e]

                    n = lax.fori_loop(0, sub, add, jnp.int32(0))
                    at = spot(n_y, n_x, p, d, w, s)
                    rows_at[at] = acc
                    rows_at[at + 1] = n
                    acc = acc + n
                if not w:
                    acc = jnp.maximum(acc, early)


def plan_rows(n_y, n_x, early, levels, place):
    most = max(n_y, n_x)
    return pl.pallas_call(
        functools.partial(plan_kernel, n_y, n_x, early),
        out_shape=jax.ShapeDtypeStruct((8 * most * most,), I32),
        in_specs=[SMEM] * 3,
        out_specs=SMEM,
        cost_estimate=COST,
        name='plan_rows',
    )(*levels, place)


def sum_kernel(n_y, n_x, passes, early, bounds, *refs):
    (lev_a, lev_b, rows_at, place, recv_a, recv_b, send_a, send_b), refs = take(refs, 8)
    tables_in = []
    for _ in BOTH:
        tok_y, refs = take(refs, n_y)
        tok_x, refs = take(refs, n_x)
        tables_in.append((tok_y, tok_x))
    early_a, refs = take(refs, len(direct_of(n_x)))
    early_b, refs = take(refs, len(direct_of(n_y)))
    chip = place[1]
    my_y, my_x = chip // n_x, chip % n_x
    sub = lev_a.shape[0] // (3 * n_y * n_x)
    words = sub * LANES
    paths = (
        Path(recv_a, send_a, early_a, my_x, n_x, my_y, n_y),
        Path(recv_b, send_b, early_b, my_y, n_y, my_x, n_x),
    )
    todo = [(p, s) for p in BOTH for s in passes if s < paths[p].steps]
    outs, refs = take(refs, 2 * len(todo))
    (tok, wgt, *bufs), refs = take(refs, 4)
    accs, (tsem, rsem, zsem) = take(refs, 2 * WAYS)
    ways = [accs[:WAYS], accs[WAYS:]]
    table_of, size = {}, 0
    for p, s in todo:
        for w in BOTH:
            table_of[p, s, w] = size
            size += paths[p].blocks * words

    def source(p, d):
        return lax.rem(paths[p].at + paths[p].blocks - d, paths[p].blocks)

    def tables(p, s, act):
        for w in BOTH:
            sender = (paths[p].steps - order_of(paths[p].steps, w)[s]) % paths[p].steps
            for d in range(paths[p].blocks):
                src = pl.ds(pl.multiple_of(source(p, d) * words, words), words)
                dst = pl.ds(table_of[p, s, w] + d * words, words)
                for held, table in zip(tables_in, (tok, wgt)):
                    act(pltpu.make_async_copy(held[p][sender].at[src], table.at[dst], tsem.at[todo.index((p, s))]))

    jobs = [(p, s, d) for p, s in todo for d in range(paths[p].blocks)]

    def fetch(job, act):
        p, s, d = jobs[job]
        path = paths[p]
        slot = job % 2
        for w in BOTH:
            first, n = (rows_at[spot(n_y, n_x, p, d, w, s) + i] for i in BOTH)
            to = bufs[w].at[slot]
            main = path.recv if d else path.send
            n_early = 0
            if not w and d in direct_of(path.blocks):
                rows = path.earlies[direct_of(path.blocks).index(d)]
                n_early = jnp.clip(early - first, 0, n)

                @pl.when(n_early > 0)
                def _():
                    act(pltpu.make_async_copy(rows.at[pl.ds(first, n_early)], to.at[pl.ds(0, n_early)], rsem.at[slot]))

            @pl.when(n > n_early)
            def _():
                act(pltpu.make_async_copy(
                    main.at[d, pl.ds(first + n_early, n - n_early)], to.at[pl.ds(n_early, n - n_early)], rsem.at[slot]))

    def zero(acc):
        def body(b, c):
            acc[pl.ds(b * BLOCK, BLOCK)] = jnp.zeros((BLOCK, *acc.shape[1:]), F32)
            return c
        lax.fori_loop(0, (acc.shape[0] - 8) // BLOCK, body, 0)

    fetch(0, start)
    for p, s in todo:
        tables(p, s, start)
    puts = []
    for job, (p, s, d) in enumerate(jobs):
        slot = job % 2
        levels = (lev_a, lev_b)[p]
        dummy = accs[0].shape[0] - 8
        if not d:
            for _, *others in ways:
                for acc in others:
                    zero(acc)
            for put in puts:
                put.wait()
            for target, *_ in ways:
                zero(target)
            tables(p, s, wait)
        fetch(job, wait)
        if job + 1 < len(jobs):
            fetch(job + 1, start)

        def one_expert(e, bases):
            counts, firsts = [], []
            for w in BOTH:
                lower, upper = (levels[list_at(n_y, n_x, sub, (my_y, my_x), p, s, w, d, w + up) + e] for up in BOTH)
                counts.append(upper - lower)
                firsts.append(table_of[p, s, w] + d * words + e * LANES + lower)
            longest = jnp.maximum(counts[0], counts[1])

            def group(b, cc):
                adds = []
                for w in BOTH:
                    for q in range(WAYS):
                        r = b * WAYS + q
                        row = bufs[w][slot, bases[w] + r].astype(F32)
                        t = jnp.where(r < counts[w], tok[firsts[w] + r], dummy)
                        adds.append((ways[w][q], t, wgt[firsts[w] + r] * row))
                for acc, t, row in adds:
                    acc[t] = acc[t] + row
                return cc

            lax.fori_loop(0, lax.shift_right_logical(longest + (WAYS - 1), 2), group, 0)
            return bases[0] + counts[0], bases[1] + counts[1]

        lax.fori_loop(0, sub, one_expert, (jnp.int32(0), jnp.int32(0)))
        if d + 1 == paths[p].blocks:
            puts = []
            for w in BOTH:
                target, second, third, fourth = ways[w]
                size = tokens_of(bounds, p, w)

                def merge(b, c):
                    rows = pl.ds(b * BLOCK, BLOCK)
                    target[rows] = (target[rows] + second[rows]) + (third[rows] + fourth[rows])
                    return c

                lax.fori_loop(0, size // BLOCK, merge, 0)
                out = outs[2 * todo.index((p, s)) + w]
                puts.append(pltpu.make_async_copy(target.at[pl.ds(0, size)], out, zsem.at[w]))
                puts[-1].start()
    for put in puts:
        put.wait()


def weighted_sums(n_y, n_x, passes, early, bounds, levels, rows_at, place, tables, recvs, sends, earlies):
    sublanes = recvs[0].shape[2]
    sub = levels[0].shape[0] // (3 * n_y * n_x)
    todo = [(p, s) for p, n in enumerate((n_y, n_x)) for s in passes if s < n]
    sizes = [tokens_of(bounds, p, w) for p, _ in todo for w in BOTH]
    table = sum((n_x if p == 0 else n_y) * 2 * sub * LANES for p, _ in todo) + 2 * LANES
    tokens = max(b - a for a, b in zip(bounds[:-1], bounds[1:]))
    ops = (*levels, rows_at, place, *recvs, *sends, *tables, *earlies)
    return pl.pallas_call(
        functools.partial(sum_kernel, n_y, n_x, passes, early, bounds),
        out_shape=tuple(jax.ShapeDtypeStruct((n, sublanes, LANES), F32) for n in sizes),
        in_specs=[SMEM] * 4 + [HBM] * (len(ops) - 4),
        out_specs=(HBM,) * len(sizes),
        scratch_shapes=[
            pltpu.SMEM((table,), I32),
            pltpu.SMEM((table,), F32),
            *[pltpu.VMEM((2, sub * LANES + LANES, sublanes, LANES), BF16) for _ in BOTH],
            *[pltpu.VMEM((tokens + 8, sublanes, LANES), F32) for _ in range(2 * WAYS)],
            pltpu.SemaphoreType.DMA((len(todo),)),
            PAIR, PAIR,
        ],
        compiler_params=LOCAL,
        cost_estimate=COST,
        name='weighted_sums',
    )(*ops)


SUM_CHUNKS = 8


def pieces_of(n):
    cuts = [BLOCK * ((n // BLOCK * j) // SUM_CHUNKS) for j in range(SUM_CHUNKS + 1)]
    return [(a, b - a) for a, b in zip(cuts[:-1], cuts[1:]) if b > a]


def reduce_kernel(n_y, n_x, bounds, *refs):
    sizes = (n_y, n_x)
    lanes = [(p, w) for p in BOTH for w in BOTH]
    got, refs = take(refs, len(lanes))
    got = dict(zip(lanes, got))
    sums = {}
    for p, n in enumerate(sizes):
        for s in range(1, n):
            for w in BOTH:
                (sums[p, s, w],), refs = take(refs, 1)
    (x_ref, y_ref), refs = take(refs, 2)
    part, own = {}, {}
    for p, w in lanes:
        for s in range(sizes[p] - 1):
            (part[p, w, s], own[p, w, s]), refs = take(refs, 2)
    zsem, gsem, rsem = refs
    rings = (Ring('y', n_y, n_x), Ring('x', n_y, n_x))
    d_model = x_ref.shape[1]
    pieces = {(p, w): pieces_of(tokens_of(bounds, p, w)) for p, w in lanes}
    order = [(p, w, j) for j in range(SUM_CHUNKS) for p, w in lanes if j < len(pieces[p, w])]

    barrier = pltpu.get_barrier_semaphore()
    for ring in rings:
        for d in (1, -1):
            pl.semaphore_signal(barrier, inc=1, device_id=ring.device(d), device_id_type=pl.DeviceIdType.MESH)
    pl.semaphore_wait(barrier, 4)

    def rows_of(p, w, j):
        return pl.ds(*pieces[p, w][j])

    def load(p, w, s, j):
        r = rows_of(p, w, j)
        return pltpu.make_async_copy(sums[p, s, w].at[r], own[p, w, s - 1].at[r], zsem.at[p, w, s - 1, j])

    def begin(p, w, j):
        r = rows_of(p, w, j)
        return pltpu.make_async_copy(got[p, w].at[r], part[p, w, 0].at[r], gsem.at[p, w, j])

    def hop(p, w, s, j):
        r = rows_of(p, w, j)
        return pltpu.make_async_remote_copy(
            src_ref=part[p, w, s - 1].at[r], dst_ref=part[p, w, s].at[r],
            send_sem=rsem.at[0, p, w, s, j], recv_sem=rsem.at[1, p, w, s, j],
            device_id=rings[p].device(1 if w == 0 else -1), device_id_type=pl.DeviceIdType.MESH)

    def arrive(p, w, s, j):
        if s == 0:
            begin(p, w, j).wait()
        else:
            hop(p, w, s, j).wait_recv()

    last = max(sizes) - 1
    for s in range(1, last + 1):
        for p, w, j in order:
            if s == 1:
                begin(p, w, j).start()
            if s < sizes[p]:
                load(p, w, s, j).start()

    for s in range(1, last):
        for p, w, j in order:
            if s >= sizes[p] - 1:
                continue
            load(p, w, s, j).wait()
            arrive(p, w, s - 1, j)
            into, more = part[p, w, s - 1], own[p, w, s - 1]
            first, n = pieces[p, w][j]

            def add(b, c):
                r = pl.ds(first + b * BLOCK, BLOCK)
                into[r] = into[r] + more[r]
                return c

            lax.fori_loop(0, n // BLOCK, add, 0)
            hop(p, w, s, j).start()

    for p, w, j in order:
        s = sizes[p] - 1
        load(p, w, s, j).wait()
        arrive(p, w, s - 1, j)
        into, more = part[p, w, s - 1], own[p, w, s - 1]
        first, n = pieces[p, w][j]
        token = bounds[2 * p + w] + first

        def finish(b, c):
            r = pl.ds(first + b * BLOCK, BLOCK)
            out = pl.ds(pl.multiple_of(token + b * BLOCK, BLOCK), BLOCK)
            total = into[r] + more[r]
            y_ref[out, :] = (x_ref[out, :].astype(F32) + total.reshape(BLOCK, d_model)).astype(BF16)
            return c

        lax.fori_loop(0, n // BLOCK, finish, 0)
    for s in range(1, last):
        for p, w, j in order:
            if s < sizes[p] - 1:
                hop(p, w, s, j).wait_send()


def reduce_back(cid, n_y, n_x, bounds, got, sums, x):
    n_tok, d_model = x.shape
    sublanes = d_model // LANES
    bufs = []
    for p, n in enumerate((n_y, n_x)):
        for w in BOTH:
            size = tokens_of(bounds, p, w)
            bufs += [pltpu.VMEM((size, sublanes, LANES), F32)] * (2 * (n - 1))
    steps = max(n_y, n_x) - 1
    ops = (*got, *sums, x)
    return pl.pallas_call(
        functools.partial(reduce_kernel, n_y, n_x, bounds),
        out_shape=jax.ShapeDtypeStruct((n_tok, d_model), BF16),
        in_specs=[HBM] * (len(ops) - 1) + [VMEM],
        out_specs=VMEM,
        scratch_shapes=[
            *bufs,
            pltpu.SemaphoreType.DMA((2, 2, steps, SUM_CHUNKS)),
            pltpu.SemaphoreType.DMA((2, 2, SUM_CHUNKS)),
            pltpu.SemaphoreType.DMA((2, 2, 2, steps, SUM_CHUNKS)),
        ],
        compiler_params=remote_params(cid),
        name='reduce_back',
    )(*ops)


def solution(mesh):
    dev_axes = ('ep2', 'ep')
    n_y, n_ep = mesh.shape['ep2'], mesh.shape['ep']
    n_x = n_ep // 2
    group = n_y * n_ep
    n_chip = n_y * n_x

    def local_step(x_loc, ids_loc, gate_loc, w_a, w_b):
        n_tok, d_model = x_loc.shape
        n_top = ids_loc.shape[1]
        e_loc = w_a.shape[0]
        sub = 2 * e_loc
        experts = e_loc * group
        cap = capacity_of(group, n_tok, n_top, experts)
        sublanes = d_model // LANES
        base_a, base_b = n_y * sub * LANES, n_x * sub * LANES
        early = min(base_a, base_b) // 8
        slots_a, slots_b = base_a + early, base_b + early
        bounds = bounds_of(n_tok)
        n_seg, n_chunk = len(bounds) - 1, len(CHUNKS) - 1
        me = lax.axis_index(dev_axes)
        core, chip = me % 2, me // 2
        place = jnp.stack([core, chip]).astype(I32)

        x3 = x_loc.reshape(n_tok, sublanes, LANES)
        chunks = [lax.all_gather(x3[bounds[CHUNKS[k]]:bounds[CHUNKS[k + 1]]], dev_axes, tiled=True) for k in range(n_chunk)]
        swap = [(i, i ^ 1) for i in range(n_ep)]
        w_a_sib = lax.ppermute(w_a, 'ep', swap)
        w_b_sib = lax.ppermute(w_b, 'ep', swap)

        toks, wgts, cnts = route(ids_loc, gate_loc, bounds)
        for_chip = toks[:experts].reshape(n_chip, 1, sub, LANES)
        table = jnp.concatenate([
            jnp.broadcast_to(for_chip, (n_chip, 2, sub, LANES)).reshape(group, sub, LANES),
            jnp.broadcast_to(cnts[None], (group, PREFIX_ROWS, LANES))], axis=1)
        table = lax.all_to_all(table, dev_axes, 0, 0, tiled=True)
        lists = build_lists(place, table.reshape(-1), cap, slots_a, slots_b, early, bounds, n_y, n_x, sub)

        prefix = table[:, sub:sub + n_seg + 1, :experts]
        totals = prefix[:, n_seg]
        offs = jnp.cumsum(totals, axis=0) - totals
        kept = jnp.clip(cap - offs, 0, totals)
        upto = jnp.minimum(prefix, kept[:, None])
        y, x = chip // n_x, chip % n_x
        level_a = lax.dynamic_slice(upto.reshape(n_y, n_ep, n_seg + 1, experts), (0, x * 2 + core, 0, y * n_x * sub), (n_y, 1, 3, n_x * sub))
        level_b = lax.dynamic_slice(upto.reshape(n_y, n_x, 2, n_seg + 1, experts), (y, 0, core, 2, 0), (1, n_x, 1, 3, experts))
        level_b = lax.dynamic_slice(level_b.reshape(n_x, 3, n_y, n_x * sub), (0, 0, 0, x * sub), (n_x, 3, n_y, sub))
        levels = (level_a.reshape(-1), level_b.reshape(-1))
        of_chip = (jnp.arange(experts)[:, None] // sub == jnp.arange(n_chip)[None, :]).astype(F32)
        per_chip = jnp.dot(upto.reshape(-1, experts).astype(F32), of_chip).reshape(group, n_seg + 1, n_chip)
        rows = (per_chip[:, 1:] - per_chip[:, :-1]).astype(I32)
        rows_a = jnp.sum(rows.reshape(n_y, n_ep, n_seg, n_chip), axis=0)
        rows_b = jnp.sum(rows.reshape(n_y, n_x, 2, n_seg, n_chip), axis=1)
        need_a = jnp.max(jnp.maximum(rows_a[:, 0], early) + rows_a[:, 1])
        need_b = jnp.max(jnp.maximum(rows_b[:, :, 2], early) + rows_b[:, :, 3])
        tiers = [(base_a * q // 256, base_b * q // 256) for q in SIZES] + [(slots_a, slots_b)]
        limits = jnp.array(tiers[:-1], I32)
        index = jnp.sum(jnp.logical_or(need_a > limits[:, 0], need_b > limits[:, 1]).astype(I32))
        within = toks[:experts]
        for lo, hi in zip(bounds[1:-1], bounds[:-2]):
            within = jnp.where(toks[:experts] >= lo, within - (lo - hi), within)
        rows_at = plan_rows(n_y, n_x, early, levels, place)

        def up_x(v, d):
            return lax.ppermute(v, 'ep', [(i, (i + 2 * d) % n_ep) for i in range(n_ep)]) if d else v

        def up_y(v, d):
            return lax.ppermute(v, 'ep2', [(i, (i + d) % n_y) for i in range(n_y)]) if d else v

        tables = []
        for v in (within, wgts[:experts]):
            grid = v.reshape(n_y, n_x, sub, LANES)
            tables += [up_y(lax.dynamic_index_in_dim(grid, (y + d) % n_y, 0).reshape(-1), d) for d in range(n_y)]
            tables += [up_x(lax.dynamic_index_in_dim(grid, (x + d) % n_x, 1).reshape(-1), d) for d in range(n_x)]
        lists, levels, rows_at, index, tables = lax.optimization_barrier((lists, levels, rows_at, index, tables))

        weights = (w_a, w_a_sib, w_b, w_b_sib)
        direct_x, direct_y = direct_of(n_x), direct_of(n_y)
        n_early = (len(direct_x), len(direct_y))
        first = run_experts(0, early, n_early, lists, place, chunks[0], *weights, (n_x * slots_a, n_y * slots_b))
        send_a, early_a = first[0], first[1:1 + n_early[0]]
        send_b, early_b = first[1 + n_early[0]], first[2 + n_early[0]:]
        earlies = [up_x(v, d) for v, d in zip(early_a, direct_x)] + [up_y(v, d) for v, d in zip(early_b, direct_y)]
        send_b, = run_experts(1, early, n_early, lists, place, chunks[1], *weights, send_b)
        sends = (send_a.reshape(n_x, slots_a, sublanes, LANES), send_b.reshape(n_y, slots_b, sublanes, LANES))

        recvs = lax.switch(index, [functools.partial(spread, a, b, early, i, n_y, n_x) for i, (a, b) in enumerate(tiers)], *sends)
        common = (early, bounds, levels, rows_at, place, tables, recvs, sends, earlies)
        head = weighted_sums(n_y, n_x, (0,), *common)
        got = (up_y(head[0], 1), up_y(head[1], -1), up_x(head[2], 1), up_x(head[3], -1))
        rest = weighted_sums(n_y, n_x, tuple(range(1, max(n_y, n_x))), *common)
        return reduce_back(len(tiers), n_y, n_x, bounds, got, rest, x_loc)

    tok_spec = P(('dp', 'ep2', 'ep'), None)
    w_spec = P(dev_axes, None, None)
    return jax.shard_map(local_step, mesh=mesh, in_specs=(tok_spec, tok_spec, tok_spec, w_spec, w_spec), out_specs=tok_spec, check_vma=False)
```

```python
import collections
import functools
import math

import jax
import jax.numpy as jnp
from jax import lax
from jax.experimental import pallas as pl
from jax.experimental.pallas import tpu as pltpu
from jax.sharding import PartitionSpec as P

LANES = 128
SEGMENTS = (0, 17, 34, 49, 64)
CHUNKS = (0, 3, 4)
SIZES = (80, 82, 84, 86, 88, 90, 92, 94, 97, 102)
TILE = 256
PREFIX_ROWS = 8
BF16 = jnp.bfloat16
F32 = jnp.float32
I32 = jnp.int32
HBM = pl.BlockSpec(memory_space=pl.ANY)
SMEM = pl.BlockSpec(memory_space=pltpu.SMEM)
VMEM = pl.BlockSpec(memory_space=pltpu.VMEM)
BOTH = range(2)
UNROLL = 8
BLOCK = 16
PAIR = pltpu.SemaphoreType.DMA((2,))
COST = pl.CostEstimate(flops=2 * 10 ** 10, bytes_accessed=10 ** 7, transcendentals=0)
VMEM_LIMIT = 64_000_000
LOCAL = pltpu.CompilerParams(vmem_limit_bytes=VMEM_LIMIT)
MIXED = pltpu.CompilerParams(vmem_limit_bytes=VMEM_LIMIT)


def remote_params(cid):
    return pltpu.CompilerParams(collective_id=cid, has_side_effects=True, vmem_limit_bytes=VMEM_LIMIT)


def take(refs, n):
    return refs[:n], refs[n:]


def start(copy):
    copy.start()


def wait(copy):
    copy.wait()


def capacity_of(group_size, n_tok, n_top, experts):
    return 8 * ((5 * group_size * n_tok * n_top) // (32 * experts))


def far_of(n):
    return n // 2 if n % 2 == 0 and n >= 4 else 0


def direct_of(n):
    return [d for d in range(1, n) if d != far_of(n)]


def bounds_of(n_tok):
    return tuple(16 * ((n_tok * q + 512) // 1024) for q in SEGMENTS)


def tokens_of(bounds, path, w):
    lo, hi = bounds[2 * path + w:][:2]
    return hi - lo


def order_of(n, w):
    return [n - 1 - s if w == 0 else (1 + s) % n for s in range(n)]


def route_kernel(bounds, ids_ref, gate_ref, tok_ref, wgt_ref, cnt_ref, code_t, gate_t, tok_acc, wgt_acc):
    n_tok, n_top = ids_ref.shape
    lane = lax.broadcasted_iota(I32, (n_tok, LANES), 1)
    member = jnp.zeros((n_tok, LANES), F32)
    gates = jnp.zeros((n_tok, LANES), F32)
    for j in range(n_top):
        hit = ids_ref[:, j:j + 1] == lane
        member = member + jnp.where(hit, 1.0, 0.0)
        gates = gates + jnp.where(hit, gate_ref[:, j:j + 1], 0.0)
    member_b = member.astype(BF16)
    row_block = min(n_tok, 128)
    for i in range(n_tok // row_block):
        rows = pl.ds(i * row_block, row_block)
        later = lax.broadcasted_iota(I32, (row_block, n_tok), 0) + i * row_block
        earlier = lax.broadcasted_iota(I32, (row_block, n_tok), 1)
        tri = jnp.where(earlier < later, 1.0, 0.0).astype(BF16)
        rank = jnp.dot(tri, member_b, preferred_element_type=F32)
        mem = member[i * row_block:(i + 1) * row_block]
        code_t[:, rows] = jnp.where(mem > 0.5, rank, -1.0).T
        gate_t[:, rows] = gates[i * row_block:(i + 1) * row_block].T
    total = jnp.zeros((1, LANES), F32)
    rows_out = [total]
    for lo, hi in zip(bounds[:-1], bounds[1:]):
        total = total + jnp.sum(member[lo:hi], axis=0, keepdims=True)
        rows_out.append(total)
    while len(rows_out) < PREFIX_ROWS:
        rows_out.append(total)
    cnt_ref[...] = jnp.concatenate(rows_out, axis=0).astype(I32)
    tok_acc[...] = jnp.zeros_like(tok_acc)
    wgt_acc[...] = jnp.zeros_like(wgt_acc)
    slot = lax.broadcasted_iota(I32, (LANES, n_tok), 0).astype(F32)
    token = lax.broadcasted_iota(I32, (1, n_tok), 1).astype(F32)
    out_lane = lax.broadcasted_iota(I32, (LANES, LANES), 1)

    def one_expert(e, carry):
        hit = slot == code_t[pl.ds(e, 1), :]
        tok = jnp.sum(jnp.where(hit, token, 0.0), axis=1, keepdims=True)
        wgt = jnp.sum(jnp.where(hit, gate_t[pl.ds(e, 1), :], 0.0), axis=1, keepdims=True)
        tok_acc[...] = jnp.where(out_lane == e, tok, tok_acc[...])
        wgt_acc[...] = jnp.where(out_lane == e, wgt, wgt_acc[...])
        return carry

    lax.fori_loop(0, LANES, one_expert, 0)
    tok_ref[...] = tok_acc[...].T.astype(I32)
    wgt_ref[...] = wgt_acc[...].T


def route(ids, gate, bounds):
    n_tok = ids.shape[0]
    return pl.pallas_call(
        functools.partial(route_kernel, bounds),
        out_shape=(
            jax.ShapeDtypeStruct((LANES, LANES), I32),
            jax.ShapeDtypeStruct((LANES, LANES), F32),
            jax.ShapeDtypeStruct((PREFIX_ROWS, LANES), I32),
        ),
        in_specs=[VMEM, VMEM],
        out_specs=(VMEM, VMEM, VMEM),
        scratch_shapes=[
            pltpu.VMEM((LANES, n_tok), F32),
            pltpu.VMEM((LANES, n_tok), F32),
            pltpu.VMEM((LANES, LANES), F32),
            pltpu.VMEM((LANES, LANES), F32),
        ],
        cost_estimate=COST,
        name='route',
    )(ids, gate)


def list_kernel(cap, slots_a, slots_b, early, bounds, n_y, n_x, sub, place_ref, info_ref,
                src_ref, start_ref, len_ref, dst_ref, lim_ref, dir_ref, span_ref, kept_ref, base_ref, lim_tab, dir_tab):
    core, chip = place_ref[0], place_ref[1]
    n_dst = n_y * n_x
    n_seg, n_chunk = len(bounds) - 1, len(CHUNKS) - 1
    dev_words = (sub + PREFIX_ROWS) * LANES
    width = src_ref.shape[0] // sub
    my_y, my_x = chip // n_x, chip % n_x

    def count(g, k, e):
        return info_ref[g * dev_words + (sub + k) * LANES + chip * sub + e]

    def per_expert(e, carry):
        def per_dev(i, off):
            for c in BOTH:
                n = count(2 * i + c, n_seg, e)
                kept = jnp.clip(cap - off, 0, n)
                off = off + n

                @pl.when(core == c)
                def _():
                    kept_ref[i * sub + e] = kept
            return off
        lax.fori_loop(0, n_dst, per_dev, 0)
        return carry

    lax.fori_loop(0, sub, per_expert, 0)

    def rows_in(k, i, e):
        g, kept = 2 * i + core, kept_ref[i * sub + e]
        return jnp.minimum(count(g, k + 1, e), kept) - jnp.minimum(count(g, k, e), kept)

    def block_bases(path, n_blocks, n_inner, slots, index):
        for d in range(n_blocks):
            acc = jnp.int32(d * slots)
            for w in BOTH:
                for r in order_of(n_inner, w):
                    i = index(d, r)

                    def add(e, acc):
                        base_ref[((2 * path + w) * n_dst + i) * sub + e] = acc
                        return acc + rows_in(2 * path + w, i, e)

                    acc = lax.fori_loop(0, sub, add, acc)
                    direct = direct_of(n_blocks)
                    lim_tab[path * n_dst + i] = d * slots + early if d in direct else 0
                    dir_tab[path * n_dst + i] = direct.index(d) if d in direct else 0
                if w == 0:
                    acc = jnp.maximum(acc, d * slots + early)

    block_bases(0, n_x, n_y, slots_a, lambda d, r: lax.rem(my_y + r, n_y) * n_x + lax.rem(my_x + d, n_x))
    block_bases(1, n_y, n_x, slots_b, lambda d, r: lax.rem(my_y + d, n_y) * n_x + lax.rem(my_x + r, n_x))

    def expert_lists(e, carry):
        pos = e * width
        for chunk, (chunk_lo, chunk_hi) in enumerate(zip(CHUNKS[:-1], CHUNKS[1:])):
            size = bounds[chunk_hi] - bounds[chunk_lo]
            start_at = pos
            for k in range(chunk_lo, chunk_hi):

                def segment(i, o):
                    g = 2 * i + core
                    kept = kept_ref[i * sub + e]
                    s0 = jnp.minimum(count(g, k, e), kept)
                    n = jnp.minimum(count(g, k + 1, e), kept) - s0
                    j = (e * n_seg + k) * n_dst + i
                    start_ref[j] = o
                    len_ref[j] = n
                    dst_ref[j] = base_ref[(k * n_dst + i) * sub + e]
                    lim_ref[j] = lim_tab[(k // 2) * n_dst + i]
                    dir_ref[j] = dir_tab[(k // 2) * n_dst + i]
                    src0 = g * size - bounds[chunk_lo]
                    tok0 = g * dev_words + e * LANES + s0

                    def block(b, c):
                        vals = [info_ref[tok0 + b * UNROLL + q] for q in range(UNROLL)]
                        for q in range(UNROLL):
                            src_ref[o + b * UNROLL + q] = src0 + vals[q]
                        return c

                    lax.fori_loop(0, pl.cdiv(n, UNROLL), block, 0)
                    return o + n

                pos = lax.fori_loop(0, n_dst, segment, pos)
            span_ref[(e * n_chunk + chunk) * 2] = start_at
            span_ref[(e * n_chunk + chunk) * 2 + 1] = pos - start_at

            def pad(b, c):
                for q in range(UNROLL):
                    src_ref[pos + b * UNROLL + q] = b * UNROLL + q
                return c

            lax.fori_loop(0, TILE // UNROLL, pad, 0)
            pos = pos + TILE
        return carry

    lax.fori_loop(0, sub, expert_lists, 0)


def build_lists(place, info, cap, slots_a, slots_b, early, bounds, n_y, n_x, sub):
    n_dst, n_seg = n_y * n_x, len(bounds) - 1
    n_chunk = len(CHUNKS) - 1
    width = LANES * n_dst + n_chunk * TILE + UNROLL
    segs = sub * n_seg * n_dst + UNROLL
    return pl.pallas_call(
        functools.partial(list_kernel, cap, slots_a, slots_b, early, bounds, n_y, n_x, sub),
        out_shape=(
            jax.ShapeDtypeStruct((sub * width,), I32),
            *[jax.ShapeDtypeStruct((segs,), I32) for _ in range(5)],
            jax.ShapeDtypeStruct((sub * n_chunk * 2,), I32),
        ),
        in_specs=[SMEM, SMEM],
        out_specs=(SMEM,) * 7,
        scratch_shapes=[
            pltpu.SMEM((n_dst * sub,), I32),
            pltpu.SMEM((n_seg * n_dst * sub,), I32),
            pltpu.SMEM((2 * n_dst,), I32),
            pltpu.SMEM((2 * n_dst,), I32),
        ],
        cost_estimate=COST,
        name='row_lists',
    )(place, info)


def gelu(v):
    return 0.5 * v * (1.0 + jnp.tanh(math.sqrt(2.0 / math.pi) * (v + 0.044715 * v * v * v)))


def expert_kernel(chunk, n_seg, early, late, n_early, *refs):
    lo_seg, hi_seg = CHUNKS[chunk:][:2]
    (src, seg_start, seg_len, seg_dst, seg_lim, seg_dir, span, place, x_hbm, wa_own, wa_sib, wb_own, wb_sib), refs = take(refs, 13)
    if lo_seg > 0:
        refs = refs[1:]
    paths, at = [], 0
    for path in BOTH:
        first, last = max(lo_seg, 2 * path), min(hi_seg, 2 * path + 2)
        if first < last:
            n = n_early[path] if lo_seg == 0 else 0
            (send, *heads), _ = take(refs[at:], 1 + 2 * n)
            paths.append((first, last, send, list(zip(*take(heads, n)))))
            at += 1 + 2 * n
    xbuf, xrows, obuf, wa, wb, t_e, t_base, t_cnt, ptr, gsem, ssem, wsem = refs[at:]
    e_loc, d_model, _ = wa_own.shape
    sub = 2 * e_loc
    core = place[0]
    sublanes = d_model // LANES
    n_dst = (seg_start.shape[0] - UNROLL) // (sub * n_seg)

    def span_of(e):
        at = (e * (len(CHUNKS) - 1) + chunk) * 2
        return span[at], span[at + 1]

    def weight_copies(e, act):
        slot = e % 2
        q = e % e_loc

        @pl.when(e // e_loc == core)
        def _():
            act(pltpu.make_async_copy(wa_own.at[q], wa.at[slot], wsem.at[slot, 0]))
            act(pltpu.make_async_copy(wb_own.at[q], wb.at[slot], wsem.at[slot, 1]))

        @pl.when(e // e_loc != core)
        def _():
            act(pltpu.make_async_copy(wa_sib.at[q], wa.at[slot], wsem.at[slot, 0]))
            act(pltpu.make_async_copy(wb_sib.at[q], wb.at[slot], wsem.at[slot, 1]))

    weight_copies(0, start)

    def plan(e, t):
        lo, n = span_of(e)

        def put(i, c):
            t_e[t + i] = e
            t_base[t + i] = lo + i * TILE
            t_cnt[t + i] = jnp.minimum(n - i * TILE, TILE)
            return c

        n_tiles = (n + TILE - 1) // TILE
        lax.fori_loop(0, n_tiles, put, 0)
        return t + n_tiles

    n_all = lax.fori_loop(0, sub, plan, 0)
    for t in BOTH:
        t_base[n_all + t], _ = span_of(0)

    def fetch_row(t, r):
        slot = t % 2
        pltpu.make_async_copy(x_hbm.at[src[t_base[t] + r]], xbuf.at[slot, r], gsem.at[slot]).start()

    def gather_wait(t):
        slot = t % 2
        pltpu.make_async_copy(x_hbm.at[pl.ds(0, TILE)], xbuf.at[slot], gsem.at[slot]).wait()

    def scatter_start(t):
        base, slot = t_base[t], t % 2
        end = base + t_cnt[t]

        for path, (_, last, send, heads) in enumerate(paths):
            j_end = (t_e[t] * n_seg + last) * n_dst

            def more(j):
                return jnp.logical_and(j < j_end, seg_start[j] < end)

            def segment(j):
                first_row = seg_start[j]
                lo = jnp.maximum(first_row, base)
                n = jnp.minimum(first_row + seg_len[j], end) - lo
                to = seg_dst[j] + lo - first_row
                n_head = jnp.clip(seg_lim[j] - to, 0, jnp.maximum(n, 0)) if heads else 0
                n_early = jnp.clip(seg_lim[j] - late - to, 0, n_head) if heads else 0
                in_head = to - seg_lim[j] + late + early

                def put(rows, first, at, n):
                    @pl.when(n > 0)
                    def _():
                        pltpu.make_async_copy(
                            obuf.at[slot, pl.ds(lo - base + first, n)], rows.at[pl.ds(at, n)], ssem.at[slot]).start()

                def put_head(q, early_rows, late_rows):
                    @pl.when(seg_dir[j] == q)
                    def _():
                        put(early_rows, 0, in_head, n_early)
                        put(late_rows, n_early, in_head + n_early - early, n_head - n_early)

                if heads:
                    @pl.when(n_head > 0)
                    def _():
                        for q, rows in enumerate(heads):
                            put_head(q, *rows)

                put(send, n_head, to + n_head, n - n_head)
                return j + 1

            start = ptr[path]
            ptr[path] = jnp.maximum(lax.while_loop(more, segment, start) - 1, start)

    def scatter_wait(t):
        n, slot = t_cnt[t], t % 2
        send = paths[0][2]
        pltpu.make_async_copy(obuf.at[slot, pl.ds(0, n)], send.at[pl.ds(0, n)], ssem.at[slot]).wait()

    def prime(r, c):
        for t in BOTH:
            fetch_row(t, r)
        return c

    lax.fori_loop(0, TILE, prime, 0, unroll=UNROLL)

    def one_expert(e, t_first):
        weight_copies(e, wait)

        @pl.when(e + 1 < sub)
        def _():
            weight_copies(e + 1, start)

        ws = e % 2
        _, n = span_of(e)
        for path, (first, _, _, _) in enumerate(paths):
            ptr[path] = (e * n_seg + first) * n_dst

        def one_tile(i, t):
            slot = t % 2
            gather_wait(t)

            @pl.when(t >= 2)
            def _():
                scatter_wait(t - 2)

            xrows[...] = xbuf[slot].reshape(TILE, d_model)
            for r in range(TILE):
                fetch_row(t + 2, r)
            hidden = gelu(jnp.dot(xrows[...], wa[ws], preferred_element_type=F32)).astype(BF16)
            out = jnp.dot(hidden, wb[ws], preferred_element_type=F32).astype(BF16)
            obuf[slot] = out.reshape(TILE, sublanes, LANES)
            scatter_start(t)
            return t + 1

        return lax.fori_loop(0, (n + TILE - 1) // TILE, one_tile, t_first)

    lax.fori_loop(0, sub, one_expert, 0)
    for back in (2, 1):
        gather_wait(n_all + back)

        @pl.when(n_all >= back)
        def _():
            scatter_wait(n_all - back)


def run_experts(chunk, early, late, n_early, lists, place, x_rows, wa, wa_sib, wb, wb_sib, rows):
    e_loc, d_model, ff = wa.shape
    sub = 2 * e_loc
    sublanes = d_model // LANES
    ops = (*lists, place, x_rows, wa, wa_sib, wb, wb_sib) + (() if chunk == 0 else (rows,))
    n_smem = len(lists) + 1
    max_tiles = sub * (pl.cdiv(lists[0].shape[0] // sub, TILE) + 1) + 2
    if chunk == 0:
        sizes = []
        for n_rows, n in zip(rows, n_early):
            sizes += [n_rows] + [early] * n + [late] * n
    else:
        sizes = [rows.shape[0]]
    return pl.pallas_call(
        functools.partial(expert_kernel, chunk, len(SEGMENTS) - 1, early, late, n_early),
        out_shape=tuple(jax.ShapeDtypeStruct((n, sublanes, LANES), BF16) for n in sizes),
        in_specs=[SMEM] * n_smem + [HBM] * (len(ops) - n_smem),
        out_specs=(HBM,) * len(sizes),
        scratch_shapes=[
            pltpu.VMEM((2, TILE, sublanes, LANES), BF16),
            pltpu.VMEM((TILE, d_model), BF16),
            pltpu.VMEM((2, TILE, sublanes, LANES), BF16),
            pltpu.VMEM((2, d_model, ff), BF16),
            pltpu.VMEM((2, ff, d_model), BF16),
            pltpu.SMEM((max_tiles,), I32),
            pltpu.SMEM((max_tiles,), I32),
            pltpu.SMEM((max_tiles,), I32),
            pltpu.SMEM((2,), I32),
            PAIR, PAIR,
            pltpu.SemaphoreType.DMA((2, 2)),
        ],
        input_output_aliases={} if chunk == 0 else {len(ops) - 1: 0},
        compiler_params=MIXED,
        cost_estimate=COST,
        name='experts',
    )(*ops)


PIECES = 4


class Ring:
    def __init__(self, axis, n_y, n_x):
        y, ec = lax.axis_index('ep2'), lax.axis_index('ep')
        self.axis, self.core = axis, ec % 2
        self.n = n_x if axis == 'x' else n_y
        self.pos = ec // 2 if axis == 'x' else y
        self.direct, self.far = direct_of(self.n), far_of(self.n)

    def place(self, d):
        return lax.rem(self.pos + d + self.n, self.n)

    def device(self, d):
        if self.axis == 'x':
            return {'ep': self.place(d) * 2 + self.core}
        return {'ep2': self.place(d)}

    def remote(self, src, dst, sems, i, d):
        return pltpu.make_async_remote_copy(
            src_ref=src, dst_ref=dst, send_sem=sems.at[0, i], recv_sem=sems.at[1, i],
            device_id=self.device(d), device_id_type=pl.DeviceIdType.MESH)

    def signal(self, barrier):
        for d in range(1, self.n):
            pl.semaphore_signal(barrier, inc=1, device_id=self.device(d), device_id_type=pl.DeviceIdType.MESH)


def spread_kernel(rows_a, rows_b, early, n_y, n_x, send_a, send_b, recv_a, recv_b, stage_a, stage_b, sem_a, sem_b):
    rings = (Ring('x', n_y, n_x), Ring('y', n_y, n_x))
    barrier = pltpu.get_barrier_semaphore()
    for ring in rings:
        ring.signal(barrier)
    pl.semaphore_wait(barrier, n_x + n_y - 2)

    sides = list(zip(rings, (rows_a, rows_b), (send_a, send_b), (recv_a, recv_b), (stage_a, stage_b), (sem_a, sem_b)))

    def lead(side, p):
        ring, rows, send, _, stage, sem = side
        hop = ring.far // 2 if p % 2 == 0 else -(ring.far // 2)
        part = pl.ds(p * (rows // PIECES), rows // PIECES)
        return ring.remote(send.at[ring.far, part], stage.at[part], sem, p, hop)

    def follow(side, p):
        ring, rows, _, recv, stage, sem = side
        hop = ring.far // 2 if p % 2 == 0 else -(ring.far // 2)
        part = pl.ds(p * (rows // PIECES), rows // PIECES)
        return ring.remote(stage.at[part], recv.at[ring.far, part], sem, PIECES + p, hop)

    def straight(side, i):
        ring, rows, send, recv, _, sem = side
        d = ring.direct[i]
        part = pl.ds(early, rows - early)
        return ring.remote(send.at[d, part], recv.at[d, part], sem, 2 * PIECES + i, d)

    relayed = [(side, p) for p in range(PIECES) for side in sides if side[0].far]
    direct = [(side, i) for side in sides for i in range(len(side[0].direct))]
    for job in relayed:
        lead(*job).start()
    for job in direct:
        straight(*job).start()
    for job in relayed:
        lead(*job).wait_recv()
        follow(*job).start()
    for job in relayed:
        lead(*job).wait_send()
    for job in direct:
        straight(*job).wait()
    for job in relayed:
        follow(*job).wait()


def spread(rows_a, rows_b, early, cid, n_y, n_x, send_a, send_b):
    return pl.pallas_call(
        functools.partial(spread_kernel, rows_a, rows_b, early, n_y, n_x),
        out_shape=tuple(jax.ShapeDtypeStruct(s, BF16) for s in (send_a.shape, send_b.shape, send_a.shape[1:], send_b.shape[1:])),
        in_specs=[HBM, HBM],
        out_specs=(HBM,) * 4,
        scratch_shapes=[
            pltpu.SemaphoreType.DMA((2, 2 * PIECES + n_x)),
            pltpu.SemaphoreType.DMA((2, 2 * PIECES + n_y)),
        ],
        compiler_params=remote_params(cid),
        name='spread_%d_%d' % (rows_a, rows_b),
    )(send_a, send_b)[:2]


WAYS = 4


Path = collections.namedtuple('Path', ('recv', 'send', 'earlies', 'lates', 'at', 'blocks', 'out_at', 'steps'))


def spot(n_y, n_x, p, d, w, s):
    most = max(n_y, n_x)
    return (((p * most + d) * 2 + w) * most + s) * 2


def list_at(n_y, n_x, sub, my, p, s, w, d, level):
    at, blocks, out_at, steps = (my[1], n_x, my[0], n_y) if p == 0 else (my[0], n_y, my[1], n_x)
    out = lax.rem(out_at + order_of(steps, w)[s], steps)
    return ((out * 3 + level) * blocks + lax.rem(at + blocks - d, blocks)) * sub


def plan_kernel(n_y, n_x, early, lev_a, lev_b, place, rows_at):
    chip = place[1]
    sub = lev_a.shape[0] // (3 * n_y * n_x)
    for p, levels in enumerate((lev_a, lev_b)):
        blocks, steps = ((n_x, n_y), (n_y, n_x))[p]
        for d in range(blocks):
            acc = jnp.int32(0)
            for w in BOTH:
                for s in range(steps):
                    lower, upper = (list_at(n_y, n_x, sub, (chip // n_x, chip % n_x), p, s, w, d, w + up) for up in BOTH)

                    def add(e, n):
                        return n + levels[upper + e] - levels[lower + e]

                    n = lax.fori_loop(0, sub, add, jnp.int32(0))
                    at = spot(n_y, n_x, p, d, w, s)
                    rows_at[at] = acc
                    rows_at[at + 1] = n
                    acc = acc + n
                if not w:
                    acc = jnp.maximum(acc, early)


def plan_rows(n_y, n_x, early, levels, place):
    most = max(n_y, n_x)
    return pl.pallas_call(
        functools.partial(plan_kernel, n_y, n_x, early),
        out_shape=jax.ShapeDtypeStruct((8 * most * most,), I32),
        in_specs=[SMEM] * 3,
        out_specs=SMEM,
        cost_estimate=COST,
        name='plan_rows',
    )(*levels, place)


def sum_kernel(n_y, n_x, passes, early, late, bounds, *refs):
    (lev_a, lev_b, rows_at, place, recv_a, recv_b, send_a, send_b), refs = take(refs, 8)
    tables_in = []
    for _ in BOTH:
        tok_y, refs = take(refs, n_y)
        tok_x, refs = take(refs, n_x)
        tables_in.append((tok_y, tok_x))
    early_a, refs = take(refs, len(direct_of(n_x)))
    early_b, refs = take(refs, len(direct_of(n_y)))
    late_a, refs = take(refs, len(direct_of(n_x)) if late else 0)
    late_b, refs = take(refs, len(direct_of(n_y)) if late else 0)
    chip = place[1]
    my_y, my_x = chip // n_x, chip % n_x
    sub = lev_a.shape[0] // (3 * n_y * n_x)
    words = sub * LANES
    paths = (
        Path(recv_a, send_a, early_a, late_a, my_x, n_x, my_y, n_y),
        Path(recv_b, send_b, early_b, late_b, my_y, n_y, my_x, n_x),
    )
    todo = [(p, s) for p in BOTH for s in passes if s < paths[p].steps]
    outs, refs = take(refs, 2 * len(todo))
    (tok, wgt, *bufs), refs = take(refs, 4)
    accs, (tsem, rsem, zsem) = take(refs, 2 * WAYS)
    ways = [accs[:WAYS], accs[WAYS:]]
    table_of, size = {}, 0
    for p, s in todo:
        for w in BOTH:
            table_of[p, s, w] = size
            size += paths[p].blocks * words

    def source(p, d):
        return lax.rem(paths[p].at + paths[p].blocks - d, paths[p].blocks)

    def tables(p, s, act):
        for w in BOTH:
            sender = (paths[p].steps - order_of(paths[p].steps, w)[s]) % paths[p].steps
            for d in range(paths[p].blocks):
                src = pl.ds(pl.multiple_of(source(p, d) * words, words), words)
                dst = pl.ds(table_of[p, s, w] + d * words, words)
                for held, table in zip(tables_in, (tok, wgt)):
                    act(pltpu.make_async_copy(held[p][sender].at[src], table.at[dst], tsem.at[todo.index((p, s))]))

    jobs = [(p, s, d) for p, s in todo for d in range(paths[p].blocks)]

    def fetch(job, act):
        p, s, d = jobs[job]
        path = paths[p]
        slot = job % 2
        for w in BOTH:
            first, n = (rows_at[spot(n_y, n_x, p, d, w, s) + i] for i in BOTH)
            to = bufs[w].at[slot]
            main = path.recv if d else path.send

            def get(rows, at, done, n):
                @pl.when(n > 0)
                def _():
                    act(pltpu.make_async_copy(rows.at[pl.ds(at, n)], to.at[pl.ds(done, n)], rsem.at[slot]))

            done = 0
            if not w and d in direct_of(path.blocks):
                q = direct_of(path.blocks).index(d)
                done = jnp.clip(early - first, 0, n)
                get(path.earlies[q], first, 0, done)
                if late:
                    n_late = jnp.clip(early + late - first, 0, n) - done
                    get(path.lates[q], first + done - early, done, n_late)
                    done = done + n_late
            get(main.at[d], first + done, done, n - done)

    def zero(acc):
        def body(b, c):
            acc[pl.ds(b * BLOCK, BLOCK)] = jnp.zeros((BLOCK, *acc.shape[1:]), F32)
            return c
        lax.fori_loop(0, (acc.shape[0] - 8) // BLOCK, body, 0)

    fetch(0, start)
    for p, s in todo:
        tables(p, s, start)
    puts = []
    for job, (p, s, d) in enumerate(jobs):
        slot = job % 2
        levels = (lev_a, lev_b)[p]
        dummy = accs[0].shape[0] - 8
        if not d:
            for _, *others in ways:
                for acc in others:
                    zero(acc)
            for put in puts:
                put.wait()
            for target, *_ in ways:
                zero(target)
            tables(p, s, wait)
        fetch(job, wait)
        if job + 1 < len(jobs):
            fetch(job + 1, start)

        def one_expert(e, bases):
            counts, firsts = [], []
            for w in BOTH:
                lower, upper = (levels[list_at(n_y, n_x, sub, (my_y, my_x), p, s, w, d, w + up) + e] for up in BOTH)
                counts.append(upper - lower)
                firsts.append(table_of[p, s, w] + d * words + e * LANES + lower)
            longest = jnp.maximum(counts[0], counts[1])

            def group(b, cc):
                adds = []
                for w in BOTH:
                    for q in range(WAYS):
                        r = b * WAYS + q
                        row = bufs[w][slot, bases[w] + r].astype(F32)
                        t = jnp.where(r < counts[w], tok[firsts[w] + r], dummy)
                        adds.append((ways[w][q], t, wgt[firsts[w] + r] * row))
                for acc, t, row in adds:
                    acc[t] = acc[t] + row
                return cc

            lax.fori_loop(0, lax.shift_right_logical(longest + (WAYS - 1), 2), group, 0)
            return bases[0] + counts[0], bases[1] + counts[1]

        lax.fori_loop(0, sub, one_expert, (jnp.int32(0), jnp.int32(0)))
        if d + 1 == paths[p].blocks:
            puts = []
            for w in BOTH:
                target, second, third, fourth = ways[w]
                size = tokens_of(bounds, p, w)

                def merge(b, c):
                    rows = pl.ds(b * BLOCK, BLOCK)
                    target[rows] = (target[rows] + second[rows]) + (third[rows] + fourth[rows])
                    return c

                lax.fori_loop(0, size // BLOCK, merge, 0)
                out = outs[2 * todo.index((p, s)) + w]
                puts.append(pltpu.make_async_copy(target.at[pl.ds(0, size)], out, zsem.at[w]))
                puts[-1].start()
    for put in puts:
        put.wait()


def weighted_sums(n_y, n_x, passes, early, late, bounds, levels, rows_at, place, tables, recvs, sends, heads):
    sublanes = recvs[0].shape[2]
    sub = levels[0].shape[0] // (3 * n_y * n_x)
    todo = [(p, s) for p, n in enumerate((n_y, n_x)) for s in passes if s < n]
    sizes = [tokens_of(bounds, p, w) for p, _ in todo for w in BOTH]
    table = sum((n_x if p == 0 else n_y) * 2 * sub * LANES for p, _ in todo) + 2 * LANES
    tokens = max(b - a for a, b in zip(bounds[:-1], bounds[1:]))
    ops = (*levels, rows_at, place, *recvs, *sends, *tables, *heads)
    return pl.pallas_call(
        functools.partial(sum_kernel, n_y, n_x, passes, early, late, bounds),
        out_shape=tuple(jax.ShapeDtypeStruct((n, sublanes, LANES), F32) for n in sizes),
        in_specs=[SMEM] * 4 + [HBM] * (len(ops) - 4),
        out_specs=(HBM,) * len(sizes),
        scratch_shapes=[
            pltpu.SMEM((table,), I32),
            pltpu.SMEM((table,), F32),
            *[pltpu.VMEM((2, sub * LANES + LANES, sublanes, LANES), BF16) for _ in BOTH],
            *[pltpu.VMEM((tokens + 8, sublanes, LANES), F32) for _ in range(2 * WAYS)],
            pltpu.SemaphoreType.DMA((len(todo),)),
            PAIR, PAIR,
        ],
        compiler_params=LOCAL,
        cost_estimate=COST,
        name='weighted_sums',
    )(*ops)


SUM_CHUNKS = 8


def pieces_of(n):
    cuts = [BLOCK * ((n // BLOCK * j) // SUM_CHUNKS) for j in range(SUM_CHUNKS + 1)]
    return [(a, b - a) for a, b in zip(cuts[:-1], cuts[1:]) if b > a]


def reduce_kernel(n_y, n_x, bounds, *refs):
    sizes = (n_y, n_x)
    lanes = [(p, w) for p in BOTH for w in BOTH]
    got, refs = take(refs, len(lanes))
    got = dict(zip(lanes, got))
    sums = {}
    for p, n in enumerate(sizes):
        for s in range(1, n):
            for w in BOTH:
                (sums[p, s, w],), refs = take(refs, 1)
    (x_ref, y_ref), refs = take(refs, 2)
    part, own = {}, {}
    for p, w in lanes:
        for s in range(sizes[p] - 1):
            (part[p, w, s], own[p, w, s]), refs = take(refs, 2)
    zsem, gsem, rsem = refs
    rings = (Ring('y', n_y, n_x), Ring('x', n_y, n_x))
    d_model = x_ref.shape[1]
    pieces = {(p, w): pieces_of(tokens_of(bounds, p, w)) for p, w in lanes}
    order = [(p, w, j) for j in range(SUM_CHUNKS) for p, w in lanes if j < len(pieces[p, w])]

    barrier = pltpu.get_barrier_semaphore()
    for ring in rings:
        for d in (1, -1):
            pl.semaphore_signal(barrier, inc=1, device_id=ring.device(d), device_id_type=pl.DeviceIdType.MESH)
    pl.semaphore_wait(barrier, 4)

    def rows_of(p, w, j):
        return pl.ds(*pieces[p, w][j])

    def load(p, w, s, j):
        r = rows_of(p, w, j)
        return pltpu.make_async_copy(sums[p, s, w].at[r], own[p, w, s - 1].at[r], zsem.at[p, w, s - 1, j])

    def begin(p, w, j):
        r = rows_of(p, w, j)
        return pltpu.make_async_copy(got[p, w].at[r], part[p, w, 0].at[r], gsem.at[p, w, j])

    def hop(p, w, s, j):
        r = rows_of(p, w, j)
        return pltpu.make_async_remote_copy(
            src_ref=part[p, w, s - 1].at[r], dst_ref=part[p, w, s].at[r],
            send_sem=rsem.at[0, p, w, s, j], recv_sem=rsem.at[1, p, w, s, j],
            device_id=rings[p].device(1 if w == 0 else -1), device_id_type=pl.DeviceIdType.MESH)

    def arrive(p, w, s, j):
        if s == 0:
            begin(p, w, j).wait()
        else:
            hop(p, w, s, j).wait_recv()

    last = max(sizes) - 1
    for s in range(1, last + 1):
        for p, w, j in order:
            if s == 1:
                begin(p, w, j).start()
            if s < sizes[p]:
                load(p, w, s, j).start()

    for s in range(1, last):
        for p, w, j in order:
            if s >= sizes[p] - 1:
                continue
            load(p, w, s, j).wait()
            arrive(p, w, s - 1, j)
            into, more = part[p, w, s - 1], own[p, w, s - 1]
            first, n = pieces[p, w][j]

            def add(b, c):
                r = pl.ds(first + b * BLOCK, BLOCK)
                into[r] = into[r] + more[r]
                return c

            lax.fori_loop(0, n // BLOCK, add, 0)
            hop(p, w, s, j).start()

    for p, w, j in order:
        s = sizes[p] - 1
        load(p, w, s, j).wait()
        arrive(p, w, s - 1, j)
        into, more = part[p, w, s - 1], own[p, w, s - 1]
        first, n = pieces[p, w][j]
        token = bounds[2 * p + w] + first

        def finish(b, c):
            r = pl.ds(first + b * BLOCK, BLOCK)
            out = pl.ds(pl.multiple_of(token + b * BLOCK, BLOCK), BLOCK)
            total = into[r] + more[r]
            y_ref[out, :] = (x_ref[out, :].astype(F32) + total.reshape(BLOCK, d_model)).astype(BF16)
            return c

        lax.fori_loop(0, n // BLOCK, finish, 0)
    for s in range(1, last):
        for p, w, j in order:
            if s < sizes[p] - 1:
                hop(p, w, s, j).wait_send()


def reduce_back(cid, n_y, n_x, bounds, got, sums, x):
    n_tok, d_model = x.shape
    sublanes = d_model // LANES
    bufs = []
    for p, n in enumerate((n_y, n_x)):
        for w in BOTH:
            size = tokens_of(bounds, p, w)
            bufs += [pltpu.VMEM((size, sublanes, LANES), F32)] * (2 * (n - 1))
    steps = max(n_y, n_x) - 1
    ops = (*got, *sums, x)
    return pl.pallas_call(
        functools.partial(reduce_kernel, n_y, n_x, bounds),
        out_shape=jax.ShapeDtypeStruct((n_tok, d_model), BF16),
        in_specs=[HBM] * (len(ops) - 1) + [VMEM],
        out_specs=VMEM,
        scratch_shapes=[
            *bufs,
            pltpu.SemaphoreType.DMA((2, 2, steps, SUM_CHUNKS)),
            pltpu.SemaphoreType.DMA((2, 2, SUM_CHUNKS)),
            pltpu.SemaphoreType.DMA((2, 2, 2, steps, SUM_CHUNKS)),
        ],
        compiler_params=remote_params(cid),
        name='reduce_back',
    )(*ops)


def solution(mesh):
    dev_axes = ('ep2', 'ep')
    n_y, n_ep = mesh.shape['ep2'], mesh.shape['ep']
    n_x = n_ep // 2
    group = n_y * n_ep
    n_chip = n_y * n_x

    def local_step(x_loc, ids_loc, gate_loc, w_a, w_b):
        n_tok, d_model = x_loc.shape
        n_top = ids_loc.shape[1]
        e_loc = w_a.shape[0]
        sub = 2 * e_loc
        experts = e_loc * group
        cap = capacity_of(group, n_tok, n_top, experts)
        sublanes = d_model // LANES
        base_a, base_b = n_y * sub * LANES, n_x * sub * LANES
        late = min(base_a, base_b) // 16
        early = late + late // 2
        head = early + late
        slots_a, slots_b = base_a + head, base_b + head
        bounds = bounds_of(n_tok)
        n_seg, n_chunk = len(bounds) - 1, len(CHUNKS) - 1
        me = lax.axis_index(dev_axes)
        core, chip = me % 2, me // 2
        place = jnp.stack([core, chip]).astype(I32)

        x3 = x_loc.reshape(n_tok, sublanes, LANES)
        chunks = [lax.all_gather(x3[bounds[CHUNKS[k]]:bounds[CHUNKS[k + 1]]], dev_axes, tiled=True) for k in range(n_chunk)]
        swap = [(i, i ^ 1) for i in range(n_ep)]
        w_a_sib = lax.ppermute(w_a, 'ep', swap)
        w_b_sib = lax.ppermute(w_b, 'ep', swap)

        toks, wgts, cnts = route(ids_loc, gate_loc, bounds)
        for_chip = toks[:experts].reshape(n_chip, 1, sub, LANES)
        table = jnp.concatenate([
            jnp.broadcast_to(for_chip, (n_chip, 2, sub, LANES)).reshape(group, sub, LANES),
            jnp.broadcast_to(cnts[None], (group, PREFIX_ROWS, LANES))], axis=1)
        table = lax.all_to_all(table, dev_axes, 0, 0, tiled=True)
        lists = build_lists(place, table.reshape(-1), cap, slots_a, slots_b, head, bounds, n_y, n_x, sub)

        prefix = table[:, sub:sub + n_seg + 1, :experts]
        totals = prefix[:, n_seg]
        offs = jnp.cumsum(totals, axis=0) - totals
        kept = jnp.clip(cap - offs, 0, totals)
        upto = jnp.minimum(prefix, kept[:, None])
        y, x = chip // n_x, chip % n_x
        level_a = lax.dynamic_slice(upto.reshape(n_y, n_ep, n_seg + 1, experts), (0, x * 2 + core, 0, y * n_x * sub), (n_y, 1, 3, n_x * sub))
        level_b = lax.dynamic_slice(upto.reshape(n_y, n_x, 2, n_seg + 1, experts), (y, 0, core, 2, 0), (1, n_x, 1, 3, experts))
        level_b = lax.dynamic_slice(level_b.reshape(n_x, 3, n_y, n_x * sub), (0, 0, 0, x * sub), (n_x, 3, n_y, sub))
        levels = (level_a.reshape(-1), level_b.reshape(-1))
        of_chip = (jnp.arange(experts)[:, None] // sub == jnp.arange(n_chip)[None, :]).astype(F32)
        per_chip = jnp.dot(upto.reshape(-1, experts).astype(F32), of_chip).reshape(group, n_seg + 1, n_chip)
        rows = (per_chip[:, 1:] - per_chip[:, :-1]).astype(I32)
        rows_a = jnp.sum(rows.reshape(n_y, n_ep, n_seg, n_chip), axis=0)
        rows_b = jnp.sum(rows.reshape(n_y, n_x, 2, n_seg, n_chip), axis=1)
        need_a = jnp.max(jnp.maximum(rows_a[:, 0], head) + rows_a[:, 1])
        need_b = jnp.max(jnp.maximum(rows_b[:, :, 2], head) + rows_b[:, :, 3])
        late_first = jnp.max(rows[:, ::2]) > early
        tiers = [(base_a * q // 256, base_b * q // 256) for q in SIZES] + [(slots_a, slots_b)]
        limits = jnp.array(tiers[:-1], I32)
        over = jnp.logical_or(need_a > limits[:, 0], need_b > limits[:, 1])
        index = jnp.sum(jnp.logical_or(over, late_first).astype(I32))
        within = toks[:experts]
        for lo, hi in zip(bounds[1:-1], bounds[:-2]):
            within = jnp.where(toks[:experts] >= lo, within - (lo - hi), within)
        rows_at = plan_rows(n_y, n_x, head, levels, place)

        def up_x(v, d):
            return lax.ppermute(v, 'ep', [(i, (i + 2 * d) % n_ep) for i in range(n_ep)]) if d else v

        def up_y(v, d):
            return lax.ppermute(v, 'ep2', [(i, (i + d) % n_y) for i in range(n_y)]) if d else v

        tables = []
        for v in (within, wgts[:experts]):
            grid = v.reshape(n_y, n_x, sub, LANES)
            tables += [up_y(lax.dynamic_index_in_dim(grid, (y + d) % n_y, 0).reshape(-1), d) for d in range(n_y)]
            tables += [up_x(lax.dynamic_index_in_dim(grid, (x + d) % n_x, 1).reshape(-1), d) for d in range(n_x)]
        lists, levels, rows_at, index, tables = lax.optimization_barrier((lists, levels, rows_at, index, tables))

        weights = (w_a, w_a_sib, w_b, w_b_sib)
        direct_x, direct_y = direct_of(n_x), direct_of(n_y)
        n_early = (len(direct_x), len(direct_y))
        first = run_experts(0, early, late, n_early, lists, place, chunks[0], *weights, (n_x * slots_a, n_y * slots_b))
        (send_a, *heads_a), (send_b, *heads_b) = take(first, 1 + 2 * n_early[0])
        early_a, late_a = take(heads_a, n_early[0])
        early_b, late_b = take(heads_b, n_early[1])

        def to_neighbours(rows_x, rows_y):
            return [up_x(v, d) for v, d in zip(rows_x, direct_x)] + [up_y(v, d) for v, d in zip(rows_y, direct_y)]

        earlies = to_neighbours(early_a, early_b)
        send_b, = run_experts(1, early, late, n_early, lists, place, chunks[1], *weights, send_b)
        sends = (send_a.reshape(n_x, slots_a, sublanes, LANES), send_b.reshape(n_y, slots_b, sublanes, LANES))

        carried = [head] * (len(tiers) - 1) + [early]
        recvs = lax.switch(index, [
            functools.partial(spread, a, b, skip, i, n_y, n_x) for i, ((a, b), skip) in enumerate(zip(tiers, carried))], *sends)
        recvs, late_a, late_b = lax.optimization_barrier((recvs, late_a, late_b))
        lates = to_neighbours(late_a, late_b)
        common = (bounds, levels, rows_at, place, tables, recvs, sends)
        begun = weighted_sums(n_y, n_x, (0,), early, 0, *common, earlies)
        got = (up_y(begun[0], 1), up_y(begun[1], -1), up_x(begun[2], 1), up_x(begun[3], -1))
        rest = weighted_sums(n_y, n_x, tuple(range(1, max(n_y, n_x))), early, late, *common, [*earlies, *lates])
        return reduce_back(len(tiers), n_y, n_x, bounds, got, rest, x_loc)

    tok_spec = P(('dp', 'ep2', 'ep'), None)
    w_spec = P(dev_axes, None, None)
    return jax.shard_map(local_step, mesh=mesh, in_specs=(tok_spec, tok_spec, tok_spec, w_spec, w_spec), out_specs=tok_spec, check_vma=False)
```

```python
import collections
import functools
import math

import jax
import jax.numpy as jnp
from jax import lax
from jax.experimental import pallas as pl
from jax.experimental.pallas import tpu as pltpu
from jax.sharding import PartitionSpec as P

LANES = 128
SEGMENTS = (0, 17, 34, 49, 64)
CHUNKS = (0, 3, 4)
SIZES = (80, 82, 84, 86, 88, 90, 92, 94, 97, 102)
TILE = 256
PREFIX_ROWS = 8
BF16 = jnp.bfloat16
F32 = jnp.float32
I32 = jnp.int32
HBM = pl.BlockSpec(memory_space=pl.ANY)
SMEM = pl.BlockSpec(memory_space=pltpu.SMEM)
VMEM = pl.BlockSpec(memory_space=pltpu.VMEM)
BOTH = range(2)
UNROLL = 8
BLOCK = 16
PAIR = pltpu.SemaphoreType.DMA((2,))
COST = pl.CostEstimate(flops=2 * 10 ** 10, bytes_accessed=10 ** 7, transcendentals=0)
VMEM_LIMIT = 64_000_000
LOCAL = pltpu.CompilerParams(vmem_limit_bytes=VMEM_LIMIT)
MIXED = pltpu.CompilerParams(vmem_limit_bytes=VMEM_LIMIT)


def remote_params(cid):
    return pltpu.CompilerParams(collective_id=cid, has_side_effects=True, vmem_limit_bytes=VMEM_LIMIT)


def take(refs, n):
    return refs[:n], refs[n:]


def start(copy):
    copy.start()


def wait(copy):
    copy.wait()


def capacity_of(group_size, n_tok, n_top, experts):
    return 8 * ((5 * group_size * n_tok * n_top) // (32 * experts))


def far_of(n):
    return n // 2 if n % 2 == 0 and n >= 4 else 0


def direct_of(n):
    return [d for d in range(1, n) if d != far_of(n)]


def bounds_of(n_tok):
    return tuple(16 * ((n_tok * q + 512) // 1024) for q in SEGMENTS)


def tokens_of(bounds, path, w):
    lo, hi = bounds[2 * path + w:][:2]
    return hi - lo


def order_of(n, w):
    return [n - 1 - s if w == 0 else (1 + s) % n for s in range(n)]


def route_kernel(bounds, ids_ref, gate_ref, tok_ref, wgt_ref, cnt_ref, code_t, gate_t, tok_acc, wgt_acc):
    n_tok, n_top = ids_ref.shape
    lane = lax.broadcasted_iota(I32, (n_tok, LANES), 1)
    member = jnp.zeros((n_tok, LANES), F32)
    gates = jnp.zeros((n_tok, LANES), F32)
    for j in range(n_top):
        hit = ids_ref[:, j:j + 1] == lane
        member = member + jnp.where(hit, 1.0, 0.0)
        gates = gates + jnp.where(hit, gate_ref[:, j:j + 1], 0.0)
    member_b = member.astype(BF16)
    row_block = min(n_tok, 128)
    for i in range(n_tok // row_block):
        rows = pl.ds(i * row_block, row_block)
        later = lax.broadcasted_iota(I32, (row_block, n_tok), 0) + i * row_block
        earlier = lax.broadcasted_iota(I32, (row_block, n_tok), 1)
        tri = jnp.where(earlier < later, 1.0, 0.0).astype(BF16)
        rank = jnp.dot(tri, member_b, preferred_element_type=F32)
        mem = member[i * row_block:(i + 1) * row_block]
        code_t[:, rows] = jnp.where(mem > 0.5, rank, -1.0).T
        gate_t[:, rows] = gates[i * row_block:(i + 1) * row_block].T
    total = jnp.zeros((1, LANES), F32)
    rows_out = [total]
    for lo, hi in zip(bounds[:-1], bounds[1:]):
        total = total + jnp.sum(member[lo:hi], axis=0, keepdims=True)
        rows_out.append(total)
    while len(rows_out) < PREFIX_ROWS:
        rows_out.append(total)
    cnt_ref[...] = jnp.concatenate(rows_out, axis=0).astype(I32)
    tok_acc[...] = jnp.zeros_like(tok_acc)
    wgt_acc[...] = jnp.zeros_like(wgt_acc)
    slot = lax.broadcasted_iota(I32, (LANES, n_tok), 0).astype(F32)
    token = lax.broadcasted_iota(I32, (1, n_tok), 1).astype(F32)
    out_lane = lax.broadcasted_iota(I32, (LANES, LANES), 1)

    def one_expert(e, carry):
        hit = slot == code_t[pl.ds(e, 1), :]
        tok = jnp.sum(jnp.where(hit, token, 0.0), axis=1, keepdims=True)
        wgt = jnp.sum(jnp.where(hit, gate_t[pl.ds(e, 1), :], 0.0), axis=1, keepdims=True)
        tok_acc[...] = jnp.where(out_lane == e, tok, tok_acc[...])
        wgt_acc[...] = jnp.where(out_lane == e, wgt, wgt_acc[...])
        return carry

    lax.fori_loop(0, LANES, one_expert, 0)
    tok_ref[...] = tok_acc[...].T.astype(I32)
    wgt_ref[...] = wgt_acc[...].T


def route(ids, gate, bounds):
    n_tok = ids.shape[0]
    return pl.pallas_call(
        functools.partial(route_kernel, bounds),
        out_shape=(
            jax.ShapeDtypeStruct((LANES, LANES), I32),
            jax.ShapeDtypeStruct((LANES, LANES), F32),
            jax.ShapeDtypeStruct((PREFIX_ROWS, LANES), I32),
        ),
        in_specs=[VMEM, VMEM],
        out_specs=(VMEM, VMEM, VMEM),
        scratch_shapes=[
            pltpu.VMEM((LANES, n_tok), F32),
            pltpu.VMEM((LANES, n_tok), F32),
            pltpu.VMEM((LANES, LANES), F32),
            pltpu.VMEM((LANES, LANES), F32),
        ],
        cost_estimate=COST,
        name='route',
    )(ids, gate)


def list_kernel(cap, slots_a, slots_b, early, bounds, n_y, n_x, sub, place_ref, info_ref,
                src_ref, start_ref, len_ref, dst_ref, lim_ref, dir_ref, span_ref, kept_ref, base_ref, lim_tab, dir_tab):
    core, chip = place_ref[0], place_ref[1]
    n_dst = n_y * n_x
    n_seg, n_chunk = len(bounds) - 1, len(CHUNKS) - 1
    dev_words = (sub + PREFIX_ROWS) * LANES
    width = src_ref.shape[0] // sub
    my_y, my_x = chip // n_x, chip % n_x

    def count(g, k, e):
        return info_ref[g * dev_words + (sub + k) * LANES + chip * sub + e]

    def per_expert(e, carry):
        def per_dev(i, off):
            for c in BOTH:
                n = count(2 * i + c, n_seg, e)
                kept = jnp.clip(cap - off, 0, n)
                off = off + n

                @pl.when(core == c)
                def _():
                    kept_ref[i * sub + e] = kept
            return off
        lax.fori_loop(0, n_dst, per_dev, 0)
        return carry

    lax.fori_loop(0, sub, per_expert, 0)

    def rows_in(k, i, e):
        g, kept = 2 * i + core, kept_ref[i * sub + e]
        return jnp.minimum(count(g, k + 1, e), kept) - jnp.minimum(count(g, k, e), kept)

    def block_bases(path, n_blocks, n_inner, slots, index):
        for d in range(n_blocks):
            acc = jnp.int32(d * slots)
            for w in BOTH:
                for r in order_of(n_inner, w):
                    i = index(d, r)

                    def add(e, acc):
                        base_ref[((2 * path + w) * n_dst + i) * sub + e] = acc
                        return acc + rows_in(2 * path + w, i, e)

                    acc = lax.fori_loop(0, sub, add, acc)
                    direct = direct_of(n_blocks)
                    lim_tab[path * n_dst + i] = d * slots + early if d in direct else 0
                    dir_tab[path * n_dst + i] = direct.index(d) if d in direct else 0
                if w == 0:
                    acc = jnp.maximum(acc, d * slots + early)

    block_bases(0, n_x, n_y, slots_a, lambda d, r: lax.rem(my_y + r, n_y) * n_x + lax.rem(my_x + d, n_x))
    block_bases(1, n_y, n_x, slots_b, lambda d, r: lax.rem(my_y + d, n_y) * n_x + lax.rem(my_x + r, n_x))

    def expert_lists(e, carry):
        pos = e * width
        for chunk, (chunk_lo, chunk_hi) in enumerate(zip(CHUNKS[:-1], CHUNKS[1:])):
            size = bounds[chunk_hi] - bounds[chunk_lo]
            start_at = pos
            for k in range(chunk_lo, chunk_hi):

                def segment(i, o):
                    g = 2 * i + core
                    kept = kept_ref[i * sub + e]
                    s0 = jnp.minimum(count(g, k, e), kept)
                    n = jnp.minimum(count(g, k + 1, e), kept) - s0
                    j = (e * n_seg + k) * n_dst + i
                    start_ref[j] = o
                    len_ref[j] = n
                    dst_ref[j] = base_ref[(k * n_dst + i) * sub + e]
                    lim_ref[j] = lim_tab[(k // 2) * n_dst + i]
                    dir_ref[j] = dir_tab[(k // 2) * n_dst + i]
                    src0 = g * size - bounds[chunk_lo]
                    tok0 = g * dev_words + e * LANES + s0

                    def block(b, c):
                        vals = [info_ref[tok0 + b * UNROLL + q] for q in range(UNROLL)]
                        for q in range(UNROLL):
                            src_ref[o + b * UNROLL + q] = src0 + vals[q]
                        return c

                    lax.fori_loop(0, pl.cdiv(n, UNROLL), block, 0)
                    return o + n

                pos = lax.fori_loop(0, n_dst, segment, pos)
            span_ref[(e * n_chunk + chunk) * 2] = start_at
            span_ref[(e * n_chunk + chunk) * 2 + 1] = pos - start_at

            def pad(b, c):
                for q in range(UNROLL):
                    src_ref[pos + b * UNROLL + q] = b * UNROLL + q
                return c

            lax.fori_loop(0, TILE // UNROLL, pad, 0)
            pos = pos + TILE
        return carry

    lax.fori_loop(0, sub, expert_lists, 0)


def build_lists(place, info, cap, slots_a, slots_b, early, bounds, n_y, n_x, sub):
    n_dst, n_seg = n_y * n_x, len(bounds) - 1
    n_chunk = len(CHUNKS) - 1
    width = LANES * n_dst + n_chunk * TILE + UNROLL
    segs = sub * n_seg * n_dst + UNROLL
    return pl.pallas_call(
        functools.partial(list_kernel, cap, slots_a, slots_b, early, bounds, n_y, n_x, sub),
        out_shape=(
            jax.ShapeDtypeStruct((sub * width,), I32),
            *[jax.ShapeDtypeStruct((segs,), I32) for _ in range(5)],
            jax.ShapeDtypeStruct((sub * n_chunk * 2,), I32),
        ),
        in_specs=[SMEM, SMEM],
        out_specs=(SMEM,) * 7,
        scratch_shapes=[
            pltpu.SMEM((n_dst * sub,), I32),
            pltpu.SMEM((n_seg * n_dst * sub,), I32),
            pltpu.SMEM((2 * n_dst,), I32),
            pltpu.SMEM((2 * n_dst,), I32),
        ],
        cost_estimate=COST,
        name='row_lists',
    )(place, info)


def gelu(v):
    return 0.5 * v * (1.0 + jnp.tanh(math.sqrt(2.0 / math.pi) * (v + 0.044715 * v * v * v)))


def expert_kernel(chunk, n_seg, early, late, n_early, *refs):
    lo_seg, hi_seg = CHUNKS[chunk:][:2]
    (src, seg_start, seg_len, seg_dst, seg_lim, seg_dir, span, place, x_hbm, wa_own, wa_sib, wb_own, wb_sib), refs = take(refs, 13)
    if lo_seg > 0:
        refs = refs[1:]
    paths, at = [], 0
    for path in BOTH:
        first, last = max(lo_seg, 2 * path), min(hi_seg, 2 * path + 2)
        if first < last:
            n = n_early[path] if lo_seg == 0 else 0
            (send, *heads), _ = take(refs[at:], 1 + 2 * n)
            paths.append((first, last, send, list(zip(*take(heads, n)))))
            at += 1 + 2 * n
    xbuf, xrows, obuf, wa, wb, t_e, t_base, t_cnt, ptr, gsem, ssem, wsem = refs[at:]
    e_loc, d_model, _ = wa_own.shape
    sub = 2 * e_loc
    core = place[0]
    sublanes = d_model // LANES
    n_dst = (seg_start.shape[0] - UNROLL) // (sub * n_seg)

    def span_of(e):
        at = (e * (len(CHUNKS) - 1) + chunk) * 2
        return span[at], span[at + 1]

    def weight_copies(e, act):
        slot = e % 2
        q = e % e_loc

        @pl.when(e // e_loc == core)
        def _():
            act(pltpu.make_async_copy(wa_own.at[q], wa.at[slot], wsem.at[slot, 0]))
            act(pltpu.make_async_copy(wb_own.at[q], wb.at[slot], wsem.at[slot, 1]))

        @pl.when(e // e_loc != core)
        def _():
            act(pltpu.make_async_copy(wa_sib.at[q], wa.at[slot], wsem.at[slot, 0]))
            act(pltpu.make_async_copy(wb_sib.at[q], wb.at[slot], wsem.at[slot, 1]))

    weight_copies(0, start)

    def plan(e, t):
        lo, n = span_of(e)

        def put(i, c):
            t_e[t + i] = e
            t_base[t + i] = lo + i * TILE
            t_cnt[t + i] = jnp.minimum(n - i * TILE, TILE)
            return c

        n_tiles = (n + TILE - 1) // TILE
        lax.fori_loop(0, n_tiles, put, 0)
        return t + n_tiles

    n_all = lax.fori_loop(0, sub, plan, 0)
    for t in BOTH:
        t_base[n_all + t], _ = span_of(0)

    def fetch_row(t, r):
        slot = t % 2
        pltpu.make_async_copy(x_hbm.at[src[t_base[t] + r]], xbuf.at[slot, r], gsem.at[slot]).start()

    def gather_wait(t):
        slot = t % 2
        pltpu.make_async_copy(x_hbm.at[pl.ds(0, TILE)], xbuf.at[slot], gsem.at[slot]).wait()

    def scatter_start(t):
        base, slot = t_base[t], t % 2
        end = base + t_cnt[t]

        for path, (_, last, send, heads) in enumerate(paths):
            j_end = (t_e[t] * n_seg + last) * n_dst

            def more(j):
                return jnp.logical_and(j < j_end, seg_start[j] < end)

            def segment(j):
                first_row = seg_start[j]
                lo = jnp.maximum(first_row, base)
                n = jnp.minimum(first_row + seg_len[j], end) - lo
                to = seg_dst[j] + lo - first_row
                n_head = jnp.clip(seg_lim[j] - to, 0, jnp.maximum(n, 0)) if heads else 0
                n_early = jnp.clip(seg_lim[j] - late - to, 0, n_head) if heads else 0
                in_head = to - seg_lim[j] + late + early

                def put(rows, first, at, n):
                    @pl.when(n > 0)
                    def _():
                        pltpu.make_async_copy(
                            obuf.at[slot, pl.ds(lo - base + first, n)], rows.at[pl.ds(at, n)], ssem.at[slot]).start()

                def put_head(q, early_rows, late_rows):
                    @pl.when(seg_dir[j] == q)
                    def _():
                        put(early_rows, 0, in_head, n_early)
                        put(late_rows, n_early, in_head + n_early - early, n_head - n_early)

                if heads:
                    @pl.when(n_head > 0)
                    def _():
                        for q, rows in enumerate(heads):
                            put_head(q, *rows)

                put(send, n_head, to + n_head, n - n_head)
                return j + 1

            start = ptr[path]
            ptr[path] = jnp.maximum(lax.while_loop(more, segment, start) - 1, start)

    def scatter_wait(t):
        n, slot = t_cnt[t], t % 2
        send = paths[0][2]
        pltpu.make_async_copy(obuf.at[slot, pl.ds(0, n)], send.at[pl.ds(0, n)], ssem.at[slot]).wait()

    def prime(r, c):
        for t in BOTH:
            fetch_row(t, r)
        return c

    lax.fori_loop(0, TILE, prime, 0, unroll=UNROLL)

    def one_expert(e, t_first):
        weight_copies(e, wait)

        @pl.when(e + 1 < sub)
        def _():
            weight_copies(e + 1, start)

        ws = e % 2
        _, n = span_of(e)
        for path, (first, _, _, _) in enumerate(paths):
            ptr[path] = (e * n_seg + first) * n_dst

        def one_tile(i, t):
            slot = t % 2
            gather_wait(t)

            @pl.when(t >= 2)
            def _():
                scatter_wait(t - 2)

            xrows[...] = xbuf[slot].reshape(TILE, d_model)
            for r in range(TILE):
                fetch_row(t + 2, r)
            hidden = gelu(jnp.dot(xrows[...], wa[ws], preferred_element_type=F32)).astype(BF16)
            out = jnp.dot(hidden, wb[ws], preferred_element_type=F32).astype(BF16)
            obuf[slot] = out.reshape(TILE, sublanes, LANES)
            scatter_start(t)
            return t + 1

        return lax.fori_loop(0, (n + TILE - 1) // TILE, one_tile, t_first)

    lax.fori_loop(0, sub, one_expert, 0)
    for back in (2, 1):
        gather_wait(n_all + back)

        @pl.when(n_all >= back)
        def _():
            scatter_wait(n_all - back)


def run_experts(chunk, early, late, n_early, lists, place, x_rows, wa, wa_sib, wb, wb_sib, rows):
    e_loc, d_model, ff = wa.shape
    sub = 2 * e_loc
    sublanes = d_model // LANES
    ops = (*lists, place, x_rows, wa, wa_sib, wb, wb_sib) + (() if chunk == 0 else (rows,))
    n_smem = len(lists) + 1
    max_tiles = sub * (pl.cdiv(lists[0].shape[0] // sub, TILE) + 1) + 2
    if chunk == 0:
        sizes = []
        for n_rows, n in zip(rows, n_early):
            sizes += [n_rows] + [early] * n + [late] * n
    else:
        sizes = [rows.shape[0]]
    return pl.pallas_call(
        functools.partial(expert_kernel, chunk, len(SEGMENTS) - 1, early, late, n_early),
        out_shape=tuple(jax.ShapeDtypeStruct((n, sublanes, LANES), BF16) for n in sizes),
        in_specs=[SMEM] * n_smem + [HBM] * (len(ops) - n_smem),
        out_specs=(HBM,) * len(sizes),
        scratch_shapes=[
            pltpu.VMEM((2, TILE, sublanes, LANES), BF16),
            pltpu.VMEM((TILE, d_model), BF16),
            pltpu.VMEM((2, TILE, sublanes, LANES), BF16),
            pltpu.VMEM((2, d_model, ff), BF16),
            pltpu.VMEM((2, ff, d_model), BF16),
            pltpu.SMEM((max_tiles,), I32),
            pltpu.SMEM((max_tiles,), I32),
            pltpu.SMEM((max_tiles,), I32),
            pltpu.SMEM((2,), I32),
            PAIR, PAIR,
            pltpu.SemaphoreType.DMA((2, 2)),
        ],
        input_output_aliases={} if chunk == 0 else {len(ops) - 1: 0},
        compiler_params=MIXED,
        cost_estimate=COST,
        name='experts',
    )(*ops)


PIECES = 4


class Ring:
    def __init__(self, axis, n_y, n_x):
        y, ec = lax.axis_index('ep2'), lax.axis_index('ep')
        self.axis, self.core = axis, ec % 2
        self.n = n_x if axis == 'x' else n_y
        self.pos = ec // 2 if axis == 'x' else y
        self.direct, self.far = direct_of(self.n), far_of(self.n)

    def place(self, d):
        return lax.rem(self.pos + d + self.n, self.n)

    def device(self, d):
        if self.axis == 'x':
            return {'ep': self.place(d) * 2 + self.core}
        return {'ep2': self.place(d)}

    def remote(self, src, dst, sems, i, d):
        return pltpu.make_async_remote_copy(
            src_ref=src, dst_ref=dst, send_sem=sems.at[0, i], recv_sem=sems.at[1, i],
            device_id=self.device(d), device_id_type=pl.DeviceIdType.MESH)

    def signal(self, barrier):
        for d in range(1, self.n):
            pl.semaphore_signal(barrier, inc=1, device_id=self.device(d), device_id_type=pl.DeviceIdType.MESH)


def spread_kernel(rows_a, rows_b, early, n_y, n_x, send_a, send_b, recv_a, recv_b, stage_a, stage_b, sem_a, sem_b):
    rings = (Ring('x', n_y, n_x), Ring('y', n_y, n_x))
    barrier = pltpu.get_barrier_semaphore()
    for ring in rings:
        ring.signal(barrier)
    pl.semaphore_wait(barrier, n_x + n_y - 2)

    sides = list(zip(rings, (rows_a, rows_b), (send_a, send_b), (recv_a, recv_b), (stage_a, stage_b), (sem_a, sem_b)))

    def lead(side, p):
        ring, rows, send, _, stage, sem = side
        hop = ring.far // 2 if p % 2 == 0 else -(ring.far // 2)
        part = pl.ds(p * (rows // PIECES), rows // PIECES)
        return ring.remote(send.at[ring.far, part], stage.at[part], sem, p, hop)

    def follow(side, p):
        ring, rows, _, recv, stage, sem = side
        hop = ring.far // 2 if p % 2 == 0 else -(ring.far // 2)
        part = pl.ds(p * (rows // PIECES), rows // PIECES)
        return ring.remote(stage.at[part], recv.at[ring.far, part], sem, PIECES + p, hop)

    def straight(side, i):
        ring, rows, send, recv, _, sem = side
        d = ring.direct[i]
        part = pl.ds(early, rows - early)
        return ring.remote(send.at[d, part], recv.at[d, part], sem, 2 * PIECES + i, d)

    relayed = [(side, p) for p in range(PIECES) for side in sides if side[0].far]
    direct = [(side, i) for side in sides for i in range(len(side[0].direct))]
    for job in relayed:
        lead(*job).start()
    for job in direct:
        straight(*job).start()
    for job in relayed:
        lead(*job).wait_recv()
        follow(*job).start()
    for job in relayed:
        lead(*job).wait_send()
    for job in direct:
        straight(*job).wait()
    for job in relayed:
        follow(*job).wait()


def spread(rows_a, rows_b, early, cid, n_y, n_x, send_a, send_b):
    return pl.pallas_call(
        functools.partial(spread_kernel, rows_a, rows_b, early, n_y, n_x),
        out_shape=tuple(jax.ShapeDtypeStruct(s, BF16) for s in (send_a.shape, send_b.shape, send_a.shape[1:], send_b.shape[1:])),
        in_specs=[HBM, HBM],
        out_specs=(HBM,) * 4,
        scratch_shapes=[
            pltpu.SemaphoreType.DMA((2, 2 * PIECES + n_x)),
            pltpu.SemaphoreType.DMA((2, 2 * PIECES + n_y)),
        ],
        compiler_params=remote_params(cid),
        name='spread_%d_%d' % (rows_a, rows_b),
    )(send_a, send_b)[:2]


WAYS = 4


Path = collections.namedtuple('Path', ('recv', 'send', 'earlies', 'lates', 'at', 'blocks', 'out_at', 'steps'))


def spot(n_y, n_x, p, d, w, s):
    most = max(n_y, n_x)
    return (((p * most + d) * 2 + w) * most + s) * 2


def list_at(n_y, n_x, sub, my, p, s, w, d, level):
    at, blocks, out_at, steps = (my[1], n_x, my[0], n_y) if p == 0 else (my[0], n_y, my[1], n_x)
    out = lax.rem(out_at + order_of(steps, w)[s], steps)
    return ((out * 3 + level) * blocks + lax.rem(at + blocks - d, blocks)) * sub


def plan_kernel(n_y, n_x, early, lev_a, lev_b, place, rows_at):
    chip = place[1]
    sub = lev_a.shape[0] // (3 * n_y * n_x)
    for p, levels in enumerate((lev_a, lev_b)):
        blocks, steps = ((n_x, n_y), (n_y, n_x))[p]
        for d in range(blocks):
            acc = jnp.int32(0)
            for w in BOTH:
                for s in range(steps):
                    lower, upper = (list_at(n_y, n_x, sub, (chip // n_x, chip % n_x), p, s, w, d, w + up) for up in BOTH)

                    def add(e, n):
                        return n + levels[upper + e] - levels[lower + e]

                    n = lax.fori_loop(0, sub, add, jnp.int32(0))
                    at = spot(n_y, n_x, p, d, w, s)
                    rows_at[at] = acc
                    rows_at[at + 1] = n
                    acc = acc + n
                if not w:
                    acc = jnp.maximum(acc, early)


def plan_rows(n_y, n_x, early, levels, place):
    most = max(n_y, n_x)
    return pl.pallas_call(
        functools.partial(plan_kernel, n_y, n_x, early),
        out_shape=jax.ShapeDtypeStruct((8 * most * most,), I32),
        in_specs=[SMEM] * 3,
        out_specs=SMEM,
        cost_estimate=COST,
        name='plan_rows',
    )(*levels, place)


def sum_kernel(n_y, n_x, passes, early, late, bounds, *refs):
    (lev_a, lev_b, rows_at, place, recv_a, recv_b, send_a, send_b), refs = take(refs, 8)
    tables_in = []
    for _ in BOTH:
        tok_y, refs = take(refs, n_y)
        tok_x, refs = take(refs, n_x)
        tables_in.append((tok_y, tok_x))
    early_a, refs = take(refs, len(direct_of(n_x)))
    early_b, refs = take(refs, len(direct_of(n_y)))
    late_a, refs = take(refs, len(direct_of(n_x)) if late else 0)
    late_b, refs = take(refs, len(direct_of(n_y)) if late else 0)
    chip = place[1]
    my_y, my_x = chip // n_x, chip % n_x
    sub = lev_a.shape[0] // (3 * n_y * n_x)
    words = sub * LANES
    paths = (
        Path(recv_a, send_a, early_a, late_a, my_x, n_x, my_y, n_y),
        Path(recv_b, send_b, early_b, late_b, my_y, n_y, my_x, n_x),
    )
    todo = [(p, s) for p in BOTH for s in passes if s < paths[p].steps]
    outs, refs = take(refs, 2 * len(todo))
    (tok, wgt, *bufs), refs = take(refs, 4)
    accs, (tsem, rsem, zsem) = take(refs, 2 * WAYS)
    ways = [accs[:WAYS], accs[WAYS:]]
    table_of, size = {}, 0
    for p, s in todo:
        for w in BOTH:
            table_of[p, s, w] = size
            size += paths[p].blocks * words

    def source(p, d):
        return lax.rem(paths[p].at + paths[p].blocks - d, paths[p].blocks)

    def tables(p, s, act):
        for w in BOTH:
            sender = (paths[p].steps - order_of(paths[p].steps, w)[s]) % paths[p].steps
            for d in range(paths[p].blocks):
                src = pl.ds(pl.multiple_of(source(p, d) * words, words), words)
                dst = pl.ds(table_of[p, s, w] + d * words, words)
                for held, table in zip(tables_in, (tok, wgt)):
                    act(pltpu.make_async_copy(held[p][sender].at[src], table.at[dst], tsem.at[todo.index((p, s))]))

    jobs = [(p, s, d) for p, s in todo for d in range(paths[p].blocks)]

    def fetch(job, act):
        p, s, d = jobs[job]
        path = paths[p]
        slot = job % 2
        for w in BOTH:
            first, n = (rows_at[spot(n_y, n_x, p, d, w, s) + i] for i in BOTH)
            to = bufs[w].at[slot]
            main = path.recv if d else path.send

            def get(rows, at, done, n):
                @pl.when(n > 0)
                def _():
                    act(pltpu.make_async_copy(rows.at[pl.ds(at, n)], to.at[pl.ds(done, n)], rsem.at[slot]))

            done = 0
            if not w and d in direct_of(path.blocks):
                q = direct_of(path.blocks).index(d)
                done = jnp.clip(early - first, 0, n)
                get(path.earlies[q], first, 0, done)
                if late:
                    n_late = jnp.clip(early + late - first, 0, n) - done
                    get(path.lates[q], first + done - early, done, n_late)
                    done = done + n_late
            get(main.at[d], first + done, done, n - done)

    def zero(acc):
        def body(b, c):
            acc[pl.ds(b * BLOCK, BLOCK)] = jnp.zeros((BLOCK, *acc.shape[1:]), F32)
            return c
        lax.fori_loop(0, (acc.shape[0] - 8) // BLOCK, body, 0)

    fetch(0, start)
    for p, s in todo:
        tables(p, s, start)
    puts = []
    for job, (p, s, d) in enumerate(jobs):
        slot = job % 2
        levels = (lev_a, lev_b)[p]
        dummy = accs[0].shape[0] - 8
        if not d:
            for _, *others in ways:
                for acc in others:
                    zero(acc)
            for put in puts:
                put.wait()
            for target, *_ in ways:
                zero(target)
            tables(p, s, wait)
        fetch(job, wait)
        if job + 1 < len(jobs):
            fetch(job + 1, start)

        def one_expert(e, bases):
            counts, firsts = [], []
            for w in BOTH:
                lower, upper = (levels[list_at(n_y, n_x, sub, (my_y, my_x), p, s, w, d, w + up) + e] for up in BOTH)
                counts.append(upper - lower)
                firsts.append(table_of[p, s, w] + d * words + e * LANES + lower)
            longest = jnp.maximum(counts[0], counts[1])

            def group(b, cc):
                adds = []
                for w in BOTH:
                    for q in range(WAYS):
                        r = b * WAYS + q
                        row = bufs[w][slot, bases[w] + r].astype(F32)
                        t = jnp.where(r < counts[w], tok[firsts[w] + r], dummy)
                        adds.append((ways[w][q], t, wgt[firsts[w] + r] * row))
                for acc, t, row in adds:
                    acc[t] = acc[t] + row
                return cc

            lax.fori_loop(0, lax.shift_right_logical(longest + (WAYS - 1), 2), group, 0)
            return bases[0] + counts[0], bases[1] + counts[1]

        lax.fori_loop(0, sub, one_expert, (jnp.int32(0), jnp.int32(0)))
        if d + 1 == paths[p].blocks:
            puts = []
            for w in BOTH:
                target, second, third, fourth = ways[w]
                size = tokens_of(bounds, p, w)

                def merge(b, c):
                    rows = pl.ds(b * BLOCK, BLOCK)
                    target[rows] = (target[rows] + second[rows]) + (third[rows] + fourth[rows])
                    return c

                lax.fori_loop(0, size // BLOCK, merge, 0)
                out = outs[2 * todo.index((p, s)) + w]
                puts.append(pltpu.make_async_copy(target.at[pl.ds(0, size)], out, zsem.at[w]))
                puts[-1].start()
    for put in puts:
        put.wait()


def weighted_sums(n_y, n_x, passes, early, late, bounds, levels, rows_at, place, tables, recvs, sends, heads):
    sublanes = recvs[0].shape[2]
    sub = levels[0].shape[0] // (3 * n_y * n_x)
    todo = [(p, s) for p, n in enumerate((n_y, n_x)) for s in passes if s < n]
    sizes = [tokens_of(bounds, p, w) for p, _ in todo for w in BOTH]
    table = sum((n_x if p == 0 else n_y) * 2 * sub * LANES for p, _ in todo) + 2 * LANES
    tokens = max(b - a for a, b in zip(bounds[:-1], bounds[1:]))
    ops = (*levels, rows_at, place, *recvs, *sends, *tables, *heads)
    return pl.pallas_call(
        functools.partial(sum_kernel, n_y, n_x, passes, early, late, bounds),
        out_shape=tuple(jax.ShapeDtypeStruct((n, sublanes, LANES), F32) for n in sizes),
        in_specs=[SMEM] * 4 + [HBM] * (len(ops) - 4),
        out_specs=(HBM,) * len(sizes),
        scratch_shapes=[
            pltpu.SMEM((table,), I32),
            pltpu.SMEM((table,), F32),
            *[pltpu.VMEM((2, sub * LANES + LANES, sublanes, LANES), BF16) for _ in BOTH],
            *[pltpu.VMEM((tokens + 8, sublanes, LANES), F32) for _ in range(2 * WAYS)],
            pltpu.SemaphoreType.DMA((len(todo),)),
            PAIR, PAIR,
        ],
        compiler_params=LOCAL,
        cost_estimate=COST,
        name='weighted_sums',
    )(*ops)


SUM_CHUNKS = 8


def pieces_of(n):
    cuts = [BLOCK * ((n // BLOCK * j) // SUM_CHUNKS) for j in range(SUM_CHUNKS + 1)]
    return [(a, b - a) for a, b in zip(cuts[:-1], cuts[1:]) if b > a]


def reduce_kernel(n_y, n_x, bounds, *refs):
    sizes = (n_y, n_x)
    lanes = [(p, w) for p in BOTH for w in BOTH]
    got, refs = take(refs, len(lanes))
    got = dict(zip(lanes, got))
    sums = {}
    for p, n in enumerate(sizes):
        for s in range(1, n):
            for w in BOTH:
                (sums[p, s, w],), refs = take(refs, 1)
    (x_ref, y_ref), refs = take(refs, 2)
    part, own = {}, {}
    for p, w in lanes:
        for s in range(sizes[p] - 1):
            (part[p, w, s], own[p, w, s]), refs = take(refs, 2)
    zsem, gsem, rsem = refs
    rings = (Ring('y', n_y, n_x), Ring('x', n_y, n_x))
    d_model = x_ref.shape[1]
    pieces = {(p, w): pieces_of(tokens_of(bounds, p, w)) for p, w in lanes}
    order = [(p, w, j) for j in range(SUM_CHUNKS) for p, w in lanes if j < len(pieces[p, w])]

    barrier = pltpu.get_barrier_semaphore()
    for ring in rings:
        for d in (1, -1):
            pl.semaphore_signal(barrier, inc=1, device_id=ring.device(d), device_id_type=pl.DeviceIdType.MESH)
    pl.semaphore_wait(barrier, 4)

    def rows_of(p, w, j):
        return pl.ds(*pieces[p, w][j])

    def load(p, w, s, j):
        r = rows_of(p, w, j)
        return pltpu.make_async_copy(sums[p, s, w].at[r], own[p, w, s - 1].at[r], zsem.at[p, w, s - 1, j])

    def begin(p, w, j):
        r = rows_of(p, w, j)
        return pltpu.make_async_copy(got[p, w].at[r], part[p, w, 0].at[r], gsem.at[p, w, j])

    def hop(p, w, s, j):
        r = rows_of(p, w, j)
        return pltpu.make_async_remote_copy(
            src_ref=part[p, w, s - 1].at[r], dst_ref=part[p, w, s].at[r],
            send_sem=rsem.at[0, p, w, s, j], recv_sem=rsem.at[1, p, w, s, j],
            device_id=rings[p].device(1 if w == 0 else -1), device_id_type=pl.DeviceIdType.MESH)

    def arrive(p, w, s, j):
        if s == 0:
            begin(p, w, j).wait()
        else:
            hop(p, w, s, j).wait_recv()

    last = max(sizes) - 1
    for p, w, j in order:
        begin(p, w, j).start()
        load(p, w, 1, j).start()

    for s in range(1, last):
        for p, w, j in order:
            if s >= sizes[p] - 1:
                continue
            load(p, w, s, j).wait()
            arrive(p, w, s - 1, j)
            into, more = part[p, w, s - 1], own[p, w, s - 1]
            first, n = pieces[p, w][j]

            def add(b, c):
                r = pl.ds(first + b * BLOCK, BLOCK)
                into[r] = into[r] + more[r]
                return c

            lax.fori_loop(0, n // BLOCK, add, 0)
            hop(p, w, s, j).start()
            load(p, w, s + 1, j).start()

    for p, w, j in order:
        s = sizes[p] - 1
        load(p, w, s, j).wait()
        arrive(p, w, s - 1, j)
        into, more = part[p, w, s - 1], own[p, w, s - 1]
        first, n = pieces[p, w][j]
        token = bounds[2 * p + w] + first

        def finish(b, c):
            r = pl.ds(first + b * BLOCK, BLOCK)
            out = pl.ds(pl.multiple_of(token + b * BLOCK, BLOCK), BLOCK)
            total = into[r] + more[r]
            y_ref[out, :] = (x_ref[out, :].astype(F32) + total.reshape(BLOCK, d_model)).astype(BF16)
            return c

        lax.fori_loop(0, n // BLOCK, finish, 0)
    for s in range(1, last):
        for p, w, j in order:
            if s < sizes[p] - 1:
                hop(p, w, s, j).wait_send()


def reduce_back(cid, n_y, n_x, bounds, got, sums, x):
    n_tok, d_model = x.shape
    sublanes = d_model // LANES
    bufs = []
    for p, n in enumerate((n_y, n_x)):
        for w in BOTH:
            size = tokens_of(bounds, p, w)
            bufs += [pltpu.VMEM((size, sublanes, LANES), F32)] * (2 * (n - 1))
    steps = max(n_y, n_x) - 1
    ops = (*got, *sums, x)
    return pl.pallas_call(
        functools.partial(reduce_kernel, n_y, n_x, bounds),
        out_shape=jax.ShapeDtypeStruct((n_tok, d_model), BF16),
        in_specs=[HBM] * (len(ops) - 1) + [VMEM],
        out_specs=VMEM,
        scratch_shapes=[
            *bufs,
            pltpu.SemaphoreType.DMA((2, 2, steps, SUM_CHUNKS)),
            pltpu.SemaphoreType.DMA((2, 2, SUM_CHUNKS)),
            pltpu.SemaphoreType.DMA((2, 2, 2, steps, SUM_CHUNKS)),
        ],
        compiler_params=remote_params(cid),
        name='reduce_back',
    )(*ops)


def solution(mesh):
    dev_axes = ('ep2', 'ep')
    n_y, n_ep = mesh.shape['ep2'], mesh.shape['ep']
    n_x = n_ep // 2
    group = n_y * n_ep
    n_chip = n_y * n_x

    def local_step(x_loc, ids_loc, gate_loc, w_a, w_b):
        n_tok, d_model = x_loc.shape
        n_top = ids_loc.shape[1]
        e_loc = w_a.shape[0]
        sub = 2 * e_loc
        experts = e_loc * group
        cap = capacity_of(group, n_tok, n_top, experts)
        sublanes = d_model // LANES
        base_a, base_b = n_y * sub * LANES, n_x * sub * LANES
        late = min(base_a, base_b) // 16
        early = late + late // 2
        head = early + late
        slots_a, slots_b = base_a + head, base_b + head
        bounds = bounds_of(n_tok)
        n_seg, n_chunk = len(bounds) - 1, len(CHUNKS) - 1
        me = lax.axis_index(dev_axes)
        core, chip = me % 2, me // 2
        place = jnp.stack([core, chip]).astype(I32)

        x3 = x_loc.reshape(n_tok, sublanes, LANES)
        chunks = [lax.all_gather(x3[bounds[CHUNKS[k]]:bounds[CHUNKS[k + 1]]], dev_axes, tiled=True) for k in range(n_chunk)]
        swap = [(i, i ^ 1) for i in range(n_ep)]
        w_a_sib = lax.ppermute(w_a, 'ep', swap)
        w_b_sib = lax.ppermute(w_b, 'ep', swap)

        toks, wgts, cnts = route(ids_loc, gate_loc, bounds)
        for_chip = toks[:experts].reshape(n_chip, 1, sub, LANES)
        table = jnp.concatenate([
            jnp.broadcast_to(for_chip, (n_chip, 2, sub, LANES)).reshape(group, sub, LANES),
            jnp.broadcast_to(cnts[None], (group, PREFIX_ROWS, LANES))], axis=1)
        table = lax.all_to_all(table, dev_axes, 0, 0, tiled=True)
        lists = build_lists(place, table.reshape(-1), cap, slots_a, slots_b, head, bounds, n_y, n_x, sub)

        prefix = table[:, sub:sub + n_seg + 1, :experts]
        totals = prefix[:, n_seg]
        offs = jnp.cumsum(totals, axis=0) - totals
        kept = jnp.clip(cap - offs, 0, totals)
        upto = jnp.minimum(prefix, kept[:, None])
        y, x = chip // n_x, chip % n_x
        level_a = lax.dynamic_slice(upto.reshape(n_y, n_ep, n_seg + 1, experts), (0, x * 2 + core, 0, y * n_x * sub), (n_y, 1, 3, n_x * sub))
        level_b = lax.dynamic_slice(upto.reshape(n_y, n_x, 2, n_seg + 1, experts), (y, 0, core, 2, 0), (1, n_x, 1, 3, experts))
        level_b = lax.dynamic_slice(level_b.reshape(n_x, 3, n_y, n_x * sub), (0, 0, 0, x * sub), (n_x, 3, n_y, sub))
        levels = (level_a.reshape(-1), level_b.reshape(-1))
        of_chip = (jnp.arange(experts)[:, None] // sub == jnp.arange(n_chip)[None, :]).astype(F32)
        per_chip = jnp.dot(upto.reshape(-1, experts).astype(F32), of_chip).reshape(group, n_seg + 1, n_chip)
        rows = (per_chip[:, 1:] - per_chip[:, :-1]).astype(I32)
        rows_a = jnp.sum(rows.reshape(n_y, n_ep, n_seg, n_chip), axis=0)
        rows_b = jnp.sum(rows.reshape(n_y, n_x, 2, n_seg, n_chip), axis=1)
        need_a = jnp.max(jnp.maximum(rows_a[:, 0], head) + rows_a[:, 1])
        need_b = jnp.max(jnp.maximum(rows_b[:, :, 2], head) + rows_b[:, :, 3])
        late_first = jnp.max(rows[:, ::2]) > early
        tiers = [(base_a * q // 256, base_b * q // 256) for q in SIZES] + [(slots_a, slots_b)]
        limits = jnp.array(tiers[:-1], I32)
        over = jnp.logical_or(need_a > limits[:, 0], need_b > limits[:, 1])
        index = jnp.sum(jnp.logical_or(over, late_first).astype(I32))
        within = toks[:experts]
        for lo, hi in zip(bounds[1:-1], bounds[:-2]):
            within = jnp.where(toks[:experts] >= lo, within - (lo - hi), within)
        rows_at = plan_rows(n_y, n_x, head, levels, place)

        def up_x(v, d):
            return lax.ppermute(v, 'ep', [(i, (i + 2 * d) % n_ep) for i in range(n_ep)]) if d else v

        def up_y(v, d):
            return lax.ppermute(v, 'ep2', [(i, (i + d) % n_y) for i in range(n_y)]) if d else v

        tables = []
        for v in (within, wgts[:experts]):
            grid = v.reshape(n_y, n_x, sub, LANES)
            tables += [up_y(lax.dynamic_index_in_dim(grid, (y + d) % n_y, 0).reshape(-1), d) for d in range(n_y)]
            tables += [up_x(lax.dynamic_index_in_dim(grid, (x + d) % n_x, 1).reshape(-1), d) for d in range(n_x)]
        lists, levels, rows_at, index, tables = lax.optimization_barrier((lists, levels, rows_at, index, tables))

        weights = (w_a, w_a_sib, w_b, w_b_sib)
        direct_x, direct_y = direct_of(n_x), direct_of(n_y)
        n_early = (len(direct_x), len(direct_y))
        first = run_experts(0, early, late, n_early, lists, place, chunks[0], *weights, (n_x * slots_a, n_y * slots_b))
        (send_a, *heads_a), (send_b, *heads_b) = take(first, 1 + 2 * n_early[0])
        early_a, late_a = take(heads_a, n_early[0])
        early_b, late_b = take(heads_b, n_early[1])

        def to_neighbours(rows_x, rows_y):
            return [up_x(v, d) for v, d in zip(rows_x, direct_x)] + [up_y(v, d) for v, d in zip(rows_y, direct_y)]

        chunks[1], early_a, early_b = lax.optimization_barrier((chunks[1], early_a, early_b))
        earlies = to_neighbours(early_a, early_b)
        send_b, = run_experts(1, early, late, n_early, lists, place, chunks[1], *weights, send_b)
        sends = (send_a.reshape(n_x, slots_a, sublanes, LANES), send_b.reshape(n_y, slots_b, sublanes, LANES))

        carried = [head] * (len(tiers) - 1) + [early]
        recvs = lax.switch(index, [
            functools.partial(spread, a, b, skip, i, n_y, n_x) for i, ((a, b), skip) in enumerate(zip(tiers, carried))], *sends)
        recvs, late_a, late_b = lax.optimization_barrier((recvs, late_a, late_b))
        lates = to_neighbours(late_a, late_b)
        common = (bounds, levels, rows_at, place, tables, recvs, sends)
        begun = weighted_sums(n_y, n_x, (0,), early, 0, *common, earlies)
        got = (up_y(begun[0], 1), up_y(begun[1], -1), up_x(begun[2], 1), up_x(begun[3], -1))
        rest = weighted_sums(n_y, n_x, tuple(range(1, max(n_y, n_x))), early, late, *common, [*earlies, *lates])
        return reduce_back(len(tiers), n_y, n_x, bounds, got, rest, x_loc)

    tok_spec = P(('dp', 'ep2', 'ep'), None)
    w_spec = P(dev_axes, None, None)
    return jax.shard_map(local_step, mesh=mesh, in_specs=(tok_spec, tok_spec, tok_spec, w_spec, w_spec), out_specs=tok_spec, check_vma=False)
```

```python
import collections
import functools
import math

import jax
import jax.numpy as jnp
from jax import lax
from jax.experimental import pallas as pl
from jax.experimental.pallas import tpu as pltpu
from jax.sharding import PartitionSpec as P

LANES = 128
SEGMENTS = (0, 17, 34, 51, 64)
CHUNKS = (0, 3, 4)
SIZES = (80, 82, 84, 86, 88, 90, 92, 94, 97, 102)
TILE = 256
PREFIX_ROWS = 8
BF16 = jnp.bfloat16
F32 = jnp.float32
I32 = jnp.int32
HBM = pl.BlockSpec(memory_space=pl.ANY)
SMEM = pl.BlockSpec(memory_space=pltpu.SMEM)
VMEM = pl.BlockSpec(memory_space=pltpu.VMEM)
BOTH = range(2)
UNROLL = 8
BLOCK = 16
PAIR = pltpu.SemaphoreType.DMA((2,))
COST = pl.CostEstimate(flops=2 * 10 ** 10, bytes_accessed=10 ** 7, transcendentals=0)
VMEM_LIMIT = 64_000_000
LOCAL = pltpu.CompilerParams(vmem_limit_bytes=VMEM_LIMIT)
MIXED = pltpu.CompilerParams(vmem_limit_bytes=VMEM_LIMIT)


def remote_params(cid):
    return pltpu.CompilerParams(collective_id=cid, has_side_effects=True, vmem_limit_bytes=VMEM_LIMIT)


def take(refs, n):
    return refs[:n], refs[n:]


def start(copy):
    copy.start()


def wait(copy):
    copy.wait()


def capacity_of(group_size, n_tok, n_top, experts):
    return 8 * ((5 * group_size * n_tok * n_top) // (32 * experts))


def far_of(n):
    return n // 2 if n % 2 == 0 and n >= 4 else 0


def direct_of(n):
    return [d for d in range(1, n) if d != far_of(n)]


def bounds_of(n_tok):
    return tuple(16 * ((n_tok * q + 512) // 1024) for q in SEGMENTS)


def tokens_of(bounds, path, w):
    lo, hi = bounds[2 * path + w:][:2]
    return hi - lo


def order_of(n, w):
    return [n - 1 - s if w == 0 else (1 + s) % n for s in range(n)]


def route_kernel(bounds, ids_ref, gate_ref, tok_ref, wgt_ref, cnt_ref, code_t, gate_t, tok_acc, wgt_acc):
    n_tok, n_top = ids_ref.shape
    lane = lax.broadcasted_iota(I32, (n_tok, LANES), 1)
    member = jnp.zeros((n_tok, LANES), F32)
    gates = jnp.zeros((n_tok, LANES), F32)
    for j in range(n_top):
        hit = ids_ref[:, j:j + 1] == lane
        member = member + jnp.where(hit, 1.0, 0.0)
        gates = gates + jnp.where(hit, gate_ref[:, j:j + 1], 0.0)
    member_b = member.astype(BF16)
    row_block = min(n_tok, 128)
    for i in range(n_tok // row_block):
        rows = pl.ds(i * row_block, row_block)
        later = lax.broadcasted_iota(I32, (row_block, n_tok), 0) + i * row_block
        earlier = lax.broadcasted_iota(I32, (row_block, n_tok), 1)
        tri = jnp.where(earlier < later, 1.0, 0.0).astype(BF16)
        rank = jnp.dot(tri, member_b, preferred_element_type=F32)
        mem = member[i * row_block:(i + 1) * row_block]
        code_t[:, rows] = jnp.where(mem > 0.5, rank, -1.0).T
        gate_t[:, rows] = gates[i * row_block:(i + 1) * row_block].T
    total = jnp.zeros((1, LANES), F32)
    rows_out = [total]
    for lo, hi in zip(bounds[:-1], bounds[1:]):
        total = total + jnp.sum(member[lo:hi], axis=0, keepdims=True)
        rows_out.append(total)
    while len(rows_out) < PREFIX_ROWS:
        rows_out.append(total)
    cnt_ref[...] = jnp.concatenate(rows_out, axis=0).astype(I32)
    tok_acc[...] = jnp.zeros_like(tok_acc)
    wgt_acc[...] = jnp.zeros_like(wgt_acc)
    slot = lax.broadcasted_iota(I32, (LANES, n_tok), 0).astype(F32)
    token = lax.broadcasted_iota(I32, (1, n_tok), 1).astype(F32)
    out_lane = lax.broadcasted_iota(I32, (LANES, LANES), 1)

    def one_expert(e, carry):
        hit = slot == code_t[pl.ds(e, 1), :]
        tok = jnp.sum(jnp.where(hit, token, 0.0), axis=1, keepdims=True)
        wgt = jnp.sum(jnp.where(hit, gate_t[pl.ds(e, 1), :], 0.0), axis=1, keepdims=True)
        tok_acc[...] = jnp.where(out_lane == e, tok, tok_acc[...])
        wgt_acc[...] = jnp.where(out_lane == e, wgt, wgt_acc[...])
        return carry

    lax.fori_loop(0, LANES, one_expert, 0)
    tok_ref[...] = tok_acc[...].T.astype(I32)
    wgt_ref[...] = wgt_acc[...].T


def route(ids, gate, bounds):
    n_tok = ids.shape[0]
    return pl.pallas_call(
        functools.partial(route_kernel, bounds),
        out_shape=(
            jax.ShapeDtypeStruct((LANES, LANES), I32),
            jax.ShapeDtypeStruct((LANES, LANES), F32),
            jax.ShapeDtypeStruct((PREFIX_ROWS, LANES), I32),
        ),
        in_specs=[VMEM, VMEM],
        out_specs=(VMEM, VMEM, VMEM),
        scratch_shapes=[
            pltpu.VMEM((LANES, n_tok), F32),
            pltpu.VMEM((LANES, n_tok), F32),
            pltpu.VMEM((LANES, LANES), F32),
            pltpu.VMEM((LANES, LANES), F32),
        ],
        cost_estimate=COST,
        name='route',
    )(ids, gate)


def list_kernel(cap, slots_a, slots_b, early, bounds, n_y, n_x, sub, place_ref, info_ref,
                src_ref, start_ref, len_ref, dst_ref, lim_ref, dir_ref, span_ref, kept_ref, base_ref, lim_tab, dir_tab):
    core, chip = place_ref[0], place_ref[1]
    n_dst = n_y * n_x
    n_seg, n_chunk = len(bounds) - 1, len(CHUNKS) - 1
    dev_words = (sub + PREFIX_ROWS) * LANES
    width = src_ref.shape[0] // sub
    my_y, my_x = chip // n_x, chip % n_x

    def count(g, k, e):
        return info_ref[g * dev_words + (sub + k) * LANES + chip * sub + e]

    def per_expert(e, carry):
        def per_dev(i, off):
            for c in BOTH:
                n = count(2 * i + c, n_seg, e)
                kept = jnp.clip(cap - off, 0, n)
                off = off + n

                @pl.when(core == c)
                def _():
                    kept_ref[i * sub + e] = kept
            return off
        lax.fori_loop(0, n_dst, per_dev, 0)
        return carry

    lax.fori_loop(0, sub, per_expert, 0)

    def rows_in(k, i, e):
        g, kept = 2 * i + core, kept_ref[i * sub + e]
        return jnp.minimum(count(g, k + 1, e), kept) - jnp.minimum(count(g, k, e), kept)

    def block_bases(path, n_blocks, n_inner, slots, index):
        for d in range(n_blocks):
            acc = jnp.int32(d * slots)
            for w in BOTH:
                for r in order_of(n_inner, w):
                    i = index(d, r)

                    def add(e, acc):
                        base_ref[((2 * path + w) * n_dst + i) * sub + e] = acc
                        return acc + rows_in(2 * path + w, i, e)

                    acc = lax.fori_loop(0, sub, add, acc)
                    direct = direct_of(n_blocks)
                    lim_tab[path * n_dst + i] = d * slots + early if d in direct else 0
                    dir_tab[path * n_dst + i] = direct.index(d) if d in direct else 0
                if w == 0:
                    acc = jnp.maximum(acc, d * slots + early)

    block_bases(0, n_x, n_y, slots_a, lambda d, r: lax.rem(my_y + r, n_y) * n_x + lax.rem(my_x + d, n_x))
    block_bases(1, n_y, n_x, slots_b, lambda d, r: lax.rem(my_y + d, n_y) * n_x + lax.rem(my_x + r, n_x))

    def expert_lists(e, carry):
        pos = e * width
        for chunk, (chunk_lo, chunk_hi) in enumerate(zip(CHUNKS[:-1], CHUNKS[1:])):
            size = bounds[chunk_hi] - bounds[chunk_lo]
            start_at = pos
            for k in range(chunk_lo, chunk_hi):

                def segment(i, o):
                    g = 2 * i + core
                    kept = kept_ref[i * sub + e]
                    s0 = jnp.minimum(count(g, k, e), kept)
                    n = jnp.minimum(count(g, k + 1, e), kept) - s0
                    j = (e * n_seg + k) * n_dst + i
                    start_ref[j] = o
                    len_ref[j] = n
                    dst_ref[j] = base_ref[(k * n_dst + i) * sub + e]
                    lim_ref[j] = lim_tab[(k // 2) * n_dst + i]
                    dir_ref[j] = dir_tab[(k // 2) * n_dst + i]
                    src0 = g * size - bounds[chunk_lo]
                    tok0 = g * dev_words + e * LANES + s0

                    def block(b, c):
                        vals = [info_ref[tok0 + b * UNROLL + q] for q in range(UNROLL)]
                        for q in range(UNROLL):
                            src_ref[o + b * UNROLL + q] = src0 + vals[q]
                        return c

                    lax.fori_loop(0, pl.cdiv(n, UNROLL), block, 0)
                    return o + n

                pos = lax.fori_loop(0, n_dst, segment, pos)
            span_ref[(e * n_chunk + chunk) * 2] = start_at
            span_ref[(e * n_chunk + chunk) * 2 + 1] = pos - start_at

            def pad(b, c):
                for q in range(UNROLL):
                    src_ref[pos + b * UNROLL + q] = b * UNROLL + q
                return c

            lax.fori_loop(0, TILE // UNROLL, pad, 0)
            pos = pos + TILE
        return carry

    lax.fori_loop(0, sub, expert_lists, 0)


def build_lists(place, info, cap, slots_a, slots_b, early, bounds, n_y, n_x, sub):
    n_dst, n_seg = n_y * n_x, len(bounds) - 1
    n_chunk = len(CHUNKS) - 1
    width = LANES * n_dst + n_chunk * TILE + UNROLL
    segs = sub * n_seg * n_dst + UNROLL
    return pl.pallas_call(
        functools.partial(list_kernel, cap, slots_a, slots_b, early, bounds, n_y, n_x, sub),
        out_shape=(
            jax.ShapeDtypeStruct((sub * width,), I32),
            *[jax.ShapeDtypeStruct((segs,), I32) for _ in range(5)],
            jax.ShapeDtypeStruct((sub * n_chunk * 2,), I32),
        ),
        in_specs=[SMEM, SMEM],
        out_specs=(SMEM,) * 7,
        scratch_shapes=[
            pltpu.SMEM((n_dst * sub,), I32),
            pltpu.SMEM((n_seg * n_dst * sub,), I32),
            pltpu.SMEM((2 * n_dst,), I32),
            pltpu.SMEM((2 * n_dst,), I32),
        ],
        cost_estimate=COST,
        name='row_lists',
    )(place, info)


def gelu(v):
    return 0.5 * v * (1.0 + jnp.tanh(math.sqrt(2.0 / math.pi) * (v + 0.044715 * v * v * v)))


def expert_kernel(chunk, n_seg, early, late, n_early, *refs):
    lo_seg, hi_seg = CHUNKS[chunk:][:2]
    (src, seg_start, seg_len, seg_dst, seg_lim, seg_dir, span, place, x_hbm, wa_own, wa_sib, wb_own, wb_sib), refs = take(refs, 13)
    if lo_seg > 0:
        refs = refs[1:]
    paths, at = [], 0
    for path in BOTH:
        first, last = max(lo_seg, 2 * path), min(hi_seg, 2 * path + 2)
        if first < last:
            n = n_early[path] if lo_seg == 0 else 0
            (send, *heads), _ = take(refs[at:], 1 + 2 * n)
            paths.append((first, last, send, list(zip(*take(heads, n)))))
            at += 1 + 2 * n
    xbuf, xrows, obuf, wa, wb, t_e, t_base, t_cnt, ptr, gsem, ssem, wsem = refs[at:]
    e_loc, d_model, _ = wa_own.shape
    sub = 2 * e_loc
    core = place[0]
    sublanes = d_model // LANES
    n_dst = (seg_start.shape[0] - UNROLL) // (sub * n_seg)

    def span_of(e):
        at = (e * (len(CHUNKS) - 1) + chunk) * 2
        return span[at], span[at + 1]

    def weight_copies(e, act):
        slot = e % 2
        q = e % e_loc

        @pl.when(e // e_loc == core)
        def _():
            act(pltpu.make_async_copy(wa_own.at[q], wa.at[slot], wsem.at[slot, 0]))
            act(pltpu.make_async_copy(wb_own.at[q], wb.at[slot], wsem.at[slot, 1]))

        @pl.when(e // e_loc != core)
        def _():
            act(pltpu.make_async_copy(wa_sib.at[q], wa.at[slot], wsem.at[slot, 0]))
            act(pltpu.make_async_copy(wb_sib.at[q], wb.at[slot], wsem.at[slot, 1]))

    weight_copies(0, start)

    def plan(e, t):
        lo, n = span_of(e)

        def put(i, c):
            t_e[t + i] = e
            t_base[t + i] = lo + i * TILE
            t_cnt[t + i] = jnp.minimum(n - i * TILE, TILE)
            return c

        n_tiles = (n + TILE - 1) // TILE
        lax.fori_loop(0, n_tiles, put, 0)
        return t + n_tiles

    n_all = lax.fori_loop(0, sub, plan, 0)
    for t in BOTH:
        t_base[n_all + t], _ = span_of(0)

    def fetch_row(t, r):
        slot = t % 2
        pltpu.make_async_copy(x_hbm.at[src[t_base[t] + r]], xbuf.at[slot, r], gsem.at[slot]).start()

    def gather_wait(t):
        slot = t % 2
        pltpu.make_async_copy(x_hbm.at[pl.ds(0, TILE)], xbuf.at[slot], gsem.at[slot]).wait()

    def scatter_start(t):
        base, slot = t_base[t], t % 2
        end = base + t_cnt[t]

        for path, (_, last, send, heads) in enumerate(paths):
            j_end = (t_e[t] * n_seg + last) * n_dst

            def more(j):
                return jnp.logical_and(j < j_end, seg_start[j] < end)

            def segment(j):
                first_row = seg_start[j]
                lo = jnp.maximum(first_row, base)
                n = jnp.minimum(first_row + seg_len[j], end) - lo
                to = seg_dst[j] + lo - first_row
                n_head = jnp.clip(seg_lim[j] - to, 0, jnp.maximum(n, 0)) if heads else 0
                n_early = jnp.clip(seg_lim[j] - late - to, 0, n_head) if heads else 0
                in_head = to - seg_lim[j] + late + early

                def put(rows, first, at, n):
                    @pl.when(n > 0)
                    def _():
                        pltpu.make_async_copy(
                            obuf.at[slot, pl.ds(lo - base + first, n)], rows.at[pl.ds(at, n)], ssem.at[slot]).start()

                def put_head(q, early_rows, late_rows):
                    @pl.when(seg_dir[j] == q)
                    def _():
                        put(early_rows, 0, in_head, n_early)
                        put(late_rows, n_early, in_head + n_early - early, n_head - n_early)

                if heads:
                    @pl.when(n_head > 0)
                    def _():
                        for q, rows in enumerate(heads):
                            put_head(q, *rows)

                put(send, n_head, to + n_head, n - n_head)
                return j + 1

            start = ptr[path]
            ptr[path] = jnp.maximum(lax.while_loop(more, segment, start) - 1, start)

    def scatter_wait(t):
        n, slot = t_cnt[t], t % 2
        send = paths[0][2]
        pltpu.make_async_copy(obuf.at[slot, pl.ds(0, n)], send.at[pl.ds(0, n)], ssem.at[slot]).wait()

    def prime(r, c):
        for t in BOTH:
            fetch_row(t, r)
        return c

    lax.fori_loop(0, TILE, prime, 0, unroll=UNROLL)

    def one_expert(e, t_first):
        weight_copies(e, wait)

        @pl.when(e + 1 < sub)
        def _():
            weight_copies(e + 1, start)

        ws = e % 2
        _, n = span_of(e)
        for path, (first, _, _, _) in enumerate(paths):
            ptr[path] = (e * n_seg + first) * n_dst

        def one_tile(i, t):
            slot = t % 2
            gather_wait(t)

            @pl.when(t >= 2)
            def _():
                scatter_wait(t - 2)

            xrows[...] = xbuf[slot].reshape(TILE, d_model)
            for r in range(TILE):
                fetch_row(t + 2, r)
            hidden = gelu(jnp.dot(xrows[...], wa[ws], preferred_element_type=F32)).astype(BF16)
            out = jnp.dot(hidden, wb[ws], preferred_element_type=F32).astype(BF16)
            obuf[slot] = out.reshape(TILE, sublanes, LANES)
            scatter_start(t)
            return t + 1

        return lax.fori_loop(0, (n + TILE - 1) // TILE, one_tile, t_first)

    lax.fori_loop(0, sub, one_expert, 0)
    for back in (2, 1):
        gather_wait(n_all + back)

        @pl.when(n_all >= back)
        def _():
            scatter_wait(n_all - back)


def run_experts(chunk, early, late, n_early, lists, place, x_rows, wa, wa_sib, wb, wb_sib, rows):
    e_loc, d_model, ff = wa.shape
    sub = 2 * e_loc
    sublanes = d_model // LANES
    ops = (*lists, place, x_rows, wa, wa_sib, wb, wb_sib) + (() if chunk == 0 else (rows,))
    n_smem = len(lists) + 1
    max_tiles = sub * (pl.cdiv(lists[0].shape[0] // sub, TILE) + 1) + 2
    if chunk == 0:
        sizes = []
        for n_rows, n in zip(rows, n_early):
            sizes += [n_rows] + [early] * n + [late] * n
    else:
        sizes = [rows.shape[0]]
    return pl.pallas_call(
        functools.partial(expert_kernel, chunk, len(SEGMENTS) - 1, early, late, n_early),
        out_shape=tuple(jax.ShapeDtypeStruct((n, sublanes, LANES), BF16) for n in sizes),
        in_specs=[SMEM] * n_smem + [HBM] * (len(ops) - n_smem),
        out_specs=(HBM,) * len(sizes),
        scratch_shapes=[
            pltpu.VMEM((2, TILE, sublanes, LANES), BF16),
            pltpu.VMEM((TILE, d_model), BF16),
            pltpu.VMEM((2, TILE, sublanes, LANES), BF16),
            pltpu.VMEM((2, d_model, ff), BF16),
            pltpu.VMEM((2, ff, d_model), BF16),
            pltpu.SMEM((max_tiles,), I32),
            pltpu.SMEM((max_tiles,), I32),
            pltpu.SMEM((max_tiles,), I32),
            pltpu.SMEM((2,), I32),
            PAIR, PAIR,
            pltpu.SemaphoreType.DMA((2, 2)),
        ],
        input_output_aliases={} if chunk == 0 else {len(ops) - 1: 0},
        compiler_params=MIXED,
        cost_estimate=COST,
        name='experts',
    )(*ops)


PIECES = 4


class Ring:
    def __init__(self, axis, n_y, n_x):
        y, ec = lax.axis_index('ep2'), lax.axis_index('ep')
        self.axis, self.core = axis, ec % 2
        self.n = n_x if axis == 'x' else n_y
        self.pos = ec // 2 if axis == 'x' else y
        self.direct, self.far = direct_of(self.n), far_of(self.n)

    def place(self, d):
        return lax.rem(self.pos + d + self.n, self.n)

    def device(self, d):
        if self.axis == 'x':
            return {'ep': self.place(d) * 2 + self.core}
        return {'ep2': self.place(d)}

    def remote(self, src, dst, sems, i, d):
        return pltpu.make_async_remote_copy(
            src_ref=src, dst_ref=dst, send_sem=sems.at[0, i], recv_sem=sems.at[1, i],
            device_id=self.device(d), device_id_type=pl.DeviceIdType.MESH)

    def signal(self, barrier):
        for d in range(1, self.n):
            pl.semaphore_signal(barrier, inc=1, device_id=self.device(d), device_id_type=pl.DeviceIdType.MESH)


def spread_kernel(rows_a, rows_b, early, n_y, n_x, send_a, send_b, recv_a, recv_b, stage_a, stage_b, sem_a, sem_b):
    rings = (Ring('x', n_y, n_x), Ring('y', n_y, n_x))
    barrier = pltpu.get_barrier_semaphore()
    for ring in rings:
        ring.signal(barrier)
    pl.semaphore_wait(barrier, n_x + n_y - 2)

    sides = list(zip(rings, (rows_a, rows_b), (send_a, send_b), (recv_a, recv_b), (stage_a, stage_b), (sem_a, sem_b)))

    def lead(side, p):
        ring, rows, send, _, stage, sem = side
        hop = ring.far // 2 if p % 2 == 0 else -(ring.far // 2)
        part = pl.ds(p * (rows // PIECES), rows // PIECES)
        return ring.remote(send.at[ring.far, part], stage.at[part], sem, p, hop)

    def follow(side, p):
        ring, rows, _, recv, stage, sem = side
        hop = ring.far // 2 if p % 2 == 0 else -(ring.far // 2)
        part = pl.ds(p * (rows // PIECES), rows // PIECES)
        return ring.remote(stage.at[part], recv.at[ring.far, part], sem, PIECES + p, hop)

    def straight(side, i):
        ring, rows, send, recv, _, sem = side
        d = ring.direct[i]
        part = pl.ds(early, rows - early)
        return ring.remote(send.at[d, part], recv.at[d, part], sem, 2 * PIECES + i, d)

    relayed = [(side, p) for p in range(PIECES) for side in sides if side[0].far]
    direct = [(side, i) for side in sides for i in range(len(side[0].direct))]
    for job in relayed:
        lead(*job).start()
    for job in direct:
        straight(*job).start()
    for job in relayed:
        lead(*job).wait_recv()
        follow(*job).start()
    for job in relayed:
        lead(*job).wait_send()
    for job in direct:
        straight(*job).wait()
    for job in relayed:
        follow(*job).wait()


def spread(rows_a, rows_b, early, cid, n_y, n_x, send_a, send_b):
    return pl.pallas_call(
        functools.partial(spread_kernel, rows_a, rows_b, early, n_y, n_x),
        out_shape=tuple(jax.ShapeDtypeStruct(s, BF16) for s in (send_a.shape, send_b.shape, send_a.shape[1:], send_b.shape[1:])),
        in_specs=[HBM, HBM],
        out_specs=(HBM,) * 4,
        scratch_shapes=[
            pltpu.SemaphoreType.DMA((2, 2 * PIECES + n_x)),
            pltpu.SemaphoreType.DMA((2, 2 * PIECES + n_y)),
        ],
        compiler_params=remote_params(cid),
        name='spread_%d_%d' % (rows_a, rows_b),
    )(send_a, send_b)[:2]


WAYS = 4


Path = collections.namedtuple('Path', ('recv', 'send', 'earlies', 'lates', 'at', 'blocks', 'out_at', 'steps'))


def spot(n_y, n_x, p, d, w, s):
    most = max(n_y, n_x)
    return (((p * most + d) * 2 + w) * most + s) * 2


def list_at(n_y, n_x, sub, my, p, s, w, d, level):
    at, blocks, out_at, steps = (my[1], n_x, my[0], n_y) if p == 0 else (my[0], n_y, my[1], n_x)
    out = lax.rem(out_at + order_of(steps, w)[s], steps)
    return ((out * 3 + level) * blocks + lax.rem(at + blocks - d, blocks)) * sub


def plan_kernel(n_y, n_x, early, lev_a, lev_b, place, rows_at):
    chip = place[1]
    sub = lev_a.shape[0] // (3 * n_y * n_x)
    for p, levels in enumerate((lev_a, lev_b)):
        blocks, steps = ((n_x, n_y), (n_y, n_x))[p]
        for d in range(blocks):
            acc = jnp.int32(0)
            for w in BOTH:
                for s in range(steps):
                    lower, upper = (list_at(n_y, n_x, sub, (chip // n_x, chip % n_x), p, s, w, d, w + up) for up in BOTH)

                    def add(e, n):
                        return n + levels[upper + e] - levels[lower + e]

                    n = lax.fori_loop(0, sub, add, jnp.int32(0))
                    at = spot(n_y, n_x, p, d, w, s)
                    rows_at[at] = acc
                    rows_at[at + 1] = n
                    acc = acc + n
                if not w:
                    acc = jnp.maximum(acc, early)


def plan_rows(n_y, n_x, early, levels, place):
    most = max(n_y, n_x)
    return pl.pallas_call(
        functools.partial(plan_kernel, n_y, n_x, early),
        out_shape=jax.ShapeDtypeStruct((8 * most * most,), I32),
        in_specs=[SMEM] * 3,
        out_specs=SMEM,
        cost_estimate=COST,
        name='plan_rows',
    )(*levels, place)


def sum_kernel(n_y, n_x, passes, early, late, bounds, *refs):
    (lev_a, lev_b, rows_at, place, recv_a, recv_b, send_a, send_b), refs = take(refs, 8)
    tables_in = []
    for _ in BOTH:
        tok_y, refs = take(refs, n_y)
        tok_x, refs = take(refs, n_x)
        tables_in.append((tok_y, tok_x))
    early_a, refs = take(refs, len(direct_of(n_x)))
    early_b, refs = take(refs, len(direct_of(n_y)))
    late_a, refs = take(refs, len(direct_of(n_x)) if late else 0)
    late_b, refs = take(refs, len(direct_of(n_y)) if late else 0)
    chip = place[1]
    my_y, my_x = chip // n_x, chip % n_x
    sub = lev_a.shape[0] // (3 * n_y * n_x)
    words = sub * LANES
    paths = (
        Path(recv_a, send_a, early_a, late_a, my_x, n_x, my_y, n_y),
        Path(recv_b, send_b, early_b, late_b, my_y, n_y, my_x, n_x),
    )
    todo = [(p, s) for p in BOTH for s in passes if s < paths[p].steps]
    outs, refs = take(refs, 2 * len(todo))
    (tok, wgt, *bufs), refs = take(refs, 4)
    accs, (tsem, rsem, zsem) = take(refs, 2 * WAYS)
    ways = [accs[:WAYS], accs[WAYS:]]
    table_of, size = {}, 0
    for p, s in todo:
        for w in BOTH:
            table_of[p, s, w] = size
            size += paths[p].blocks * words

    def source(p, d):
        return lax.rem(paths[p].at + paths[p].blocks - d, paths[p].blocks)

    def tables(p, s, act):
        for w in BOTH:
            sender = (paths[p].steps - order_of(paths[p].steps, w)[s]) % paths[p].steps
            for d in range(paths[p].blocks):
                src = pl.ds(pl.multiple_of(source(p, d) * words, words), words)
                dst = pl.ds(table_of[p, s, w] + d * words, words)
                for held, table in zip(tables_in, (tok, wgt)):
                    act(pltpu.make_async_copy(held[p][sender].at[src], table.at[dst], tsem.at[todo.index((p, s))]))

    jobs = [(p, s, d) for p, s in todo for d in range(paths[p].blocks)]

    def fetch(job, act):
        p, s, d = jobs[job]
        path = paths[p]
        slot = job % 2
        for w in BOTH:
            first, n = (rows_at[spot(n_y, n_x, p, d, w, s) + i] for i in BOTH)
            to = bufs[w].at[slot]
            main = path.recv if d else path.send

            def get(rows, at, done, n):
                @pl.when(n > 0)
                def _():
                    act(pltpu.make_async_copy(rows.at[pl.ds(at, n)], to.at[pl.ds(done, n)], rsem.at[slot]))

            done = 0
            if not w and d in direct_of(path.blocks):
                q = direct_of(path.blocks).index(d)
                done = jnp.clip(early - first, 0, n)
                get(path.earlies[q], first, 0, done)
                if late:
                    n_late = jnp.clip(early + late - first, 0, n) - done
                    get(path.lates[q], first + done - early, done, n_late)
                    done = done + n_late
            get(main.at[d], first + done, done, n - done)

    def zero(acc):
        def body(b, c):
            acc[pl.ds(b * BLOCK, BLOCK)] = jnp.zeros((BLOCK, *acc.shape[1:]), F32)
            return c
        lax.fori_loop(0, (acc.shape[0] - 8) // BLOCK, body, 0)

    fetch(0, start)
    for p, s in todo:
        tables(p, s, start)
    puts = []
    for job, (p, s, d) in enumerate(jobs):
        slot = job % 2
        levels = (lev_a, lev_b)[p]
        dummy = accs[0].shape[0] - 8
        if not d:
            for _, *others in ways:
                for acc in others:
                    zero(acc)
            for put in puts:
                put.wait()
            for target, *_ in ways:
                zero(target)
            tables(p, s, wait)
        fetch(job, wait)
        if job + 1 < len(jobs):
            fetch(job + 1, start)

        def one_expert(e, bases):
            counts, firsts = [], []
            for w in BOTH:
                lower, upper = (levels[list_at(n_y, n_x, sub, (my_y, my_x), p, s, w, d, w + up) + e] for up in BOTH)
                counts.append(upper - lower)
                firsts.append(table_of[p, s, w] + d * words + e * LANES + lower)
            longest = jnp.maximum(counts[0], counts[1])

            def group(b, cc):
                adds = []
                for w in BOTH:
                    for q in range(WAYS):
                        r = b * WAYS + q
                        row = bufs[w][slot, bases[w] + r].astype(F32)
                        t = jnp.where(r < counts[w], tok[firsts[w] + r], dummy)
                        adds.append((ways[w][q], t, wgt[firsts[w] + r] * row))
                for acc, t, row in adds:
                    acc[t] = acc[t] + row
                return cc

            lax.fori_loop(0, lax.shift_right_logical(longest + (WAYS - 1), 2), group, 0)
            return bases[0] + counts[0], bases[1] + counts[1]

        lax.fori_loop(0, sub, one_expert, (jnp.int32(0), jnp.int32(0)))
        if d + 1 == paths[p].blocks:
            puts = []
            for w in BOTH:
                target, second, third, fourth = ways[w]
                size = tokens_of(bounds, p, w)

                def merge(b, c):
                    rows = pl.ds(b * BLOCK, BLOCK)
                    target[rows] = (target[rows] + second[rows]) + (third[rows] + fourth[rows])
                    return c

                lax.fori_loop(0, size // BLOCK, merge, 0)
                out = outs[2 * todo.index((p, s)) + w]
                puts.append(pltpu.make_async_copy(target.at[pl.ds(0, size)], out, zsem.at[w]))
                puts[-1].start()
    for put in puts:
        put.wait()


def weighted_sums(n_y, n_x, passes, early, late, bounds, levels, rows_at, place, tables, recvs, sends, heads):
    sublanes = recvs[0].shape[2]
    sub = levels[0].shape[0] // (3 * n_y * n_x)
    todo = [(p, s) for p, n in enumerate((n_y, n_x)) for s in passes if s < n]
    sizes = [tokens_of(bounds, p, w) for p, _ in todo for w in BOTH]
    table = sum((n_x if p == 0 else n_y) * 2 * sub * LANES for p, _ in todo) + 2 * LANES
    tokens = max(b - a for a, b in zip(bounds[:-1], bounds[1:]))
    ops = (*levels, rows_at, place, *recvs, *sends, *tables, *heads)
    return pl.pallas_call(
        functools.partial(sum_kernel, n_y, n_x, passes, early, late, bounds),
        out_shape=tuple(jax.ShapeDtypeStruct((n, sublanes, LANES), F32) for n in sizes),
        in_specs=[SMEM] * 4 + [HBM] * (len(ops) - 4),
        out_specs=(HBM,) * len(sizes),
        scratch_shapes=[
            pltpu.SMEM((table,), I32),
            pltpu.SMEM((table,), F32),
            *[pltpu.VMEM((2, sub * LANES + LANES, sublanes, LANES), BF16) for _ in BOTH],
            *[pltpu.VMEM((tokens + 8, sublanes, LANES), F32) for _ in range(2 * WAYS)],
            pltpu.SemaphoreType.DMA((len(todo),)),
            PAIR, PAIR,
        ],
        compiler_params=LOCAL,
        cost_estimate=COST,
        name='weighted_sums',
    )(*ops)


SUM_CHUNKS = 8


def pieces_of(n):
    cuts = [BLOCK * ((n // BLOCK * j) // SUM_CHUNKS) for j in range(SUM_CHUNKS + 1)]
    return [(a, b - a) for a, b in zip(cuts[:-1], cuts[1:]) if b > a]


def reduce_kernel(n_y, n_x, bounds, *refs):
    sizes = (n_y, n_x)
    lanes = [(p, w) for p in BOTH for w in BOTH]
    got, refs = take(refs, len(lanes))
    got = dict(zip(lanes, got))
    sums = {}
    for p, n in enumerate(sizes):
        for s in range(1, n):
            for w in BOTH:
                (sums[p, s, w],), refs = take(refs, 1)
    (x_ref, y_ref), refs = take(refs, 2)
    part, own = {}, {}
    for p, w in lanes:
        for s in range(sizes[p] - 1):
            (part[p, w, s], own[p, w, s]), refs = take(refs, 2)
    zsem, gsem, rsem = refs
    rings = (Ring('y', n_y, n_x), Ring('x', n_y, n_x))
    d_model = x_ref.shape[1]
    pieces = {(p, w): pieces_of(tokens_of(bounds, p, w)) for p, w in lanes}
    order = [(p, w, j) for j in range(SUM_CHUNKS) for p, w in lanes if j < len(pieces[p, w])]

    barrier = pltpu.get_barrier_semaphore()
    for ring in rings:
        for d in (1, -1):
            pl.semaphore_signal(barrier, inc=1, device_id=ring.device(d), device_id_type=pl.DeviceIdType.MESH)
    pl.semaphore_wait(barrier, 4)

    def rows_of(p, w, j):
        return pl.ds(*pieces[p, w][j])

    def load(p, w, s, j):
        r = rows_of(p, w, j)
        return pltpu.make_async_copy(sums[p, s, w].at[r], own[p, w, s - 1].at[r], zsem.at[p, w, s - 1, j])

    def begin(p, w, j):
        r = rows_of(p, w, j)
        return pltpu.make_async_copy(got[p, w].at[r], part[p, w, 0].at[r], gsem.at[p, w, j])

    def hop(p, w, s, j):
        r = rows_of(p, w, j)
        return pltpu.make_async_remote_copy(
            src_ref=part[p, w, s - 1].at[r], dst_ref=part[p, w, s].at[r],
            send_sem=rsem.at[0, p, w, s, j], recv_sem=rsem.at[1, p, w, s, j],
            device_id=rings[p].device(1 if w == 0 else -1), device_id_type=pl.DeviceIdType.MESH)

    def arrive(p, w, s, j):
        if s == 0:
            begin(p, w, j).wait()
        else:
            hop(p, w, s, j).wait_recv()

    last = max(sizes) - 1
    for p, w, j in order:
        begin(p, w, j).start()
        load(p, w, 1, j).start()

    for s in range(1, last):
        for p, w, j in order:
            if s >= sizes[p] - 1:
                continue
            load(p, w, s, j).wait()
            arrive(p, w, s - 1, j)
            into, more = part[p, w, s - 1], own[p, w, s - 1]
            first, n = pieces[p, w][j]

            def add(b, c):
                r = pl.ds(first + b * BLOCK, BLOCK)
                into[r] = into[r] + more[r]
                return c

            lax.fori_loop(0, n // BLOCK, add, 0)
            hop(p, w, s, j).start()
            load(p, w, s + 1, j).start()

    for p, w, j in order:
        s = sizes[p] - 1
        load(p, w, s, j).wait()
        arrive(p, w, s - 1, j)
        into, more = part[p, w, s - 1], own[p, w, s - 1]
        first, n = pieces[p, w][j]
        token = bounds[2 * p + w] + first

        def finish(b, c):
            r = pl.ds(first + b * BLOCK, BLOCK)
            out = pl.ds(pl.multiple_of(token + b * BLOCK, BLOCK), BLOCK)
            total = into[r] + more[r]
            y_ref[out, :] = (x_ref[out, :].astype(F32) + total.reshape(BLOCK, d_model)).astype(BF16)
            return c

        lax.fori_loop(0, n // BLOCK, finish, 0)
    for s in range(1, last):
        for p, w, j in order:
            if s < sizes[p] - 1:
                hop(p, w, s, j).wait_send()


def reduce_back(cid, n_y, n_x, bounds, got, sums, x):
    n_tok, d_model = x.shape
    sublanes = d_model // LANES
    bufs = []
    for p, n in enumerate((n_y, n_x)):
        for w in BOTH:
            size = tokens_of(bounds, p, w)
            bufs += [pltpu.VMEM((size, sublanes, LANES), F32)] * (2 * (n - 1))
    steps = max(n_y, n_x) - 1
    ops = (*got, *sums, x)
    return pl.pallas_call(
        functools.partial(reduce_kernel, n_y, n_x, bounds),
        out_shape=jax.ShapeDtypeStruct((n_tok, d_model), BF16),
        in_specs=[HBM] * (len(ops) - 1) + [VMEM],
        out_specs=VMEM,
        scratch_shapes=[
            *bufs,
            pltpu.SemaphoreType.DMA((2, 2, steps, SUM_CHUNKS)),
            pltpu.SemaphoreType.DMA((2, 2, SUM_CHUNKS)),
            pltpu.SemaphoreType.DMA((2, 2, 2, steps, SUM_CHUNKS)),
        ],
        compiler_params=remote_params(cid),
        name='reduce_back',
    )(*ops)


def solution(mesh):
    dev_axes = ('ep2', 'ep')
    n_y, n_ep = mesh.shape['ep2'], mesh.shape['ep']
    n_x = n_ep // 2
    group = n_y * n_ep
    n_chip = n_y * n_x

    def local_step(x_loc, ids_loc, gate_loc, w_a, w_b):
        n_tok, d_model = x_loc.shape
        n_top = ids_loc.shape[1]
        e_loc = w_a.shape[0]
        sub = 2 * e_loc
        experts = e_loc * group
        cap = capacity_of(group, n_tok, n_top, experts)
        sublanes = d_model // LANES
        base_a, base_b = n_y * sub * LANES, n_x * sub * LANES
        late = min(base_a, base_b) // 16
        early = late + late // 2
        head = early + late
        slots_a, slots_b = base_a + head, base_b + head
        bounds = bounds_of(n_tok)
        n_seg, n_chunk = len(bounds) - 1, len(CHUNKS) - 1
        me = lax.axis_index(dev_axes)
        core, chip = me % 2, me // 2
        place = jnp.stack([core, chip]).astype(I32)

        x3 = x_loc.reshape(n_tok, sublanes, LANES)
        chunks = [lax.all_gather(x3[bounds[CHUNKS[k]]:bounds[CHUNKS[k + 1]]], dev_axes, tiled=True) for k in range(n_chunk)]
        swap = [(i, i ^ 1) for i in range(n_ep)]
        w_a_sib = lax.ppermute(w_a, 'ep', swap)
        w_b_sib = lax.ppermute(w_b, 'ep', swap)

        toks, wgts, cnts = route(ids_loc, gate_loc, bounds)
        for_chip = toks[:experts].reshape(n_chip, 1, sub, LANES)
        table = jnp.concatenate([
            jnp.broadcast_to(for_chip, (n_chip, 2, sub, LANES)).reshape(group, sub, LANES),
            jnp.broadcast_to(cnts[None], (group, PREFIX_ROWS, LANES))], axis=1)
        table = lax.all_to_all(table, dev_axes, 0, 0, tiled=True)
        lists = build_lists(place, table.reshape(-1), cap, slots_a, slots_b, head, bounds, n_y, n_x, sub)

        prefix = table[:, sub:sub + n_seg + 1, :experts]
        totals = prefix[:, n_seg]
        offs = jnp.cumsum(totals, axis=0) - totals
        kept = jnp.clip(cap - offs, 0, totals)
        upto = jnp.minimum(prefix, kept[:, None])
        y, x = chip // n_x, chip % n_x
        level_a = lax.dynamic_slice(upto.reshape(n_y, n_ep, n_seg + 1, experts), (0, x * 2 + core, 0, y * n_x * sub), (n_y, 1, 3, n_x * sub))
        level_b = lax.dynamic_slice(upto.reshape(n_y, n_x, 2, n_seg + 1, experts), (y, 0, core, 2, 0), (1, n_x, 1, 3, experts))
        level_b = lax.dynamic_slice(level_b.reshape(n_x, 3, n_y, n_x * sub), (0, 0, 0, x * sub), (n_x, 3, n_y, sub))
        levels = (level_a.reshape(-1), level_b.reshape(-1))
        of_chip = (jnp.arange(experts)[:, None] // sub == jnp.arange(n_chip)[None, :]).astype(F32)
        per_chip = jnp.dot(upto.reshape(-1, experts).astype(F32), of_chip).reshape(group, n_seg + 1, n_chip)
        rows = (per_chip[:, 1:] - per_chip[:, :-1]).astype(I32)
        rows_a = jnp.sum(rows.reshape(n_y, n_ep, n_seg, n_chip), axis=0)
        rows_b = jnp.sum(rows.reshape(n_y, n_x, 2, n_seg, n_chip), axis=1)
        need_a = jnp.max(jnp.maximum(rows_a[:, 0], head) + rows_a[:, 1])
        need_b = jnp.max(jnp.maximum(rows_b[:, :, 2], head) + rows_b[:, :, 3])
        late_first = jnp.max(rows[:, ::2]) > early
        tiers = [(base_a * q // 256, base_b * q // 256) for q in SIZES] + [(slots_a, slots_b)]
        limits = jnp.array(tiers[:-1], I32)
        over = jnp.logical_or(need_a > limits[:, 0], need_b > limits[:, 1])
        index = jnp.sum(jnp.logical_or(over, late_first).astype(I32))
        within = toks[:experts]
        for lo, hi in zip(bounds[1:-1], bounds[:-2]):
            within = jnp.where(toks[:experts] >= lo, within - (lo - hi), within)
        rows_at = plan_rows(n_y, n_x, head, levels, place)

        def up_x(v, d):
            return lax.ppermute(v, 'ep', [(i, (i + 2 * d) % n_ep) for i in range(n_ep)]) if d else v

        def up_y(v, d):
            return lax.ppermute(v, 'ep2', [(i, (i + d) % n_y) for i in range(n_y)]) if d else v

        tables = []
        for v in (within, wgts[:experts]):
            grid = v.reshape(n_y, n_x, sub, LANES)
            tables += [up_y(lax.dynamic_index_in_dim(grid, (y + d) % n_y, 0).reshape(-1), d) for d in range(n_y)]
            tables += [up_x(lax.dynamic_index_in_dim(grid, (x + d) % n_x, 1).reshape(-1), d) for d in range(n_x)]
        lists, levels, rows_at, index, tables = lax.optimization_barrier((lists, levels, rows_at, index, tables))

        weights = (w_a, w_a_sib, w_b, w_b_sib)
        direct_x, direct_y = direct_of(n_x), direct_of(n_y)
        n_early = (len(direct_x), len(direct_y))
        first = run_experts(0, early, late, n_early, lists, place, chunks[0], *weights, (n_x * slots_a, n_y * slots_b))
        (send_a, *heads_a), (send_b, *heads_b) = take(first, 1 + 2 * n_early[0])
        early_a, late_a = take(heads_a, n_early[0])
        early_b, late_b = take(heads_b, n_early[1])

        def to_neighbours(rows_x, rows_y):
            return [up_x(v, d) for v, d in zip(rows_x, direct_x)] + [up_y(v, d) for v, d in zip(rows_y, direct_y)]

        chunks[1], early_a, early_b = lax.optimization_barrier((chunks[1], early_a, early_b))
        earlies = to_neighbours(early_a, early_b)
        send_b, = run_experts(1, early, late, n_early, lists, place, chunks[1], *weights, send_b)
        sends = (send_a.reshape(n_x, slots_a, sublanes, LANES), send_b.reshape(n_y, slots_b, sublanes, LANES))

        carried = [head] * (len(tiers) - 1) + [early]
        recvs = lax.switch(index, [
            functools.partial(spread, a, b, skip, i, n_y, n_x) for i, ((a, b), skip) in enumerate(zip(tiers, carried))], *sends)
        recvs, late_a, late_b = lax.optimization_barrier((recvs, late_a, late_b))
        lates = to_neighbours(late_a, late_b)
        common = (bounds, levels, rows_at, place, tables, recvs, sends)
        begun = weighted_sums(n_y, n_x, (0,), early, 0, *common, earlies)
        got = (up_y(begun[0], 1), up_y(begun[1], -1), up_x(begun[2], 1), up_x(begun[3], -1))
        rest = weighted_sums(n_y, n_x, tuple(range(1, max(n_y, n_x))), early, late, *common, [*earlies, *lates])
        return reduce_back(len(tiers), n_y, n_x, bounds, got, rest, x_loc)

    tok_spec = P(('dp', 'ep2', 'ep'), None)
    w_spec = P(dev_axes, None, None)
    return jax.shard_map(local_step, mesh=mesh, in_specs=(tok_spec, tok_spec, tok_spec, w_spec, w_spec), out_specs=tok_spec, check_vma=False)
```
